128 devices in a mesh: gx: 8 (over y, x_lo), gy: 4 (over x_hi, core), gz: 4 (over z).
Axes of the slice: x: 4 (x_hi: 2, x_lo: 2; x = x_hi * 2 + x_lo), y: 4, z: 4, core: 2. Of those that a mesh axis runs over, the one named last changes fastest.
Arguments:
- features: bfloat16 [24, 8, 32, 8, 128], P('gx', 'gy', 'gz'), may hold values from -6 to 6
- positions: float32 [24, 8, 32, 24], P('gx', 'gy', 'gz'), may hold values from 0 to 256, as said below
- grid_anchor: int32 [24, 8, 32, 24], P('gx', 'gy', 'gz'), may hold values from -1 to 254, as said below
- species: int32 [24, 8, 32, 8], P('gx', 'gy', 'gz'), may hold values from 0 to 1
- neighbours: int32 [24, 8, 32, 512], P('gx', 'gy', 'gz'), may hold values from 0 to 49151, as said below
- neighbour_count: int32 [24, 8, 32, 8], P('gx', 'gy', 'gz'), may hold values from 32 to 64
- w_self: bfloat16 [128, 128], replicated, may hold values from -0.5 to 0.5
- w_neighbour: bfloat16 [128, 128], replicated, may hold values from -0.5 to 0.5
- w_radial: bfloat16 [8, 128], replicated, may hold values from -2 to 2
- radial_rates: float32 [8], replicated, may hold values from 0.05 to 2
- w_pair1: bfloat16 [128, 128], replicated, may hold values from -0.5 to 0.5
- w_pair2: bfloat16 [128, 128], replicated, may hold values from -0.5 to 0.5
- w_vector: bfloat16 [128, 128], replicated, may hold values from -0.5 to 0.5
- w_out: bfloat16 [128, 128], replicated, may hold values from -0.5 to 0.5
- w_charge: bfloat16 [128], replicated, may hold values from -0.5 to 0.5
- species_charge: float32 [2], replicated, may hold values from -1 to 1
Outputs:
- features_out: bfloat16 [24, 8, 32, 8, 128], P('gx', 'gy', 'gz')
- site_potential: float32 [24, 8, 32, 8], P('gx', 'gy', 'gz')
The draws below stay inside these ranges and needn't reach their ends.
Inputs may be any that keep to these rules, and one draw needn't show every extreme that they name: `positions`: component d of slot s of cell (cx, cy, cz) lies in that cell: between c_d * 8 and (c_d + 1) * 8. `grid_anchor`: at the same place as in positions, the whole part of the coordinate minus 1; the coordinate lies between grid_anchor + 1 and grid_anchor + 2. `neighbours`: each entry is the index ((cx * 8 + cy) * 32 + cz) * 8 + s of an atom whose cell differs from the listing atom's cell by at most one along each dimension, periodically; never the listing atom itself.
All inputs are finite; a program needn't handle non-finite values.
Results may differ from the reference program's by a relative error of at most 0.0039.
The reference program's roundings to bfloat16 on the way count: a program that leaves them out, or rounds other values in their place, can miss the bound.
Values may be sent and summed in bfloat16 or wider, within the bound.
A program may use at most 64 MiB of HBM per device.

```python
import math
import jax
import jax.numpy as jnp
from jax import lax

C = 128
K = 8
NBR = 64
SPECIES = 2
CELL = 8
BLOCK = 128
SLOTS = 8
NCX = 24
NCY = 8
NCZ = 32
NX = 192
NY = 64
NZ = 256
SCREEN = 32


def cell_corners():
    cell_x = jnp.broadcast_to(jnp.arange(NCX, dtype=jnp.int32)[:, None, None], (NCX, NCY, NCZ))
    cell_y = jnp.broadcast_to(jnp.arange(NCY, dtype=jnp.int32)[None, :, None], (NCX, NCY, NCZ))
    cell_z = jnp.broadcast_to(jnp.arange(NCZ, dtype=jnp.int32)[None, None, :], (NCX, NCY, NCZ))
    return (jnp.stack([cell_x, cell_y, cell_z], axis=3) * CELL)[:, :, :, :, None]


def placement_parts(key):
    inner_cell = jax.random.randint(jax.random.fold_in(key, 11), (NCX, NCY, NCZ, 3, SLOTS), 0, CELL)
    return cell_corners() + inner_cell


def draw_positions(key, part):
    whole_cells = placement_parts(key)
    uniform_draw = jax.random.uniform(jax.random.fold_in(key, 12), (NCX, NCY, NCZ, 3, SLOTS), jnp.float32)
    fraction = uniform_draw
    return (whole_cells.astype(jnp.float32) + fraction).reshape(NCX, NCY, NCZ, 3 * SLOTS)


def draw_grid_anchor(key, part):
    return (placement_parts(key) - 1).reshape(NCX, NCY, NCZ, 3 * SLOTS).astype(jnp.int32)


def draw_neighbours(key, part):
    draw_shape = (NCX, NCY, NCZ, SLOTS, NBR)
    steps_x = jax.random.randint(jax.random.fold_in(key, 21), draw_shape, -1, 2)
    steps_y = jax.random.randint(jax.random.fold_in(key, 22), draw_shape, -1, 2)
    steps_z = jax.random.randint(jax.random.fold_in(key, 23), draw_shape, -1, 2)
    pick_slot = jax.random.randint(jax.random.fold_in(key, 24), draw_shape, 0, SLOTS)
    cell_x = jnp.arange(NCX, dtype=jnp.int32)[:, None, None, None, None]
    cell_y = jnp.arange(NCY, dtype=jnp.int32)[None, :, None, None, None]
    cell_z = jnp.arange(NCZ, dtype=jnp.int32)[None, None, :, None, None]
    own_slot = jnp.arange(SLOTS, dtype=jnp.int32)[None, None, None, :, None]
    self_pair = (steps_x == 0) & (steps_y == 0) & (steps_z == 0) & (pick_slot == own_slot)
    pick_slot = jnp.where(self_pair, (pick_slot + 1) % SLOTS, pick_slot)
    other_x = (cell_x + steps_x) % NCX
    other_y = (cell_y + steps_y) % NCY
    other_z = (cell_z + steps_z) % NCZ
    atom_ids = ((other_x * NCY + other_y) * NCZ + other_z) * SLOTS + pick_slot
    return atom_ids.reshape(NCX, NCY, NCZ, SLOTS * NBR).astype(jnp.int32)


def with_ends(entries, own_key, smallest, high):
    shape = entries.shape
    spot = [jax.random.randint(jax.random.fold_in(own_key, axis), (), 0, shape[axis]) for axis in range(len(shape))]
    entries = entries.at[tuple(spot)].set(smallest)
    longest = shape.index(max(shape))
    spot[longest] = (spot[longest] + 1) % shape[longest]
    return entries.at[tuple(spot)].set(high)


def levels(key, shape, shards, low, largest):
    level, own = 1.0, jax.random.fold_in(key, 6)
    for axis_at, blocks in shards:
        heights = jnp.exp(jax.random.uniform(jax.random.fold_in(own, axis_at), (blocks,), jnp.float32, low / len(shards), largest / len(shards)))
        level = level * jnp.repeat(heights, shape[axis_at] // blocks).reshape([-1 if axis == axis_at else 1 for axis in range(len(shape))])
    return level


def noise(rng, shape, scale, most, pieces=(), kind=jnp.bfloat16):
    entries = scale * jax.random.normal(rng, shape, jnp.float32)
    if pieces:
        entries = entries * levels(rng, shape, pieces, -0.22, 0.18)
    return jnp.clip(entries, -most, most).astype(kind)


def setup_inputs(seed: int = 0) -> dict:
    key_of = jax.random.split(jax.random.key(seed), 17)
    return {
        "features": noise(key_of[0], (NCX, NCY, NCZ, SLOTS, C), 1.0, 6.0, ((0, 8), (1, 4), (2, 4))),
        "positions": draw_positions(jax.random.fold_in(key_of[16], 71), 0),
        "grid_anchor": draw_grid_anchor(jax.random.fold_in(key_of[16], 71), 0),
        "species": with_ends(jax.random.randint(key_of[3], (NCX, NCY, NCZ, SLOTS), 0, SPECIES), jax.random.fold_in(key_of[3], 1), 0, SPECIES - 1).astype(jnp.int32),
        "neighbours": draw_neighbours(jax.random.fold_in(key_of[16], 71), 0),
        "neighbour_count": with_ends(jax.random.randint(key_of[5], (NCX, NCY, NCZ, SLOTS), NBR // 2, NBR + 1), jax.random.fold_in(key_of[5], 1), NBR // 2, NBR).astype(jnp.int32),
        "w_self": noise(key_of[6], (C, C), C ** -0.5, 0.5),
        "w_neighbour": noise(key_of[7], (C, C), C ** -0.5, 0.5),
        "w_radial": noise(key_of[8], (K, C), K ** -0.5, 2.0),
        "radial_rates": jnp.clip(jnp.exp(jax.random.uniform(key_of[9], (K,), jnp.float32, math.log(0.05), math.log(2.0))), 0.05, 2.0),
        "w_pair1": noise(key_of[10], (C, C), C ** -0.5, 0.5),
        "w_pair2": noise(key_of[11], (C, C), C ** -0.5, 0.5),
        "w_vector": noise(key_of[12], (C, C), C ** -0.5, 0.5),
        "w_out": noise(key_of[13], (C, C), C ** -0.5, 0.5),
        "w_charge": noise(key_of[14], (C,), C ** -0.5, 0.5),
        "species_charge": jnp.clip(jax.random.uniform(key_of[15], (SPECIES,), jnp.float32, -1.0, 1.0), -1.0, 1.0),
    }


coulomb_scale = 0.25
smearing = 1.0
highest = lax.Precision.HIGHEST

def spline_weights(fraction):
    square = fraction * fraction
    cube_part = square * fraction
    remain = 1.0 - fraction
    return jnp.stack([remain * remain * remain / 6.0, (3.0 * cube_part - 6.0 * square + 4.0) / 6.0, (-3.0 * cube_part + 3.0 * square + 3.0 * fraction + 1.0) / 6.0, cube_part / 6.0], axis=-1)

def wave_squared(mode_ids, length):
    signed_modes = jnp.where(mode_ids > length // 2, mode_ids - length, mode_ids).astype(jnp.float32)
    wavenumber = signed_modes * (2.0 * math.pi / length)
    return wavenumber * wavenumber

def spline_modulus(mode_ids, length):
    real_part = jnp.zeros(mode_ids.shape, jnp.float32)
    imag_part = jnp.zeros(mode_ids.shape, jnp.float32)
    for tap_shift, coefficient in ((0, 1.0 / 6.0), (1, 4.0 / 6.0), (2, 1.0 / 6.0)):
        angles = (mode_ids * tap_shift % length).astype(jnp.float32) * (2.0 * math.pi / length)
        real_part = real_part + coefficient * jnp.cos(angles)
        imag_part = imag_part + coefficient * jnp.sin(angles)
    return real_part * real_part + imag_part * imag_part

def green_values(mode_x, mode_y, mode_z, length_x, length_y, length_z, screen_length):
    total_sq = wave_squared(mode_x, length_x) + wave_squared(mode_y, length_y) + wave_squared(mode_z, length_z)
    moduli = spline_modulus(mode_x, length_x) * spline_modulus(mode_y, length_y) * spline_modulus(mode_z, length_z)
    kernel = coulomb_scale * 4.0 * math.pi * jnp.exp(-0.5 * smearing * smearing * total_sq) / ((total_sq + 1.0 / (screen_length * screen_length)) * moduli)
    zero_mode = (mode_x == 0) & (mode_y == 0) & (mode_z == 0)
    return jnp.where(zero_mode, 0.0, kernel)

def atom_table(values):
    cell_shape = values.shape[:3]
    slot_count = values.shape[3] // 3
    grouped = values.reshape(cell_shape + (3, slot_count))
    return jnp.moveaxis(grouped, 3, 4).reshape(-1, 3)

def atom_update(hidden_rows, own_proj, sent_rows, displace, live_slots, w_radial, radial_rates, w_pair1, w_pair2, w_vector, w_out):
    row_count, list_length, channels = sent_rows.shape
    scaled = displace / CELL
    square = lax.optimization_barrier(jnp.sum(scaled * scaled, axis=2))
    radial_basis = jnp.exp(-square[:, :, None] * radial_rates[None, None, :]).astype(jnp.bfloat16)
    radial_part = jnp.dot(radial_basis.reshape(row_count * list_length, -1), w_radial, preferred_element_type=jnp.float32)
    pre_active = own_proj[:, None, :] + sent_rows.astype(jnp.float32) + radial_part.reshape(row_count, list_length, channels)
    latent = jax.nn.silu(pre_active).astype(jnp.bfloat16).reshape(row_count * list_length, channels)
    second = jax.nn.silu(jnp.dot(latent, w_pair1, preferred_element_type=jnp.float32)).astype(jnp.bfloat16)
    third_layer = jax.nn.silu(jnp.dot(second, w_pair2, preferred_element_type=jnp.float32)).astype(jnp.bfloat16)
    vector_weights = jnp.dot(third_layer, w_vector, preferred_element_type=jnp.float32).reshape(row_count, list_length, channels)
    live_float = live_slots.astype(jnp.float32)
    message = jnp.einsum('rn,rnc->rc', live_float, third_layer.reshape(row_count, list_length, channels).astype(jnp.float32), precision=highest) / NBR
    weighted = live_float[:, :, None] * scaled
    vector = jnp.einsum('rnd,rnc->rdc', weighted, vector_weights, precision=highest) / math.sqrt(NBR)
    invariant = lax.optimization_barrier(jnp.sum(vector * vector, axis=1))
    update = (message + invariant).astype(jnp.bfloat16)
    return (hidden_rows.astype(jnp.float32) + jnp.dot(update, w_out, preferred_element_type=jnp.float32)).astype(jnp.bfloat16)

def reference(features, positions, grid_anchor, species, neighbours, neighbour_count, w_self, w_neighbour, w_radial, radial_rates, w_pair1, w_pair2, w_vector, w_out, w_charge, species_charge):
    atom_count = NCX * NCY * NCZ * SLOTS
    hidden_rows = features.reshape(atom_count, C)
    place_rows = atom_table(positions)
    anchor_rows = atom_table(grid_anchor)
    species_rows = species.reshape(atom_count)
    neighbour_rows = neighbours.reshape(atom_count, NBR)
    counts = neighbour_count.reshape(atom_count)
    own_proj = jnp.dot(hidden_rows, w_self, preferred_element_type=jnp.float32)
    sent_proj = jnp.dot(hidden_rows, w_neighbour, preferred_element_type=jnp.float32).astype(jnp.bfloat16)
    box_length = jnp.array([NCX * CELL, NCY * CELL, NCZ * CELL], jnp.float32)
    list_ids = jnp.arange(NBR, dtype=jnp.int32)

    def pair_block(block_index):
        block_start = (block_index * BLOCK).astype(jnp.int32)
        block_ids = lax.dynamic_slice_in_dim(neighbour_rows, block_start, BLOCK, 0)
        own_place = lax.dynamic_slice_in_dim(place_rows, block_start, BLOCK, 0)
        displace = place_rows[block_ids] - own_place[:, None, :]
        displace = displace - box_length * jnp.floor(displace / box_length + 0.5)
        live_slots = list_ids[None, :] < lax.dynamic_slice_in_dim(counts, block_start, BLOCK, 0)[:, None]
        return atom_update(lax.dynamic_slice_in_dim(hidden_rows, block_start, BLOCK, 0), lax.dynamic_slice_in_dim(own_proj, block_start, BLOCK, 0), sent_proj[block_ids], displace, live_slots, w_radial, radial_rates, w_pair1, w_pair2, w_vector, w_out)
    updated = lax.map(pair_block, jnp.arange(atom_count // BLOCK, dtype=jnp.int32))
    features_out = updated.reshape(NCX, NCY, NCZ, SLOTS, C)
    charge = species_charge[species_rows] + jnp.dot(hidden_rows, w_charge, preferred_element_type=jnp.float32)
    tap_weights = spline_weights(place_rows - (anchor_rows + 1).astype(jnp.float32))
    tap_ids = jnp.arange(4, dtype=jnp.int32)
    index_x = (anchor_rows[:, 0:1] + tap_ids[None, :]) % NX
    index_y = (anchor_rows[:, 1:2] + tap_ids[None, :]) % NY
    index_z = (anchor_rows[:, 2:3] + tap_ids[None, :]) % NZ
    stencil = tap_weights[:, 0, :, None, None] * tap_weights[:, 1, None, :, None] * tap_weights[:, 2, None, None, :]
    amounts = charge[:, None, None, None] * stencil
    charge_grid = jnp.zeros((NX, NY, NZ), jnp.float32).at[index_x[:, :, None, None], index_y[:, None, :, None], index_z[:, None, None, :]].add(amounts)
    spectrum = jnp.fft.fftn(charge_grid)
    green = green_values(jnp.arange(NX, dtype=jnp.int32)[:, None, None], jnp.arange(NY, dtype=jnp.int32)[None, :, None], jnp.arange(NZ, dtype=jnp.int32)[None, None, :], NX, NY, NZ, SCREEN)
    potential_grid = jnp.real(jnp.fft.ifftn(spectrum * green)).astype(jnp.float32)
    sampled = potential_grid[index_x[:, :, None, None], index_y[:, None, :, None], index_z[:, None, None, :]]
    site_potential = lax.optimization_barrier(jnp.sum(sampled * stencil, axis=(1, 2, 3))).reshape(NCX, NCY, NCZ, SLOTS)
    return (features_out, site_potential)
```

```python
import functools
import math

import jax
import jax.numpy as jnp
from jax import lax
from jax.experimental import pallas as pl
from jax.experimental.pallas import tpu as pltpu
from jax.sharding import PartitionSpec as P

NBR = 64
CELL = 8
BLOCK = 128


coulomb_scale = 0.25
smearing = 1.0
highest = lax.Precision.HIGHEST


def padded_2(block, sides, width):
    for axis, dim in sides:
        count = lax.axis_size(axis)
        forward = [(i, i + 1) for i in range(count - 1)]
        forward.append((count - 1, 0))
        backward = [(target, source) for source, target in forward]
        low = lax.ppermute(
            lax.slice_in_dim(block, block.shape[dim] - width, None, axis=dim), axis, forward
        )
        high = lax.ppermute(lax.slice_in_dim(block, 0, width, axis=dim), axis, backward)
        block = jnp.concatenate([low, block, high], axis=dim)
    return block


def spline_weights(fraction):
    square = fraction * fraction
    cube_part = square * fraction
    remain = 1.0 - fraction
    return jnp.stack(
        [
            remain * remain * remain / 6.0,
            (3.0 * cube_part - 6.0 * square + 4.0) / 6.0,
            (-3.0 * cube_part + 3.0 * square + 3.0 * fraction + 1.0) / 6.0,
            cube_part / 6.0,
        ],
        axis=-1,
    )


def wave_squared(mode_ids, length):
    signed_modes = jnp.where(mode_ids > length // 2, mode_ids - length, mode_ids).astype(
        jnp.float32
    )
    wavenumber = signed_modes * (2.0 * math.pi / length)
    return wavenumber * wavenumber


def spline_modulus(mode_ids, length):
    real_part = jnp.zeros(mode_ids.shape, jnp.float32)
    imag_part = jnp.zeros(mode_ids.shape, jnp.float32)
    for tap_shift, coefficient in ((0, 1.0 / 6.0), (1, 4.0 / 6.0), (2, 1.0 / 6.0)):
        angles = (mode_ids * tap_shift % length).astype(jnp.float32) * (2.0 * math.pi / length)
        real_part = real_part + coefficient * jnp.cos(angles)
        imag_part = imag_part + coefficient * jnp.sin(angles)
    return real_part * real_part + imag_part * imag_part


def green_values(mode_x, mode_y, mode_z, length_x, length_y, length_z, screen_length):
    total_sq = (
        wave_squared(mode_x, length_x)
        + wave_squared(mode_y, length_y)
        + wave_squared(mode_z, length_z)
    )
    moduli = (
        spline_modulus(mode_x, length_x)
        * spline_modulus(mode_y, length_y)
        * spline_modulus(mode_z, length_z)
    )
    kernel = (
        coulomb_scale
        * 4.0
        * math.pi
        * jnp.exp(-0.5 * smearing * smearing * total_sq)
        / ((total_sq + 1.0 / (screen_length * screen_length)) * moduli)
    )
    zero_mode = (mode_x == 0) & (mode_y == 0) & (mode_z == 0)
    return jnp.where(zero_mode, 0.0, kernel)


def atom_columns(values):
    slot_count = values.shape[3] // 3
    grouped = values.reshape(-1, 3, slot_count)
    return jnp.moveaxis(grouped, 1, 0).reshape(3, -1)


NT = (((1,), (1,)), ((), ()))


def pair_kernel(
    unroll,
    feat_ref,
    pos_ref,
    nbr_ref,
    count_ref,
    wn_ref,
    ws_ref,
    wr_ref,
    rate_ref,
    w1_ref,
    w2_ref,
    wv_ref,
    wo_ref,
    hid_ref,
    out_ref,
    feat32,
    first_w,
    pair1_w,
    pair2_w,
    hot_row,
    lane_row,
    live_row,
    sums,
):
    f32, bf16 = jnp.float32, jnp.bfloat16
    feat32[...] = feat_ref[...].astype(f32)
    first_w[:, 0:128] = (wn_ref[...].astype(f32) * 0.5).T.astype(bf16)
    first_w[:, 128:256] = (ws_ref[...].astype(f32) * 0.5).T.astype(bf16)
    pair1_w[...] = (w1_ref[...].astype(f32) * 0.5).T.astype(bf16)
    pair2_w[...] = (w2_ref[...].astype(f32) * 0.5).T.astype(bf16)
    radial_pad = jnp.concatenate(
        [jnp.zeros((88, 128), f32), wr_ref[...].astype(f32) * 0.5, jnp.zeros((32, 128), f32)], axis=0
    ).T
    cell_x0 = lax.axis_index("gx") * 3
    cell_y0 = lax.axis_index("gy") * 2
    cell_z0 = lax.axis_index("gz") * 8
    rates = rate_ref[...]

    sub8 = lax.broadcasted_iota(jnp.int32, (8, 512), 0)
    lane8 = lax.broadcasted_iota(jnp.int32, (8, 512), 1)
    sub_l = lax.broadcasted_iota(jnp.int32, (8, 128), 0)
    own_mask = (lane8 // 64) == sub8
    own_hot = jnp.where(own_mask, 1.0, 0.0).astype(f32)
    own_hot32 = jnp.concatenate([own_hot, own_hot, jnp.zeros((16, 512), f32)], axis=0).astype(bf16)
    lane_t = lax.broadcasted_iota(jnp.int32, (128, 128), 1)
    low_part = (lane_t >= 104) & (lane_t < 112)
    half_sub = sub_l // 4
    axis_sub = sub_l % 4
    box = jnp.where(axis_sub == 0, 192.0, jnp.where(axis_sub == 1, 64.0, 256.0)).astype(f32)
    box_inv = 1.0 / box
    atom_lane = lax.broadcasted_iota(jnp.int32, (8, 128), 1) // 64

    def column(col, carry):
        cx = col // 2
        cy = col % 2
        ids = nbr_ref[col]
        slot = ids & 7
        z = (ids >> 3) & 31
        y = (ids >> 8) & 7
        x = ids >> 11
        dz = (z - (cell_z0 + sub8) + 1) & 31
        dy = (y - (cell_y0 + cy) + 1) & 7
        dx = x - (cell_x0 + cx) + 1
        dx = jnp.where(dx < 0, dx + 24, dx)
        dx = jnp.where(dx >= 24, dx - 24, dx)
        strip = dx * 3 + dy
        hot_row[...] = strip * 24 + dz * 8 + slot
        lane_row[...] = ((dz + sub8) * 8 + slot) * 16 + strip
        counts = count_ref[col]
        pieces = []
        for g in range(4):
            owner = atom_lane + 2 * g
            count_g = jnp.take_along_axis(counts, owner, axis=1)
            slot_g = lax.broadcasted_iota(jnp.int32, (8, 128), 1) % 64
            pieces.append(jnp.where(slot_g < count_g, 1.0, 0.0).astype(f32))
        live_row[...] = jnp.concatenate(pieces, axis=1)

        def cell(cz):
            rows = []
            for dx_ in range(3):
                for dy_ in range(3):
                    base = ((cx + dx_) * 4 + cy + dy_) * 80 + cz * 8
                    rows.append(feat32[pl.ds(pl.multiple_of(base, 8), 24), :])
            own_base = ((cx + 1) * 4 + cy + 1) * 80 + cz * 8 + 8
            own = feat32[pl.ds(pl.multiple_of(own_base, 8), 8), :]
            left = jnp.concatenate(rows + [jnp.zeros((40, 128), f32)], axis=0)
            right = jnp.concatenate(
                [jnp.zeros((224, 128), f32), own, own, jnp.zeros((16, 128), f32)], axis=0
            )
            table = jnp.concatenate([left, right], axis=1).astype(bf16)
            proj = lax.dot_general(first_w[...], table, NT, preferred_element_type=f32)
            tail = proj[:, 128:256]
            tail_hi = tail.astype(bf16).astype(f32)
            tail = jnp.where(low_part, tail - tail_hi, tail_hi) + radial_pad
            lhs = jnp.concatenate([proj[:, 0:128].astype(bf16), tail.astype(bf16)], axis=1)

            place = []
            hot = hot_row[pl.ds(cz, 1), :]
            packed = lane_row[pl.ds(cz, 1), :]
            live = live_row[pl.ds(cz, 1), :]
            for g in range(4):
                packed_g = jnp.broadcast_to(packed[:, g * 128 : g * 128 + 128], (8, 128))
                where_g = packed_g >> 4
                strip_g = packed_g & 15
                got = jnp.zeros((8, 128), f32)
                for t in range(5):
                    hit = strip_g == (2 * t + half_sub)
                    got = jnp.where(
                        hit,
                        jnp.take_along_axis(pos_ref[col, t * 8 : t * 8 + 8, :], where_g, axis=1),
                        got,
                    )
                got = got + pltpu.roll(got, 4, 0)
                mine = jnp.take_along_axis(
                    pos_ref[col, 40:48, :], atom_lane + 2 * g + (cz + 1) * 8, axis=1
                )
                gap = got - mine
                gap = gap - box * jnp.floor(gap * box_inv + 0.5)
                place.append(gap * 0.125)
            scaled = jnp.concatenate(place, axis=1)
            square = scaled * scaled
            square = square[0:1] + square[1:2] + square[2:3]
            basis = jnp.exp(-jnp.broadcast_to(square, (8, 512)) * rates)
            cell_iota = lax.broadcasted_iota(jnp.int32, (216, 512), 0)
            hots = jnp.where(cell_iota == hot, 1.0, 0.0).astype(f32)
            rhs = jnp.concatenate(
                [jnp.concatenate([hots, basis], axis=0).astype(bf16), own_hot32], axis=0
            )
            half = jnp.dot(lhs, rhs, preferred_element_type=f32)
            latent = (half + half * jnp.tanh(half)).astype(bf16)
            half = jnp.dot(pair1_w[...], latent, preferred_element_type=f32)
            second = (half + half * jnp.tanh(half)).astype(bf16)
            half = jnp.dot(pair2_w[...], second, preferred_element_type=f32)
            third = (half + half * jnp.tanh(half)).astype(bf16)

            weighted = scaled * live
            w_hi = weighted.astype(bf16).astype(f32)
            w_lo = weighted - w_hi
            parts = [live]
            for d in range(3):
                parts += [w_hi[d : d + 1], w_lo[d : d + 1]]
            spread = jnp.concatenate(
                [jnp.where(own_mask, jnp.broadcast_to(p, (8, 512)), 0.0) for p in parts]
                + [jnp.zeros((8, 512), f32)],
                axis=0,
            ).astype(bf16)
            total = lax.dot_general(spread, third, NT, preferred_element_type=f32)
            at = pl.multiple_of((col * 8 + cz) * 8, 8)
            sums[0, pl.ds(at, 8), :] = total[0:8]
            for d in range(3):
                sums[1 + d, pl.ds(at, 8), :] = (
                    total[8 + 16 * d : 16 + 16 * d] + total[16 + 16 * d : 24 + 16 * d]
                )

        def step(i, c):
            for u in range(unroll):
                cell(i * unroll + u)
            return c

        lax.fori_loop(0, 8 // unroll, step, 0)
        return carry

    lax.fori_loop(0, 6, column, 0)
    wv = wv_ref[...]
    invariant = jnp.zeros((384, 128), f32)
    for d in range(3):
        t = sums[1 + d]
        hi = t.astype(bf16)
        lo = (t - hi.astype(f32)).astype(bf16)
        vec = jnp.dot(hi, wv, preferred_element_type=f32) + jnp.dot(
            lo, wv, preferred_element_type=f32
        )
        invariant = invariant + vec * vec
    update = (sums[0] * (1.0 / 64.0) + invariant * (1.0 / 64.0)).astype(bf16)
    out_ref[...] = (
        hid_ref[...].astype(f32) + jnp.dot(update, wo_ref[...], preferred_element_type=f32)
    ).astype(bf16)


def pair_update(
    feat_ext, pos_tab, nbr, counts, wn, ws, wr, rates, w1, w2, wv, wo, hidden, unroll=2
):
    f32, bf16 = jnp.float32, jnp.bfloat16
    vm = pl.BlockSpec(memory_space=pltpu.VMEM)
    return pl.pallas_call(
        functools.partial(pair_kernel, unroll),
        out_shape=jax.ShapeDtypeStruct((384, 128), bf16),
        in_specs=[vm] * 13,
        out_specs=vm,
        scratch_shapes=[
            pltpu.VMEM((1600, 128), f32),
            pltpu.VMEM((128, 256), bf16),
            pltpu.VMEM((128, 128), bf16),
            pltpu.VMEM((128, 128), bf16),
            pltpu.VMEM((8, 512), jnp.int32),
            pltpu.VMEM((8, 512), jnp.int32),
            pltpu.VMEM((8, 512), f32),
            pltpu.VMEM((4, 384, 128), f32),
        ],
        compiler_params=pltpu.CompilerParams(vmem_limit_bytes=40 * 1024 * 1024),
        name="pair_update",
    )(feat_ext, pos_tab, nbr, counts, wn, ws, wr, rates, w1, w2, wv, wo, hidden)


def stencil_rows(first_cell, tap_weights, length):
    cell_ids = jnp.arange(length, dtype=jnp.int32)
    offsets = cell_ids[None, :] - first_cell[:, None]
    tap_ids = jnp.arange(4, dtype=jnp.int32)
    return jnp.sum(
        jnp.where(offsets[:, :, None] == tap_ids[None, None, :], tap_weights[:, None, :], 0.0),
        axis=2,
    )


def spread_grid(first_cols, tap_cols, charge, size_x, size_y, size_z):
    block_count = first_cols.shape[1] // BLOCK

    def spread_block(running, block_index):
        block_start = block_index * BLOCK
        block_first = lax.dynamic_slice_in_dim(first_cols, block_start, BLOCK, 1)
        block_taps = lax.dynamic_slice_in_dim(tap_cols, block_start, BLOCK, 1)
        block_charge = lax.dynamic_slice_in_dim(charge, block_start, BLOCK, 0)
        rows_x = stencil_rows(block_first[0], block_taps[0], size_x) * block_charge[:, None]
        rows_y = stencil_rows(block_first[1], block_taps[1], size_y)
        rows_z = stencil_rows(block_first[2], block_taps[2], size_z)
        plane = (rows_y[:, :, None] * rows_z[:, None, :]).reshape(BLOCK, -1)
        return (running + jnp.dot(rows_x.T, plane, precision=highest), None)

    grid_sum, _ = lax.scan(
        spread_block,
        jnp.zeros((size_x, size_y * size_z), jnp.float32),
        jnp.arange(block_count, dtype=jnp.int32),
    )
    return grid_sum.reshape(size_x, size_y, size_z)


def fold_rims(padded, fold_axis, length):
    core_cells = lax.slice_in_dim(padded, 3, 3 + length, axis=fold_axis)
    lower_rim = lax.slice_in_dim(padded, 0, 2, axis=fold_axis)
    upper_rim = lax.slice_in_dim(padded, length + 5, length + 6, axis=fold_axis)
    lower_pad = [(0, 0)] * padded.ndim
    lower_pad[fold_axis] = (0, length - 2)
    upper_pad = [(0, 0)] * padded.ndim
    upper_pad[fold_axis] = (length - 1, 0)
    return core_cells + jnp.pad(lower_rim, lower_pad) + jnp.pad(upper_rim, upper_pad)


def dft_tables(row_ids, col_ids, length):
    phase_turns = row_ids[:, None] * col_ids[None, :] % length
    angles = phase_turns.astype(jnp.float32) * (2.0 * math.pi / length)
    return (jnp.cos(angles), jnp.sin(angles))


def lines_along_z(pieces, cos_rows, sin_rows):
    return jnp.stack(
        [
            jnp.einsum("nyz,zk->nky", pieces, cos_rows, precision=highest),
            -jnp.einsum("nyz,zk->nky", pieces, sin_rows, precision=highest),
        ],
        axis=1,
    )


def lines_along_y(pieces, cos_rows, sin_rows):
    real_in = pieces[:, 0]
    imag_in = pieces[:, 1]
    real_out = jnp.einsum("nky,yq->nkq", real_in, cos_rows, precision=highest) + jnp.einsum(
        "nky,yq->nkq", imag_in, sin_rows, precision=highest
    )
    imag_out = jnp.einsum("nky,yq->nkq", imag_in, cos_rows, precision=highest) - jnp.einsum(
        "nky,yq->nkq", real_in, sin_rows, precision=highest
    )
    return jnp.stack([real_out, imag_out], axis=1)


def inverse_y(pieces, cos_rows, sin_rows):
    real_in = pieces[:, 0]
    imag_in = pieces[:, 1]
    real_out = jnp.einsum("nmq,qy->nmy", real_in, cos_rows, precision=highest) - jnp.einsum(
        "nmq,qy->nmy", imag_in, sin_rows, precision=highest
    )
    imag_out = jnp.einsum("nmq,qy->nmy", imag_in, cos_rows, precision=highest) + jnp.einsum(
        "nmq,qy->nmy", real_in, sin_rows, precision=highest
    )
    return jnp.stack([real_out, imag_out], axis=1)


def inverse_z(pieces, cos_rows, sin_rows):
    real_in = pieces[:, 0]
    imag_in = pieces[:, 1]
    return jnp.einsum("nky,kz->nyz", real_in, cos_rows, precision=highest) - jnp.einsum(
        "nky,kz->nyz", imag_in, sin_rows, precision=highest
    )


def shards(
    features,
    positions,
    grid_anchor,
    species,
    neighbours,
    neighbour_count,
    w_self,
    w_neighbour,
    w_radial,
    radial_rates,
    w_pair1,
    w_pair2,
    w_vector,
    w_out,
    w_charge,
    species_charge,
):
    cells_x, cells_y, cells_z, slot_count, channels = features.shape
    atom_count = cells_x * cells_y * cells_z * slot_count
    block_count = atom_count // BLOCK
    grid_x, grid_y, grid_z = (cells_x * CELL, cells_y * CELL, cells_z * CELL)
    devices_x, devices_y, devices_z = (
        lax.axis_size("gx"),
        lax.axis_size("gy"),
        lax.axis_size("gz"),
    )
    length_x, length_y, length_z = (grid_x * devices_x, grid_y * devices_y, grid_z * devices_z)
    hidden_rows = features.reshape(atom_count, channels)
    species_rows = species.reshape(atom_count)
    kind_ids = jnp.arange(species_charge.shape[0], dtype=jnp.int32)
    base_charge = jnp.sum(
        jnp.where(species_rows[:, None] == kind_ids[None, :], species_charge[None, :], 0.0), axis=1
    )
    charge = base_charge + jnp.dot(hidden_rows, w_charge, preferred_element_type=jnp.float32)
    feat_ext = padded_2(features, (("gx", 0), ("gy", 1), ("gz", 2)), 1)
    rim_ext = padded_2(positions, (("gx", 0), ("gy", 1), ("gz", 2)), 1)
    place_cols = atom_columns(positions)
    anchor_cols = atom_columns(grid_anchor)
    tap_cols = spline_weights(place_cols - (anchor_cols + 1).astype(jnp.float32))
    grid_start = jnp.stack(
        [
            lax.axis_index("gx") * grid_x,
            lax.axis_index("gy") * grid_y,
            lax.axis_index("gz") * grid_z,
        ]
    )
    first_cols = anchor_cols - grid_start[:, None] + 1
    charge_padded = spread_grid(first_cols, tap_cols, charge, grid_x + 3, grid_y + 3, grid_z + 3)
    charge_halo = padded_2(charge_padded, (("gx", 0), ("gy", 1), ("gz", 2)), 2)
    brick_charge = fold_rims(fold_rims(fold_rims(charge_halo, 0, grid_x), 1, grid_y), 2, grid_z)
    lines_kz = length_z // (devices_y * devices_z)
    lines_ky = length_y // devices_x
    natural_x = jnp.arange(length_x, dtype=jnp.int32)
    natural_y = jnp.arange(length_y, dtype=jnp.int32)
    natural_z = jnp.arange(length_z, dtype=jnp.int32)
    cos_x, sin_x = dft_tables(natural_x, natural_x, length_x)
    cos_y, sin_y = dft_tables(natural_y, natural_y, length_y)
    cos_z, sin_z = dft_tables(natural_z, natural_z, length_z)
    spec_z = lines_along_z(
        lax.all_to_all(brick_charge, "gz", split_axis=1, concat_axis=2, tiled=True),
        cos_rows=cos_z,
        sin_rows=sin_z,
    )
    spec_y = lines_along_y(
        lax.all_to_all(spec_z, ("gy", "gz"), split_axis=2, concat_axis=3, tiled=True),
        cos_rows=cos_y,
        sin_rows=sin_y,
    )
    spec_x = lax.all_to_all(spec_y, "gx", split_axis=3, concat_axis=0, tiled=True)
    real_x = spec_x[:, 0].reshape(length_x, -1)
    imag_x = spec_x[:, 1].reshape(length_x, -1)
    real_k = jnp.dot(cos_x, real_x, precision=highest) + jnp.dot(sin_x, imag_x, precision=highest)
    imag_k = jnp.dot(cos_x, imag_x, precision=highest) - jnp.dot(sin_x, real_x, precision=highest)
    mode_kz = lax.axis_index(("gy", "gz")) * lines_kz + jnp.arange(lines_kz, dtype=jnp.int32)
    mode_ky = lax.axis_index("gx") * lines_ky + jnp.arange(lines_ky, dtype=jnp.int32)
    green = green_values(
        natural_x[:, None, None],
        mode_ky[None, None, :],
        mode_kz[None, :, None],
        length_x,
        length_y,
        length_z,
        2 * grid_y,
    )
    green = green.reshape(length_x, -1) * (1.0 / (length_x * length_y * length_z))
    real_g = real_k * green
    imag_g = imag_k * green
    back_real = jnp.dot(cos_x, real_g, precision=highest) - jnp.dot(
        sin_x, imag_g, precision=highest
    )
    back_imag = jnp.dot(cos_x, imag_g, precision=highest) + jnp.dot(
        sin_x, real_g, precision=highest
    )
    back_x = jnp.stack(
        [
            back_real.reshape(length_x, lines_kz, lines_ky),
            back_imag.reshape(length_x, lines_kz, lines_ky),
        ],
        axis=1,
    )
    back_y = inverse_y(
        lax.all_to_all(back_x, "gx", split_axis=0, concat_axis=3, tiled=True),
        cos_rows=cos_y,
        sin_rows=sin_y,
    )
    potential_lines = inverse_z(
        lax.all_to_all(back_y, ("gy", "gz"), split_axis=3, concat_axis=2, tiled=True),
        cos_rows=cos_z,
        sin_rows=sin_z,
    )
    brick_potential = lax.all_to_all(potential_lines, "gz", split_axis=2, concat_axis=1, tiled=True)
    strips = rim_ext.reshape(cells_x + 2, cells_y + 2, cells_z + 2, 3, slot_count)
    strips = jnp.moveaxis(strips, 3, 2).reshape(cells_x + 2, cells_y + 2, 3, 80)
    strips = jnp.pad(strips, ((0, 0), (0, 0), (0, 1), (0, 48)))
    columns = []
    for cx in range(cells_x):
        for cy in range(cells_y):
            near = strips[cx : cx + 3, cy : cy + 3].reshape(9, 4, 128)
            columns.append(jnp.concatenate([near, near[4:5], near[4:5], near[4:5]]))
    pos_tab = jnp.stack(columns).reshape(6, 48, 128)
    counts = jnp.pad(neighbour_count.reshape(6, 8, 8), ((0, 0), (0, 0), (0, 120)))
    updated = pair_update(
        feat_ext.reshape(-1, channels),
        pos_tab,
        neighbours.reshape(6, 8, 512),
        counts,
        w_neighbour,
        w_self,
        w_radial,
        radial_rates.reshape(8, 1),
        w_pair1,
        w_pair2,
        w_vector,
        w_out,
        hidden_rows,
    )
    features_out = updated.reshape(cells_x, cells_y, cells_z, slot_count, channels)
    potential_ext = padded_2(brick_potential, (("gx", 0), ("gy", 1), ("gz", 2)), 2)
    potential_flat = potential_ext.reshape(grid_x + 4, -1)

    def sample_block(block_index):
        block_start = block_index * BLOCK
        block_first = lax.dynamic_slice_in_dim(first_cols, block_start, BLOCK, 1) + 1
        block_taps = lax.dynamic_slice_in_dim(tap_cols, block_start, BLOCK, 1)
        rows_x = stencil_rows(block_first[0], block_taps[0], grid_x + 4)
        rows_y = stencil_rows(block_first[1], block_taps[1], grid_y + 4)
        rows_z = stencil_rows(block_first[2], block_taps[2], grid_z + 4)
        values = jnp.dot(rows_x, potential_flat, precision=highest).reshape(
            BLOCK, grid_y + 4, grid_z + 4
        )
        partial_sum = jnp.einsum("byz,by->bz", values, rows_y, precision=highest)
        return jnp.sum(partial_sum * rows_z, axis=1)

    site_potential = lax.map(sample_block, jnp.arange(block_count, dtype=jnp.int32))
    site_potential = site_potential.reshape(cells_x, cells_y, cells_z, slot_count)
    return (features_out, site_potential)


def solution(mesh):
    return jax.shard_map(
        shards,
        mesh=mesh,
        in_specs=(
            P("gx", "gy", "gz", None, None),
            P("gx", "gy", "gz", None),
            P("gx", "gy", "gz", None),
            P("gx", "gy", "gz", None),
            P("gx", "gy", "gz", None),
            P("gx", "gy", "gz", None),
            P(),
            P(),
            P(),
            P(),
            P(),
            P(),
            P(),
            P(),
            P(),
            P(),
        ),
        out_specs=(P("gx", "gy", "gz", None, None), P("gx", "gy", "gz", None)),
        check_vma=False,
    )
```

```python
import functools

import jax
import jax.numpy as jnp
import numpy as np
from jax import lax
from jax.experimental import pallas as pl
from jax.experimental.pallas import tpu as pltpu
from jax.sharding import PartitionSpec as P


coulomb_scale = 0.25
smearing = 1.0


def padded_2(block, sides, width):
    for axis, dim in sides:
        count = lax.axis_size(axis)
        forward = [(i, i + 1) for i in range(count - 1)]
        forward.append((count - 1, 0))
        backward = [(target, source) for source, target in forward]
        low = lax.ppermute(
            lax.slice_in_dim(block, block.shape[dim] - width, None, axis=dim), axis, forward
        )
        high = lax.ppermute(lax.slice_in_dim(block, 0, width, axis=dim), axis, backward)
        block = jnp.concatenate([low, block, high], axis=dim)
    return block


NT = (((1,), (1,)), ((), ()))


def pair_kernel(
    unroll,
    feat_ref,
    pos_ref,
    nbr_ref,
    count_ref,
    wn_ref,
    ws_ref,
    wr_ref,
    rate_ref,
    w1_ref,
    w2_ref,
    wv_ref,
    wo_ref,
    hid_ref,
    out_ref,
    feat32,
    first_w,
    pair1_w,
    pair2_w,
    hot_row,
    lane_row,
    live_row,
    sums,
):
    f32, bf16 = jnp.float32, jnp.bfloat16
    feat32[...] = feat_ref[...].astype(f32)
    first_w[:, 0:128] = (wn_ref[...].astype(f32) * 0.5).T.astype(bf16)
    first_w[:, 128:256] = (ws_ref[...].astype(f32) * 0.5).T.astype(bf16)
    pair1_w[...] = (w1_ref[...].astype(f32) * 0.5).T.astype(bf16)
    pair2_w[...] = (w2_ref[...].astype(f32) * 0.5).T.astype(bf16)
    radial_pad = jnp.concatenate(
        [jnp.zeros((88, 128), f32), wr_ref[...].astype(f32) * 0.5, jnp.zeros((32, 128), f32)], axis=0
    ).T
    cell_x0 = lax.axis_index("gx") * 3
    cell_y0 = lax.axis_index("gy") * 2
    cell_z0 = lax.axis_index("gz") * 8
    rates = rate_ref[...]

    sub8 = lax.broadcasted_iota(jnp.int32, (8, 512), 0)
    lane8 = lax.broadcasted_iota(jnp.int32, (8, 512), 1)
    sub_l = lax.broadcasted_iota(jnp.int32, (8, 128), 0)
    own_mask = (lane8 // 64) == sub8
    own_hot = jnp.where(own_mask, 1.0, 0.0).astype(f32)
    own_hot32 = jnp.concatenate([own_hot, own_hot, jnp.zeros((16, 512), f32)], axis=0).astype(bf16)
    lane_t = lax.broadcasted_iota(jnp.int32, (128, 128), 1)
    low_part = (lane_t >= 104) & (lane_t < 112)
    half_sub = sub_l // 4
    axis_sub = sub_l % 4
    box = jnp.where(axis_sub == 0, 192.0, jnp.where(axis_sub == 1, 64.0, 256.0)).astype(f32)
    box_inv = 1.0 / box
    atom_lane = lax.broadcasted_iota(jnp.int32, (8, 128), 1) // 64

    def column(col, carry):
        cx = col // 2
        cy = col % 2
        ids = nbr_ref[col]
        slot = ids & 7
        z = (ids >> 3) & 31
        y = (ids >> 8) & 7
        x = ids >> 11
        dz = (z - (cell_z0 + sub8) + 1) & 31
        dy = (y - (cell_y0 + cy) + 1) & 7
        dx = x - (cell_x0 + cx) + 1
        dx = jnp.where(dx < 0, dx + 24, dx)
        dx = jnp.where(dx >= 24, dx - 24, dx)
        strip = dx * 3 + dy
        hot_row[...] = strip * 24 + dz * 8 + slot
        lane_row[...] = ((dz + sub8) * 8 + slot) * 16 + strip
        counts = count_ref[col]
        pieces = []
        for g in range(4):
            owner = atom_lane + 2 * g
            count_g = jnp.take_along_axis(counts, owner, axis=1)
            slot_g = lax.broadcasted_iota(jnp.int32, (8, 128), 1) % 64
            pieces.append(jnp.where(slot_g < count_g, 1.0, 0.0).astype(f32))
        live_row[...] = jnp.concatenate(pieces, axis=1)

        def cell(cz):
            rows = []
            for dx_ in range(3):
                for dy_ in range(3):
                    base = ((cx + dx_) * 4 + cy + dy_) * 80 + cz * 8
                    rows.append(feat32[pl.ds(pl.multiple_of(base, 8), 24), :])
            own_base = ((cx + 1) * 4 + cy + 1) * 80 + cz * 8 + 8
            own = feat32[pl.ds(pl.multiple_of(own_base, 8), 8), :]
            left = jnp.concatenate(rows + [jnp.zeros((40, 128), f32)], axis=0)
            right = jnp.concatenate(
                [jnp.zeros((224, 128), f32), own, own, jnp.zeros((16, 128), f32)], axis=0
            )
            table = jnp.concatenate([left, right], axis=1).astype(bf16)
            proj = lax.dot_general(first_w[...], table, NT, preferred_element_type=f32)
            tail = proj[:, 128:256]
            tail_hi = tail.astype(bf16).astype(f32)
            tail = jnp.where(low_part, tail - tail_hi, tail_hi) + radial_pad
            lhs = jnp.concatenate([proj[:, 0:128].astype(bf16), tail.astype(bf16)], axis=1)

            place = []
            hot = hot_row[pl.ds(cz, 1), :]
            packed = lane_row[pl.ds(cz, 1), :]
            live = live_row[pl.ds(cz, 1), :]
            for g in range(4):
                packed_g = jnp.broadcast_to(packed[:, g * 128 : g * 128 + 128], (8, 128))
                where_g = packed_g >> 4
                strip_g = packed_g & 15
                got = jnp.zeros((8, 128), f32)
                for t in range(5):
                    hit = strip_g == (2 * t + half_sub)
                    got = jnp.where(
                        hit,
                        jnp.take_along_axis(pos_ref[col, t * 8 : t * 8 + 8, :], where_g, axis=1),
                        got,
                    )
                got = got + pltpu.roll(got, 4, 0)
                mine = jnp.take_along_axis(
                    pos_ref[col, 40:48, :], atom_lane + 2 * g + (cz + 1) * 8, axis=1
                )
                gap = got - mine
                gap = gap - box * jnp.floor(gap * box_inv + 0.5)
                place.append(gap * 0.125)
            scaled = jnp.concatenate(place, axis=1)
            square = scaled * scaled
            square = square[0:1] + square[1:2] + square[2:3]
            basis = jnp.exp(-jnp.broadcast_to(square, (8, 512)) * rates)
            cell_iota = lax.broadcasted_iota(jnp.int32, (216, 512), 0)
            hots = jnp.where(cell_iota == hot, 1.0, 0.0).astype(f32)
            rhs = jnp.concatenate(
                [jnp.concatenate([hots, basis], axis=0).astype(bf16), own_hot32], axis=0
            )
            half = jnp.dot(lhs, rhs, preferred_element_type=f32)
            latent = (half + half * jnp.tanh(half)).astype(bf16)
            half = jnp.dot(pair1_w[...], latent, preferred_element_type=f32)
            second = (half + half * jnp.tanh(half)).astype(bf16)
            half = jnp.dot(pair2_w[...], second, preferred_element_type=f32)
            third = (half + half * jnp.tanh(half)).astype(bf16)

            weighted = scaled * live
            w_hi = weighted.astype(bf16).astype(f32)
            w_lo = weighted - w_hi
            parts = [live]
            for d in range(3):
                parts += [w_hi[d : d + 1], w_lo[d : d + 1]]
            spread = jnp.concatenate(
                [jnp.where(own_mask, jnp.broadcast_to(p, (8, 512)), 0.0) for p in parts]
                + [jnp.zeros((8, 512), f32)],
                axis=0,
            ).astype(bf16)
            total = lax.dot_general(spread, third, NT, preferred_element_type=f32)
            at = pl.multiple_of((col * 8 + cz) * 8, 8)
            sums[0, pl.ds(at, 8), :] = total[0:8]
            for d in range(3):
                sums[1 + d, pl.ds(at, 8), :] = (
                    total[8 + 16 * d : 16 + 16 * d] + total[16 + 16 * d : 24 + 16 * d]
                )

        def step(i, c):
            for u in range(unroll):
                cell(i * unroll + u)
            return c

        lax.fori_loop(0, 8 // unroll, step, 0)
        return carry

    lax.fori_loop(0, 6, column, 0)
    wv = wv_ref[...]
    invariant = jnp.zeros((384, 128), f32)
    for d in range(3):
        t = sums[1 + d]
        hi = t.astype(bf16)
        lo = (t - hi.astype(f32)).astype(bf16)
        vec = jnp.dot(hi, wv, preferred_element_type=f32) + jnp.dot(
            lo, wv, preferred_element_type=f32
        )
        invariant = invariant + vec * vec
    update = (sums[0] * (1.0 / 64.0) + invariant * (1.0 / 64.0)).astype(bf16)
    out_ref[...] = (
        hid_ref[...].astype(f32) + jnp.dot(update, wo_ref[...], preferred_element_type=f32)
    ).astype(bf16)


def pair_update(
    feat_ext, pos_tab, nbr, counts, wn, ws, wr, rates, w1, w2, wv, wo, hidden, unroll=2
):
    f32, bf16 = jnp.float32, jnp.bfloat16
    vm = pl.BlockSpec(memory_space=pltpu.VMEM)
    return pl.pallas_call(
        functools.partial(pair_kernel, unroll),
        out_shape=jax.ShapeDtypeStruct((384, 128), bf16),
        in_specs=[vm] * 13,
        out_specs=vm,
        scratch_shapes=[
            pltpu.VMEM((1600, 128), f32),
            pltpu.VMEM((128, 256), bf16),
            pltpu.VMEM((128, 128), bf16),
            pltpu.VMEM((128, 128), bf16),
            pltpu.VMEM((8, 512), jnp.int32),
            pltpu.VMEM((8, 512), jnp.int32),
            pltpu.VMEM((8, 512), f32),
            pltpu.VMEM((4, 384, 128), f32),
        ],
        compiler_params=pltpu.CompilerParams(vmem_limit_bytes=40 * 1024 * 1024),
        name="pair_update",
    )(feat_ext, pos_tab, nbr, counts, wn, ws, wr, rates, w1, w2, wv, wo, hidden)

def real_basis(length):
    modes = np.arange(length)[:, None]
    cells = np.arange(length)[None, :]
    turns = 2.0 * np.pi * ((modes * cells) % length) / length
    flipped = 2.0 * np.pi * (((length - modes) * cells) % length) / length
    return np.where(modes <= length // 2, np.cos(turns), np.sin(flipped))


def two_parts(table):
    table = np.asarray(table, np.float32)
    high = table.astype(jnp.bfloat16)
    low = (table - high.astype(np.float32)).astype(jnp.bfloat16)
    return np.stack([high, low])


def mode_tables(length):
    modes = np.arange(length)
    signed = np.where(modes > length // 2, modes - length, modes)
    wave = signed * (2.0 * np.pi / length)
    modulus = ((4.0 + 2.0 * np.cos(2.0 * np.pi * modes / length)) / 6.0) ** 2
    weight = np.where((modes == 0) | (modes == length // 2), 1.0, 2.0) / length
    return np.exp(-0.5 * smearing * smearing * wave * wave) / modulus * weight, wave * wave


def ewald_tables():
    basis_z = two_parts(real_basis(256))
    order_y = np.array([4 * p + i for i in range(4) for p in range(16)])
    forward_y = real_basis(64)[:, order_y]
    basis_y = np.stack([two_parts(forward_y), two_parts(forward_y.T)])
    wide = np.zeros((256, 256))
    full_x = real_basis(192)
    for g in range(8):
        wide[:192, 32 * g : 32 * g + 27] = full_x[:, (24 * g - 1 + np.arange(27)) % 192]
    basis_x = two_parts(wide)
    green_x = np.zeros((2, 8, 256))
    gain, square = mode_tables(192)
    green_x[0, :, :192] = gain * (coulomb_scale * 4.0 * np.pi)
    green_x[1, :, :192] = square
    green_x[1, :, 192:] = 1.0
    green_y = np.repeat(np.stack(mode_tables(64))[:, :, None], 128, 2)
    green_z = np.repeat(np.stack(mode_tables(256))[:, :, None], 128, 2)
    return (
        basis_z,
        basis_y,
        basis_x,
        green_x.astype(np.float32),
        green_y.astype(np.float32),
        green_z.astype(np.float32),
    )


def split(value):
    high = value.astype(jnp.bfloat16)
    return high, (value - high.astype(jnp.float32)).astype(jnp.bfloat16)


def dot3(a, b, dims=(((1,), (0,)), ((), ()))):
    def one(u, v):
        return lax.dot_general(u, v, dims, preferred_element_type=jnp.float32)

    return one(a[0], b[0]) + (one(a[0], b[1]) + one(a[1], b[0]))


def swap_groups(pieces, shift):
    lane = lax.broadcasted_iota(jnp.int32, pieces[0].shape, 1) // 32
    out = None
    for k, piece in enumerate(pieces):
        moved = pltpu.roll(piece, (32 * (k - shift)) % 128, 1) if k != shift else piece
        out = moved if out is None else jnp.where(lane == k, moved, out)
    return out


def tap_rows(fraction):
    square = fraction * fraction
    cube = square * fraction
    remain = 1.0 - fraction
    return (
        remain * remain * remain / 6.0,
        (3.0 * cube - 6.0 * square + 4.0) / 6.0,
        (-3.0 * cube + 3.0 * square + 3.0 * fraction + 1.0) / 6.0,
        cube / 6.0,
    )


def pick_taps(offset, taps):
    out = jnp.zeros(offset.shape, jnp.float32)
    for t in range(4):
        out = jnp.where(offset == t, taps[t], out)
    return out


def ewald_kernel(
    atoms_ref,
    bz_ref,
    by_ref,
    bx_ref,
    gx_ref,
    gy_ref,
    gz_ref,
    out_ref,
    rx_atoms,
    z_high,
    z_low,
    stencil,
    tx_b,
    rx_b,
    tx_c,
    rx_c,
    tx_c2,
    rx_c2,
    tx_b2,
    rx_b2,
    parts,
    rx_parts,
    sa,
    ra,
    sb,
    rb,
    sc,
    rc,
    sc2,
    rc2,
    sb2,
    rb2,
    sp,
    rp,
):
    f32 = jnp.float32
    MESH = pl.DeviceIdType.MESH
    ix, iy, iz = lax.axis_index("gx"), lax.axis_index("gy"), lax.axis_index("gz")
    me = iy * 4 + iz
    barrier = pltpu.get_barrier_semaphore()

    def yz_peer(r):
        other = lax.rem(me + r, 16)
        return other, (ix, other // 4, lax.rem(other, 4))

    def x_peer(r):
        other = lax.rem(ix + r, 8)
        return other, (other, iy, iz)

    def greet_yz(r, c):
        pl.semaphore_signal(barrier, inc=1, device_id=yz_peer(r)[1], device_id_type=MESH)
        return c

    def greet_x(r, c):
        pl.semaphore_signal(barrier, inc=1, device_id=x_peer(r)[1], device_id_type=MESH)
        return c

    lax.fori_loop(1, 16, greet_yz, 0)
    lax.fori_loop(1, 8, greet_x, 0)
    pl.semaphore_wait(barrier, 22)

    routes = [(0, 3, 3, 1), (0, 0, 0, 1), (0, 1, 0, 0), (0, 2, 0, 0)]
    routes += [(1, 1, 0, 1), (1, 2, 0, 1), (1, 3, 0, 0), (1, 0, 1, 0)]

    def atom_copy(half, to_z, step_y, place):
        return pltpu.make_async_remote_copy(
            src_ref=atoms_ref.at[half],
            dst_ref=rx_atoms.at[iz, place],
            send_sem=sa.at[half, to_z],
            recv_sem=ra.at[iz, place],
            device_id=(ix, lax.rem(iy + step_y, 4), to_z),
            device_id_type=MESH,
        )

    for half, to_z, step_y, place in routes:
        if step_y:
            atom_copy(half, to_z, step_y, place).start()
        else:

            @pl.when(iz != to_z)
            def _():
                atom_copy(half, to_z, step_y, place).start()

            @pl.when(iz == to_z)
            def _():
                rx_atoms[iz, place] = atoms_ref[half]

    from_y = [
        lax.rem(iy + jnp.where(iz == 0, 3, 0), 4),
        lax.rem(iy + jnp.where(iz == 3, 1, 0), 4),
    ]
    edge = jnp.where((iz == 0) | (iz == 3), 1, 0)
    from_half = [edge, 1 - edge]

    def atom_wait(s, u):
        @pl.when((s != iz) | (from_y[u] != iy))
        def _():
            pltpu.make_async_remote_copy(
                src_ref=atoms_ref.at[0],
                dst_ref=rx_atoms.at[s, u],
                send_sem=sa.at[0, 0],
                recv_sem=ra.at[s, u],
                device_id=(ix, from_y[u], s),
                device_id_type=MESH,
            ).wait_recv()

    for s in range(4):
        for u in range(2):
            atom_wait(s, u)

    z_ids = lax.broadcasted_iota(jnp.int32, (256, 256), 0)
    x_ids = lax.broadcasted_iota(jnp.int32, (32, 256), 0) + (ix * 24 - 1)
    y_first = iy * 16 + iz * 4

    def spread(slot, total):
        rows = rx_atoms[slot // 2, lax.rem(slot, 2)]
        anchor = rows[3:6].astype(jnp.int32)
        weights_z = pick_taps((z_ids - anchor[2:3]) & 255, tap_rows(rows[2:3]))
        high, low = split(weights_z)
        at = pl.ds(pl.multiple_of(slot * 256, 256), 256)
        z_high[:, at] = high
        z_low[:, at] = low
        weights_x = pick_taps(x_ids - anchor[0:1], tap_rows(rows[0:1]))
        taps_y = tap_rows(rows[1:2])
        blocks = [
            weights_x * pick_taps((y_first + i - anchor[1:2]) & 63, taps_y) for i in range(4)
        ]
        both = jnp.concatenate(blocks, axis=0)
        stencil[:, at] = both
        return total + dot3((high, low), split(both * rows[6:7]), NT)

    lines = lax.fori_loop(0, 8, spread, jnp.zeros((256, 128), f32))
    spectrum = dot3((bz_ref[0], bz_ref[1]), split(lines))
    tx_b[...] = spectrum.reshape(16, 16, 128)
    rx_b[me] = tx_b[me]

    def exchange(tx, rx, send, recv, peer, count, mine):
        def copy(r):
            other, where = peer(r)
            return pltpu.make_async_remote_copy(
                src_ref=tx.at[other],
                dst_ref=rx.at[mine],
                send_sem=send.at[other],
                recv_sem=recv.at[mine],
                device_id=where,
                device_id_type=MESH,
            )

        def arrival(r):
            other, where = peer(r)
            return pltpu.make_async_remote_copy(
                src_ref=tx.at[other],
                dst_ref=rx.at[other],
                send_sem=send.at[other],
                recv_sem=recv.at[other],
                device_id=where,
                device_id_type=MESH,
            )

        def start(r, c):
            copy(r).start()
            return c

        def wait(r, c):
            arrival(r).wait_recv()
            return c

        def drain(r, c):
            copy(r).wait_send()
            return c

        lax.fori_loop(1, count, start, 0)
        return (
            lambda: lax.fori_loop(1, count, wait, 0),
            lambda: lax.fori_loop(1, count, drain, 0),
        )

    arrive_b, drain_b = exchange(tx_b, rx_b, sb, rb, yz_peer, 16, me)
    arrive_b()
    flat_b = rx_b.reshape(256, 128)
    columns = []
    for group in range(4):
        pieces = [flat_b[pl.ds(group * 4 + k, 16, 16), :] for k in range(4)]
        columns.append(jnp.concatenate([swap_groups(pieces, i) for i in range(4)], axis=0))
    lines_y = jnp.concatenate(columns, axis=1)
    modes_y = dot3((by_ref[0, 0], by_ref[0, 1]), split(lines_y))
    tx_c[...] = modes_y.reshape(8, 8, 512)
    rx_c[ix] = tx_c[ix]
    arrive_c, drain_c = exchange(tx_c, rx_c, sc, rc, x_peer, 8, ix)

    gain_z = gz_ref[0, pl.ds(pl.multiple_of(me * 16, 16), 16), :]
    square_z = gz_ref[1, pl.ds(pl.multiple_of(me * 16, 16), 16), :]
    gain_y = gy_ref[0, pl.ds(pl.multiple_of(ix * 8, 8), 8), :]
    square_y = gy_ref[1, pl.ds(pl.multiple_of(ix * 8, 8), 8), :]
    gain_yz = (gain_z[:, None, :] * gain_y[None, :, :]).reshape(128, 128)
    square_yz = (square_z[:, None, :] + square_y[None, :, :]).reshape(128, 128)
    greens = []
    for h in range(2):
        lanes = slice(128 * h, 128 * h + 128)
        total = square_yz + gx_ref[1, 0:1, lanes]
        value = gain_yz * gx_ref[0, 0:1, lanes] / (total + 1.0 / 1024.0)
        greens.append(jnp.where(total == 0.0, 0.0, value))
    green = jnp.concatenate(greens, axis=1)

    arrive_c()
    rows_x = []
    for group in range(4):
        for k in range(4):
            halves = [
                swap_groups(
                    [rx_c[4 * h + g, :, group * 128 : group * 128 + 128] for g in range(4)], k
                )
                for h in range(2)
            ]
            rows_x.append(jnp.concatenate(halves, axis=1))
    lines_x = jnp.concatenate(rows_x, axis=0)
    basis_x = (bx_ref[0], bx_ref[1])
    filtered = dot3(split(lines_x), basis_x, NT) * green
    back_x = dot3(split(filtered), basis_x)
    for g in range(8):
        half = g // 4
        for group in range(4):
            pieces = [
                back_x[(group * 4 + k) * 8 : (group * 4 + k) * 8 + 8, half * 128 : half * 128 + 128]
                for k in range(4)
            ]
            tx_c2[g, :, group * 128 : group * 128 + 128] = swap_groups(pieces, g % 4)
    rx_c2[ix] = tx_c2[ix]
    arrive_c2, drain_c2 = exchange(tx_c2, rx_c2, sc2, rc2, x_peer, 8, ix)
    arrive_c2()
    back_y = dot3((by_ref[1, 0], by_ref[1, 1]), split(rx_c2[...].reshape(64, 512)))
    flat_b2 = tx_b2.reshape(256, 128)
    for group in range(4):
        pieces = [back_y[16 * i : 16 * i + 16, group * 128 : group * 128 + 128] for i in range(4)]
        for k in range(4):
            flat_b2[pl.ds(group * 4 + k, 16, 16), :] = swap_groups(pieces, k)
    rx_b2[me] = tx_b2[me]
    arrive_b2, drain_b2 = exchange(tx_b2, rx_b2, sb2, rb2, yz_peer, 16, me)
    arrive_b2()
    back_z = rx_b2[...].reshape(256, 128).T
    potential = split(dot3(split(back_z), (bz_ref[0], bz_ref[1])))

    def sample(slot, c):
        at = pl.ds(pl.multiple_of(slot * 256, 256), 256)
        values = dot3(potential, (z_high[:, at], z_low[:, at]))
        parts[slot] = jnp.sum(values * stencil[:, at], axis=0, keepdims=True)
        return c

    lax.fori_loop(0, 8, sample, 0)

    def part_copy(s, u):
        return pltpu.make_async_remote_copy(
            src_ref=parts.at[2 * s + u],
            dst_ref=rx_parts.at[from_half[u], iz],
            send_sem=sp.at[s, u],
            recv_sem=rp.at[from_half[u], iz],
            device_id=(ix, from_y[u], s),
            device_id_type=MESH,
        )

    for s in range(4):
        for u in range(2):

            @pl.when((s != iz) | (from_y[u] != iy))
            def _():
                part_copy(s, u).start()

            @pl.when((s == iz) & (from_y[u] == iy))
            def _():
                rx_parts[from_half[u], iz] = parts[2 * s + u]

    def part_wait(half, to_z, step_y):
        pltpu.make_async_remote_copy(
            src_ref=parts.at[0],
            dst_ref=rx_parts.at[half, to_z],
            send_sem=sp.at[0, 0],
            recv_sem=rp.at[half, to_z],
            device_id=(ix, lax.rem(iy + step_y, 4), to_z),
            device_id_type=MESH,
        ).wait_recv()

    for half, to_z, step_y, place in routes:
        if step_y:
            part_wait(half, to_z, step_y)
        else:

            @pl.when(iz != to_z)
            def _():
                part_wait(half, to_z, step_y)

    for half in range(2):
        out_ref[half] = (
            (rx_parts[half, 0] + rx_parts[half, 1]) + (rx_parts[half, 2] + rx_parts[half, 3])
        )

    for half, to_z, step_y, place in routes:
        if step_y:
            atom_copy(half, to_z, step_y, place).wait_send()
        else:

            @pl.when(iz != to_z)
            def _():
                atom_copy(half, to_z, step_y, place).wait_send()

    drain_b()
    drain_c()
    drain_c2()
    drain_b2()
    for s in range(4):
        for u in range(2):

            @pl.when((s != iz) | (from_y[u] != iy))
            def _():
                part_copy(s, u).wait_send()


def ewald(atoms):
    f32, bf16 = jnp.float32, jnp.bfloat16
    vm = pl.BlockSpec(memory_space=pltpu.VMEM)
    dma = pltpu.SemaphoreType.DMA
    tables = [jnp.asarray(t) for t in ewald_tables()]
    return pl.pallas_call(
        ewald_kernel,
        out_shape=jax.ShapeDtypeStruct((2, 1, 256), f32),
        in_specs=[vm] * 7,
        out_specs=vm,
        scratch_shapes=[
            pltpu.VMEM((4, 2, 8, 256), f32),
            pltpu.VMEM((256, 2048), bf16),
            pltpu.VMEM((256, 2048), bf16),
            pltpu.VMEM((128, 2048), f32),
            pltpu.VMEM((16, 16, 128), f32),
            pltpu.VMEM((16, 16, 128), f32),
            pltpu.VMEM((8, 8, 512), f32),
            pltpu.VMEM((8, 8, 512), f32),
            pltpu.VMEM((8, 8, 512), f32),
            pltpu.VMEM((8, 8, 512), f32),
            pltpu.VMEM((16, 16, 128), f32),
            pltpu.VMEM((16, 16, 128), f32),
            pltpu.VMEM((8, 1, 256), f32),
            pltpu.VMEM((2, 4, 1, 256), f32),
            dma((2, 4)),
            dma((4, 2)),
            dma((16,)),
            dma((16,)),
            dma((8,)),
            dma((8,)),
            dma((8,)),
            dma((8,)),
            dma((16,)),
            dma((16,)),
            dma((4, 2)),
            dma((2, 4)),
        ],
        compiler_params=pltpu.CompilerParams(
            collective_id=0, has_side_effects=True, vmem_limit_bytes=40 * 1024 * 1024
        ),
        name="ewald",
    )(atoms, *tables)


def shards(
    features,
    positions,
    grid_anchor,
    species,
    neighbours,
    neighbour_count,
    w_self,
    w_neighbour,
    w_radial,
    radial_rates,
    w_pair1,
    w_pair2,
    w_vector,
    w_out,
    w_charge,
    species_charge,
):
    cells_x, cells_y, cells_z, slot_count, channels = features.shape
    atom_count = cells_x * cells_y * cells_z * slot_count
    hidden_rows = features.reshape(atom_count, channels)
    species_rows = species.reshape(atom_count)
    kind_ids = jnp.arange(species_charge.shape[0], dtype=jnp.int32)
    base_charge = jnp.sum(
        jnp.where(species_rows[:, None] == kind_ids[None, :], species_charge[None, :], 0.0), axis=1
    )
    charge = base_charge + jnp.dot(hidden_rows, w_charge, preferred_element_type=jnp.float32)
    feat_ext = padded_2(features, (("gx", 0), ("gy", 1), ("gz", 2)), 1)
    rim_ext = padded_2(positions, (("gx", 0), ("gy", 1), ("gz", 2)), 1)

    def by_half(values, width):
        grouped = values.reshape(cells_x, cells_y, cells_z, width, slot_count)
        return grouped.transpose(1, 3, 0, 2, 4).reshape(cells_y, width, -1)

    place = by_half(positions, 3)
    anchor = by_half(grid_anchor, 3).astype(jnp.float32)
    atoms = jnp.concatenate(
        [place - (anchor + 1.0), anchor, by_half(charge, 1), jnp.zeros((2, 1, 192), jnp.float32)],
        axis=1,
    )
    site = ewald(jnp.pad(atoms, ((0, 0), (0, 0), (0, 64))))
    site_potential = site[:, 0, :192].reshape(cells_y, cells_x, cells_z, slot_count)
    site_potential = site_potential.transpose(1, 0, 2, 3)
    strips = rim_ext.reshape(cells_x + 2, cells_y + 2, cells_z + 2, 3, slot_count)
    strips = jnp.moveaxis(strips, 3, 2).reshape(cells_x + 2, cells_y + 2, 3, 80)
    strips = jnp.pad(strips, ((0, 0), (0, 0), (0, 1), (0, 48)))
    columns = []
    for cx in range(cells_x):
        for cy in range(cells_y):
            near = strips[cx : cx + 3, cy : cy + 3].reshape(9, 4, 128)
            columns.append(jnp.concatenate([near, near[4:5], near[4:5], near[4:5]]))
    pos_tab = jnp.stack(columns).reshape(6, 48, 128)
    counts = jnp.pad(neighbour_count.reshape(6, 8, 8), ((0, 0), (0, 0), (0, 120)))
    updated = pair_update(
        feat_ext.reshape(-1, channels),
        pos_tab,
        neighbours.reshape(6, 8, 512),
        counts,
        w_neighbour,
        w_self,
        w_radial,
        radial_rates.reshape(8, 1),
        w_pair1,
        w_pair2,
        w_vector,
        w_out,
        hidden_rows,
    )
    features_out = updated.reshape(cells_x, cells_y, cells_z, slot_count, channels)
    return (features_out, site_potential)


def solution(mesh):
    return jax.shard_map(
        shards,
        mesh=mesh,
        in_specs=(
            P("gx", "gy", "gz", None, None),
            P("gx", "gy", "gz", None),
            P("gx", "gy", "gz", None),
            P("gx", "gy", "gz", None),
            P("gx", "gy", "gz", None),
            P("gx", "gy", "gz", None),
            P(),
            P(),
            P(),
            P(),
            P(),
            P(),
            P(),
            P(),
            P(),
            P(),
        ),
        out_specs=(P("gx", "gy", "gz", None, None), P("gx", "gy", "gz", None)),
        check_vma=False,
    )
```

```python
import functools

import jax
import jax.numpy as jnp
import numpy as np
from jax import lax
from jax.experimental import pallas as pl
from jax.experimental.pallas import tpu as pltpu
from jax.sharding import PartitionSpec as P


coulomb_scale = 0.25
smearing = 1.0


NT = (((1,), (1,)), ((), ()))


def real_basis(length):
    modes = np.arange(length)[:, None]
    cells = np.arange(length)[None, :]
    turns = 2.0 * np.pi * ((modes * cells) % length) / length
    flipped = 2.0 * np.pi * (((length - modes) * cells) % length) / length
    return np.where(modes <= length // 2, np.cos(turns), np.sin(flipped))


def two_parts(table):
    table = np.asarray(table, np.float32)
    high = table.astype(jnp.bfloat16)
    low = (table - high.astype(np.float32)).astype(jnp.bfloat16)
    return np.stack([high, low])


def mode_tables(length):
    modes = np.arange(length)
    signed = np.where(modes > length // 2, modes - length, modes)
    wave = signed * (2.0 * np.pi / length)
    modulus = ((4.0 + 2.0 * np.cos(2.0 * np.pi * modes / length)) / 6.0) ** 2
    weight = np.where((modes == 0) | (modes == length // 2), 1.0, 2.0) / length
    return np.exp(-0.5 * smearing * smearing * wave * wave) / modulus * weight, wave * wave


def ewald_tables():
    basis_z = two_parts(real_basis(256))
    order_y = np.array([4 * p + i for i in range(4) for p in range(16)])
    forward_y = real_basis(64)[:, order_y]
    basis_y = np.stack([two_parts(forward_y), two_parts(forward_y.T)])
    wide = np.zeros((256, 256))
    full_x = real_basis(192)
    for g in range(8):
        wide[:192, 32 * g : 32 * g + 27] = full_x[:, (24 * g - 1 + np.arange(27)) % 192]
    basis_x = two_parts(wide)
    green_x = np.zeros((2, 8, 256))
    gain, square = mode_tables(192)
    green_x[0, :, :192] = gain * (coulomb_scale * 4.0 * np.pi)
    green_x[1, :, :192] = square
    green_x[1, :, 192:] = 1.0
    green_y = np.repeat(np.stack(mode_tables(64))[:, :, None], 128, 2)
    green_z = np.repeat(np.stack(mode_tables(256))[:, :, None], 128, 2)
    return (
        basis_z,
        basis_y,
        basis_x,
        green_x.astype(np.float32),
        green_y.astype(np.float32),
        green_z.astype(np.float32),
    )


def split(value):
    high = value.astype(jnp.bfloat16)
    return high, (value - high.astype(jnp.float32)).astype(jnp.bfloat16)


def dot3(a, b, dims=(((1,), (0,)), ((), ()))):
    def one(u, v):
        return lax.dot_general(u, v, dims, preferred_element_type=jnp.float32)

    return one(a[0], b[0]) + (one(a[0], b[1]) + one(a[1], b[0]))


def swap_groups(pieces, shift):
    lane = lax.broadcasted_iota(jnp.int32, pieces[0].shape, 1) // 32
    out = None
    for k, piece in enumerate(pieces):
        moved = pltpu.roll(piece, (32 * (k - shift)) % 128, 1) if k != shift else piece
        out = moved if out is None else jnp.where(lane == k, moved, out)
    return out


def tap_rows(fraction):
    square = fraction * fraction
    cube = square * fraction
    remain = 1.0 - fraction
    return (
        remain * remain * remain / 6.0,
        (3.0 * cube - 6.0 * square + 4.0) / 6.0,
        (-3.0 * cube + 3.0 * square + 3.0 * fraction + 1.0) / 6.0,
        cube / 6.0,
    )


def pick_taps(offset, taps):
    out = jnp.zeros(offset.shape, jnp.float32)
    for t in range(4):
        out = jnp.where(offset == t, taps[t], out)
    return out


def layer_kernel(
    unroll,
    feat_ref,
    pos_ref,
    atoms_ref,
    nbr_ref,
    count_ref,
    wn_ref,
    ws_ref,
    wr_ref,
    rate_ref,
    w1_ref,
    w2_ref,
    wv_ref,
    wo_ref,
    wc_ref,
    kind_ref,
    bz_ref,
    by_ref,
    bx_ref,
    gx_ref,
    gy_ref,
    gz_ref,
    out_ref,
    site_ref,
    feat_ext,
    pos_ext,
    pos_tab,
    feat32,
    first_w,
    pair1_w,
    pair2_w,
    hot_row,
    lane_row,
    live_row,
    sums,
    tx_atoms,
    rx_atoms,
    z_high,
    z_low,
    stencil,
    tx_b,
    rx_b,
    tx_c,
    rx_c,
    tx_c2,
    rx_c2,
    tx_b2,
    rx_b2,
    parts,
    rx_parts,
    sa,
    ra,
    sb,
    rb,
    sc,
    rc,
    sc2,
    rc2,
    sb2,
    rb2,
    sp,
    rp,
    sf,
    rf,
    sq,
    rq,
):
    bf16 = jnp.bfloat16
    f32 = jnp.float32
    MESH = pl.DeviceIdType.MESH
    ix, iy, iz = lax.axis_index("gx"), lax.axis_index("gy"), lax.axis_index("gz")
    me = iy * 4 + iz
    barrier = pltpu.get_barrier_semaphore()

    def yz_peer(r):
        other = lax.rem(me + r, 16)
        return other, (ix, other // 4, lax.rem(other, 4))

    def x_peer(r):
        other = lax.rem(ix + r, 8)
        return other, (other, iy, iz)

    def greet_yz(r, c):
        pl.semaphore_signal(barrier, inc=1, device_id=yz_peer(r)[1], device_id_type=MESH)
        return c

    def greet_x(r, c):
        pl.semaphore_signal(barrier, inc=1, device_id=x_peer(r)[1], device_id_type=MESH)
        return c

    lax.fori_loop(1, 16, greet_yz, 0)
    lax.fori_loop(1, 8, greet_x, 0)

    def halo_peer(index):
        ox, oy, oz = index // 9 - 1, index // 3 % 3 - 1, index % 3 - 1
        return (lax.rem(ix + ox + 8, 8), lax.rem(iy + oy + 4, 4), lax.rem(iz + oz + 4, 4))

    def halo_span(step, cells):
        if step == 0:
            return pl.ds(0, cells), pl.ds(1, cells)
        return (pl.ds(cells - 1, 1), pl.ds(0, 1)) if step > 0 else (pl.ds(0, 1), pl.ds(cells + 1, 1))

    halo_ids = [n for n in range(27) if n != 13]

    def halo_copies(index):
        steps = (index // 9 - 1, index // 3 % 3 - 1, index % 3 - 1)
        spans = [halo_span(step, cells) for step, cells in zip(steps, (3, 2, 8))]
        source = tuple(span[0] for span in spans)
        target = tuple(span[1] for span in spans)
        return [
            pltpu.make_async_remote_copy(
                src_ref=src.at[source],
                dst_ref=dst.at[target],
                send_sem=send.at[index],
                recv_sem=recv.at[index],
                device_id=halo_peer(index),
                device_id_type=MESH,
            )
            for src, dst, send, recv in ((feat_ref, feat_ext, sf, rf), (pos_ref, pos_ext, sq, rq))
        ]

    for index in halo_ids:
        pl.semaphore_signal(barrier, inc=1, device_id=halo_peer(index), device_id_type=MESH)

    for half in range(2):
        own_rows = feat_ref[:, half].astype(f32).reshape(192, 128).astype(bf16)
        readout = lax.dot_general(wc_ref[...], own_rows, NT, preferred_element_type=f32)[0:1]
        rows = atoms_ref[half]
        kinds = rows[6:7]
        base = jnp.where(kinds == 0.0, kind_ref[0], jnp.where(kinds == 1.0, kind_ref[1], 0.0))
        total = jnp.concatenate([base[:, 0:192] + readout, jnp.zeros((1, 64), f32)], axis=1)
        tx_atoms[half, 0:3, :] = rows[0:3] - (rows[3:6] + 1.0)
        tx_atoms[half, 3:6, :] = rows[3:6]
        tx_atoms[half, 6:7, :] = total
        tx_atoms[half, 7:8, :] = jnp.zeros((1, 256), f32)

    pl.semaphore_wait(barrier, 48)

    routes = [(0, 3, 3, 1), (0, 0, 0, 1), (0, 1, 0, 0), (0, 2, 0, 0)]
    routes += [(1, 1, 0, 1), (1, 2, 0, 1), (1, 3, 0, 0), (1, 0, 1, 0)]

    def atom_copy(half, to_z, step_y, place):
        return pltpu.make_async_remote_copy(
            src_ref=tx_atoms.at[half],
            dst_ref=rx_atoms.at[iz, place],
            send_sem=sa.at[half, to_z],
            recv_sem=ra.at[iz, place],
            device_id=(ix, lax.rem(iy + step_y, 4), to_z),
            device_id_type=MESH,
        )

    for half, to_z, step_y, place in routes:
        if step_y:
            atom_copy(half, to_z, step_y, place).start()
        else:

            @pl.when(iz != to_z)
            def _():
                atom_copy(half, to_z, step_y, place).start()

            @pl.when(iz == to_z)
            def _():
                rx_atoms[iz, place] = tx_atoms[half]

    for index in halo_ids:
        for copy in halo_copies(index):
            copy.start()
    feat_ext[1:4, 1:3, 1:9] = feat_ref[...]
    pos_ext[1:4, 1:3, 1:9] = pos_ref[...]
    first_w[:, 0:128] = (wn_ref[...].astype(f32) * 0.5).T.astype(bf16)
    first_w[:, 128:256] = (ws_ref[...].astype(f32) * 0.5).T.astype(bf16)
    pair1_w[...] = (w1_ref[...].astype(f32) * 0.5).T.astype(bf16)
    pair2_w[...] = (w2_ref[...].astype(f32) * 0.5).T.astype(bf16)
    radial_pad = jnp.concatenate(
        [jnp.zeros((88, 128), f32), wr_ref[...].astype(f32) * 0.5, jnp.zeros((32, 128), f32)], axis=0
    ).T
    cell_x0, cell_y0, cell_z0 = ix * 3, iy * 2, iz * 8
    rates = rate_ref[...]

    sub8 = lax.broadcasted_iota(jnp.int32, (8, 512), 0)
    lane8 = lax.broadcasted_iota(jnp.int32, (8, 512), 1)
    sub_l = lax.broadcasted_iota(jnp.int32, (8, 128), 0)
    own_mask = (lane8 // 64) == sub8
    own_hot = jnp.where(own_mask, 1.0, 0.0).astype(f32)
    own_hot32 = jnp.concatenate([own_hot, own_hot, jnp.zeros((16, 512), f32)], axis=0).astype(bf16)
    lane_t = lax.broadcasted_iota(jnp.int32, (128, 128), 1)
    low_part = (lane_t >= 104) & (lane_t < 112)
    half_sub = sub_l // 4
    axis_sub = sub_l % 4
    box = jnp.where(axis_sub == 0, 192.0, jnp.where(axis_sub == 1, 64.0, 256.0)).astype(f32)
    box_inv = 1.0 / box
    atom_lane = lax.broadcasted_iota(jnp.int32, (8, 128), 1) // 64


    def column(col):
        cx = col // 2
        cy = col % 2
        ids = nbr_ref[col]
        slot = ids & 7
        z = (ids >> 3) & 31
        y = (ids >> 8) & 7
        x = ids >> 11
        dz = (z - (cell_z0 + sub8) + 1) & 31
        dy = (y - (cell_y0 + cy) + 1) & 7
        dx = x - (cell_x0 + cx) + 1
        dx = jnp.where(dx < 0, dx + 24, dx)
        dx = jnp.where(dx >= 24, dx - 24, dx)
        strip = dx * 3 + dy
        hot_row[...] = strip * 24 + dz * 8 + slot
        lane_row[...] = ((dz + sub8) * 8 + slot) * 16 + strip
        counts = count_ref[col]
        pieces = []
        for g in range(4):
            owner = atom_lane + 2 * g
            count_g = jnp.take_along_axis(counts, owner, axis=1)
            slot_g = lax.broadcasted_iota(jnp.int32, (8, 128), 1) % 64
            pieces.append(jnp.where(slot_g < count_g, 1.0, 0.0).astype(f32))
        live_row[...] = jnp.concatenate(pieces, axis=1)

        def cell(cz):
            rows = []
            for dx_ in range(3):
                for dy_ in range(3):
                    base = ((cx + dx_) * 4 + cy + dy_) * 80 + cz * 8
                    rows.append(feat32[pl.ds(pl.multiple_of(base, 8), 24), :])
            own_base = ((cx + 1) * 4 + cy + 1) * 80 + cz * 8 + 8
            own = feat32[pl.ds(pl.multiple_of(own_base, 8), 8), :]
            left = jnp.concatenate(rows + [jnp.zeros((40, 128), f32)], axis=0)
            right = jnp.concatenate(
                [jnp.zeros((224, 128), f32), own, own, jnp.zeros((16, 128), f32)], axis=0
            )
            table = jnp.concatenate([left, right], axis=1).astype(bf16)
            proj = lax.dot_general(first_w[...], table, NT, preferred_element_type=f32)
            tail = proj[:, 128:256]
            tail_hi = tail.astype(bf16).astype(f32)
            tail = jnp.where(low_part, tail - tail_hi, tail_hi) + radial_pad
            lhs = jnp.concatenate([proj[:, 0:128].astype(bf16), tail.astype(bf16)], axis=1)

            place = []
            hot = hot_row[pl.ds(cz, 1), :]
            packed = lane_row[pl.ds(cz, 1), :]
            live = live_row[pl.ds(cz, 1), :]
            for g in range(4):
                packed_g = jnp.broadcast_to(packed[:, g * 128 : g * 128 + 128], (8, 128))
                where_g = packed_g >> 4
                strip_g = packed_g & 15
                got = jnp.zeros((8, 128), f32)
                for t in range(5):
                    hit = strip_g == (2 * t + half_sub)
                    got = jnp.where(
                        hit,
                        jnp.take_along_axis(pos_tab[col, t * 8 : t * 8 + 8, :], where_g, axis=1),
                        got,
                    )
                got = got + pltpu.roll(got, 4, 0)
                mine = jnp.take_along_axis(
                    pos_tab[col, 40:48, :], atom_lane + 2 * g + (cz + 1) * 8, axis=1
                )
                gap = got - mine
                gap = gap - box * jnp.floor(gap * box_inv + 0.5)
                place.append(gap * 0.125)
            scaled = jnp.concatenate(place, axis=1)
            square = scaled * scaled
            square = square[0:1] + square[1:2] + square[2:3]
            basis = jnp.exp(-jnp.broadcast_to(square, (8, 512)) * rates)
            cell_iota = lax.broadcasted_iota(jnp.int32, (216, 512), 0)
            hots = jnp.where(cell_iota == hot, 1.0, 0.0).astype(f32)
            rhs = jnp.concatenate(
                [jnp.concatenate([hots, basis], axis=0).astype(bf16), own_hot32], axis=0
            )
            half = jnp.dot(lhs, rhs, preferred_element_type=f32)
            latent = (half + half * jnp.tanh(half)).astype(bf16)
            half = jnp.dot(pair1_w[...], latent, preferred_element_type=f32)
            second = (half + half * jnp.tanh(half)).astype(bf16)
            half = jnp.dot(pair2_w[...], second, preferred_element_type=f32)
            third = (half + half * jnp.tanh(half)).astype(bf16)

            weighted = scaled * live
            w_hi = weighted.astype(bf16).astype(f32)
            w_lo = weighted - w_hi
            parts = [live]
            for d in range(3):
                parts += [w_hi[d : d + 1], w_lo[d : d + 1]]
            spread = jnp.concatenate(
                [jnp.where(own_mask, jnp.broadcast_to(p, (8, 512)), 0.0) for p in parts]
                + [jnp.zeros((8, 512), f32)],
                axis=0,
            ).astype(bf16)
            total = lax.dot_general(spread, third, NT, preferred_element_type=f32)
            at = pl.multiple_of((col * 8 + cz) * 8, 8)
            sums[0, pl.ds(at, 8), :] = total[0:8]
            for d in range(3):
                sums[1 + d, pl.ds(at, 8), :] = (
                    total[8 + 16 * d : 16 + 16 * d] + total[16 + 16 * d : 24 + 16 * d]
                )

        def step(i, c):
            for u in range(unroll):
                cell(i * unroll + u)
            return c

        lax.fori_loop(0, 8 // unroll, step, 0)

    from_y = [
        lax.rem(iy + jnp.where(iz == 0, 3, 0), 4),
        lax.rem(iy + jnp.where(iz == 3, 1, 0), 4),
    ]
    edge = jnp.where((iz == 0) | (iz == 3), 1, 0)
    from_half = [edge, 1 - edge]

    def atom_wait(s, u):
        @pl.when((s != iz) | (from_y[u] != iy))
        def _():
            pltpu.make_async_remote_copy(
                src_ref=tx_atoms.at[0],
                dst_ref=rx_atoms.at[s, u],
                send_sem=sa.at[0, 0],
                recv_sem=ra.at[s, u],
                device_id=(ix, from_y[u], s),
                device_id_type=MESH,
            ).wait_recv()

    for s in range(4):
        for u in range(2):
            atom_wait(s, u)

    z_ids = lax.broadcasted_iota(jnp.int32, (256, 256), 0)
    x_ids = lax.broadcasted_iota(jnp.int32, (32, 256), 0) + (ix * 24 - 1)
    y_first = iy * 16 + iz * 4

    def spread(slot, total):
        rows = rx_atoms[slot // 2, lax.rem(slot, 2)]
        anchor = rows[3:6].astype(jnp.int32)
        weights_z = pick_taps((z_ids - anchor[2:3]) & 255, tap_rows(rows[2:3]))
        high, low = split(weights_z)
        at = pl.ds(pl.multiple_of(slot * 256, 256), 256)
        z_high[:, at] = high
        z_low[:, at] = low
        weights_x = pick_taps(x_ids - anchor[0:1], tap_rows(rows[0:1]))
        taps_y = tap_rows(rows[1:2])
        blocks = [
            weights_x * pick_taps((y_first + i - anchor[1:2]) & 63, taps_y) for i in range(4)
        ]
        both = jnp.concatenate(blocks, axis=0)
        stencil[:, at] = both
        return total + dot3((high, low), split(both * rows[6:7]), NT)

    lines = lax.fori_loop(0, 8, spread, jnp.zeros((256, 128), f32))
    spectrum = dot3((bz_ref[0], bz_ref[1]), split(lines))
    tx_b[...] = spectrum.reshape(16, 16, 128)
    rx_b[me] = tx_b[me]

    def exchange(tx, rx, send, recv, peer, count, mine):
        def copy(r):
            other, where = peer(r)
            return pltpu.make_async_remote_copy(
                src_ref=tx.at[other],
                dst_ref=rx.at[mine],
                send_sem=send.at[other],
                recv_sem=recv.at[mine],
                device_id=where,
                device_id_type=MESH,
            )

        def arrival(r):
            other, where = peer(r)
            return pltpu.make_async_remote_copy(
                src_ref=tx.at[other],
                dst_ref=rx.at[other],
                send_sem=send.at[other],
                recv_sem=recv.at[other],
                device_id=where,
                device_id_type=MESH,
            )

        def start(r, c):
            copy(r).start()
            return c

        def wait(r, c):
            arrival(r).wait_recv()
            return c

        def drain(r, c):
            copy(r).wait_send()
            return c

        lax.fori_loop(1, count, start, 0)
        return (
            lambda: lax.fori_loop(1, count, wait, 0),
            lambda: lax.fori_loop(1, count, drain, 0),
        )

    arrive_b, drain_b = exchange(tx_b, rx_b, sb, rb, yz_peer, 16, me)

    for index in halo_ids:
        for copy in halo_copies(26 - index):
            copy.wait_recv()
    feat32[...] = feat_ext[...].astype(f32).reshape(1600, 128)
    strip_axis = axis_sub * 8 + lax.broadcasted_iota(jnp.int32, (8, 128), 1) % 8
    strip_cell = lax.broadcasted_iota(jnp.int32, (8, 128), 1) // 8
    strips = []
    for sx in range(5):
        for sy in range(4):
            rows = pos_ext[sx, sy].reshape(10, 128)
            table = jnp.zeros((8, 128), f32)
            for z in range(10):
                row = jnp.broadcast_to(rows[z : z + 1], (8, 128))
                moved = jnp.take_along_axis(row, strip_axis, axis=1)
                table = jnp.where(strip_cell == z, moved, table)
            strips.append(table)
    for n in range(6):
        near = [strips[(n // 2 + d // 3) * 4 + n % 2 + d % 3] for d in range(9)]
        near += [near[4]] * 3
        for t in range(6):
            pos_tab[n, 8 * t : 8 * t + 8, :] = jnp.where(half_sub == 0, near[2 * t], near[2 * t + 1])
    column(0)
    arrive_b()
    flat_b = rx_b.reshape(256, 128)
    columns = []
    for group in range(4):
        pieces = [flat_b[pl.ds(group * 4 + k, 16, 16), :] for k in range(4)]
        columns.append(jnp.concatenate([swap_groups(pieces, i) for i in range(4)], axis=0))
    lines_y = jnp.concatenate(columns, axis=1)
    modes_y = dot3((by_ref[0, 0], by_ref[0, 1]), split(lines_y))
    tx_c[...] = modes_y.reshape(8, 8, 512)
    rx_c[ix] = tx_c[ix]
    arrive_c, drain_c = exchange(tx_c, rx_c, sc, rc, x_peer, 8, ix)

    gain_z = gz_ref[0, pl.ds(pl.multiple_of(me * 16, 16), 16), :]
    square_z = gz_ref[1, pl.ds(pl.multiple_of(me * 16, 16), 16), :]
    gain_y = gy_ref[0, pl.ds(pl.multiple_of(ix * 8, 8), 8), :]
    square_y = gy_ref[1, pl.ds(pl.multiple_of(ix * 8, 8), 8), :]
    gain_yz = (gain_z[:, None, :] * gain_y[None, :, :]).reshape(128, 128)
    square_yz = (square_z[:, None, :] + square_y[None, :, :]).reshape(128, 128)
    greens = []
    for h in range(2):
        lanes = slice(128 * h, 128 * h + 128)
        total = square_yz + gx_ref[1, 0:1, lanes]
        value = gain_yz * gx_ref[0, 0:1, lanes] / (total + 1.0 / 1024.0)
        greens.append(jnp.where(total == 0.0, 0.0, value))
    green = jnp.concatenate(greens, axis=1)
    column(1)

    arrive_c()
    rows_x = []
    for group in range(4):
        for k in range(4):
            halves = [
                swap_groups(
                    [rx_c[4 * h + g, :, group * 128 : group * 128 + 128] for g in range(4)], k
                )
                for h in range(2)
            ]
            rows_x.append(jnp.concatenate(halves, axis=1))
    lines_x = jnp.concatenate(rows_x, axis=0)
    basis_x = (bx_ref[0], bx_ref[1])
    filtered = dot3(split(lines_x), basis_x, NT) * green
    back_x = dot3(split(filtered), basis_x)
    for g in range(8):
        half = g // 4
        for group in range(4):
            pieces = [
                back_x[(group * 4 + k) * 8 : (group * 4 + k) * 8 + 8, half * 128 : half * 128 + 128]
                for k in range(4)
            ]
            tx_c2[g, :, group * 128 : group * 128 + 128] = swap_groups(pieces, g % 4)
    rx_c2[ix] = tx_c2[ix]
    arrive_c2, drain_c2 = exchange(tx_c2, rx_c2, sc2, rc2, x_peer, 8, ix)
    column(2)
    arrive_c2()
    back_y = dot3((by_ref[1, 0], by_ref[1, 1]), split(rx_c2[...].reshape(64, 512)))
    flat_b2 = tx_b2.reshape(256, 128)
    for group in range(4):
        pieces = [back_y[16 * i : 16 * i + 16, group * 128 : group * 128 + 128] for i in range(4)]
        for k in range(4):
            flat_b2[pl.ds(group * 4 + k, 16, 16), :] = swap_groups(pieces, k)
    rx_b2[me] = tx_b2[me]
    arrive_b2, drain_b2 = exchange(tx_b2, rx_b2, sb2, rb2, yz_peer, 16, me)
    column(3)
    arrive_b2()
    back_z = rx_b2[...].reshape(256, 128).T
    potential = split(dot3(split(back_z), (bz_ref[0], bz_ref[1])))

    def sample(slot, c):
        at = pl.ds(pl.multiple_of(slot * 256, 256), 256)
        values = dot3(potential, (z_high[:, at], z_low[:, at]))
        parts[slot] = jnp.sum(values * stencil[:, at], axis=0, keepdims=True)
        return c

    lax.fori_loop(0, 8, sample, 0)

    def part_copy(s, u):
        return pltpu.make_async_remote_copy(
            src_ref=parts.at[2 * s + u],
            dst_ref=rx_parts.at[from_half[u], iz],
            send_sem=sp.at[s, u],
            recv_sem=rp.at[from_half[u], iz],
            device_id=(ix, from_y[u], s),
            device_id_type=MESH,
        )

    for s in range(4):
        for u in range(2):

            @pl.when((s != iz) | (from_y[u] != iy))
            def _():
                part_copy(s, u).start()

            @pl.when((s == iz) & (from_y[u] == iy))
            def _():
                rx_parts[from_half[u], iz] = parts[2 * s + u]

    column(4)
    column(5)
    wv = wv_ref[...]
    invariant = jnp.zeros((384, 128), f32)
    for d in range(3):
        t = sums[1 + d]
        hi = t.astype(bf16)
        lo = (t - hi.astype(f32)).astype(bf16)
        vec = jnp.dot(hi, wv, preferred_element_type=f32) + jnp.dot(
            lo, wv, preferred_element_type=f32
        )
        invariant = invariant + vec * vec
    update = (sums[0] * (1.0 / 64.0) + invariant * (1.0 / 64.0)).astype(bf16)
    out_ref[...] = (
        feat_ref[...].astype(f32).reshape(384, 128) + jnp.dot(update, wo_ref[...], preferred_element_type=f32)
    ).astype(bf16)

    def part_wait(half, to_z, step_y):
        pltpu.make_async_remote_copy(
            src_ref=parts.at[0],
            dst_ref=rx_parts.at[half, to_z],
            send_sem=sp.at[0, 0],
            recv_sem=rp.at[half, to_z],
            device_id=(ix, lax.rem(iy + step_y, 4), to_z),
            device_id_type=MESH,
        ).wait_recv()

    for half, to_z, step_y, place in routes:
        if step_y:
            part_wait(half, to_z, step_y)
        else:

            @pl.when(iz != to_z)
            def _():
                part_wait(half, to_z, step_y)

    for half in range(2):
        site_ref[half] = (
            (rx_parts[half, 0] + rx_parts[half, 1]) + (rx_parts[half, 2] + rx_parts[half, 3])
        )

    for half, to_z, step_y, place in routes:
        if step_y:
            atom_copy(half, to_z, step_y, place).wait_send()
        else:

            @pl.when(iz != to_z)
            def _():
                atom_copy(half, to_z, step_y, place).wait_send()

    drain_b()
    drain_c()
    drain_c2()
    drain_b2()
    for s in range(4):
        for u in range(2):

            @pl.when((s != iz) | (from_y[u] != iy))
            def _():
                part_copy(s, u).wait_send()
    for index in halo_ids:
        for copy in halo_copies(index):
            copy.wait_send()


def layer(operands, unroll=2):
    f32, bf16 = jnp.float32, jnp.bfloat16
    vm = pl.BlockSpec(memory_space=pltpu.VMEM)
    dma = pltpu.SemaphoreType.DMA
    tables = [jnp.asarray(t) for t in ewald_tables()]
    specs = [vm] * 14 + [pl.BlockSpec(memory_space=pltpu.SMEM)] + [vm] * 6
    return pl.pallas_call(
        functools.partial(layer_kernel, unroll),
        out_shape=(
            jax.ShapeDtypeStruct((384, 128), bf16),
            jax.ShapeDtypeStruct((2, 1, 256), f32),
        ),
        in_specs=specs,
        out_specs=(vm, vm),
        scratch_shapes=[
            pltpu.VMEM((5, 4, 10, 8, 128), bf16),
            pltpu.VMEM((5, 4, 10, 1, 128), f32),
            pltpu.VMEM((6, 48, 128), f32),
            pltpu.VMEM((1600, 128), f32),
            pltpu.VMEM((128, 256), bf16),
            pltpu.VMEM((128, 128), bf16),
            pltpu.VMEM((128, 128), bf16),
            pltpu.VMEM((8, 512), jnp.int32),
            pltpu.VMEM((8, 512), jnp.int32),
            pltpu.VMEM((8, 512), f32),
            pltpu.VMEM((4, 384, 128), f32),
            pltpu.VMEM((2, 8, 256), f32),
            pltpu.VMEM((4, 2, 8, 256), f32),
            pltpu.VMEM((256, 2048), bf16),
            pltpu.VMEM((256, 2048), bf16),
            pltpu.VMEM((128, 2048), f32),
            pltpu.VMEM((16, 16, 128), f32),
            pltpu.VMEM((16, 16, 128), f32),
            pltpu.VMEM((8, 8, 512), f32),
            pltpu.VMEM((8, 8, 512), f32),
            pltpu.VMEM((8, 8, 512), f32),
            pltpu.VMEM((8, 8, 512), f32),
            pltpu.VMEM((16, 16, 128), f32),
            pltpu.VMEM((16, 16, 128), f32),
            pltpu.VMEM((8, 1, 256), f32),
            pltpu.VMEM((2, 4, 1, 256), f32),
            dma((2, 4)),
            dma((4, 2)),
            dma((16,)),
            dma((16,)),
            dma((8,)),
            dma((8,)),
            dma((8,)),
            dma((8,)),
            dma((16,)),
            dma((16,)),
            dma((4, 2)),
            dma((2, 4)),
            dma((27,)),
            dma((27,)),
            dma((27,)),
            dma((27,)),
        ],
        compiler_params=pltpu.CompilerParams(
            collective_id=0, has_side_effects=True, vmem_limit_bytes=40 * 1024 * 1024
        ),
        cost_estimate=pl.CostEstimate(flops=4 * 10**9, bytes_accessed=4 * 10**6, transcendentals=10**7),
        name="layer",
    )(*operands, *tables)


def shards(
    features,
    positions,
    grid_anchor,
    species,
    neighbours,
    neighbour_count,
    w_self,
    w_neighbour,
    w_radial,
    radial_rates,
    w_pair1,
    w_pair2,
    w_vector,
    w_out,
    w_charge,
    species_charge,
):
    cells_x, cells_y, cells_z, slot_count, channels = features.shape

    def by_half(values, width):
        grouped = values.reshape(cells_x, cells_y, cells_z, width, slot_count)
        return grouped.transpose(1, 3, 0, 2, 4).reshape(cells_y, width, -1)

    atoms = jnp.concatenate(
        [
            by_half(positions, 3),
            by_half(grid_anchor, 3).astype(jnp.float32),
            by_half(species, 1).astype(jnp.float32),
        ],
        axis=1,
    )
    counts = neighbour_count.reshape(6, 8, 8)
    pos_rows = positions.reshape(cells_x, cells_y, cells_z, 1, 24)
    updated, site = layer(
        (
            features,
            jnp.pad(pos_rows, ((0, 0),) * 4 + ((0, 104),)),
            jnp.pad(atoms, ((0, 0), (0, 1), (0, 64))),
            neighbours.reshape(6, 8, 512),
            jnp.pad(counts, ((0, 0), (0, 0), (0, 120))),
            w_neighbour,
            w_self,
            w_radial,
            radial_rates.reshape(8, 1),
            w_pair1,
            w_pair2,
            w_vector,
            w_out,
            jnp.broadcast_to(w_charge[None, :], (8, channels)),
            species_charge,
        )
    )
    features_out = updated.reshape(cells_x, cells_y, cells_z, slot_count, channels)
    site_potential = site[:, 0, :192].reshape(cells_y, cells_x, cells_z, slot_count)
    site_potential = site_potential.transpose(1, 0, 2, 3)
    return (features_out, site_potential)


def solution(mesh):
    return jax.shard_map(
        shards,
        mesh=mesh,
        in_specs=(
            P("gx", "gy", "gz", None, None),
            P("gx", "gy", "gz", None),
            P("gx", "gy", "gz", None),
            P("gx", "gy", "gz", None),
            P("gx", "gy", "gz", None),
            P("gx", "gy", "gz", None),
            P(),
            P(),
            P(),
            P(),
            P(),
            P(),
            P(),
            P(),
            P(),
            P(),
        ),
        out_specs=(P("gx", "gy", "gz", None, None), P("gx", "gy", "gz", None)),
        check_vma=False,
    )
```

```python
import jax
import jax.numpy as jnp
import numpy as np
from jax import lax
from jax.experimental import pallas as pl
from jax.experimental.pallas import tpu as pltpu
from jax.sharding import PartitionSpec as P


coulomb_scale = 0.25
smearing = 1.0


NT = (((1,), (1,)), ((), ()))
CUTS = (0, 2, 5, 7, 10)


def real_basis(length):
    modes = np.arange(length)[:, None]
    cells = np.arange(length)[None, :]
    turns = 2.0 * np.pi * ((modes * cells) % length) / length
    flipped = 2.0 * np.pi * (((length - modes) * cells) % length) / length
    return np.where(modes <= length // 2, np.cos(turns), np.sin(flipped))


def two_parts(table):
    table = np.asarray(table, np.float32)
    high = table.astype(jnp.bfloat16)
    low = (table - high.astype(np.float32)).astype(jnp.bfloat16)
    return np.stack([high, low])


def mode_tables(length):
    modes = np.arange(length)
    signed = np.where(modes > length // 2, modes - length, modes)
    wave = signed * (2.0 * np.pi / length)
    modulus = ((4.0 + 2.0 * np.cos(2.0 * np.pi * modes / length)) / 6.0) ** 2
    weight = np.where((modes == 0) | (modes == length // 2), 1.0, 2.0) / length
    return np.exp(-0.5 * smearing * smearing * wave * wave) / modulus * weight, wave * wave


def ewald_tables():
    basis_z = two_parts(real_basis(256))
    order_y = np.array([4 * p + i for i in range(4) for p in range(16)])
    forward_y = real_basis(64)[:, order_y]
    basis_y = np.stack([two_parts(forward_y), two_parts(forward_y.T)])
    wide = np.zeros((256, 256))
    full_x = real_basis(192)
    for g in range(8):
        wide[:192, 32 * g : 32 * g + 27] = full_x[:, (24 * g - 1 + np.arange(27)) % 192]
    basis_x = two_parts(wide)
    green_x = np.zeros((2, 8, 256))
    gain, square = mode_tables(192)
    green_x[0, :, :192] = gain * (coulomb_scale * 4.0 * np.pi)
    green_x[1, :, :192] = square
    green_x[1, :, 192:] = 1.0
    green_y = np.repeat(np.stack(mode_tables(64))[:, :, None], 128, 2)
    green_z = np.repeat(np.stack(mode_tables(256))[:, :, None], 128, 2)
    return (
        basis_z,
        basis_y,
        basis_x,
        green_x.astype(np.float32),
        green_y.astype(np.float32),
        green_z.astype(np.float32),
    )


def split(value):
    high = value.astype(jnp.bfloat16)
    return high, (value - high.astype(jnp.float32)).astype(jnp.bfloat16)


def dot3(a, b, dims=(((1,), (0,)), ((), ()))):
    def one(u, v):
        return lax.dot_general(u, v, dims, preferred_element_type=jnp.float32)

    return one(a[0], b[0]) + (one(a[0], b[1]) + one(a[1], b[0]))


def swap_groups(pieces, shift):
    lane = lax.broadcasted_iota(jnp.int32, pieces[0].shape, 1) // 32
    out = None
    for k, piece in enumerate(pieces):
        moved = pltpu.roll(piece, (32 * (k - shift)) % 128, 1) if k != shift else piece
        out = moved if out is None else jnp.where(lane == k, moved, out)
    return out


def tap_rows(fraction):
    square = fraction * fraction
    cube = square * fraction
    remain = 1.0 - fraction
    return (
        remain * remain * remain / 6.0,
        (3.0 * cube - 6.0 * square + 4.0) / 6.0,
        (-3.0 * cube + 3.0 * square + 3.0 * fraction + 1.0) / 6.0,
        cube / 6.0,
    )


def pick_taps(offset, taps):
    out = jnp.zeros(offset.shape, jnp.float32)
    for t in range(4):
        out = jnp.where(offset == t, taps[t], out)
    return out


def layer_kernel(
    feat_ref,
    place_ref,
    anchor_ref,
    species_ref,
    nbr_hbm,
    count_ref,
    wn_ref,
    ws_ref,
    wr_ref,
    rate_ref,
    w1_ref,
    w2_ref,
    wv_ref,
    wo_ref,
    wc_ref,
    kind_ref,
    bz_hbm,
    by_hbm,
    bx_hbm,
    gx_ref,
    gy_hbm,
    gz_hbm,
    out_ref,
    site_ref,
    nbr,
    bz_ref,
    by_ref,
    bx_ref,
    gy_ref,
    gz_ref,
    load_sem,
    pos_ref,
    feat_ext,
    pos_ext,
    pos_tab,
    feat32,
    first_w,
    pair1_w,
    pair2_w,
    hot_row,
    lane_row,
    live_row,
    sums,
    tx_atoms,
    rx_atoms,
    z_high,
    z_low,
    stencil,
    tx_b,
    rx_b,
    tx_c,
    rx_c,
    tx_c2,
    rx_c2,
    tx_b2,
    rx_b2,
    parts,
    rx_parts,
    sa,
    ra,
    sb,
    rb,
    sc,
    rc,
    sc2,
    rc2,
    sb2,
    rb2,
    sp,
    rp,
    sf,
    rf,
    sq,
    rq,
):
    bf16 = jnp.bfloat16
    f32 = jnp.float32
    MESH = pl.DeviceIdType.MESH
    ix, iy, iz = lax.axis_index("gx"), lax.axis_index("gy"), lax.axis_index("gz")
    me = iy * 4 + iz
    barrier = pltpu.get_barrier_semaphore()
    loads = [
        pltpu.make_async_copy(src, dst, load_sem.at[n])
        for n, (src, dst) in enumerate(
            (
                (bz_hbm, bz_ref),
                (nbr_hbm, nbr),
                (by_hbm, by_ref),
                (bx_hbm, bx_ref),
                (gy_hbm, gy_ref),
                (gz_hbm, gz_ref),
            )
        )
    ]
    for load in loads:
        load.start()

    def yz_peer(r):
        other = lax.rem(me + r, 16)
        return other, (ix, other // 4, lax.rem(other, 4))

    def x_peer(r):
        other = lax.rem(ix + r, 8)
        return other, (other, iy, iz)

    def greet_yz(r, c):
        pl.semaphore_signal(barrier, inc=1, device_id=yz_peer(r)[1], device_id_type=MESH)
        return c

    def greet_x(r, c):
        pl.semaphore_signal(barrier, inc=1, device_id=x_peer(r)[1], device_id_type=MESH)
        return c

    lax.fori_loop(1, 16, greet_yz, 0)
    lax.fori_loop(1, 8, greet_x, 0)

    def halo_peer(index):
        ox, oy, oz = index // 9 - 1, index // 3 % 3 - 1, index % 3 - 1
        return (lax.rem(ix + ox + 8, 8), lax.rem(iy + oy + 4, 4), lax.rem(iz + oz + 4, 4))

    def halo_span(step, cells):
        if step == 0:
            return pl.ds(0, cells), pl.ds(1, cells)
        return (pl.ds(cells - 1, 1), pl.ds(0, 1)) if step > 0 else (pl.ds(0, 1), pl.ds(cells + 1, 1))

    halo_ids = [n for n in range(27) if n != 13]

    def halo_copies(index):
        steps = (index // 9 - 1, index // 3 % 3 - 1, index % 3 - 1)
        spans = [halo_span(step, cells) for step, cells in zip(steps, (3, 2, 8))]
        source = tuple(span[0] for span in spans)
        target = tuple(span[1] for span in spans)
        return [
            pltpu.make_async_remote_copy(
                src_ref=src.at[source],
                dst_ref=dst.at[target],
                send_sem=send.at[index],
                recv_sem=recv.at[index],
                device_id=halo_peer(index),
                device_id_type=MESH,
            )
            for src, dst, send, recv in ((feat_ref, feat_ext, sf, rf), (pos_ref, pos_ext, sq, rq))
        ]

    for index in halo_ids:
        pl.semaphore_signal(barrier, inc=1, device_id=halo_peer(index), device_id_type=MESH)

    sub_l = lax.broadcasted_iota(jnp.int32, (8, 128), 0)
    lane_l = lax.broadcasted_iota(jnp.int32, (8, 128), 1)
    for half in range(2):
        own_rows = feat_ref[:, half].astype(f32).reshape(192, 128).astype(bf16)
        weights = jnp.broadcast_to(wc_ref[...].astype(f32), (16, 128)).astype(bf16)
        readout = lax.dot_general(weights, own_rows, NT, preferred_element_type=f32)[0:8]
        laid = []
        for cx in range(3):
            place = place_ref[cx, half]
            for cz in range(8):
                pos_ref[cx, half, cz, :, 0:24] = place[cz : cz + 1]
                pos_ref[cx, half, cz, :, 24:128] = jnp.zeros((1, 104), f32)
            source = jnp.concatenate(
                [
                    place,
                    anchor_ref[cx, half].astype(f32),
                    species_ref[cx, half].astype(f32),
                    jnp.zeros((8, 72), f32),
                ],
                axis=1,
            )
            rows = jnp.zeros((8, 128), f32)
            for cz in range(8):
                row = jnp.broadcast_to(source[cz : cz + 1], (8, 128))
                moved = jnp.take_along_axis(row, sub_l * 8 + lane_l % 8, axis=1)
                rows = jnp.where(lane_l // 8 == cz, moved, rows)
            laid.append(rows)
        rows = jnp.concatenate(
            [jnp.where(lane_l < 64, laid[0], pltpu.roll(laid[1], 64, 1)), laid[2]], axis=1
        )
        kinds = rows[6:7]
        base = jnp.where(kinds == 0.0, kind_ref[0], jnp.where(kinds == 1.0, kind_ref[1], 0.0))
        total = jnp.concatenate(
            [base[:, 0:192] + readout[0:1, :], jnp.zeros((1, 64), f32)], axis=1
        )
        tx_atoms[half, 0:3, :] = rows[0:3] - (rows[3:6] + 1.0)
        tx_atoms[half, 3:6, :] = rows[3:6]
        tx_atoms[half, 6:7, :] = total
        tx_atoms[half, 7:8, :] = jnp.zeros((1, 256), f32)

    pl.semaphore_wait(barrier, 48)

    routes = [(0, 3, 3, 1), (0, 0, 0, 1), (0, 1, 0, 0), (0, 2, 0, 0)]
    routes += [(1, 1, 0, 1), (1, 2, 0, 1), (1, 3, 0, 0), (1, 0, 1, 0)]

    def atom_copy(half, to_z, step_y, place):
        return pltpu.make_async_remote_copy(
            src_ref=tx_atoms.at[half],
            dst_ref=rx_atoms.at[iz, place],
            send_sem=sa.at[half, to_z],
            recv_sem=ra.at[iz, place],
            device_id=(ix, lax.rem(iy + step_y, 4), to_z),
            device_id_type=MESH,
        )

    for half, to_z, step_y, place in routes:
        if step_y:
            atom_copy(half, to_z, step_y, place).start()
        else:

            @pl.when(iz != to_z)
            def _():
                atom_copy(half, to_z, step_y, place).start()

            @pl.when(iz == to_z)
            def _():
                rx_atoms[iz, place] = tx_atoms[half]

    for index in halo_ids:
        for copy in halo_copies(index):
            copy.start()
    feat_ext[1:4, 1:3, 1:9] = feat_ref[...]
    pos_ext[1:4, 1:3, 1:9] = pos_ref[...]
    first_w[:, 0:128] = (wn_ref[...].astype(f32) * 0.5).T.astype(bf16)
    first_w[:, 128:256] = (ws_ref[...].astype(f32) * 0.5).T.astype(bf16)
    pair1_w[...] = (w1_ref[...].astype(f32) * 0.5).T.astype(bf16)
    pair2_w[...] = (w2_ref[...].astype(f32) * 0.5).T.astype(bf16)
    radial_pad = jnp.concatenate(
        [jnp.zeros((88, 128), f32), wr_ref[...].astype(f32) * 0.5, jnp.zeros((32, 128), f32)], axis=0
    ).T
    cell_x0, cell_y0, cell_z0 = ix * 3, iy * 2, iz * 8

    sub8 = lax.broadcasted_iota(jnp.int32, (8, 512), 0)
    lane8 = lax.broadcasted_iota(jnp.int32, (8, 512), 1)
    rates = jnp.zeros((8, 512), f32)
    for k in range(8):
        rates = jnp.where(sub8 == k, rate_ref[k], rates)
    sub_l = lax.broadcasted_iota(jnp.int32, (8, 128), 0)
    own_mask = (lane8 // 64) == sub8
    own_hot = jnp.where(own_mask, 1.0, 0.0).astype(f32)
    own_hot32 = jnp.concatenate([own_hot, own_hot, jnp.zeros((16, 512), f32)], axis=0).astype(bf16)
    lane_t = lax.broadcasted_iota(jnp.int32, (128, 128), 1)
    low_part = (lane_t >= 104) & (lane_t < 112)
    half_sub = sub_l // 4
    axis_sub = sub_l % 4
    box = jnp.where(axis_sub == 0, 192.0, jnp.where(axis_sub == 1, 64.0, 256.0)).astype(f32)
    box_inv = 1.0 / box
    atom_lane = lax.broadcasted_iota(jnp.int32, (8, 128), 1) // 64


    def half_column(index, carry):
        col = index // 2
        cx = col // 2
        cy = lax.rem(col, 2)
        ids = nbr[cx, cy]
        slot = ids & 7
        z = (ids >> 3) & 31
        y = (ids >> 8) & 7
        x = ids >> 11
        dz = (z - (cell_z0 + sub8) + 1) & 31
        dy = (y - (cell_y0 + cy) + 1) & 7
        dx = x - (cell_x0 + cx) + 1
        dx = jnp.where(dx < 0, dx + 24, dx)
        dx = jnp.where(dx >= 24, dx - 24, dx)
        strip = dx * 3 + dy
        hot_row[...] = strip * 24 + dz * 8 + slot
        lane_row[...] = ((dz + sub8) * 8 + slot) * 16 + strip
        counts = jnp.concatenate([count_ref[cx, cy], jnp.zeros((8, 120), jnp.int32)], axis=1)
        pieces = []
        for g in range(4):
            owner = atom_lane + 2 * g
            count_g = jnp.take_along_axis(counts, owner, axis=1)
            slot_g = lax.broadcasted_iota(jnp.int32, (8, 128), 1) % 64
            pieces.append(jnp.where(slot_g < count_g, 1.0, 0.0).astype(f32))
        live_row[...] = jnp.concatenate(pieces, axis=1)

        def cell(cz):
            rows = []
            for dx_ in range(3):
                for dy_ in range(3):
                    base = ((cx + dx_) * 4 + cy + dy_) * 80 + cz * 8
                    rows.append(feat32[pl.ds(pl.multiple_of(base, 8), 24), :])
            own_base = ((cx + 1) * 4 + cy + 1) * 80 + cz * 8 + 8
            own = feat32[pl.ds(pl.multiple_of(own_base, 8), 8), :]
            left = jnp.concatenate(rows + [jnp.zeros((40, 128), f32)], axis=0)
            right = jnp.concatenate(
                [jnp.zeros((224, 128), f32), own, own, jnp.zeros((16, 128), f32)], axis=0
            )
            table = jnp.concatenate([left, right], axis=1).astype(bf16)
            proj = lax.dot_general(first_w[...], table, NT, preferred_element_type=f32)
            tail = proj[:, 128:256]
            tail_hi = tail.astype(bf16).astype(f32)
            tail = jnp.where(low_part, tail - tail_hi, tail_hi) + radial_pad
            lhs = jnp.concatenate([proj[:, 0:128].astype(bf16), tail.astype(bf16)], axis=1)

            place = []
            hot = hot_row[pl.ds(cz, 1), :]
            packed = lane_row[pl.ds(cz, 1), :]
            live = live_row[pl.ds(cz, 1), :]
            for g in range(4):
                packed_g = jnp.broadcast_to(packed[:, g * 128 : g * 128 + 128], (8, 128))
                where_g = packed_g >> 4
                strip_g = packed_g & 15
                got = jnp.zeros((8, 128), f32)
                for t in range(5):
                    hit = strip_g == (2 * t + half_sub)
                    got = jnp.where(
                        hit,
                        jnp.take_along_axis(pos_tab[col, t * 8 : t * 8 + 8, :], where_g, axis=1),
                        got,
                    )
                got = got + pltpu.roll(got, 4, 0)
                mine = jnp.take_along_axis(
                    pos_tab[col, 40:48, :], atom_lane + 2 * g + (cz + 1) * 8, axis=1
                )
                gap = got - mine
                gap = gap - box * jnp.floor(gap * box_inv + 0.5)
                place.append(gap * 0.125)
            scaled = jnp.concatenate(place, axis=1)
            square = scaled * scaled
            square = square[0:1] + square[1:2] + square[2:3]
            basis = jnp.exp(-jnp.broadcast_to(square, (8, 512)) * rates)
            cell_iota = lax.broadcasted_iota(jnp.int32, (216, 512), 0)
            hots = jnp.where(cell_iota == hot, 1.0, 0.0).astype(f32)
            rhs = jnp.concatenate(
                [jnp.concatenate([hots, basis], axis=0).astype(bf16), own_hot32], axis=0
            )
            half = jnp.dot(lhs, rhs, preferred_element_type=f32)
            yield
            latent = (half + half * jnp.tanh(half)).astype(bf16)
            half = jnp.dot(pair1_w[...], latent, preferred_element_type=f32)
            yield
            second = (half + half * jnp.tanh(half)).astype(bf16)
            half = jnp.dot(pair2_w[...], second, preferred_element_type=f32)
            yield
            third = (half + half * jnp.tanh(half)).astype(bf16)

            weighted = scaled * live
            w_hi = weighted.astype(bf16).astype(f32)
            w_lo = weighted - w_hi
            parts = [live]
            for d in range(3):
                parts += [w_hi[d : d + 1], w_lo[d : d + 1]]
            spread = jnp.concatenate(
                [jnp.where(own_mask, jnp.broadcast_to(p, (8, 512)), 0.0) for p in parts]
                + [jnp.zeros((8, 512), f32)],
                axis=0,
            ).astype(bf16)
            total = lax.dot_general(spread, third, NT, preferred_element_type=f32)
            yield
            at = pl.multiple_of((col * 8 + cz) * 8, 8)
            sums[0, pl.ds(at, 8), :] = total[0:8]
            for d in range(3):
                sums[1 + d, pl.ds(at, 8), :] = (
                    total[8 + 16 * d : 16 + 16 * d] + total[16 + 16 * d : 24 + 16 * d]
                )

        running = [cell(lax.rem(index, 2) * 4 + u) for u in range(4)]
        while running:
            running = [one for one in running if next(one, 1) is None]
        return carry

    def half_columns(first, last):
        lax.fori_loop(first, last, half_column, 0)

    from_y = [
        lax.rem(iy + jnp.where(iz == 0, 3, 0), 4),
        lax.rem(iy + jnp.where(iz == 3, 1, 0), 4),
    ]
    edge = jnp.where((iz == 0) | (iz == 3), 1, 0)
    from_half = [edge, 1 - edge]

    def atom_wait(s, u):
        @pl.when((s != iz) | (from_y[u] != iy))
        def _():
            pltpu.make_async_remote_copy(
                src_ref=tx_atoms.at[0],
                dst_ref=rx_atoms.at[s, u],
                send_sem=sa.at[0, 0],
                recv_sem=ra.at[s, u],
                device_id=(ix, from_y[u], s),
                device_id_type=MESH,
            ).wait_recv()

    z_ids = lax.broadcasted_iota(jnp.int32, (256, 256), 0)
    x_ids = lax.broadcasted_iota(jnp.int32, (32, 256), 0) + (ix * 24 - 1)
    y_first = iy * 16 + iz * 4

    loads[0].wait()

    def spread(turn, total):
        source = lax.rem(iz + turn, 4)
        for u in range(2):
            atom_wait(source, u)
        for u in range(2):
            total = spread_one(source * 2 + u, rx_atoms[source, u], total)
        return total

    def spread_one(slot, rows, total):
        anchor = rows[3:6].astype(jnp.int32)
        weights_z = pick_taps((z_ids - anchor[2:3]) & 255, tap_rows(rows[2:3]))
        high, low = split(weights_z)
        at = pl.ds(pl.multiple_of(slot * 256, 256), 256)
        z_high[:, at] = high
        z_low[:, at] = low
        weights_x = pick_taps(x_ids - anchor[0:1], tap_rows(rows[0:1]))
        taps_y = tap_rows(rows[1:2])
        blocks = [
            weights_x * pick_taps((y_first + i - anchor[1:2]) & 63, taps_y) for i in range(4)
        ]
        both = jnp.concatenate(blocks, axis=0)
        stencil[:, at] = both
        return total + dot3((high, low), split(both * rows[6:7]), NT)

    lines = lax.fori_loop(0, 4, spread, jnp.zeros((256, 128), f32))
    spectrum = dot3((bz_ref[0], bz_ref[1]), split(lines))
    tx_b[...] = spectrum.reshape(16, 16, 128)
    rx_b[me] = tx_b[me]

    def exchange(tx, rx, send, recv, peer, count, mine):
        def copy(r):
            other, where = peer(r)
            return pltpu.make_async_remote_copy(
                src_ref=tx.at[other],
                dst_ref=rx.at[mine],
                send_sem=send.at[other],
                recv_sem=recv.at[mine],
                device_id=where,
                device_id_type=MESH,
            )

        def arrival(r):
            other, where = peer(r)
            return pltpu.make_async_remote_copy(
                src_ref=tx.at[other],
                dst_ref=rx.at[other],
                send_sem=send.at[other],
                recv_sem=recv.at[other],
                device_id=where,
                device_id_type=MESH,
            )

        def start(r, c):
            copy(r).start()
            return c

        def wait(r, c):
            arrival(r).wait_recv()
            return c

        def drain(r, c):
            copy(r).wait_send()
            return c

        lax.fori_loop(1, count, start, 0)
        return (
            lambda: lax.fori_loop(1, count, wait, 0),
            lambda: lax.fori_loop(1, count, drain, 0),
        )

    arrive_b, drain_b = exchange(tx_b, rx_b, sb, rb, yz_peer, 16, me)

    for index in halo_ids:
        for copy in halo_copies(26 - index):
            copy.wait_recv()
    for load in loads[1:]:
        load.wait()
    feat32[...] = feat_ext[...].astype(f32).reshape(1600, 128)
    strip_axis = axis_sub * 8 + lax.broadcasted_iota(jnp.int32, (8, 128), 1) % 8
    strip_cell = lax.broadcasted_iota(jnp.int32, (8, 128), 1) // 8
    strips = []
    for sx in range(5):
        for sy in range(4):
            rows = pos_ext[sx, sy].reshape(10, 128)
            table = jnp.zeros((8, 128), f32)
            for z in range(10):
                row = jnp.broadcast_to(rows[z : z + 1], (8, 128))
                moved = jnp.take_along_axis(row, strip_axis, axis=1)
                table = jnp.where(strip_cell == z, moved, table)
            strips.append(table)
    for n in range(6):
        near = [strips[(n // 2 + d // 3) * 4 + n % 2 + d % 3] for d in range(9)]
        near += [near[4]] * 3
        for t in range(6):
            pos_tab[n, 8 * t : 8 * t + 8, :] = jnp.where(half_sub == 0, near[2 * t], near[2 * t + 1])
    half_columns(CUTS[0], CUTS[1])
    arrive_b()
    flat_b = rx_b.reshape(256, 128)
    columns = []
    for group in range(4):
        pieces = [flat_b[pl.ds(group * 4 + k, 16, 16), :] for k in range(4)]
        columns.append(jnp.concatenate([swap_groups(pieces, i) for i in range(4)], axis=0))
    lines_y = jnp.concatenate(columns, axis=1)
    modes_y = dot3((by_ref[0, 0], by_ref[0, 1]), split(lines_y))
    tx_c[...] = modes_y.reshape(8, 8, 512)
    rx_c[ix] = tx_c[ix]
    arrive_c, drain_c = exchange(tx_c, rx_c, sc, rc, x_peer, 8, ix)

    gain_z = gz_ref[0, pl.ds(pl.multiple_of(me * 16, 16), 16), :]
    square_z = gz_ref[1, pl.ds(pl.multiple_of(me * 16, 16), 16), :]
    gain_y = gy_ref[0, pl.ds(pl.multiple_of(ix * 8, 8), 8), :]
    square_y = gy_ref[1, pl.ds(pl.multiple_of(ix * 8, 8), 8), :]
    gain_yz = (gain_z[:, None, :] * gain_y[None, :, :]).reshape(128, 128)
    square_yz = (square_z[:, None, :] + square_y[None, :, :]).reshape(128, 128)
    greens = []
    for h in range(2):
        lanes = slice(128 * h, 128 * h + 128)
        total = square_yz + gx_ref[1, 0:1, lanes]
        value = gain_yz * gx_ref[0, 0:1, lanes] / (total + 1.0 / 1024.0)
        greens.append(jnp.where(total == 0.0, 0.0, value))
    green = jnp.concatenate(greens, axis=1)
    half_columns(CUTS[1], CUTS[2])

    arrive_c()
    rows_x = []
    for group in range(4):
        for k in range(4):
            halves = [
                swap_groups(
                    [rx_c[4 * h + g, :, group * 128 : group * 128 + 128] for g in range(4)], k
                )
                for h in range(2)
            ]
            rows_x.append(jnp.concatenate(halves, axis=1))
    lines_x = jnp.concatenate(rows_x, axis=0)
    basis_x = (bx_ref[0], bx_ref[1])
    filtered = dot3(split(lines_x), basis_x, NT) * green
    back_x = dot3(split(filtered), basis_x)
    for g in range(8):
        half = g // 4
        for group in range(4):
            pieces = [
                back_x[(group * 4 + k) * 8 : (group * 4 + k) * 8 + 8, half * 128 : half * 128 + 128]
                for k in range(4)
            ]
            tx_c2[g, :, group * 128 : group * 128 + 128] = swap_groups(pieces, g % 4)
    rx_c2[ix] = tx_c2[ix]
    arrive_c2, drain_c2 = exchange(tx_c2, rx_c2, sc2, rc2, x_peer, 8, ix)
    half_columns(CUTS[2], CUTS[3])
    arrive_c2()
    back_y = dot3((by_ref[1, 0], by_ref[1, 1]), split(rx_c2[...].reshape(64, 512)))
    flat_b2 = tx_b2.reshape(256, 128)
    for group in range(4):
        pieces = [back_y[16 * i : 16 * i + 16, group * 128 : group * 128 + 128] for i in range(4)]
        for k in range(4):
            flat_b2[pl.ds(group * 4 + k, 16, 16), :] = swap_groups(pieces, k)
    rx_b2[me] = tx_b2[me]
    arrive_b2, drain_b2 = exchange(tx_b2, rx_b2, sb2, rb2, yz_peer, 16, me)
    half_columns(CUTS[3], CUTS[4])
    arrive_b2()
    back_z = rx_b2[...].reshape(256, 128).T
    potential = split(dot3(split(back_z), (bz_ref[0], bz_ref[1])))

    def sample(slot, c):
        at = pl.ds(pl.multiple_of(slot * 256, 256), 256)
        values = dot3(potential, (z_high[:, at], z_low[:, at]))
        parts[slot] = jnp.sum(values * stencil[:, at], axis=0, keepdims=True)
        return c

    lax.fori_loop(0, 8, sample, 0)

    def part_copy(s, u):
        return pltpu.make_async_remote_copy(
            src_ref=parts.at[2 * s + u],
            dst_ref=rx_parts.at[from_half[u], iz],
            send_sem=sp.at[s, u],
            recv_sem=rp.at[from_half[u], iz],
            device_id=(ix, from_y[u], s),
            device_id_type=MESH,
        )

    for s in range(4):
        for u in range(2):

            @pl.when((s != iz) | (from_y[u] != iy))
            def _():
                part_copy(s, u).start()

            @pl.when((s == iz) & (from_y[u] == iy))
            def _():
                rx_parts[from_half[u], iz] = parts[2 * s + u]

    half_columns(CUTS[4], 12)
    wv = wv_ref[...]
    invariant = jnp.zeros((384, 128), f32)
    for d in range(3):
        t = sums[1 + d]
        hi = t.astype(bf16)
        lo = (t - hi.astype(f32)).astype(bf16)
        vec = jnp.dot(hi, wv, preferred_element_type=f32) + jnp.dot(
            lo, wv, preferred_element_type=f32
        )
        invariant = invariant + vec * vec
    update = (sums[0] * (1.0 / 64.0) + invariant * (1.0 / 64.0)).astype(bf16)
    out_ref[...] = (
        feat_ref[...].astype(f32).reshape(384, 128) + jnp.dot(update, wo_ref[...], preferred_element_type=f32)
    ).astype(bf16)

    def part_wait(half, to_z, step_y):
        pltpu.make_async_remote_copy(
            src_ref=parts.at[0],
            dst_ref=rx_parts.at[half, to_z],
            send_sem=sp.at[0, 0],
            recv_sem=rp.at[half, to_z],
            device_id=(ix, lax.rem(iy + step_y, 4), to_z),
            device_id_type=MESH,
        ).wait_recv()

    for half, to_z, step_y, place in routes:
        if step_y:
            part_wait(half, to_z, step_y)
        else:

            @pl.when(iz != to_z)
            def _():
                part_wait(half, to_z, step_y)

    for half in range(2):
        site = (rx_parts[half, 0] + rx_parts[half, 1]) + (rx_parts[half, 2] + rx_parts[half, 3])
        for cx in range(3):
            block = site[:, 0:128] if cx < 2 else site[:, 128:256]
            block = jnp.broadcast_to(block, (8, 128))
            at = sub_l * 8 + lane_l % 8 + 64 * (cx % 2)
            site_ref[cx, half] = jnp.take_along_axis(block, at, axis=1)[:, 0:8]

    for half, to_z, step_y, place in routes:
        if step_y:
            atom_copy(half, to_z, step_y, place).wait_send()
        else:

            @pl.when(iz != to_z)
            def _():
                atom_copy(half, to_z, step_y, place).wait_send()

    drain_b()
    drain_c()
    drain_c2()
    drain_b2()
    for s in range(4):
        for u in range(2):

            @pl.when((s != iz) | (from_y[u] != iy))
            def _():
                part_copy(s, u).wait_send()
    for index in halo_ids:
        for copy in halo_copies(index):
            copy.wait_send()


def layer(operands):
    f32, bf16 = jnp.float32, jnp.bfloat16
    vm = pl.BlockSpec(memory_space=pltpu.VMEM)
    dma = pltpu.SemaphoreType.DMA
    tables = [jnp.asarray(t) for t in ewald_tables()]
    hbm = pl.BlockSpec(memory_space=pltpu.HBM)
    smem = pl.BlockSpec(memory_space=pltpu.SMEM)
    specs = [vm] * 4 + [hbm] + [vm] * 4 + [smem] + [vm] * 5 + [smem]
    specs += [hbm] * 3 + [vm] + [hbm] * 2
    return pl.pallas_call(
        layer_kernel,
        out_shape=(
            jax.ShapeDtypeStruct((384, 128), bf16),
            jax.ShapeDtypeStruct((3, 2, 8, 8), f32),
        ),
        in_specs=specs,
        out_specs=(vm, vm),
        scratch_shapes=[
            pltpu.VMEM((3, 2, 8, 512), jnp.int32),
            pltpu.VMEM((2, 256, 256), bf16),
            pltpu.VMEM((2, 2, 64, 64), bf16),
            pltpu.VMEM((2, 256, 256), bf16),
            pltpu.VMEM((2, 64, 128), f32),
            pltpu.VMEM((2, 256, 128), f32),
            dma((6,)),
            pltpu.VMEM((3, 2, 8, 1, 128), f32),
            pltpu.VMEM((5, 4, 10, 8, 128), bf16),
            pltpu.VMEM((5, 4, 10, 1, 128), f32),
            pltpu.VMEM((6, 48, 128), f32),
            pltpu.VMEM((1600, 128), f32),
            pltpu.VMEM((128, 256), bf16),
            pltpu.VMEM((128, 128), bf16),
            pltpu.VMEM((128, 128), bf16),
            pltpu.VMEM((8, 512), jnp.int32),
            pltpu.VMEM((8, 512), jnp.int32),
            pltpu.VMEM((8, 512), f32),
            pltpu.VMEM((4, 384, 128), f32),
            pltpu.VMEM((2, 8, 256), f32),
            pltpu.VMEM((4, 2, 8, 256), f32),
            pltpu.VMEM((256, 2048), bf16),
            pltpu.VMEM((256, 2048), bf16),
            pltpu.VMEM((128, 2048), f32),
            pltpu.VMEM((16, 16, 128), f32),
            pltpu.VMEM((16, 16, 128), f32),
            pltpu.VMEM((8, 8, 512), f32),
            pltpu.VMEM((8, 8, 512), f32),
            pltpu.VMEM((8, 8, 512), f32),
            pltpu.VMEM((8, 8, 512), f32),
            pltpu.VMEM((16, 16, 128), f32),
            pltpu.VMEM((16, 16, 128), f32),
            pltpu.VMEM((8, 1, 256), f32),
            pltpu.VMEM((2, 4, 1, 256), f32),
            dma((2, 4)),
            dma((4, 2)),
            dma((16,)),
            dma((16,)),
            dma((8,)),
            dma((8,)),
            dma((8,)),
            dma((8,)),
            dma((16,)),
            dma((16,)),
            dma((4, 2)),
            dma((2, 4)),
            dma((27,)),
            dma((27,)),
            dma((27,)),
            dma((27,)),
        ],
        compiler_params=pltpu.CompilerParams(
            collective_id=0, has_side_effects=True, vmem_limit_bytes=67043328
        ),
        cost_estimate=pl.CostEstimate(flops=4 * 10**9, bytes_accessed=4 * 10**6, transcendentals=10**7),
        name="layer",
    )(*operands, *tables)


def shards(
    features,
    positions,
    grid_anchor,
    species,
    neighbours,
    neighbour_count,
    w_self,
    w_neighbour,
    w_radial,
    radial_rates,
    w_pair1,
    w_pair2,
    w_vector,
    w_out,
    w_charge,
    species_charge,
):
    updated, site_potential = layer(
        (
            features,
            positions,
            grid_anchor,
            species,
            neighbours,
            neighbour_count,
            w_neighbour,
            w_self,
            w_radial,
            radial_rates,
            w_pair1,
            w_pair2,
            w_vector,
            w_out,
            w_charge.reshape(1, 128),
            species_charge,
        )
    )
    return (updated.reshape(features.shape), site_potential)


def solution(mesh):
    return jax.shard_map(
        shards,
        mesh=mesh,
        in_specs=(
            P("gx", "gy", "gz", None, None),
            P("gx", "gy", "gz", None),
            P("gx", "gy", "gz", None),
            P("gx", "gy", "gz", None),
            P("gx", "gy", "gz", None),
            P("gx", "gy", "gz", None),
            P(),
            P(),
            P(),
            P(),
            P(),
            P(),
            P(),
            P(),
            P(),
            P(),
        ),
        out_specs=(P("gx", "gy", "gz", None, None), P("gx", "gy", "gz", None)),
        check_vma=False,
    )
```

```python
import jax
import jax.numpy as jnp
import numpy as np
from jax import lax
from jax.experimental import pallas as pl
from jax.experimental.pallas import tpu as pltpu
from jax.sharding import PartitionSpec as P


coulomb_scale = 0.25
smearing = 1.0


NT = (((1,), (1,)), ((), ()))
CUTS = (0, 4, 6, 8, 11)


def real_basis(length):
    modes = np.arange(length)[:, None]
    cells = np.arange(length)[None, :]
    turns = 2.0 * np.pi * ((modes * cells) % length) / length
    flipped = 2.0 * np.pi * (((length - modes) * cells) % length) / length
    return np.where(modes <= length // 2, np.cos(turns), np.sin(flipped))


def two_parts(table):
    table = np.asarray(table, np.float32)
    high = table.astype(jnp.bfloat16)
    low = (table - high.astype(np.float32)).astype(jnp.bfloat16)
    return np.stack([high, low])


def mode_tables(length):
    modes = np.arange(length)
    signed = np.where(modes > length // 2, modes - length, modes)
    wave = signed * (2.0 * np.pi / length)
    modulus = ((4.0 + 2.0 * np.cos(2.0 * np.pi * modes / length)) / 6.0) ** 2
    weight = np.where((modes == 0) | (modes == length // 2), 1.0, 2.0) / length
    return np.exp(-0.5 * smearing * smearing * wave * wave) / modulus * weight, wave * wave


def ewald_tables():
    basis_z = two_parts(real_basis(256))
    order_y = np.array([4 * p + i for i in range(4) for p in range(16)])
    forward_y = real_basis(64)[:, order_y]
    basis_y = np.stack([two_parts(forward_y), two_parts(forward_y.T)])
    wide = np.zeros((256, 256))
    full_x = real_basis(192)
    for g in range(8):
        wide[:192, 32 * g : 32 * g + 27] = full_x[:, (24 * g - 1 + np.arange(27)) % 192]
    basis_x = two_parts(wide)
    green_x = np.zeros((2, 8, 256))
    gain, square = mode_tables(192)
    green_x[0, :, :192] = gain * (coulomb_scale * 4.0 * np.pi)
    green_x[1, :, :192] = square
    green_x[1, :, 192:] = 1.0
    green_y = np.repeat(np.stack(mode_tables(64))[:, :, None], 128, 2)
    green_z = np.repeat(np.stack(mode_tables(256))[:, :, None], 128, 2)
    return (
        basis_z,
        basis_y,
        basis_x,
        green_x.astype(np.float32),
        green_y.astype(np.float32),
        green_z.astype(np.float32),
    )


def split(value):
    high = value.astype(jnp.bfloat16)
    return high, (value - high.astype(jnp.float32)).astype(jnp.bfloat16)


def dot3(a, b, dims=(((1,), (0,)), ((), ()))):
    def one(u, v):
        return lax.dot_general(u, v, dims, preferred_element_type=jnp.float32)

    return one(a[0], b[0]) + (one(a[0], b[1]) + one(a[1], b[0]))


def swap_groups(pieces, shift):
    lane = lax.broadcasted_iota(jnp.int32, pieces[0].shape, 1) // 32
    out = None
    for k, piece in enumerate(pieces):
        moved = pltpu.roll(piece, (32 * (k - shift)) % 128, 1) if k != shift else piece
        out = moved if out is None else jnp.where(lane == k, moved, out)
    return out


def tap_rows(fraction):
    square = fraction * fraction
    cube = square * fraction
    remain = 1.0 - fraction
    return (
        remain * remain * remain / 6.0,
        (3.0 * cube - 6.0 * square + 4.0) / 6.0,
        (-3.0 * cube + 3.0 * square + 3.0 * fraction + 1.0) / 6.0,
        cube / 6.0,
    )


def pick_taps(offset, taps):
    out = jnp.zeros(offset.shape, jnp.float32)
    for t in range(4):
        out = jnp.where(offset == t, taps[t], out)
    return out


def layer_kernel(
    feat_hbm,
    place_hbm,
    anchor_hbm,
    species_hbm,
    nbr_hbm,
    count_hbm,
    wn_hbm,
    ws_hbm,
    wr_hbm,
    rate_ref,
    w1_hbm,
    w2_hbm,
    wv_hbm,
    wo_hbm,
    wc_hbm,
    kind_ref,
    bz_hbm,
    by_hbm,
    bx_hbm,
    gx_hbm,
    gy_hbm,
    gz_hbm,
    out_ref,
    site_ref,
    feat_ref,
    place_ref,
    anchor_ref,
    species_ref,
    wc_ref,
    wn_ref,
    ws_ref,
    wr_ref,
    w1_ref,
    w2_ref,
    nbr_ref,
    count_ref,
    bz_ref,
    by_ref,
    bx_ref,
    gx_ref,
    gy_ref,
    gz_ref,
    wv_ref,
    wo_ref,
    load_sem,
    pos_ref,
    feat_ext,
    pos_ext,
    pos_tab,
    feat32,
    first_w,
    pair1_w,
    pair2_w,
    hot_row,
    lane_row,
    live_row,
    sums,
    tx_atoms,
    rx_atoms,
    z_high,
    z_low,
    stencil,
    tx_b,
    rx_b,
    tx_c,
    rx_c,
    tx_c2,
    rx_c2,
    tx_b2,
    rx_b2,
    parts,
    rx_parts,
    sa,
    ra,
    sb,
    rb,
    sc,
    rc,
    sc2,
    rc2,
    sb2,
    rb2,
    sp,
    rp,
    sf,
    rf,
    sq,
    rq,
):
    bf16 = jnp.bfloat16
    f32 = jnp.float32
    MESH = pl.DeviceIdType.MESH
    ix, iy, iz = lax.axis_index("gx"), lax.axis_index("gy"), lax.axis_index("gz")
    me = iy * 4 + iz
    barrier = pltpu.get_barrier_semaphore()
    pairs = (
        (feat_hbm, feat_ref),
        (place_hbm, place_ref),
        (anchor_hbm, anchor_ref),
        (species_hbm, species_ref),
        (wc_hbm, wc_ref),
        (wn_hbm, wn_ref),
        (ws_hbm, ws_ref),
        (wr_hbm, wr_ref),
        (w1_hbm, w1_ref),
        (w2_hbm, w2_ref),
        (nbr_hbm, nbr_ref),
        (count_hbm, count_ref),
        (bz_hbm, bz_ref),
        (by_hbm, by_ref),
        (bx_hbm, bx_ref),
        (gx_hbm, gx_ref),
        (gy_hbm, gy_ref),
        (gz_hbm, gz_ref),
        (wv_hbm, wv_ref),
        (wo_hbm, wo_ref),
    )
    loads = [
        pltpu.make_async_copy(src, dst, load_sem.at[n]) for n, (src, dst) in enumerate(pairs)
    ]
    for load in loads:
        load.start()

    def yz_peer(r):
        other = lax.rem(me + r, 16)
        return other, (ix, other // 4, lax.rem(other, 4))

    def x_peer(r):
        other = lax.rem(ix + r, 8)
        return other, (other, iy, iz)

    def greet_yz(r, c):
        pl.semaphore_signal(barrier, inc=1, device_id=yz_peer(r)[1], device_id_type=MESH)
        return c

    def greet_x(r, c):
        pl.semaphore_signal(barrier, inc=1, device_id=x_peer(r)[1], device_id_type=MESH)
        return c

    lax.fori_loop(1, 16, greet_yz, 0)
    lax.fori_loop(1, 8, greet_x, 0)

    def halo_peer(index):
        ox, oy, oz = index // 9 - 1, index // 3 % 3 - 1, index % 3 - 1
        return (lax.rem(ix + ox + 8, 8), lax.rem(iy + oy + 4, 4), lax.rem(iz + oz + 4, 4))

    def halo_span(step, cells):
        if step == 0:
            return pl.ds(0, cells), pl.ds(1, cells)
        return (pl.ds(cells - 1, 1), pl.ds(0, 1)) if step > 0 else (pl.ds(0, 1), pl.ds(cells + 1, 1))

    halo_ids = [n for n in range(27) if n != 13]
    near_ids = [n for n in halo_ids if n // 9 == 1]
    far_ids = [n for n in halo_ids if n // 9 != 1]

    def halo_copies(index):
        steps = (index // 9 - 1, index // 3 % 3 - 1, index % 3 - 1)
        spans = [halo_span(step, cells) for step, cells in zip(steps, (3, 2, 8))]
        source = tuple(span[0] for span in spans)
        target = tuple(span[1] for span in spans)
        row = {0: pl.ds(1, 2), 1: pl.ds(0, 1), -1: pl.ds(3, 1)}[steps[2]]
        return [
            pltpu.make_async_remote_copy(
                src_ref=src.at[source[:2] + (from_z,)],
                dst_ref=dst.at[target[:2] + (to_z,)],
                send_sem=send.at[index],
                recv_sem=recv.at[index],
                device_id=halo_peer(index),
                device_id_type=MESH,
            )
            for src, dst, send, recv, from_z, to_z in (
                (feat_ref, feat_ext, sf, rf, source[2], target[2]),
                (pos_ref, pos_ext, sq, rq, row, row),
            )
        ]

    for index in halo_ids:
        pl.semaphore_signal(barrier, inc=1, device_id=halo_peer(index), device_id_type=MESH)

    for load in loads[:5]:
        load.wait()

    sub_l = lax.broadcasted_iota(jnp.int32, (8, 128), 0)
    lane_l = lax.broadcasted_iota(jnp.int32, (8, 128), 1)
    for half in range(2):
        own_rows = feat_ref[:, half].astype(f32).reshape(192, 128).astype(bf16)
        weights = jnp.broadcast_to(wc_ref[...].astype(f32), (16, 128)).astype(bf16)
        readout = lax.dot_general(weights, own_rows, NT, preferred_element_type=f32)[0:8]
        laid = []
        for cx in range(3):
            place = place_ref[cx, half]
            for row, cells in ((0, (7,)), (1, (0, 1, 2, 3)), (2, (4, 5, 6, 7)), (3, (0,))):
                pieces = [place[cz : cz + 1] for cz in cells]
                pieces.append(jnp.zeros((1, 128 - 24 * len(cells)), f32))
                pos_ref[cx, half, row] = jnp.concatenate(pieces, axis=1)
            source = jnp.concatenate(
                [
                    place,
                    anchor_ref[cx, half].astype(f32),
                    species_ref[cx, half].astype(f32),
                    jnp.zeros((8, 72), f32),
                ],
                axis=1,
            )
            rows = jnp.zeros((8, 128), f32)
            for cz in range(8):
                row = jnp.broadcast_to(source[cz : cz + 1], (8, 128))
                moved = jnp.take_along_axis(row, sub_l * 8 + lane_l % 8, axis=1)
                rows = jnp.where(lane_l // 8 == cz, moved, rows)
            laid.append(rows)
        rows = jnp.concatenate(
            [jnp.where(lane_l < 64, laid[0], pltpu.roll(laid[1], 64, 1)), laid[2]], axis=1
        )
        kinds = rows[6:7]
        base = jnp.where(kinds == 0.0, kind_ref[0], jnp.where(kinds == 1.0, kind_ref[1], 0.0))
        total = jnp.concatenate(
            [base[:, 0:192] + readout[0:1, :], jnp.zeros((1, 64), f32)], axis=1
        )
        tx_atoms[half, 0:3, :] = rows[0:3] - (rows[3:6] + 1.0)
        tx_atoms[half, 3:6, :] = rows[3:6]
        tx_atoms[half, 6:7, :] = total
        tx_atoms[half, 7:8, :] = jnp.zeros((1, 256), f32)

    for load in loads[5:10]:
        load.wait()
    first_w[:, 0:128] = (wn_ref[...].astype(f32) * 0.5).T.astype(bf16)
    first_w[:, 128:256] = (ws_ref[...].astype(f32) * 0.5).T.astype(bf16)
    pair1_w[...] = (w1_ref[...].astype(f32) * 0.5).T.astype(bf16)
    pair2_w[...] = (w2_ref[...].astype(f32) * 0.5).T.astype(bf16)
    radial_pad = jnp.concatenate(
        [jnp.zeros((88, 128), f32), wr_ref[...].astype(f32) * 0.5, jnp.zeros((32, 128), f32)], axis=0
    ).T
    cell_x0, cell_y0, cell_z0 = ix * 3, iy * 2, iz * 8

    sub8 = lax.broadcasted_iota(jnp.int32, (8, 512), 0)
    lane8 = lax.broadcasted_iota(jnp.int32, (8, 512), 1)
    rates = jnp.zeros((8, 512), f32)
    for k in range(8):
        rates = jnp.where(sub8 == k, rate_ref[k], rates)
    own_mask = (lane8 // 64) == sub8
    own_hot = jnp.where(own_mask, 1.0, 0.0).astype(f32)
    own_hot32 = jnp.concatenate([own_hot, own_hot, jnp.zeros((16, 512), f32)], axis=0).astype(bf16)
    lane_t = lax.broadcasted_iota(jnp.int32, (128, 128), 1)
    low_part = (lane_t >= 104) & (lane_t < 112)
    half_sub = sub_l // 4
    axis_sub = sub_l % 4
    box = jnp.where(axis_sub == 0, 192.0, jnp.where(axis_sub == 1, 64.0, 256.0)).astype(f32)
    box_inv = 1.0 / box
    atom_lane = lax.broadcasted_iota(jnp.int32, (8, 128), 1) // 64
    pl.semaphore_wait(barrier, 48)

    routes = [(0, 3, 3, 1), (0, 0, 0, 1), (0, 1, 0, 0), (0, 2, 0, 0)]
    routes += [(1, 1, 0, 1), (1, 2, 0, 1), (1, 3, 0, 0), (1, 0, 1, 0)]

    def atom_copy(half, to_z, step_y, place):
        return pltpu.make_async_remote_copy(
            src_ref=tx_atoms.at[half],
            dst_ref=rx_atoms.at[iz, place],
            send_sem=sa.at[half, to_z],
            recv_sem=ra.at[iz, place],
            device_id=(ix, lax.rem(iy + step_y, 4), to_z),
            device_id_type=MESH,
        )

    for half, to_z, step_y, place in routes:
        if step_y:
            atom_copy(half, to_z, step_y, place).start()
        else:

            @pl.when(iz != to_z)
            def _():
                atom_copy(half, to_z, step_y, place).start()

            @pl.when(iz == to_z)
            def _():
                rx_atoms[iz, place] = tx_atoms[half]

    for index in near_ids:
        for copy in halo_copies(index):
            copy.start()
    feat_ext[1:4, 1:3, 1:9] = feat_ref[...]
    pos_ext[1:4, 1:3, 1:3] = pos_ref[:, :, 1:3]
    def half_column(index, carry):
        later = (index - 4) // 2
        col = jnp.where(index < 4, 2 + index // 2, jnp.where(later < 2, later, later + 2))
        cx = col // 2
        cy = lax.rem(col, 2)
        ids = nbr_ref[cx, cy]
        slot = ids & 7
        z = (ids >> 3) & 31
        y = (ids >> 8) & 7
        x = ids >> 11
        dz = (z - (cell_z0 + sub8) + 1) & 31
        dy = (y - (cell_y0 + cy) + 1) & 7
        dx = x - (cell_x0 + cx) + 1
        dx = jnp.where(dx < 0, dx + 24, dx)
        dx = jnp.where(dx >= 24, dx - 24, dx)
        strip = dx * 3 + dy
        hot_row[...] = strip * 24 + dz * 8 + slot
        lane_row[...] = ((dz + sub8) * 8 + slot) * 16 + strip
        counts = jnp.concatenate([count_ref[cx, cy], jnp.zeros((8, 120), jnp.int32)], axis=1)
        pieces = []
        for g in range(4):
            owner = atom_lane + 2 * g
            count_g = jnp.take_along_axis(counts, owner, axis=1)
            slot_g = lax.broadcasted_iota(jnp.int32, (8, 128), 1) % 64
            pieces.append(jnp.where(slot_g < count_g, 1.0, 0.0).astype(f32))
        live_row[...] = jnp.concatenate(pieces, axis=1)

        def cell(cz):
            rows = []
            for dx_ in range(3):
                for dy_ in range(3):
                    base = ((cx + dx_) * 4 + cy + dy_) * 80 + cz * 8
                    rows.append(feat32[pl.ds(pl.multiple_of(base, 8), 24), :])
            own_base = ((cx + 1) * 4 + cy + 1) * 80 + cz * 8 + 8
            own = feat32[pl.ds(pl.multiple_of(own_base, 8), 8), :]
            left = jnp.concatenate(rows + [jnp.zeros((40, 128), f32)], axis=0)
            right = jnp.concatenate(
                [jnp.zeros((224, 128), f32), own, own, jnp.zeros((16, 128), f32)], axis=0
            )
            table = jnp.concatenate([left, right], axis=1).astype(bf16)
            proj = lax.dot_general(first_w[...], table, NT, preferred_element_type=f32)
            tail = proj[:, 128:256]
            tail_hi = tail.astype(bf16).astype(f32)
            tail = jnp.where(low_part, tail - tail_hi, tail_hi) + radial_pad
            lhs = jnp.concatenate([proj[:, 0:128].astype(bf16), tail.astype(bf16)], axis=1)

            place = []
            hot = hot_row[pl.ds(cz, 1), :]
            packed = lane_row[pl.ds(cz, 1), :]
            live = live_row[pl.ds(cz, 1), :]
            for g in range(4):
                packed_g = jnp.broadcast_to(packed[:, g * 128 : g * 128 + 128], (8, 128))
                where_g = packed_g >> 4
                strip_g = packed_g & 15
                got = jnp.zeros((8, 128), f32)
                for t in range(5):
                    hit = strip_g == (2 * t + half_sub)
                    got = jnp.where(
                        hit,
                        jnp.take_along_axis(pos_tab[col, t * 8 : t * 8 + 8, :], where_g, axis=1),
                        got,
                    )
                got = got + pltpu.roll(got, 4, 0)
                mine = jnp.take_along_axis(
                    pos_tab[col, 40:48, :], atom_lane + 2 * g + (cz + 1) * 8, axis=1
                )
                gap = got - mine
                gap = gap - box * jnp.floor(gap * box_inv + 0.5)
                place.append(gap * 0.125)
            scaled = jnp.concatenate(place, axis=1)
            square = scaled * scaled
            square = square[0:1] + square[1:2] + square[2:3]
            basis = jnp.exp(-jnp.broadcast_to(square, (8, 512)) * rates)
            cell_iota = lax.broadcasted_iota(jnp.int32, (216, 512), 0)
            hots = jnp.where(cell_iota == hot, 1.0, 0.0).astype(f32)
            rhs = jnp.concatenate(
                [jnp.concatenate([hots, basis], axis=0).astype(bf16), own_hot32], axis=0
            )
            half = jnp.dot(lhs, rhs, preferred_element_type=f32)
            yield
            latent = (half + half * jnp.tanh(half)).astype(bf16)
            half = jnp.dot(pair1_w[...], latent, preferred_element_type=f32)
            yield
            second = (half + half * jnp.tanh(half)).astype(bf16)
            half = jnp.dot(pair2_w[...], second, preferred_element_type=f32)
            yield
            third = (half + half * jnp.tanh(half)).astype(bf16)

            weighted = scaled * live
            w_hi = weighted.astype(bf16).astype(f32)
            w_lo = weighted - w_hi
            parts = [live]
            for d in range(3):
                parts += [w_hi[d : d + 1], w_lo[d : d + 1]]
            spread = jnp.concatenate(
                [jnp.where(own_mask, jnp.broadcast_to(p, (8, 512)), 0.0) for p in parts]
                + [jnp.zeros((8, 512), f32)],
                axis=0,
            ).astype(bf16)
            total = lax.dot_general(spread, third, NT, preferred_element_type=f32)
            yield
            at = pl.multiple_of((col * 8 + cz) * 8, 8)
            sums[0, pl.ds(at, 8), :] = total[0:8]
            for d in range(3):
                sums[1 + d, pl.ds(at, 8), :] = (
                    total[8 + 16 * d : 16 + 16 * d] + total[16 + 16 * d : 24 + 16 * d]
                )

        running = [cell(lax.rem(index, 2) * 4 + u) for u in range(4)]
        while running:
            running = [one for one in running if next(one, 1) is None]
        return carry

    def half_columns(first, last):
        lax.fori_loop(first, last, half_column, 0)

    from_y = [
        lax.rem(iy + jnp.where(iz == 0, 3, 0), 4),
        lax.rem(iy + jnp.where(iz == 3, 1, 0), 4),
    ]
    edge = jnp.where((iz == 0) | (iz == 3), 1, 0)
    from_half = [edge, 1 - edge]

    def atom_wait(s, u):
        @pl.when((s != iz) | (from_y[u] != iy))
        def _():
            pltpu.make_async_remote_copy(
                src_ref=tx_atoms.at[0],
                dst_ref=rx_atoms.at[s, u],
                send_sem=sa.at[0, 0],
                recv_sem=ra.at[s, u],
                device_id=(ix, from_y[u], s),
                device_id_type=MESH,
            ).wait_recv()

    y_first = iy * 16 + iz * 4

    for load in loads[10:]:
        load.wait()
    z_ids = lax.broadcasted_iota(jnp.int32, (256, 384), 0)
    x_ids = lax.broadcasted_iota(jnp.int32, (32, 384), 0) + (ix * 24 - 1)
    lane_384 = lax.broadcasted_iota(jnp.int32, (8, 128), 1)

    def spread(turn, total):
        source = lax.rem(iz + turn, 4)
        for u in range(2):
            atom_wait(source, u)
        low_part_, high_part_ = rx_atoms[source, 0], rx_atoms[source, 1]
        moved = pltpu.roll(high_part_, 64, 1)
        rows = jnp.concatenate(
            [
                low_part_[:, 0:128],
                jnp.where(lane_384 < 64, low_part_[:, 128:256], moved[:, 0:128]),
                moved[:, 128:256],
            ],
            axis=1,
        )
        anchor = rows[3:6].astype(jnp.int32)
        weights_z = pick_taps((z_ids - anchor[2:3]) & 255, tap_rows(rows[2:3]))
        high, low = split(weights_z)
        z_high[source] = high
        z_low[source] = low
        weights_x = pick_taps(x_ids - anchor[0:1], tap_rows(rows[0:1]))
        taps_y = tap_rows(rows[1:2])
        blocks = [
            weights_x * pick_taps((y_first + i - anchor[1:2]) & 63, taps_y) for i in range(4)
        ]
        both = jnp.concatenate(blocks, axis=0)
        stencil[source] = both
        return total + dot3((high, low), split(both * rows[6:7]), NT)

    lines = lax.fori_loop(0, 4, spread, jnp.zeros((256, 128), f32))
    spectrum = dot3((bz_ref[0], bz_ref[1]), split(lines))
    tx_b[...] = spectrum.reshape(16, 16, 128)
    rx_b[me] = tx_b[me]

    def exchange(tx, rx, send, recv, peer, count, mine):
        def copy(r):
            other, where = peer(r)
            return pltpu.make_async_remote_copy(
                src_ref=tx.at[other],
                dst_ref=rx.at[mine],
                send_sem=send.at[other],
                recv_sem=recv.at[mine],
                device_id=where,
                device_id_type=MESH,
            )

        def arrival(r):
            other, where = peer(r)
            return pltpu.make_async_remote_copy(
                src_ref=tx.at[other],
                dst_ref=rx.at[other],
                send_sem=send.at[other],
                recv_sem=recv.at[other],
                device_id=where,
                device_id_type=MESH,
            )

        def start(r, c):
            copy(r).start()
            return c

        def wait(r, c):
            arrival(r).wait_recv()
            return c

        def drain(r, c):
            copy(r).wait_send()
            return c

        lax.fori_loop(1, count, start, 0)
        return (
            lambda: lax.fori_loop(1, count, wait, 0),
            lambda: lax.fori_loop(1, count, drain, 0),
        )

    arrive_b, drain_b = exchange(tx_b, rx_b, sb, rb, yz_peer, 16, me)

    for index in far_ids:
        for copy in halo_copies(index):
            copy.start()
    strip_lane = lax.broadcasted_iota(jnp.int32, (8, 128), 1)
    strip_cell = strip_lane // 8
    within = axis_sub * 8 + strip_lane % 8
    starts = jnp.where(strip_cell == 0, 0, jnp.where(strip_cell == 9, 0, lax.rem(strip_cell + 3, 4)))
    strip_at = jnp.where(axis_sub == 3, 127, jnp.minimum(starts * 24 + within, 127))
    strips = {}

    def lay_strips(sx):
        feat32[320 * sx : 320 * sx + 320, :] = feat_ext[sx].astype(f32).reshape(320, 128)
        for sy in range(4):
            table = jnp.zeros((8, 128), f32)
            for row, first, last in ((0, 0, 1), (1, 1, 5), (2, 5, 9), (3, 9, 10)):
                source = jnp.broadcast_to(pos_ext[sx, sy, row], (8, 128))
                moved = jnp.take_along_axis(source, strip_at, axis=1)
                table = jnp.where((strip_cell >= first) & (strip_cell < last), moved, table)
            strips[sx, sy] = table

    def lay_column(n):
        near = [strips[n // 2 + d // 3, n % 2 + d % 3] for d in range(9)]
        near += [near[4]] * 3
        for t in range(6):
            pos_tab[n, 8 * t : 8 * t + 8, :] = jnp.where(half_sub == 0, near[2 * t], near[2 * t + 1])

    for index in near_ids:
        for copy in halo_copies(26 - index):
            copy.wait_recv()
    for sx in (1, 2, 3):
        lay_strips(sx)
    for n in (2, 3):
        lay_column(n)
    half_columns(CUTS[0], CUTS[1])
    arrive_b()
    flat_b = rx_b.reshape(256, 128)
    columns = []
    for group in range(4):
        pieces = [flat_b[pl.ds(group * 4 + k, 16, 16), :] for k in range(4)]
        columns.append(jnp.concatenate([swap_groups(pieces, i) for i in range(4)], axis=0))
    lines_y = jnp.concatenate(columns, axis=1)
    modes_y = dot3((by_ref[0, 0], by_ref[0, 1]), split(lines_y))
    tx_c[...] = modes_y.reshape(8, 8, 512)
    rx_c[ix] = tx_c[ix]
    arrive_c, drain_c = exchange(tx_c, rx_c, sc, rc, x_peer, 8, ix)

    gain_z = gz_ref[0, pl.ds(pl.multiple_of(me * 16, 16), 16), :]
    square_z = gz_ref[1, pl.ds(pl.multiple_of(me * 16, 16), 16), :]
    gain_y = gy_ref[0, pl.ds(pl.multiple_of(ix * 8, 8), 8), :]
    square_y = gy_ref[1, pl.ds(pl.multiple_of(ix * 8, 8), 8), :]
    gain_yz = (gain_z[:, None, :] * gain_y[None, :, :]).reshape(128, 128)
    square_yz = (square_z[:, None, :] + square_y[None, :, :]).reshape(128, 128)
    greens = []
    for h in range(2):
        lanes = slice(128 * h, 128 * h + 128)
        total = square_yz + gx_ref[1, 0:1, lanes]
        value = gain_yz * gx_ref[0, 0:1, lanes] / (total + 1.0 / 1024.0)
        greens.append(jnp.where(total == 0.0, 0.0, value))
    green = jnp.concatenate(greens, axis=1)
    for index in far_ids:
        for copy in halo_copies(26 - index):
            copy.wait_recv()
    for sx in (0, 4):
        lay_strips(sx)
    for n in (0, 1, 4, 5):
        lay_column(n)
    half_columns(CUTS[1], CUTS[2])

    arrive_c()
    rows_x = []
    for group in range(4):
        for k in range(4):
            halves = [
                swap_groups(
                    [rx_c[4 * h + g, :, group * 128 : group * 128 + 128] for g in range(4)], k
                )
                for h in range(2)
            ]
            rows_x.append(jnp.concatenate(halves, axis=1))
    lines_x = jnp.concatenate(rows_x, axis=0)
    basis_x = (bx_ref[0], bx_ref[1])
    filtered = dot3(split(lines_x), basis_x, NT) * green
    back_x = dot3(split(filtered), basis_x)
    for g in range(8):
        half = g // 4
        for group in range(4):
            pieces = [
                back_x[(group * 4 + k) * 8 : (group * 4 + k) * 8 + 8, half * 128 : half * 128 + 128]
                for k in range(4)
            ]
            tx_c2[g, :, group * 128 : group * 128 + 128] = swap_groups(pieces, g % 4)
    rx_c2[ix] = tx_c2[ix]
    arrive_c2, drain_c2 = exchange(tx_c2, rx_c2, sc2, rc2, x_peer, 8, ix)
    half_columns(CUTS[2], CUTS[3])
    arrive_c2()
    back_y = dot3((by_ref[1, 0], by_ref[1, 1]), split(rx_c2[...].reshape(64, 512)))
    flat_b2 = tx_b2.reshape(256, 128)
    for group in range(4):
        pieces = [back_y[16 * i : 16 * i + 16, group * 128 : group * 128 + 128] for i in range(4)]
        for k in range(4):
            flat_b2[pl.ds(group * 4 + k, 16, 16), :] = swap_groups(pieces, k)
    rx_b2[me] = tx_b2[me]
    arrive_b2, drain_b2 = exchange(tx_b2, rx_b2, sb2, rb2, yz_peer, 16, me)
    half_columns(CUTS[3], CUTS[4])
    arrive_b2()
    back_z = rx_b2[...].reshape(256, 128).T
    potential = split(dot3(split(back_z), (bz_ref[0], bz_ref[1])))

    def sample(source, c):
        values = dot3(potential, (z_high[source], z_low[source]))
        sums_ = jnp.sum(values * stencil[source], axis=0, keepdims=True)
        parts[2 * source] = sums_[:, 0:256]
        tail = jnp.broadcast_to(sums_[:, 128:384], (8, 256))
        parts[2 * source + 1] = pltpu.roll(tail, 192, 1)[0:1]
        return c

    lax.fori_loop(0, 4, sample, 0)

    def part_copy(s, u):
        return pltpu.make_async_remote_copy(
            src_ref=parts.at[2 * s + u],
            dst_ref=rx_parts.at[from_half[u], iz],
            send_sem=sp.at[s, u],
            recv_sem=rp.at[from_half[u], iz],
            device_id=(ix, from_y[u], s),
            device_id_type=MESH,
        )

    for s in range(4):
        for u in range(2):

            @pl.when((s != iz) | (from_y[u] != iy))
            def _():
                part_copy(s, u).start()

            @pl.when((s == iz) & (from_y[u] == iy))
            def _():
                rx_parts[from_half[u], iz] = parts[2 * s + u]

    half_columns(CUTS[4], 12)
    wv = wv_ref[...]
    invariant = jnp.zeros((384, 128), f32)
    for d in range(3):
        t = sums[1 + d]
        hi = t.astype(bf16)
        lo = (t - hi.astype(f32)).astype(bf16)
        vec = jnp.dot(hi, wv, preferred_element_type=f32) + jnp.dot(
            lo, wv, preferred_element_type=f32
        )
        invariant = invariant + vec * vec
    update = (sums[0] * (1.0 / 64.0) + invariant * (1.0 / 64.0)).astype(bf16)
    out_ref[...] = (
        feat_ref[...].astype(f32).reshape(384, 128) + jnp.dot(update, wo_ref[...], preferred_element_type=f32)
    ).astype(bf16)

    for half, to_z, step_y, place in routes:
        if step_y:
            atom_copy(half, to_z, step_y, place).wait_send()
        else:

            @pl.when(iz != to_z)
            def _():
                atom_copy(half, to_z, step_y, place).wait_send()

    drain_b()
    drain_c()
    drain_c2()
    drain_b2()
    for index in halo_ids:
        for copy in halo_copies(index):
            copy.wait_send()

    def part_wait(half, to_z, step_y):
        pltpu.make_async_remote_copy(
            src_ref=parts.at[0],
            dst_ref=rx_parts.at[half, to_z],
            send_sem=sp.at[0, 0],
            recv_sem=rp.at[half, to_z],
            device_id=(ix, lax.rem(iy + step_y, 4), to_z),
            device_id_type=MESH,
        ).wait_recv()

    for half, to_z, step_y, place in routes:
        if step_y:
            part_wait(half, to_z, step_y)
        else:

            @pl.when(iz != to_z)
            def _():
                part_wait(half, to_z, step_y)

    for half in range(2):
        site = (rx_parts[half, 0] + rx_parts[half, 1]) + (rx_parts[half, 2] + rx_parts[half, 3])
        for cx in range(3):
            block = site[:, 0:128] if cx < 2 else site[:, 128:256]
            block = jnp.broadcast_to(block, (8, 128))
            at = sub_l * 8 + lane_l % 8 + 64 * (cx % 2)
            site_ref[cx, half] = jnp.take_along_axis(block, at, axis=1)[:, 0:8]

    for s in range(4):
        for u in range(2):

            @pl.when((s != iz) | (from_y[u] != iy))
            def _():
                part_copy(s, u).wait_send()


def layer(operands):
    f32, bf16 = jnp.float32, jnp.bfloat16
    vm = pl.BlockSpec(memory_space=pltpu.VMEM)
    dma = pltpu.SemaphoreType.DMA
    tables = [jnp.asarray(t) for t in ewald_tables()]
    hbm = pl.BlockSpec(memory_space=pltpu.HBM)
    smem = pl.BlockSpec(memory_space=pltpu.SMEM)
    specs = [hbm] * 9 + [smem] + [hbm] * 5 + [smem] + [hbm] * 6
    shapes = [operands[n] for n in (0, 1, 2, 3, 14, 6, 7, 8, 10, 11, 4, 5)] + tables
    shapes += [operands[n] for n in (12, 13)]
    staged = [pltpu.VMEM(x.shape, x.dtype) for x in shapes]
    return pl.pallas_call(
        layer_kernel,
        out_shape=(
            jax.ShapeDtypeStruct((384, 128), bf16),
            jax.ShapeDtypeStruct((3, 2, 8, 8), f32),
        ),
        in_specs=specs,
        out_specs=(vm, vm),
        scratch_shapes=staged
        + [
            dma((20,)),
            pltpu.VMEM((3, 2, 4, 1, 128), f32),
            pltpu.VMEM((5, 4, 10, 8, 128), bf16),
            pltpu.VMEM((5, 4, 4, 1, 128), f32),
            pltpu.VMEM((6, 48, 128), f32),
            pltpu.VMEM((1600, 128), f32),
            pltpu.VMEM((128, 256), bf16),
            pltpu.VMEM((128, 128), bf16),
            pltpu.VMEM((128, 128), bf16),
            pltpu.VMEM((8, 512), jnp.int32),
            pltpu.VMEM((8, 512), jnp.int32),
            pltpu.VMEM((8, 512), f32),
            pltpu.VMEM((4, 384, 128), f32),
            pltpu.VMEM((2, 8, 256), f32),
            pltpu.VMEM((4, 2, 8, 256), f32),
            pltpu.VMEM((4, 256, 384), bf16),
            pltpu.VMEM((4, 256, 384), bf16),
            pltpu.VMEM((4, 128, 384), f32),
            pltpu.VMEM((16, 16, 128), f32),
            pltpu.VMEM((16, 16, 128), f32),
            pltpu.VMEM((8, 8, 512), f32),
            pltpu.VMEM((8, 8, 512), f32),
            pltpu.VMEM((8, 8, 512), f32),
            pltpu.VMEM((8, 8, 512), f32),
            pltpu.VMEM((16, 16, 128), f32),
            pltpu.VMEM((16, 16, 128), f32),
            pltpu.VMEM((8, 1, 256), f32),
            pltpu.VMEM((2, 4, 1, 256), f32),
            dma((2, 4)),
            dma((4, 2)),
            dma((16,)),
            dma((16,)),
            dma((8,)),
            dma((8,)),
            dma((8,)),
            dma((8,)),
            dma((16,)),
            dma((16,)),
            dma((4, 2)),
            dma((2, 4)),
            dma((27,)),
            dma((27,)),
            dma((27,)),
            dma((27,)),
        ],
        compiler_params=pltpu.CompilerParams(
            collective_id=0, has_side_effects=True, vmem_limit_bytes=67043328
        ),
        cost_estimate=pl.CostEstimate(flops=4 * 10**9, bytes_accessed=4 * 10**6, transcendentals=10**7),
        name="layer",
    )(*operands, *tables)


def shards(
    features,
    positions,
    grid_anchor,
    species,
    neighbours,
    neighbour_count,
    w_self,
    w_neighbour,
    w_radial,
    radial_rates,
    w_pair1,
    w_pair2,
    w_vector,
    w_out,
    w_charge,
    species_charge,
):
    updated, site_potential = layer(
        (
            features,
            positions,
            grid_anchor,
            species,
            neighbours,
            neighbour_count,
            w_neighbour,
            w_self,
            w_radial,
            radial_rates,
            w_pair1,
            w_pair2,
            w_vector,
            w_out,
            w_charge.reshape(1, 128),
            species_charge,
        )
    )
    return (updated.reshape(features.shape), site_potential)


def solution(mesh):
    return jax.shard_map(
        shards,
        mesh=mesh,
        in_specs=(
            P("gx", "gy", "gz", None, None),
            P("gx", "gy", "gz", None),
            P("gx", "gy", "gz", None),
            P("gx", "gy", "gz", None),
            P("gx", "gy", "gz", None),
            P("gx", "gy", "gz", None),
            P(),
            P(),
            P(),
            P(),
            P(),
            P(),
            P(),
            P(),
            P(),
            P(),
        ),
        out_specs=(P("gx", "gy", "gz", None, None), P("gx", "gy", "gz", None)),
        check_vma=False,
    )
```

```python
import jax
import jax.numpy as jnp
import numpy as np
from jax import lax
from jax.experimental import pallas as pl
from jax.experimental.pallas import tpu as pltpu
from jax.sharding import PartitionSpec as P


coulomb_scale = 0.25
smearing = 1.0


NT = (((1,), (1,)), ((), ()))
CUTS = (0, 4, 6, 8, 11)


def real_basis(length):
    modes = np.arange(length)[:, None]
    cells = np.arange(length)[None, :]
    turns = 2.0 * np.pi * ((modes * cells) % length) / length
    flipped = 2.0 * np.pi * (((length - modes) * cells) % length) / length
    return np.where(modes <= length // 2, np.cos(turns), np.sin(flipped))


def two_parts(table):
    table = np.asarray(table, np.float32)
    high = table.astype(jnp.bfloat16)
    low = (table - high.astype(np.float32)).astype(jnp.bfloat16)
    return np.stack([high, low])


def mode_tables(length):
    modes = np.arange(length)
    signed = np.where(modes > length // 2, modes - length, modes)
    wave = signed * (2.0 * np.pi / length)
    modulus = ((4.0 + 2.0 * np.cos(2.0 * np.pi * modes / length)) / 6.0) ** 2
    weight = np.where((modes == 0) | (modes == length // 2), 1.0, 2.0) / length
    return np.exp(-0.5 * smearing * smearing * wave * wave) / modulus * weight, wave * wave


def ewald_tables():
    basis_z = two_parts(real_basis(256))
    order_y = np.array([4 * p + i for i in range(4) for p in range(16)])
    forward_y = real_basis(64)[:, order_y]
    basis_y = np.stack([two_parts(forward_y), two_parts(forward_y.T)])
    wide = np.zeros((256, 256))
    full_x = real_basis(192)
    for g in range(8):
        wide[:192, 32 * g : 32 * g + 27] = full_x[:, (24 * g - 1 + np.arange(27)) % 192]
    basis_x = two_parts(wide)
    green_x = np.zeros((2, 8, 256))
    gain, square = mode_tables(192)
    green_x[0, :, :192] = gain * (coulomb_scale * 4.0 * np.pi)
    green_x[1, :, :192] = square
    green_x[1, :, 192:] = 1.0
    green_y = np.repeat(np.stack(mode_tables(64))[:, :, None], 128, 2)
    green_z = np.repeat(np.stack(mode_tables(256))[:, :, None], 128, 2)
    return (
        basis_z,
        basis_y,
        basis_x,
        green_x.astype(np.float32),
        green_y.astype(np.float32),
        green_z.astype(np.float32),
    )


def split(value):
    high = value.astype(jnp.bfloat16)
    return high, (value - high.astype(jnp.float32)).astype(jnp.bfloat16)


def dot3(a, b, dims=(((1,), (0,)), ((), ()))):
    def one(u, v):
        return lax.dot_general(u, v, dims, preferred_element_type=jnp.float32)

    return one(a[0], b[0]) + (one(a[0], b[1]) + one(a[1], b[0]))


def swap_groups(pieces, shift):
    lane = lax.broadcasted_iota(jnp.int32, pieces[0].shape, 1) // 32
    out = None
    for k, piece in enumerate(pieces):
        moved = pltpu.roll(piece, (32 * (k - shift)) % 128, 1) if k != shift else piece
        out = moved if out is None else jnp.where(lane == k, moved, out)
    return out


def tap_rows(fraction):
    square = fraction * fraction
    cube = square * fraction
    remain = 1.0 - fraction
    return (
        remain * remain * remain / 6.0,
        (3.0 * cube - 6.0 * square + 4.0) / 6.0,
        (-3.0 * cube + 3.0 * square + 3.0 * fraction + 1.0) / 6.0,
        cube / 6.0,
    )


def pick_taps(offset, taps):
    out = jnp.zeros(offset.shape, jnp.float32)
    for t in range(4):
        out = jnp.where(offset == t, taps[t], out)
    return out


def layer_kernel(
    feat_hbm,
    place_hbm,
    anchor_hbm,
    species_hbm,
    nbr_hbm,
    count_hbm,
    wn_hbm,
    ws_hbm,
    wr_hbm,
    rate_hbm,
    w1_hbm,
    w2_hbm,
    wv_hbm,
    wo_hbm,
    wc_hbm,
    kind_hbm,
    bz_hbm,
    by_hbm,
    bx_hbm,
    gx_hbm,
    gy_hbm,
    gz_hbm,
    out_ref,
    site_ref,
    feat_ref,
    place_ref,
    anchor_ref,
    species_ref,
    wc_ref,
    wn_ref,
    ws_ref,
    wr_ref,
    w1_ref,
    w2_ref,
    nbr_ref,
    count_ref,
    bz_ref,
    by_ref,
    bx_ref,
    gx_ref,
    gy_ref,
    gz_ref,
    wv_ref,
    wo_ref,
    kind_ref,
    rate_ref,
    load_sem,
    small_sem,
    pos_ref,
    feat_ext,
    pos_ext,
    pos_tab,
    feat32,
    first_w,
    pair1_w,
    pair2_w,
    hot_row,
    lane_row,
    live_row,
    sums,
    tx_atoms,
    rx_atoms,
    z_high,
    z_low,
    stencil,
    tx_b,
    rx_b,
    tx_c,
    rx_c,
    tx_c2,
    rx_c2,
    tx_b2,
    rx_b2,
    parts,
    rx_parts,
    sa,
    ra,
    sb,
    rb,
    sc,
    rc,
    sc2,
    rc2,
    sb2,
    rb2,
    sp,
    rp,
    sf,
    rf,
    sq,
    rq,
):
    bf16 = jnp.bfloat16
    f32 = jnp.float32
    MESH = pl.DeviceIdType.MESH
    ix, iy, iz = lax.axis_index("gx"), lax.axis_index("gy"), lax.axis_index("gz")
    me = iy * 4 + iz
    barrier = pltpu.get_barrier_semaphore()
    def yz_peer(r):
        other = lax.rem(me + r, 16)
        return other, (ix, other // 4, lax.rem(other, 4))

    def x_peer(r):
        other = lax.rem(ix + r, 8)
        return other, (other, iy, iz)

    def greet_yz(r, c):
        pl.semaphore_signal(barrier, inc=1, device_id=yz_peer(r)[1], device_id_type=MESH)
        return c

    def greet_x(r, c):
        pl.semaphore_signal(barrier, inc=1, device_id=x_peer(r)[1], device_id_type=MESH)
        return c

    lax.fori_loop(1, 16, greet_yz, 0)
    lax.fori_loop(1, 8, greet_x, 0)

    def halo_peer(index):
        ox, oy, oz = index // 9 - 1, index // 3 % 3 - 1, index % 3 - 1
        return (lax.rem(ix + ox + 8, 8), lax.rem(iy + oy + 4, 4), lax.rem(iz + oz + 4, 4))

    def halo_span(step, cells):
        if step == 0:
            return pl.ds(0, cells), pl.ds(1, cells)
        return (pl.ds(cells - 1, 1), pl.ds(0, 1)) if step > 0 else (pl.ds(0, 1), pl.ds(cells + 1, 1))

    halo_ids = [n for n in range(27) if n != 13]
    near_ids = [n for n in halo_ids if n // 9 == 1]
    far_ids = [n for n in halo_ids if n // 9 != 1]

    def halo_copies(index):
        steps = (index // 9 - 1, index // 3 % 3 - 1, index % 3 - 1)
        spans = [halo_span(step, cells) for step, cells in zip(steps, (3, 2, 8))]
        group = 0 if steps[0] == 0 else 1
        source = tuple(span[0] for span in spans)
        target = tuple(span[1] for span in spans)
        row = {0: pl.ds(1, 2), 1: pl.ds(0, 1), -1: pl.ds(3, 1)}[steps[2]]
        return [
            pltpu.make_async_remote_copy(
                src_ref=src.at[source[:2] + (from_z,)],
                dst_ref=dst.at[target[:2] + (to_z,)],
                send_sem=send.at[group],
                recv_sem=recv.at[group],
                device_id=halo_peer(index),
                device_id_type=MESH,
            )
            for src, dst, send, recv, from_z, to_z in (
                (feat_ref, feat_ext, sf, rf, source[2], target[2]),
                (pos_ref, pos_ext, sq, rq, row, row),
            )
        ]

    def halo_group(group):
        cells = (pl.ds(0, 2 if group else 3), pl.ds(0, 4), pl.ds(0, 10 if group else 6))
        rows = (pl.ds(0, 2 if group else 3), pl.ds(0, 4), pl.ds(0, 4 if group else 3))
        return [
            pltpu.make_async_remote_copy(
                src_ref=ext.at[part],
                dst_ref=ext.at[part],
                send_sem=send.at[group],
                recv_sem=recv.at[group],
                device_id=halo_peer(0),
                device_id_type=MESH,
            )
            for ext, part, send, recv in ((feat_ext, cells, sf, rf), (pos_ext, rows, sq, rq))
        ]

    for index in halo_ids:
        pl.semaphore_signal(barrier, inc=1, device_id=halo_peer(index), device_id_type=MESH)

    pairs = (
        (feat_hbm, feat_ref),
        (place_hbm, place_ref),
        (anchor_hbm, anchor_ref),
        (species_hbm, species_ref),
        (wc_hbm, wc_ref),
        (wn_hbm, wn_ref),
        (ws_hbm, ws_ref),
        (wr_hbm, wr_ref),
        (w1_hbm, w1_ref),
        (w2_hbm, w2_ref),
        (nbr_hbm, nbr_ref),
        (count_hbm, count_ref),
        (bz_hbm, bz_ref),
        (by_hbm, by_ref),
        (bx_hbm, bx_ref),
        (gx_hbm, gx_ref),
        (gy_hbm, gy_ref),
        (gz_hbm, gz_ref),
        (wv_hbm, wv_ref),
        (wo_hbm, wo_ref),
    )
    loads = [
        pltpu.make_async_copy(src, dst, load_sem.at[n]) for n, (src, dst) in enumerate(pairs)
    ]
    small = [
        pltpu.make_async_copy(kind_hbm, kind_ref, small_sem.at[0]),
        pltpu.make_async_copy(rate_hbm, rate_ref, small_sem.at[1]),
    ]
    for load in small + loads:
        load.start()

    for load in small + loads[:5]:
        load.wait()

    sub_l = lax.broadcasted_iota(jnp.int32, (8, 128), 0)
    lane_l = lax.broadcasted_iota(jnp.int32, (8, 128), 1)
    for half in range(2):
        own_rows = feat_ref[:, half].astype(f32).reshape(192, 128).astype(bf16)
        weights = jnp.broadcast_to(wc_ref[...].astype(f32), (16, 128)).astype(bf16)
        readout = lax.dot_general(weights, own_rows, NT, preferred_element_type=f32)[0:8]
        laid = []
        for cx in range(3):
            place = place_ref[cx, half]
            for row, cells in ((0, (7,)), (1, (0, 1, 2, 3)), (2, (4, 5, 6, 7)), (3, (0,))):
                pieces = [place[cz : cz + 1] for cz in cells]
                pieces.append(jnp.zeros((1, 128 - 24 * len(cells)), f32))
                pos_ref[cx, half, row] = jnp.concatenate(pieces, axis=1)
            source = jnp.concatenate(
                [
                    place,
                    anchor_ref[cx, half].astype(f32),
                    species_ref[cx, half].astype(f32),
                    jnp.zeros((8, 72), f32),
                ],
                axis=1,
            )
            rows = jnp.zeros((8, 128), f32)
            for cz in range(8):
                row = jnp.broadcast_to(source[cz : cz + 1], (8, 128))
                moved = jnp.take_along_axis(row, sub_l * 8 + lane_l % 8, axis=1)
                rows = jnp.where(lane_l // 8 == cz, moved, rows)
            laid.append(rows)
        rows = jnp.concatenate(
            [jnp.where(lane_l < 64, laid[0], pltpu.roll(laid[1], 64, 1)), laid[2]], axis=1
        )
        kinds = rows[6:7]
        base = jnp.where(kinds == 0.0, kind_ref[0], jnp.where(kinds == 1.0, kind_ref[1], 0.0))
        total = jnp.concatenate(
            [base[:, 0:192] + readout[0:1, :], jnp.zeros((1, 64), f32)], axis=1
        )
        tx_atoms[half, 0:3, :] = rows[0:3] - (rows[3:6] + 1.0)
        tx_atoms[half, 3:6, :] = rows[3:6]
        tx_atoms[half, 6:7, :] = total
        tx_atoms[half, 7:8, :] = jnp.zeros((1, 256), f32)

    for load in loads[5:10]:
        load.wait()
    first_w[:, 0:128] = (wn_ref[...].astype(f32) * 0.5).T.astype(bf16)
    first_w[:, 128:256] = (ws_ref[...].astype(f32) * 0.5).T.astype(bf16)
    pair1_w[...] = (w1_ref[...].astype(f32) * 0.5).T.astype(bf16)
    pair2_w[...] = (w2_ref[...].astype(f32) * 0.5).T.astype(bf16)
    radial_pad = jnp.concatenate(
        [jnp.zeros((88, 128), f32), wr_ref[...].astype(f32) * 0.5, jnp.zeros((32, 128), f32)], axis=0
    ).T
    cell_x0, cell_y0, cell_z0 = ix * 3, iy * 2, iz * 8

    sub8 = lax.broadcasted_iota(jnp.int32, (8, 512), 0)
    lane8 = lax.broadcasted_iota(jnp.int32, (8, 512), 1)
    rates = jnp.zeros((8, 512), f32)
    for k in range(8):
        rates = jnp.where(sub8 == k, rate_ref[k], rates)
    own_mask = (lane8 // 64) == sub8
    own_hot = jnp.where(own_mask, 1.0, 0.0).astype(f32)
    own_hot32 = jnp.concatenate([own_hot, own_hot, jnp.zeros((16, 512), f32)], axis=0).astype(bf16)
    lane_t = lax.broadcasted_iota(jnp.int32, (128, 128), 1)
    low_part = (lane_t >= 104) & (lane_t < 112)
    half_sub = sub_l // 4
    axis_sub = sub_l % 4
    box = jnp.where(axis_sub == 0, 192.0, jnp.where(axis_sub == 1, 64.0, 256.0)).astype(f32)
    box_inv = 1.0 / box
    atom_lane = lax.broadcasted_iota(jnp.int32, (8, 128), 1) // 64
    pl.semaphore_wait(barrier, 48)

    routes = [(0, 3, 3, 1), (0, 0, 0, 1), (0, 1, 0, 0), (0, 2, 0, 0)]
    routes += [(1, 1, 0, 1), (1, 2, 0, 1), (1, 3, 0, 0), (1, 0, 1, 0)]

    def atom_copy(half, to_z, step_y, place):
        return pltpu.make_async_remote_copy(
            src_ref=tx_atoms.at[half],
            dst_ref=rx_atoms.at[iz, place],
            send_sem=sa.at[half, to_z],
            recv_sem=ra.at[iz, place],
            device_id=(ix, lax.rem(iy + step_y, 4), to_z),
            device_id_type=MESH,
        )

    for half, to_z, step_y, place in routes:
        if step_y:
            atom_copy(half, to_z, step_y, place).start()
        else:

            @pl.when(iz != to_z)
            def _():
                atom_copy(half, to_z, step_y, place).start()

            @pl.when(iz == to_z)
            def _():
                rx_atoms[iz, place] = tx_atoms[half]

    for index in near_ids:
        for copy in halo_copies(index):
            copy.start()
    feat_ext[1:4, 1:3, 1:9] = feat_ref[...]
    pos_ext[1:4, 1:3, 1:3] = pos_ref[:, :, 1:3]
    def half_column(index, carry):
        later = (index - 4) // 2
        col = jnp.where(index < 4, 2 + index // 2, jnp.where(later < 2, later, later + 2))
        cx = col // 2
        cy = lax.rem(col, 2)
        ids = nbr_ref[cx, cy]
        slot = ids & 7
        z = (ids >> 3) & 31
        y = (ids >> 8) & 7
        x = ids >> 11
        dz = (z - (cell_z0 + sub8) + 1) & 31
        dy = (y - (cell_y0 + cy) + 1) & 7
        dx = x - (cell_x0 + cx) + 1
        dx = jnp.where(dx < 0, dx + 24, dx)
        dx = jnp.where(dx >= 24, dx - 24, dx)
        strip = dx * 3 + dy
        hot_row[...] = strip * 24 + dz * 8 + slot
        lane_row[...] = ((dz + sub8) * 8 + slot) * 16 + strip
        counts = jnp.concatenate([count_ref[cx, cy], jnp.zeros((8, 120), jnp.int32)], axis=1)
        pieces = []
        for g in range(4):
            owner = atom_lane + 2 * g
            count_g = jnp.take_along_axis(counts, owner, axis=1)
            slot_g = lax.broadcasted_iota(jnp.int32, (8, 128), 1) % 64
            pieces.append(jnp.where(slot_g < count_g, 1.0, 0.0).astype(f32))
        live_row[...] = jnp.concatenate(pieces, axis=1)

        def cell(cz):
            rows = []
            for dx_ in range(3):
                for dy_ in range(3):
                    base = ((cx + dx_) * 4 + cy + dy_) * 80 + cz * 8
                    rows.append(feat32[pl.ds(pl.multiple_of(base, 8), 24), :])
            own_base = ((cx + 1) * 4 + cy + 1) * 80 + cz * 8 + 8
            own = feat32[pl.ds(pl.multiple_of(own_base, 8), 8), :]
            left = jnp.concatenate(rows + [jnp.zeros((40, 128), f32)], axis=0)
            right = jnp.concatenate(
                [jnp.zeros((224, 128), f32), own, own, jnp.zeros((16, 128), f32)], axis=0
            )
            table = jnp.concatenate([left, right], axis=1).astype(bf16)
            proj = lax.dot_general(first_w[...], table, NT, preferred_element_type=f32)
            tail = proj[:, 128:256]
            tail_hi = tail.astype(bf16).astype(f32)
            tail = jnp.where(low_part, tail - tail_hi, tail_hi) + radial_pad
            lhs = jnp.concatenate([proj[:, 0:128].astype(bf16), tail.astype(bf16)], axis=1)

            place = []
            hot = hot_row[pl.ds(cz, 1), :]
            packed = lane_row[pl.ds(cz, 1), :]
            live = live_row[pl.ds(cz, 1), :]
            for g in range(4):
                packed_g = jnp.broadcast_to(packed[:, g * 128 : g * 128 + 128], (8, 128))
                where_g = packed_g >> 4
                strip_g = packed_g & 15
                got = jnp.zeros((8, 128), f32)
                for t in range(5):
                    hit = strip_g == (2 * t + half_sub)
                    got = jnp.where(
                        hit,
                        jnp.take_along_axis(pos_tab[col, t * 8 : t * 8 + 8, :], where_g, axis=1),
                        got,
                    )
                got = got + pltpu.roll(got, 4, 0)
                mine = jnp.take_along_axis(
                    pos_tab[col, 40:48, :], atom_lane + 2 * g + (cz + 1) * 8, axis=1
                )
                gap = got - mine
                gap = gap - box * jnp.floor(gap * box_inv + 0.5)
                place.append(gap * 0.125)
            scaled = jnp.concatenate(place, axis=1)
            square = scaled * scaled
            square = square[0:1] + square[1:2] + square[2:3]
            basis = jnp.exp(-jnp.broadcast_to(square, (8, 512)) * rates)
            cell_iota = lax.broadcasted_iota(jnp.int32, (216, 512), 0)
            hots = jnp.where(cell_iota == hot, 1.0, 0.0).astype(f32)
            rhs = jnp.concatenate(
                [jnp.concatenate([hots, basis], axis=0).astype(bf16), own_hot32], axis=0
            )
            half = jnp.dot(lhs, rhs, preferred_element_type=f32)
            yield
            latent = (half + half * jnp.tanh(half)).astype(bf16)
            half = jnp.dot(pair1_w[...], latent, preferred_element_type=f32)
            yield
            second = (half + half * jnp.tanh(half)).astype(bf16)
            half = jnp.dot(pair2_w[...], second, preferred_element_type=f32)
            yield
            third = (half + half * jnp.tanh(half)).astype(bf16)

            weighted = scaled * live
            w_hi = weighted.astype(bf16).astype(f32)
            w_lo = weighted - w_hi
            parts = [live]
            for d in range(3):
                parts += [w_hi[d : d + 1], w_lo[d : d + 1]]
            spread = jnp.concatenate(
                [jnp.where(own_mask, jnp.broadcast_to(p, (8, 512)), 0.0) for p in parts]
                + [jnp.zeros((8, 512), f32)],
                axis=0,
            ).astype(bf16)
            total = lax.dot_general(spread, third, NT, preferred_element_type=f32)
            yield
            at = pl.multiple_of((col * 8 + cz) * 8, 8)
            sums[0, pl.ds(at, 8), :] = total[0:8]
            for d in range(3):
                sums[1 + d, pl.ds(at, 8), :] = (
                    total[8 + 16 * d : 16 + 16 * d] + total[16 + 16 * d : 24 + 16 * d]
                )

        running = [cell(lax.rem(index, 2) * 4 + u) for u in range(4)]
        while running:
            running = [one for one in running if next(one, 1) is None]
        return carry

    def half_columns(first, last):
        lax.fori_loop(first, last, half_column, 0)

    from_y = [
        lax.rem(iy + jnp.where(iz == 0, 3, 0), 4),
        lax.rem(iy + jnp.where(iz == 3, 1, 0), 4),
    ]
    edge = jnp.where((iz == 0) | (iz == 3), 1, 0)
    from_half = [edge, 1 - edge]

    def atom_wait(s, u):
        @pl.when((s != iz) | (from_y[u] != iy))
        def _():
            pltpu.make_async_remote_copy(
                src_ref=tx_atoms.at[0],
                dst_ref=rx_atoms.at[s, u],
                send_sem=sa.at[0, 0],
                recv_sem=ra.at[s, u],
                device_id=(ix, from_y[u], s),
                device_id_type=MESH,
            ).wait_recv()

    y_first = iy * 16 + iz * 4

    for load in loads[10:]:
        load.wait()
    z_ids = lax.broadcasted_iota(jnp.int32, (256, 384), 0)
    x_ids = lax.broadcasted_iota(jnp.int32, (32, 384), 0) + (ix * 24 - 1)
    lane_384 = lax.broadcasted_iota(jnp.int32, (8, 128), 1)

    def spread(turn, total):
        step = jnp.where(turn < 2, turn, 5 - turn)
        source = lax.rem(iz + step, 4)
        for u in range(2):
            atom_wait(source, u)
        low_part_, high_part_ = rx_atoms[source, 0], rx_atoms[source, 1]
        moved = pltpu.roll(high_part_, 64, 1)
        rows = jnp.concatenate(
            [
                low_part_[:, 0:128],
                jnp.where(lane_384 < 64, low_part_[:, 128:256], moved[:, 0:128]),
                moved[:, 128:256],
            ],
            axis=1,
        )
        anchor = rows[3:6].astype(jnp.int32)
        weights_z = pick_taps((z_ids - anchor[2:3]) & 255, tap_rows(rows[2:3]))
        high, low = split(weights_z)
        z_high[source] = high
        z_low[source] = low
        weights_x = pick_taps(x_ids - anchor[0:1], tap_rows(rows[0:1]))
        taps_y = tap_rows(rows[1:2])
        blocks = [
            weights_x * pick_taps((y_first + i - anchor[1:2]) & 63, taps_y) for i in range(4)
        ]
        both = jnp.concatenate(blocks, axis=0)
        stencil[source] = both
        return total + dot3(split(both * rows[6:7]), (high, low), NT)

    lines = lax.fori_loop(0, 4, spread, jnp.zeros((128, 256), f32))
    spectrum = dot3((bz_ref[0], bz_ref[1]), split(lines), NT)
    tx_b[...] = spectrum.reshape(16, 16, 128)
    rx_b[me] = tx_b[me]

    def exchange(tx, rx, send, recv, peer, count, mine):
        def start(r, c):
            other, where = peer(r)
            pltpu.make_async_remote_copy(
                src_ref=tx.at[other],
                dst_ref=rx.at[mine],
                send_sem=send,
                recv_sem=recv,
                device_id=where,
                device_id_type=MESH,
            ).start()
            return c

        lax.fori_loop(1, count, start, 0)
        whole = pltpu.make_async_remote_copy(
            src_ref=tx.at[pl.ds(0, count - 1)],
            dst_ref=rx.at[pl.ds(0, count - 1)],
            send_sem=send,
            recv_sem=recv,
            device_id=peer(1)[1],
            device_id_type=MESH,
        )
        return whole.wait_recv, whole.wait_send

    arrive_b, drain_b = exchange(tx_b, rx_b, sb, rb, yz_peer, 16, me)

    for index in far_ids:
        for copy in halo_copies(index):
            copy.start()
    strip_lane = lax.broadcasted_iota(jnp.int32, (8, 128), 1)
    strip_cell = strip_lane // 8
    within = axis_sub * 8 + strip_lane % 8
    starts = jnp.where(strip_cell == 0, 0, jnp.where(strip_cell == 9, 0, lax.rem(strip_cell + 3, 4)))
    strip_at = jnp.where(axis_sub == 3, 127, jnp.minimum(starts * 24 + within, 127))
    strips = {}

    def lay_strips(sx):
        feat32[320 * sx : 320 * sx + 320, :] = feat_ext[sx].astype(f32).reshape(320, 128)
        for sy in range(4):
            table = jnp.zeros((8, 128), f32)
            for row, first, last in ((0, 0, 1), (1, 1, 5), (2, 5, 9), (3, 9, 10)):
                source = jnp.broadcast_to(pos_ext[sx, sy, row], (8, 128))
                moved = jnp.take_along_axis(source, strip_at, axis=1)
                table = jnp.where((strip_cell >= first) & (strip_cell < last), moved, table)
            strips[sx, sy] = table

    def lay_column(n):
        near = [strips[n // 2 + d // 3, n % 2 + d % 3] for d in range(9)]
        near += [near[4]] * 3
        for t in range(6):
            pos_tab[n, 8 * t : 8 * t + 8, :] = jnp.where(half_sub == 0, near[2 * t], near[2 * t + 1])

    for copy in halo_group(0):
        copy.wait_recv()
    for sx in (1, 2, 3):
        lay_strips(sx)
    for n in (2, 3):
        lay_column(n)
    half_columns(CUTS[0], CUTS[1])
    arrive_b()
    flat_b = rx_b.reshape(256, 128)
    columns = []
    for group in range(4):
        pieces = [flat_b[pl.ds(group * 4 + k, 16, 16), :] for k in range(4)]
        columns.append(jnp.concatenate([swap_groups(pieces, i) for i in range(4)], axis=0))
    lines_y = jnp.concatenate(columns, axis=1)
    modes_y = dot3((by_ref[0, 0], by_ref[0, 1]), split(lines_y))
    tx_c[...] = modes_y.reshape(8, 8, 512)
    rx_c[ix] = tx_c[ix]
    arrive_c, drain_c = exchange(tx_c, rx_c, sc, rc, x_peer, 8, ix)

    gain_z = gz_ref[0, pl.ds(pl.multiple_of(me * 16, 16), 16), :]
    square_z = gz_ref[1, pl.ds(pl.multiple_of(me * 16, 16), 16), :]
    gain_y = gy_ref[0, pl.ds(pl.multiple_of(ix * 8, 8), 8), :]
    square_y = gy_ref[1, pl.ds(pl.multiple_of(ix * 8, 8), 8), :]
    gain_yz = (gain_z[:, None, :] * gain_y[None, :, :]).reshape(128, 128)
    square_yz = (square_z[:, None, :] + square_y[None, :, :]).reshape(128, 128)
    greens = []
    for h in range(2):
        lanes = slice(128 * h, 128 * h + 128)
        total = square_yz + gx_ref[1, 0:1, lanes]
        value = gain_yz * gx_ref[0, 0:1, lanes] / (total + 1.0 / 1024.0)
        greens.append(jnp.where(total == 0.0, 0.0, value))
    green = jnp.concatenate(greens, axis=1)
    for copy in halo_group(1):
        copy.wait_recv()
    for sx in (0, 4):
        lay_strips(sx)
    for n in (0, 1, 4, 5):
        lay_column(n)
    half_columns(CUTS[1], CUTS[2])

    arrive_c()
    rows_x = []
    for group in range(4):
        for k in range(4):
            halves = [
                swap_groups(
                    [rx_c[4 * h + g, :, group * 128 : group * 128 + 128] for g in range(4)], k
                )
                for h in range(2)
            ]
            rows_x.append(jnp.concatenate(halves, axis=1))
    lines_x = jnp.concatenate(rows_x, axis=0)
    basis_x = (bx_ref[0], bx_ref[1])
    filtered = dot3(split(lines_x), basis_x, NT) * green
    back_x = dot3(split(filtered), basis_x)
    for g in range(8):
        half = g // 4
        for group in range(4):
            pieces = [
                back_x[(group * 4 + k) * 8 : (group * 4 + k) * 8 + 8, half * 128 : half * 128 + 128]
                for k in range(4)
            ]
            tx_c2[g, :, group * 128 : group * 128 + 128] = swap_groups(pieces, g % 4)
    rx_c2[ix] = tx_c2[ix]
    arrive_c2, drain_c2 = exchange(tx_c2, rx_c2, sc2, rc2, x_peer, 8, ix)
    half_columns(CUTS[2], CUTS[3])
    arrive_c2()
    back_y = dot3((by_ref[1, 0], by_ref[1, 1]), split(rx_c2[...].reshape(64, 512)))
    flat_b2 = tx_b2.reshape(256, 128)
    for group in range(4):
        pieces = [back_y[16 * i : 16 * i + 16, group * 128 : group * 128 + 128] for i in range(4)]
        for k in range(4):
            flat_b2[pl.ds(group * 4 + k, 16, 16), :] = swap_groups(pieces, k)
    rx_b2[me] = tx_b2[me]
    arrive_b2, drain_b2 = exchange(tx_b2, rx_b2, sb2, rb2, yz_peer, 16, me)
    half_columns(CUTS[3], CUTS[4])
    arrive_b2()
    back_z = rx_b2[...].reshape(256, 128).T
    potential = split(dot3(split(back_z), (bz_ref[0], bz_ref[1])))

    def sample(source, c):
        values = dot3(potential, (z_high[source], z_low[source]))
        sums_ = jnp.sum(values * stencil[source], axis=0, keepdims=True)
        parts[2 * source] = sums_[:, 0:256]
        tail = jnp.broadcast_to(sums_[:, 128:384], (8, 256))
        parts[2 * source + 1] = pltpu.roll(tail, 192, 1)[0:1]
        return c

    lax.fori_loop(0, 4, sample, 0)

    def part_copy(s, u):
        return pltpu.make_async_remote_copy(
            src_ref=parts.at[2 * s + u],
            dst_ref=rx_parts.at[from_half[u], iz],
            send_sem=sp.at[s, u],
            recv_sem=rp.at[from_half[u], iz],
            device_id=(ix, from_y[u], s),
            device_id_type=MESH,
        )

    for s in range(4):
        for u in range(2):

            @pl.when((s != iz) | (from_y[u] != iy))
            def _():
                part_copy(s, u).start()

            @pl.when((s == iz) & (from_y[u] == iy))
            def _():
                rx_parts[from_half[u], iz] = parts[2 * s + u]

    half_columns(CUTS[4], 12)
    wv = wv_ref[...]
    invariant = jnp.zeros((384, 128), f32)
    for d in range(3):
        t = sums[1 + d]
        hi = t.astype(bf16)
        lo = (t - hi.astype(f32)).astype(bf16)
        vec = jnp.dot(hi, wv, preferred_element_type=f32) + jnp.dot(
            lo, wv, preferred_element_type=f32
        )
        invariant = invariant + vec * vec
    update = (sums[0] * (1.0 / 64.0) + invariant * (1.0 / 64.0)).astype(bf16)
    out_ref[...] = (
        feat_ref[...].astype(f32).reshape(384, 128) + jnp.dot(update, wo_ref[...], preferred_element_type=f32)
    ).astype(bf16)

    for half, to_z, step_y, place in routes:
        if step_y:
            atom_copy(half, to_z, step_y, place).wait_send()
        else:

            @pl.when(iz != to_z)
            def _():
                atom_copy(half, to_z, step_y, place).wait_send()

    drain_b()
    drain_c()
    drain_c2()
    drain_b2()
    for group in range(2):
        for copy in halo_group(group):
            copy.wait_send()

    def part_wait(half, to_z, step_y):
        pltpu.make_async_remote_copy(
            src_ref=parts.at[0],
            dst_ref=rx_parts.at[half, to_z],
            send_sem=sp.at[0, 0],
            recv_sem=rp.at[half, to_z],
            device_id=(ix, lax.rem(iy + step_y, 4), to_z),
            device_id_type=MESH,
        ).wait_recv()

    for half, to_z, step_y, place in routes:
        if step_y:
            part_wait(half, to_z, step_y)
        else:

            @pl.when(iz != to_z)
            def _():
                part_wait(half, to_z, step_y)

    for half in range(2):
        site = (rx_parts[half, 0] + rx_parts[half, 1]) + (rx_parts[half, 2] + rx_parts[half, 3])
        for cx in range(3):
            block = site[:, 0:128] if cx < 2 else site[:, 128:256]
            block = jnp.broadcast_to(block, (8, 128))
            at = sub_l * 8 + lane_l % 8 + 64 * (cx % 2)
            site_ref[cx, half] = jnp.take_along_axis(block, at, axis=1)[:, 0:8]

    for s in range(4):
        for u in range(2):

            @pl.when((s != iz) | (from_y[u] != iy))
            def _():
                part_copy(s, u).wait_send()


def layer(operands):
    f32, bf16 = jnp.float32, jnp.bfloat16
    vm = pl.BlockSpec(memory_space=pltpu.VMEM)
    dma = pltpu.SemaphoreType.DMA
    tables = [jnp.asarray(t) for t in ewald_tables()]
    hbm = pl.BlockSpec(memory_space=pltpu.HBM)
    specs = [hbm] * 22
    shapes = [operands[n] for n in (0, 1, 2, 3, 14, 6, 7, 8, 10, 11, 4, 5)] + tables
    shapes += [operands[n] for n in (12, 13)]
    staged = [pltpu.VMEM(x.shape, x.dtype) for x in shapes]
    return pl.pallas_call(
        layer_kernel,
        out_shape=(
            jax.ShapeDtypeStruct((384, 128), bf16),
            jax.ShapeDtypeStruct((3, 2, 8, 8), f32),
        ),
        in_specs=specs,
        out_specs=(vm, vm),
        scratch_shapes=staged
        + [
            pltpu.SMEM((2,), f32),
            pltpu.SMEM((8,), f32),
            dma((20,)),
            dma((2,)),
            pltpu.VMEM((3, 2, 4, 1, 128), f32),
            pltpu.VMEM((5, 4, 10, 8, 128), bf16),
            pltpu.VMEM((5, 4, 4, 1, 128), f32),
            pltpu.VMEM((6, 48, 128), f32),
            pltpu.VMEM((1600, 128), f32),
            pltpu.VMEM((128, 256), bf16),
            pltpu.VMEM((128, 128), bf16),
            pltpu.VMEM((128, 128), bf16),
            pltpu.VMEM((8, 512), jnp.int32),
            pltpu.VMEM((8, 512), jnp.int32),
            pltpu.VMEM((8, 512), f32),
            pltpu.VMEM((4, 384, 128), f32),
            pltpu.VMEM((2, 8, 256), f32),
            pltpu.VMEM((4, 2, 8, 256), f32),
            pltpu.VMEM((4, 256, 384), bf16),
            pltpu.VMEM((4, 256, 384), bf16),
            pltpu.VMEM((4, 128, 384), f32),
            pltpu.VMEM((16, 16, 128), f32),
            pltpu.VMEM((16, 16, 128), f32),
            pltpu.VMEM((8, 8, 512), f32),
            pltpu.VMEM((8, 8, 512), f32),
            pltpu.VMEM((8, 8, 512), f32),
            pltpu.VMEM((8, 8, 512), f32),
            pltpu.VMEM((16, 16, 128), f32),
            pltpu.VMEM((16, 16, 128), f32),
            pltpu.VMEM((8, 1, 256), f32),
            pltpu.VMEM((2, 4, 1, 256), f32),
            dma((2, 4)),
            dma((4, 2)),
            *[pltpu.SemaphoreType.DMA] * 8,
            dma((4, 2)),
            dma((2, 4)),
            dma((2,)),
            dma((2,)),
            dma((2,)),
            dma((2,)),
        ],
        compiler_params=pltpu.CompilerParams(
            collective_id=0, has_side_effects=True, vmem_limit_bytes=48 * 1024 * 1024
        ),
        cost_estimate=pl.CostEstimate(flops=4 * 10**9, bytes_accessed=4 * 10**6, transcendentals=10**7),
        name="layer",
    )(*[pltpu.with_memory_space_constraint(x, pltpu.HBM) for x in (*operands, *tables)])


def shards(
    features,
    positions,
    grid_anchor,
    species,
    neighbours,
    neighbour_count,
    w_self,
    w_neighbour,
    w_radial,
    radial_rates,
    w_pair1,
    w_pair2,
    w_vector,
    w_out,
    w_charge,
    species_charge,
):
    updated, site_potential = layer(
        (
            features,
            positions,
            grid_anchor,
            species,
            neighbours,
            neighbour_count,
            w_neighbour,
            w_self,
            w_radial,
            radial_rates,
            w_pair1,
            w_pair2,
            w_vector,
            w_out,
            w_charge.reshape(1, 128),
            species_charge,
        )
    )
    return (updated.reshape(features.shape), site_potential)


def solution(mesh):
    return jax.shard_map(
        shards,
        mesh=mesh,
        in_specs=(
            P("gx", "gy", "gz", None, None),
            P("gx", "gy", "gz", None),
            P("gx", "gy", "gz", None),
            P("gx", "gy", "gz", None),
            P("gx", "gy", "gz", None),
            P("gx", "gy", "gz", None),
            P(),
            P(),
            P(),
            P(),
            P(),
            P(),
            P(),
            P(),
            P(),
            P(),
        ),
        out_specs=(P("gx", "gy", "gz", None, None), P("gx", "gy", "gz", None)),
        check_vma=False,
    )
```

```python
import jax
import jax.numpy as jnp
import numpy as np
from jax import lax
from jax.experimental import pallas as pl
from jax.experimental.pallas import tpu as pltpu
from jax.sharding import PartitionSpec as P


coulomb_scale = 0.25
smearing = 1.0


NT = (((1,), (1,)), ((), ()))
CUTS = (0, 4, 6, 8, 11)


def real_basis(length):
    modes = np.arange(length)[:, None]
    cells = np.arange(length)[None, :]
    turns = 2.0 * np.pi * ((modes * cells) % length) / length
    flipped = 2.0 * np.pi * (((length - modes) * cells) % length) / length
    return np.where(modes <= length // 2, np.cos(turns), np.sin(flipped))


def two_parts(table):
    table = np.asarray(table, np.float32)
    high = table.astype(jnp.bfloat16)
    low = (table - high.astype(np.float32)).astype(jnp.bfloat16)
    return np.stack([high, low])


def mode_tables(length):
    modes = np.arange(length)
    signed = np.where(modes > length // 2, modes - length, modes)
    wave = signed * (2.0 * np.pi / length)
    modulus = ((4.0 + 2.0 * np.cos(2.0 * np.pi * modes / length)) / 6.0) ** 2
    weight = np.where((modes == 0) | (modes == length // 2), 1.0, 2.0) / length
    return np.exp(-0.5 * smearing * smearing * wave * wave) / modulus * weight, wave * wave


def ewald_tables():
    basis_z = two_parts(real_basis(256))
    order_y = np.array([4 * p + i for i in range(4) for p in range(16)])
    forward_y = real_basis(64)[:, order_y]
    basis_y = np.stack([two_parts(forward_y), two_parts(forward_y.T)])
    wide = np.zeros((256, 256))
    full_x = real_basis(192)
    for g in range(8):
        wide[:192, 32 * g : 32 * g + 27] = full_x[:, (24 * g - 1 + np.arange(27)) % 192]
    basis_x = two_parts(wide)
    green_x = np.zeros((2, 8, 256))
    gain, square = mode_tables(192)
    green_x[0, :, :192] = gain * (coulomb_scale * 4.0 * np.pi)
    green_x[1, :, :192] = square
    green_x[1, :, 192:] = 1.0
    green_y = np.repeat(np.stack(mode_tables(64))[:, :, None], 128, 2)
    green_z = np.repeat(np.stack(mode_tables(256))[:, :, None], 128, 2)
    return (
        basis_z,
        basis_y,
        basis_x,
        green_x.astype(np.float32),
        green_y.astype(np.float32),
        green_z.astype(np.float32),
    )


def split(value):
    high = value.astype(jnp.bfloat16)
    return high, (value - high.astype(jnp.float32)).astype(jnp.bfloat16)


def dot3(a, b, dims=(((1,), (0,)), ((), ()))):
    def one(u, v):
        return lax.dot_general(u, v, dims, preferred_element_type=jnp.float32)

    return one(a[0], b[0]) + (one(a[0], b[1]) + one(a[1], b[0]))


def swap_groups(pieces, shift):
    lane = lax.broadcasted_iota(jnp.int32, pieces[0].shape, 1) // 32
    out = None
    for k, piece in enumerate(pieces):
        moved = pltpu.roll(piece, (32 * (k - shift)) % 128, 1) if k != shift else piece
        out = moved if out is None else jnp.where(lane == k, moved, out)
    return out


def tap_rows(fraction):
    square = fraction * fraction
    cube = square * fraction
    remain = 1.0 - fraction
    return (
        remain * remain * remain / 6.0,
        (3.0 * cube - 6.0 * square + 4.0) / 6.0,
        (-3.0 * cube + 3.0 * square + 3.0 * fraction + 1.0) / 6.0,
        cube / 6.0,
    )


def pick_taps(offset, taps):
    out = jnp.zeros(offset.shape, jnp.float32)
    for t in range(4):
        out = jnp.where(offset == t, taps[t], out)
    return out


def layer_kernel(
    feat_hbm,
    place_hbm,
    anchor_hbm,
    species_hbm,
    nbr_hbm,
    count_hbm,
    wn_hbm,
    ws_hbm,
    wr_hbm,
    rate_hbm,
    w1_hbm,
    w2_hbm,
    wv_hbm,
    wo_hbm,
    wc_hbm,
    kind_hbm,
    bz_hbm,
    by_hbm,
    bx_hbm,
    gx_hbm,
    gy_hbm,
    gz_hbm,
    out_ref,
    site_ref,
    feat_ref,
    place_ref,
    anchor_ref,
    species_ref,
    wc_ref,
    wn_ref,
    ws_ref,
    wr_ref,
    w1_ref,
    w2_ref,
    nbr_ref,
    count_ref,
    bz_ref,
    by_ref,
    bx_ref,
    gx_ref,
    gy_ref,
    gz_ref,
    wv_ref,
    wo_ref,
    kind_ref,
    rate_ref,
    load_sem,
    small_sem,
    pos_ref,
    feat_ext,
    pos_ext,
    pos_tab,
    feat32,
    first_w,
    pair1_w,
    pair2_w,
    hot_row,
    lane_row,
    live_row,
    sums,
    tx_atoms,
    rx_atoms,
    z_high,
    z_low,
    stencil,
    tx_b,
    rx_b,
    tx_c,
    rx_c,
    tx_c2,
    rx_c2,
    tx_b2,
    rx_b2,
    flat_b,
    parts,
    rx_parts,
    sa,
    ra,
    sb,
    rb,
    sc,
    rc,
    sc2,
    rc2,
    sb2,
    rb2,
    sp,
    rp,
    sf,
    rf,
    sq,
    rq,
):
    bf16 = jnp.bfloat16
    f32 = jnp.float32
    MESH = pl.DeviceIdType.MESH
    ix, iy, iz = lax.axis_index("gx"), lax.axis_index("gy"), lax.axis_index("gz")
    me = iy * 4 + iz
    barrier = pltpu.get_barrier_semaphore()
    def yz_peer(r):
        other = lax.rem(me + r, 16)
        return other, (ix, other // 4, lax.rem(other, 4))

    def x_peer(r):
        other = lax.rem(ix + r, 8)
        return other, (other, iy, iz)

    def greet_yz(r, c):
        pl.semaphore_signal(barrier, inc=1, device_id=yz_peer(r)[1], device_id_type=MESH)
        return c

    def greet_x(r, c):
        pl.semaphore_signal(barrier, inc=1, device_id=x_peer(r)[1], device_id_type=MESH)
        return c

    lax.fori_loop(1, 16, greet_yz, 0)
    lax.fori_loop(1, 8, greet_x, 0)

    def halo_peer(index):
        ox, oy, oz = index // 9 - 1, index // 3 % 3 - 1, index % 3 - 1
        return (lax.rem(ix + ox + 8, 8), lax.rem(iy + oy + 4, 4), lax.rem(iz + oz + 4, 4))

    def halo_span(step, cells):
        if step == 0:
            return pl.ds(0, cells), pl.ds(1, cells)
        return (pl.ds(cells - 1, 1), pl.ds(0, 1)) if step > 0 else (pl.ds(0, 1), pl.ds(cells + 1, 1))

    halo_ids = [n for n in range(27) if n != 13]
    near_ids = [n for n in halo_ids if n // 9 == 1]
    far_ids = [n for n in halo_ids if n // 9 != 1]

    def halo_copies(index):
        steps = (index // 9 - 1, index // 3 % 3 - 1, index % 3 - 1)
        spans = [halo_span(step, cells) for step, cells in zip(steps, (3, 2, 8))]
        group = 0 if steps[0] == 0 else 1
        source = tuple(span[0] for span in spans)
        target = tuple(span[1] for span in spans)
        row = {0: pl.ds(1, 2), 1: pl.ds(0, 1), -1: pl.ds(3, 1)}[steps[2]]
        return [
            pltpu.make_async_remote_copy(
                src_ref=src.at[source[:2] + (from_z,)],
                dst_ref=dst.at[target[:2] + (to_z,)],
                send_sem=send.at[group],
                recv_sem=recv.at[group],
                device_id=halo_peer(index),
                device_id_type=MESH,
            )
            for src, dst, send, recv, from_z, to_z in (
                (feat_ref, feat_ext, sf, rf, source[2], target[2]),
                (pos_ref, pos_ext, sq, rq, row, row),
            )
        ]

    def halo_group(group):
        cells = (pl.ds(0, 2 if group else 3), pl.ds(0, 4), pl.ds(0, 10 if group else 6))
        rows = (pl.ds(0, 2 if group else 3), pl.ds(0, 4), pl.ds(0, 4 if group else 3))
        return [
            pltpu.make_async_remote_copy(
                src_ref=ext.at[part],
                dst_ref=ext.at[part],
                send_sem=send.at[group],
                recv_sem=recv.at[group],
                device_id=halo_peer(0),
                device_id_type=MESH,
            )
            for ext, part, send, recv in ((feat_ext, cells, sf, rf), (pos_ext, rows, sq, rq))
        ]

    for index in halo_ids:
        pl.semaphore_signal(barrier, inc=1, device_id=halo_peer(index), device_id_type=MESH)

    pairs = (
        (feat_hbm, feat_ref),
        (place_hbm, place_ref),
        (anchor_hbm, anchor_ref),
        (species_hbm, species_ref),
        (wc_hbm, wc_ref),
        (wn_hbm, wn_ref),
        (ws_hbm, ws_ref),
        (wr_hbm, wr_ref),
        (w1_hbm, w1_ref),
        (w2_hbm, w2_ref),
        (nbr_hbm, nbr_ref),
        (count_hbm, count_ref),
        (bz_hbm, bz_ref),
        (by_hbm, by_ref),
        (bx_hbm, bx_ref),
        (gx_hbm, gx_ref),
        (gy_hbm, gy_ref),
        (gz_hbm, gz_ref),
        (wv_hbm, wv_ref),
        (wo_hbm, wo_ref),
    )
    loads = [
        pltpu.make_async_copy(src, dst, load_sem.at[n]) for n, (src, dst) in enumerate(pairs)
    ]
    small = [
        pltpu.make_async_copy(kind_hbm, kind_ref, small_sem.at[0]),
        pltpu.make_async_copy(rate_hbm, rate_ref, small_sem.at[1]),
    ]
    for load in small + loads:
        load.start()

    for load in small + loads[:5]:
        load.wait()

    sub_l = lax.broadcasted_iota(jnp.int32, (8, 128), 0)
    lane_l = lax.broadcasted_iota(jnp.int32, (8, 128), 1)
    for half in range(2):
        own_rows = feat_ref[:, half].astype(f32).reshape(192, 128).astype(bf16)
        weights = jnp.broadcast_to(wc_ref[...].astype(f32), (16, 128)).astype(bf16)
        readout = lax.dot_general(weights, own_rows, NT, preferred_element_type=f32)[0:8]
        laid = []
        for cx in range(3):
            place = place_ref[cx, half]
            for row, cells in ((0, (7,)), (1, (0, 1, 2, 3)), (2, (4, 5, 6, 7)), (3, (0,))):
                pieces = [place[cz : cz + 1] for cz in cells]
                pieces.append(jnp.zeros((1, 128 - 24 * len(cells)), f32))
                pos_ref[cx, half, row] = jnp.concatenate(pieces, axis=1)
            source = jnp.concatenate(
                [
                    place,
                    anchor_ref[cx, half].astype(f32),
                    species_ref[cx, half].astype(f32),
                    jnp.zeros((8, 72), f32),
                ],
                axis=1,
            )
            rows = jnp.zeros((8, 128), f32)
            for cz in range(8):
                row = jnp.broadcast_to(source[cz : cz + 1], (8, 128))
                moved = jnp.take_along_axis(row, sub_l * 8 + lane_l % 8, axis=1)
                rows = jnp.where(lane_l // 8 == cz, moved, rows)
            laid.append(rows)
        rows = jnp.concatenate(
            [jnp.where(lane_l < 64, laid[0], pltpu.roll(laid[1], 64, 1)), laid[2]], axis=1
        )
        kinds = rows[6:7]
        base = jnp.where(kinds == 0.0, kind_ref[0], jnp.where(kinds == 1.0, kind_ref[1], 0.0))
        total = jnp.concatenate(
            [base[:, 0:192] + readout[0:1, :], jnp.zeros((1, 64), f32)], axis=1
        )
        tx_atoms[half, 0:3, :] = rows[0:3] - (rows[3:6] + 1.0)
        tx_atoms[half, 3:6, :] = rows[3:6]
        tx_atoms[half, 6:7, :] = total
        tx_atoms[half, 7:8, :] = jnp.zeros((1, 256), f32)

    for load in loads[5:10]:
        load.wait()
    first_w[:, 0:128] = (wn_ref[...].astype(f32) * 0.5).T.astype(bf16)
    first_w[:, 128:256] = (ws_ref[...].astype(f32) * 0.5).T.astype(bf16)
    pair1_w[...] = (w1_ref[...].astype(f32) * 0.5).T.astype(bf16)
    pair2_w[...] = (w2_ref[...].astype(f32) * 0.5).T.astype(bf16)
    radial_pad = jnp.concatenate(
        [jnp.zeros((88, 128), f32), wr_ref[...].astype(f32) * 0.5, jnp.zeros((32, 128), f32)], axis=0
    ).T
    cell_x0, cell_y0, cell_z0 = ix * 3, iy * 2, iz * 8

    sub8 = lax.broadcasted_iota(jnp.int32, (8, 512), 0)
    lane8 = lax.broadcasted_iota(jnp.int32, (8, 512), 1)
    rates = jnp.zeros((8, 512), f32)
    for k in range(8):
        rates = jnp.where(sub8 == k, rate_ref[k], rates)
    own_mask = (lane8 // 64) == sub8
    own_hot = jnp.where(own_mask, 1.0, 0.0).astype(f32)
    own_hot32 = jnp.concatenate([own_hot, own_hot, jnp.zeros((16, 512), f32)], axis=0).astype(bf16)
    lane_t = lax.broadcasted_iota(jnp.int32, (128, 128), 1)
    low_part = (lane_t >= 104) & (lane_t < 112)
    half_sub = sub_l // 4
    axis_sub = sub_l % 4
    box = jnp.where(axis_sub == 0, 192.0, jnp.where(axis_sub == 1, 64.0, 256.0)).astype(f32)
    box_inv = 1.0 / box
    atom_lane = lax.broadcasted_iota(jnp.int32, (8, 128), 1) // 64
    pl.semaphore_wait(barrier, 48)

    routes = [(0, 3, 3, 1), (0, 0, 0, 1), (0, 1, 0, 0), (0, 2, 0, 0)]
    routes += [(1, 1, 0, 1), (1, 2, 0, 1), (1, 3, 0, 0), (1, 0, 1, 0)]

    def atom_copy(half, to_z, step_y, place):
        return pltpu.make_async_remote_copy(
            src_ref=tx_atoms.at[half],
            dst_ref=rx_atoms.at[iz, place],
            send_sem=sa.at[half, to_z],
            recv_sem=ra.at[iz, place],
            device_id=(ix, lax.rem(iy + step_y, 4), to_z),
            device_id_type=MESH,
        )

    for half, to_z, step_y, place in routes:
        if step_y:
            atom_copy(half, to_z, step_y, place).start()
        else:

            @pl.when(iz != to_z)
            def _():
                atom_copy(half, to_z, step_y, place).start()

            @pl.when(iz == to_z)
            def _():
                rx_atoms[iz, place] = tx_atoms[half]

    for index in near_ids:
        for copy in halo_copies(index):
            copy.start()
    feat_ext[1:4, 1:3, 1:9] = feat_ref[...]
    pos_ext[1:4, 1:3, 1:3] = pos_ref[:, :, 1:3]
    def half_column(index, carry):
        later = (index - 4) // 2
        col = jnp.where(index < 4, 2 + index // 2, jnp.where(later < 2, later, later + 2))
        cx = col // 2
        cy = lax.rem(col, 2)
        ids = nbr_ref[cx, cy]
        slot = ids & 7
        z = (ids >> 3) & 31
        y = (ids >> 8) & 7
        x = ids >> 11
        dz = (z - (cell_z0 + sub8) + 1) & 31
        dy = (y - (cell_y0 + cy) + 1) & 7
        dx = x - (cell_x0 + cx) + 1
        dx = jnp.where(dx < 0, dx + 24, dx)
        dx = jnp.where(dx >= 24, dx - 24, dx)
        strip = dx * 3 + dy
        hot_row[...] = strip * 24 + dz * 8 + slot
        lane_row[...] = ((dz + sub8) * 8 + slot) * 16 + strip
        counts = jnp.concatenate([count_ref[cx, cy], jnp.zeros((8, 120), jnp.int32)], axis=1)
        pieces = []
        for g in range(4):
            owner = atom_lane + 2 * g
            count_g = jnp.take_along_axis(counts, owner, axis=1)
            slot_g = lax.broadcasted_iota(jnp.int32, (8, 128), 1) % 64
            pieces.append(jnp.where(slot_g < count_g, 1.0, 0.0).astype(f32))
        live_row[...] = jnp.concatenate(pieces, axis=1)

        def cell(cz):
            rows = []
            for dx_ in range(3):
                for dy_ in range(3):
                    base = ((cx + dx_) * 4 + cy + dy_) * 80 + cz * 8
                    rows.append(feat32[pl.ds(pl.multiple_of(base, 8), 24), :])
            own_base = ((cx + 1) * 4 + cy + 1) * 80 + cz * 8 + 8
            own = feat32[pl.ds(pl.multiple_of(own_base, 8), 8), :]
            left = jnp.concatenate(rows + [jnp.zeros((40, 128), f32)], axis=0)
            right = jnp.concatenate(
                [jnp.zeros((224, 128), f32), own, own, jnp.zeros((16, 128), f32)], axis=0
            )
            table = jnp.concatenate([left, right], axis=1).astype(bf16)
            proj = lax.dot_general(first_w[...], table, NT, preferred_element_type=f32)
            tail = proj[:, 128:256]
            tail_hi = tail.astype(bf16).astype(f32)
            tail = jnp.where(low_part, tail - tail_hi, tail_hi) + radial_pad
            lhs = jnp.concatenate([proj[:, 0:128].astype(bf16), tail.astype(bf16)], axis=1)

            place = []
            hot = hot_row[pl.ds(cz, 1), :]
            packed = lane_row[pl.ds(cz, 1), :]
            live = live_row[pl.ds(cz, 1), :]
            for g in range(4):
                packed_g = jnp.broadcast_to(packed[:, g * 128 : g * 128 + 128], (8, 128))
                where_g = packed_g >> 4
                strip_g = packed_g & 15
                got = jnp.zeros((8, 128), f32)
                for t in range(5):
                    hit = strip_g == (2 * t + half_sub)
                    got = jnp.where(
                        hit,
                        jnp.take_along_axis(pos_tab[col, t * 8 : t * 8 + 8, :], where_g, axis=1),
                        got,
                    )
                got = got + pltpu.roll(got, 4, 0)
                mine = jnp.take_along_axis(
                    pos_tab[col, 40:48, :], atom_lane + 2 * g + (cz + 1) * 8, axis=1
                )
                gap = got - mine
                gap = gap - box * jnp.floor(gap * box_inv + 0.5)
                place.append(gap * 0.125)
            scaled = jnp.concatenate(place, axis=1)
            square = scaled * scaled
            square = square[0:1] + square[1:2] + square[2:3]
            basis = jnp.exp(-jnp.broadcast_to(square, (8, 512)) * rates)
            cell_iota = lax.broadcasted_iota(jnp.int32, (216, 512), 0)
            hots = jnp.where(cell_iota == hot, 1.0, 0.0).astype(f32)
            rhs = jnp.concatenate(
                [jnp.concatenate([hots, basis], axis=0).astype(bf16), own_hot32], axis=0
            )
            half = jnp.dot(lhs, rhs, preferred_element_type=f32)
            yield
            latent = (half + half * jnp.tanh(half)).astype(bf16)
            half = jnp.dot(pair1_w[...], latent, preferred_element_type=f32)
            yield
            second = (half + half * jnp.tanh(half)).astype(bf16)
            half = jnp.dot(pair2_w[...], second, preferred_element_type=f32)
            yield
            third = (half + half * jnp.tanh(half)).astype(bf16)

            weighted = scaled * live
            w_hi = weighted.astype(bf16).astype(f32)
            w_lo = weighted - w_hi
            parts = [live]
            for d in range(3):
                parts += [w_hi[d : d + 1], w_lo[d : d + 1]]
            spread = jnp.concatenate(
                [jnp.where(own_mask, jnp.broadcast_to(p, (8, 512)), 0.0) for p in parts]
                + [jnp.zeros((8, 512), f32)],
                axis=0,
            ).astype(bf16)
            total = lax.dot_general(spread, third, NT, preferred_element_type=f32)
            yield
            at = pl.multiple_of((col * 8 + cz) * 8, 8)
            sums[0, pl.ds(at, 8), :] = total[0:8]
            for d in range(3):
                sums[1 + d, pl.ds(at, 8), :] = (
                    total[8 + 16 * d : 16 + 16 * d] + total[16 + 16 * d : 24 + 16 * d]
                )

        running = [cell(lax.rem(index, 2) * 4 + u) for u in range(4)]
        while running:
            running = [one for one in running if next(one, 1) is None]
        return carry

    def half_columns(first, last):
        lax.fori_loop(first, last, half_column, 0)

    from_y = [
        lax.rem(iy + jnp.where(iz == 0, 3, 0), 4),
        lax.rem(iy + jnp.where(iz == 3, 1, 0), 4),
    ]
    edge = jnp.where((iz == 0) | (iz == 3), 1, 0)
    from_half = [edge, 1 - edge]

    def atom_wait(s, u):
        @pl.when((s != iz) | (from_y[u] != iy))
        def _():
            pltpu.make_async_remote_copy(
                src_ref=tx_atoms.at[0],
                dst_ref=rx_atoms.at[s, u],
                send_sem=sa.at[0, 0],
                recv_sem=ra.at[s, u],
                device_id=(ix, from_y[u], s),
                device_id_type=MESH,
            ).wait_recv()

    y_first = iy * 16 + iz * 4

    for load in loads[10:]:
        load.wait()
    z_ids = lax.broadcasted_iota(jnp.int32, (256, 384), 0)
    x_ids = lax.broadcasted_iota(jnp.int32, (32, 384), 0) + (ix * 24 - 1)
    lane_384 = lax.broadcasted_iota(jnp.int32, (8, 128), 1)

    def spread(turn, total):
        step = jnp.where(turn < 2, turn, 5 - turn)
        source = lax.rem(iz + step, 4)
        for u in range(2):
            atom_wait(source, u)
        low_part_, high_part_ = rx_atoms[source, 0], rx_atoms[source, 1]
        moved = pltpu.roll(high_part_, 64, 1)
        rows = jnp.concatenate(
            [
                low_part_[:, 0:128],
                jnp.where(lane_384 < 64, low_part_[:, 128:256], moved[:, 0:128]),
                moved[:, 128:256],
            ],
            axis=1,
        )
        anchor = rows[3:6].astype(jnp.int32)
        weights_z = pick_taps((z_ids - anchor[2:3]) & 255, tap_rows(rows[2:3]))
        high, low = split(weights_z)
        z_high[source] = high
        z_low[source] = low
        weights_x = pick_taps(x_ids - anchor[0:1], tap_rows(rows[0:1]))
        taps_y = tap_rows(rows[1:2])
        blocks = [
            weights_x * pick_taps((y_first + i - anchor[1:2]) & 63, taps_y) for i in range(4)
        ]
        both = jnp.concatenate(blocks, axis=0)
        stencil[source] = both
        return total + dot3(split(both * rows[6:7]), (high, low), NT)

    lines = lax.fori_loop(0, 4, spread, jnp.zeros((128, 256), f32))
    spectrum = dot3((bz_ref[0], bz_ref[1]), split(lines), NT)
    tx_b[...] = spectrum.astype(bf16).reshape(16, 16, 128)
    rx_b[me] = tx_b[me]

    def exchange(tx, rx, send, recv, peer, count, mine):
        def start(r, c):
            other, where = peer(r)
            pltpu.make_async_remote_copy(
                src_ref=tx.at[other],
                dst_ref=rx.at[mine],
                send_sem=send,
                recv_sem=recv,
                device_id=where,
                device_id_type=MESH,
            ).start()
            return c

        lax.fori_loop(1, count, start, 0)
        whole = pltpu.make_async_remote_copy(
            src_ref=tx.at[pl.ds(0, count - 1)],
            dst_ref=rx.at[pl.ds(0, count - 1)],
            send_sem=send,
            recv_sem=recv,
            device_id=peer(1)[1],
            device_id_type=MESH,
        )
        return whole.wait_recv, whole.wait_send

    arrive_b, drain_b = exchange(tx_b, rx_b, sb, rb, yz_peer, 16, me)

    for index in far_ids:
        for copy in halo_copies(index):
            copy.start()
    strip_lane = lax.broadcasted_iota(jnp.int32, (8, 128), 1)
    strip_cell = strip_lane // 8
    within = axis_sub * 8 + strip_lane % 8
    starts = jnp.where(strip_cell == 0, 0, jnp.where(strip_cell == 9, 0, lax.rem(strip_cell + 3, 4)))
    strip_at = jnp.where(axis_sub == 3, 127, jnp.minimum(starts * 24 + within, 127))
    strips = {}

    def lay_strips(sx):
        feat32[320 * sx : 320 * sx + 320, :] = feat_ext[sx].astype(f32).reshape(320, 128)
        for sy in range(4):
            table = jnp.zeros((8, 128), f32)
            for row, first, last in ((0, 0, 1), (1, 1, 5), (2, 5, 9), (3, 9, 10)):
                source = jnp.broadcast_to(pos_ext[sx, sy, row], (8, 128))
                moved = jnp.take_along_axis(source, strip_at, axis=1)
                table = jnp.where((strip_cell >= first) & (strip_cell < last), moved, table)
            strips[sx, sy] = table

    def lay_column(n):
        near = [strips[n // 2 + d // 3, n % 2 + d % 3] for d in range(9)]
        near += [near[4]] * 3
        for t in range(6):
            pos_tab[n, 8 * t : 8 * t + 8, :] = jnp.where(half_sub == 0, near[2 * t], near[2 * t + 1])

    for copy in halo_group(0):
        copy.wait_recv()
    for sx in (1, 2, 3):
        lay_strips(sx)
    for n in (2, 3):
        lay_column(n)
    half_columns(CUTS[0], CUTS[1])
    arrive_b()
    flat_b[...] = rx_b[...].astype(f32).reshape(256, 128)
    columns = []
    for group in range(4):
        pieces = [flat_b[pl.ds(group * 4 + k, 16, 16), :] for k in range(4)]
        columns.append(jnp.concatenate([swap_groups(pieces, i) for i in range(4)], axis=0))
    lines_y = jnp.concatenate(columns, axis=1)
    lines_y = lines_y.astype(bf16)
    modes_y = jnp.dot(by_ref[0, 0], lines_y, preferred_element_type=f32)
    modes_y = modes_y + jnp.dot(by_ref[0, 1], lines_y, preferred_element_type=f32)
    tx_c[...] = modes_y.reshape(8, 8, 512)
    rx_c[ix] = tx_c[ix]
    arrive_c, drain_c = exchange(tx_c, rx_c, sc, rc, x_peer, 8, ix)

    gain_z = gz_ref[0, pl.ds(pl.multiple_of(me * 16, 16), 16), :]
    square_z = gz_ref[1, pl.ds(pl.multiple_of(me * 16, 16), 16), :]
    gain_y = gy_ref[0, pl.ds(pl.multiple_of(ix * 8, 8), 8), :]
    square_y = gy_ref[1, pl.ds(pl.multiple_of(ix * 8, 8), 8), :]
    gain_yz = (gain_z[:, None, :] * gain_y[None, :, :]).reshape(128, 128)
    square_yz = (square_z[:, None, :] + square_y[None, :, :]).reshape(128, 128)
    greens = []
    for h in range(2):
        lanes = slice(128 * h, 128 * h + 128)
        total = square_yz + gx_ref[1, 0:1, lanes]
        value = gain_yz * gx_ref[0, 0:1, lanes] / (total + 1.0 / 1024.0)
        greens.append(jnp.where(total == 0.0, 0.0, value))
    green = jnp.concatenate(greens, axis=1)
    for copy in halo_group(1):
        copy.wait_recv()
    for sx in (0, 4):
        lay_strips(sx)
    for n in (0, 1, 4, 5):
        lay_column(n)
    half_columns(CUTS[1], CUTS[2])

    arrive_c()
    rows_x = []
    for group in range(4):
        for k in range(4):
            halves = [
                swap_groups(
                    [rx_c[4 * h + g, :, group * 128 : group * 128 + 128] for g in range(4)], k
                )
                for h in range(2)
            ]
            rows_x.append(jnp.concatenate(halves, axis=1))
    lines_x = jnp.concatenate(rows_x, axis=0)
    basis_x = (bx_ref[0], bx_ref[1])
    filtered = dot3(split(lines_x), basis_x, NT) * green
    back_x = dot3(split(filtered), basis_x)
    for g in range(8):
        half = g // 4
        for group in range(4):
            pieces = [
                back_x[(group * 4 + k) * 8 : (group * 4 + k) * 8 + 8, half * 128 : half * 128 + 128]
                for k in range(4)
            ]
            tx_c2[g, :, group * 128 : group * 128 + 128] = swap_groups(pieces, g % 4)
    rx_c2[ix] = tx_c2[ix]
    arrive_c2, drain_c2 = exchange(tx_c2, rx_c2, sc2, rc2, x_peer, 8, ix)
    half_columns(CUTS[2], CUTS[3])
    arrive_c2()
    back_y = dot3((by_ref[1, 0], by_ref[1, 1]), split(rx_c2[...].reshape(64, 512)))
    for group in range(4):
        pieces = [back_y[16 * i : 16 * i + 16, group * 128 : group * 128 + 128] for i in range(4)]
        for k in range(4):
            flat_b[pl.ds(group * 4 + k, 16, 16), :] = swap_groups(pieces, k)
    tx_b2[...] = flat_b[...].astype(bf16).reshape(16, 16, 128)
    rx_b2[me] = tx_b2[me]
    arrive_b2, drain_b2 = exchange(tx_b2, rx_b2, sb2, rb2, yz_peer, 16, me)
    half_columns(CUTS[3], CUTS[4])
    arrive_b2()
    back_z = rx_b2[...].astype(f32).reshape(256, 128).T.astype(bf16)
    lines_z = jnp.dot(back_z, bz_ref[0], preferred_element_type=f32)
    potential = split(lines_z + jnp.dot(back_z, bz_ref[1], preferred_element_type=f32))

    sampled = [dot3(potential, (z_high[n], z_low[n])) for n in range(4)]
    for n in range(4):
        total = jnp.sum(sampled[n] * stencil[n], axis=0, keepdims=True)
        parts[2 * n] = total[:, 0:256]
        tail = jnp.broadcast_to(total[:, 128:384], (8, 256))
        parts[2 * n + 1] = pltpu.roll(tail, 192, 1)[0:1]

    def part_copy(s, u):
        return pltpu.make_async_remote_copy(
            src_ref=parts.at[2 * s + u],
            dst_ref=rx_parts.at[from_half[u], iz],
            send_sem=sp.at[s, u],
            recv_sem=rp.at[from_half[u], iz],
            device_id=(ix, from_y[u], s),
            device_id_type=MESH,
        )

    for s in range(4):
        for u in range(2):

            @pl.when((s != iz) | (from_y[u] != iy))
            def _():
                part_copy(s, u).start()

            @pl.when((s == iz) & (from_y[u] == iy))
            def _():
                rx_parts[from_half[u], iz] = parts[2 * s + u]

    half_columns(CUTS[4], 12)
    wv = wv_ref[...]
    invariant = jnp.zeros((384, 128), f32)
    for d in range(3):
        t = sums[1 + d]
        hi = t.astype(bf16)
        lo = (t - hi.astype(f32)).astype(bf16)
        vec = jnp.dot(hi, wv, preferred_element_type=f32) + jnp.dot(
            lo, wv, preferred_element_type=f32
        )
        invariant = invariant + vec * vec
    update = (sums[0] * (1.0 / 64.0) + invariant * (1.0 / 64.0)).astype(bf16)
    out_ref[...] = (
        feat_ref[...].astype(f32).reshape(384, 128) + jnp.dot(update, wo_ref[...], preferred_element_type=f32)
    ).astype(bf16)

    for half, to_z, step_y, place in routes:
        if step_y:
            atom_copy(half, to_z, step_y, place).wait_send()
        else:

            @pl.when(iz != to_z)
            def _():
                atom_copy(half, to_z, step_y, place).wait_send()

    drain_b()
    drain_c()
    drain_c2()
    drain_b2()
    for group in range(2):
        for copy in halo_group(group):
            copy.wait_send()

    def part_wait(half, to_z, step_y):
        pltpu.make_async_remote_copy(
            src_ref=parts.at[0],
            dst_ref=rx_parts.at[half, to_z],
            send_sem=sp.at[0, 0],
            recv_sem=rp.at[half, to_z],
            device_id=(ix, lax.rem(iy + step_y, 4), to_z),
            device_id_type=MESH,
        ).wait_recv()

    for half, to_z, step_y, place in routes:
        if step_y:
            part_wait(half, to_z, step_y)
        else:

            @pl.when(iz != to_z)
            def _():
                part_wait(half, to_z, step_y)

    for half in range(2):
        site = (rx_parts[half, 0] + rx_parts[half, 1]) + (rx_parts[half, 2] + rx_parts[half, 3])
        for cx in range(3):
            block = site[:, 0:128] if cx < 2 else site[:, 128:256]
            block = jnp.broadcast_to(block, (8, 128))
            at = sub_l * 8 + lane_l % 8 + 64 * (cx % 2)
            site_ref[cx, half] = jnp.take_along_axis(block, at, axis=1)[:, 0:8]

    for s in range(4):
        for u in range(2):

            @pl.when((s != iz) | (from_y[u] != iy))
            def _():
                part_copy(s, u).wait_send()


def layer(operands):
    f32, bf16 = jnp.float32, jnp.bfloat16
    vm = pl.BlockSpec(memory_space=pltpu.VMEM)
    dma = pltpu.SemaphoreType.DMA
    tables = [jnp.asarray(t) for t in ewald_tables()]
    hbm = pl.BlockSpec(memory_space=pltpu.HBM)
    specs = [hbm] * 22
    shapes = [operands[n] for n in (0, 1, 2, 3, 14, 6, 7, 8, 10, 11, 4, 5)] + tables
    shapes += [operands[n] for n in (12, 13)]
    staged = [pltpu.VMEM(x.shape, x.dtype) for x in shapes]
    return pl.pallas_call(
        layer_kernel,
        out_shape=(
            jax.ShapeDtypeStruct((384, 128), bf16),
            jax.ShapeDtypeStruct((3, 2, 8, 8), f32),
        ),
        in_specs=specs,
        out_specs=(vm, vm),
        scratch_shapes=staged
        + [
            pltpu.SMEM((2,), f32),
            pltpu.SMEM((8,), f32),
            dma((20,)),
            dma((2,)),
            pltpu.VMEM((3, 2, 4, 1, 128), f32),
            pltpu.VMEM((5, 4, 10, 8, 128), bf16),
            pltpu.VMEM((5, 4, 4, 1, 128), f32),
            pltpu.VMEM((6, 48, 128), f32),
            pltpu.VMEM((1600, 128), f32),
            pltpu.VMEM((128, 256), bf16),
            pltpu.VMEM((128, 128), bf16),
            pltpu.VMEM((128, 128), bf16),
            pltpu.VMEM((8, 512), jnp.int32),
            pltpu.VMEM((8, 512), jnp.int32),
            pltpu.VMEM((8, 512), f32),
            pltpu.VMEM((4, 384, 128), f32),
            pltpu.VMEM((2, 8, 256), f32),
            pltpu.VMEM((4, 2, 8, 256), f32),
            pltpu.VMEM((4, 256, 384), bf16),
            pltpu.VMEM((4, 256, 384), bf16),
            pltpu.VMEM((4, 128, 384), f32),
            pltpu.VMEM((16, 16, 128), bf16),
            pltpu.VMEM((16, 16, 128), bf16),
            pltpu.VMEM((8, 8, 512), f32),
            pltpu.VMEM((8, 8, 512), f32),
            pltpu.VMEM((8, 8, 512), f32),
            pltpu.VMEM((8, 8, 512), f32),
            pltpu.VMEM((16, 16, 128), bf16),
            pltpu.VMEM((16, 16, 128), bf16),
            pltpu.VMEM((256, 128), f32),
            pltpu.VMEM((8, 1, 256), f32),
            pltpu.VMEM((2, 4, 1, 256), f32),
            dma((2, 4)),
            dma((4, 2)),
            *[pltpu.SemaphoreType.DMA] * 8,
            dma((4, 2)),
            dma((2, 4)),
            dma((2,)),
            dma((2,)),
            dma((2,)),
            dma((2,)),
        ],
        compiler_params=pltpu.CompilerParams(
            collective_id=0, has_side_effects=True, vmem_limit_bytes=48 * 1024 * 1024
        ),
        cost_estimate=pl.CostEstimate(flops=4 * 10**9, bytes_accessed=4 * 10**6, transcendentals=10**7),
        name="layer",
    )(*[pltpu.with_memory_space_constraint(x, pltpu.HBM) for x in (*operands, *tables)])


def shards(
    features,
    positions,
    grid_anchor,
    species,
    neighbours,
    neighbour_count,
    w_self,
    w_neighbour,
    w_radial,
    radial_rates,
    w_pair1,
    w_pair2,
    w_vector,
    w_out,
    w_charge,
    species_charge,
):
    updated, site_potential = layer(
        (
            features,
            positions,
            grid_anchor,
            species,
            neighbours,
            neighbour_count,
            w_neighbour,
            w_self,
            w_radial,
            radial_rates,
            w_pair1,
            w_pair2,
            w_vector,
            w_out,
            w_charge.reshape(1, 128),
            species_charge,
        )
    )
    return (updated.reshape(features.shape), site_potential)


def solution(mesh):
    return jax.shard_map(
        shards,
        mesh=mesh,
        in_specs=(
            P("gx", "gy", "gz", None, None),
            P("gx", "gy", "gz", None),
            P("gx", "gy", "gz", None),
            P("gx", "gy", "gz", None),
            P("gx", "gy", "gz", None),
            P("gx", "gy", "gz", None),
            P(),
            P(),
            P(),
            P(),
            P(),
            P(),
            P(),
            P(),
            P(),
            P(),
        ),
        out_specs=(P("gx", "gy", "gz", None, None), P("gx", "gy", "gz", None)),
        check_vma=False,
    )
```

```python
import jax
import jax.numpy as jnp
import numpy as np
from jax import lax
from jax.experimental import pallas as pl
from jax.experimental.pallas import tpu as pltpu
from jax.sharding import PartitionSpec as P


coulomb_scale = 0.25
smearing = 1.0


NT = (((1,), (1,)), ((), ()))
CUTS = (0, 4, 6, 8, 11)


def real_basis(length):
    modes = np.arange(length)[:, None]
    cells = np.arange(length)[None, :]
    turns = 2.0 * np.pi * ((modes * cells) % length) / length
    flipped = 2.0 * np.pi * (((length - modes) * cells) % length) / length
    return np.where(modes <= length // 2, np.cos(turns), np.sin(flipped))


def two_parts(table):
    table = np.asarray(table, np.float32)
    high = table.astype(jnp.bfloat16)
    low = (table - high.astype(np.float32)).astype(jnp.bfloat16)
    return np.stack([high, low])


def mode_tables(length):
    modes = np.arange(length)
    signed = np.where(modes > length // 2, modes - length, modes)
    wave = signed * (2.0 * np.pi / length)
    modulus = ((4.0 + 2.0 * np.cos(2.0 * np.pi * modes / length)) / 6.0) ** 2
    weight = np.where((modes == 0) | (modes == length // 2), 1.0, 2.0) / length
    return np.exp(-0.5 * smearing * smearing * wave * wave) / modulus * weight, wave * wave


def ewald_tables():
    basis_z = two_parts(real_basis(256))
    order_y = np.array([4 * p + i for i in range(4) for p in range(16)])
    forward_y = real_basis(64)[:, order_y]
    basis_y = np.stack([two_parts(forward_y), two_parts(forward_y.T)])
    wide = np.zeros((256, 256))
    full_x = real_basis(192)
    for g in range(8):
        wide[:192, 32 * g : 32 * g + 27] = full_x[:, (24 * g - 1 + np.arange(27)) % 192]
    basis_x = two_parts(wide)
    green_x = np.zeros((2, 8, 256))
    gain, square = mode_tables(192)
    green_x[0, :, :192] = gain * (coulomb_scale * 4.0 * np.pi)
    green_x[1, :, :192] = square
    green_x[1, :, 192:] = 1.0
    green_y = np.repeat(np.stack(mode_tables(64))[:, :, None], 128, 2)
    green_z = np.repeat(np.stack(mode_tables(256))[:, :, None], 128, 2)
    return (
        basis_z,
        basis_y,
        basis_x,
        green_x.astype(np.float32),
        green_y.astype(np.float32),
        green_z.astype(np.float32),
    )


def split(value):
    high = value.astype(jnp.bfloat16)
    return high, (value - high.astype(jnp.float32)).astype(jnp.bfloat16)


def dot3(a, b, dims=(((1,), (0,)), ((), ()))):
    def one(u, v):
        return lax.dot_general(u, v, dims, preferred_element_type=jnp.float32)

    rows = a[0].shape[0]
    both = one(jnp.concatenate([a[0], a[1]], axis=0), b[0])
    return both[0:rows] + (one(a[0], b[1]) + both[rows : 2 * rows])


def swap_groups(pieces, shift):
    lane = lax.broadcasted_iota(jnp.int32, pieces[0].shape, 1) // 32
    out = None
    for k, piece in enumerate(pieces):
        moved = pltpu.roll(piece, (32 * (k - shift)) % 128, 1) if k != shift else piece
        out = moved if out is None else jnp.where(lane == k, moved, out)
    return out


def tap_rows(fraction):
    square = fraction * fraction
    cube = square * fraction
    remain = 1.0 - fraction
    return (
        remain * remain * remain / 6.0,
        (3.0 * cube - 6.0 * square + 4.0) / 6.0,
        (-3.0 * cube + 3.0 * square + 3.0 * fraction + 1.0) / 6.0,
        cube / 6.0,
    )


def pick_taps(offset, taps):
    out = jnp.zeros(offset.shape, jnp.float32)
    for t in range(4):
        out = jnp.where(offset == t, taps[t], out)
    return out


def layer_kernel(
    feat_hbm,
    place_hbm,
    anchor_hbm,
    species_hbm,
    nbr_hbm,
    count_hbm,
    wn_hbm,
    ws_hbm,
    wr_hbm,
    rate_hbm,
    w1_hbm,
    w2_hbm,
    wv_hbm,
    wo_hbm,
    wc_hbm,
    kind_hbm,
    bz_hbm,
    by_hbm,
    bx_hbm,
    gx_hbm,
    gy_hbm,
    gz_hbm,
    out_ref,
    site_ref,
    feat_ref,
    place_ref,
    anchor_ref,
    species_ref,
    wc_ref,
    wn_ref,
    ws_ref,
    wr_ref,
    w1_ref,
    w2_ref,
    nbr_ref,
    count_ref,
    bz_ref,
    by_ref,
    bx_ref,
    gx_ref,
    gy_ref,
    gz_ref,
    wv_ref,
    wo_ref,
    kind_ref,
    rate_ref,
    load_sem,
    small_sem,
    pos_ref,
    feat_ext,
    pos_ext,
    pos_tab,
    feat32,
    first_w,
    pair1_w,
    pair2_w,
    hot_row,
    lane_row,
    live_row,
    sums,
    tx_atoms,
    rx_atoms,
    z_high,
    z_low,
    stencil,
    tx_b,
    rx_b,
    tx_c,
    rx_c,
    tx_c2,
    rx_c2,
    tx_b2,
    rx_b2,
    flat_b,
    flat_c,
    parts,
    rx_parts,
    sa,
    ra,
    sb,
    rb,
    sc,
    rc,
    sc2,
    rc2,
    sb2,
    rb2,
    sp,
    rp,
    sf,
    rf,
    sq,
    rq,
):
    bf16 = jnp.bfloat16
    f32 = jnp.float32
    MESH = pl.DeviceIdType.MESH
    ix, iy, iz = lax.axis_index("gx"), lax.axis_index("gy"), lax.axis_index("gz")
    me = iy * 4 + iz
    barrier = pltpu.get_barrier_semaphore()
    pairs = (
        (feat_hbm, feat_ref),
        (place_hbm, place_ref),
        (anchor_hbm, anchor_ref),
        (species_hbm, species_ref),
        (wc_hbm, wc_ref),
        (wn_hbm, wn_ref),
        (ws_hbm, ws_ref),
        (wr_hbm, wr_ref),
        (w1_hbm, w1_ref),
        (w2_hbm, w2_ref),
        (nbr_hbm, nbr_ref),
        (count_hbm, count_ref),
        (bz_hbm, bz_ref),
        (by_hbm, by_ref),
        (bx_hbm, bx_ref),
        (gx_hbm, gx_ref),
        (gy_hbm, gy_ref),
        (gz_hbm, gz_ref),
        (wv_hbm, wv_ref),
        (wo_hbm, wo_ref),
    )
    loads = [
        pltpu.make_async_copy(src, dst, load_sem.at[n]) for n, (src, dst) in enumerate(pairs)
    ]
    small = [
        pltpu.make_async_copy(kind_hbm, kind_ref, small_sem.at[0]),
        pltpu.make_async_copy(rate_hbm, rate_ref, small_sem.at[1]),
    ]
    for load in loads[:5] + small[:1]:
        load.start()

    def yz_peer(r):
        other = lax.rem(me + r, 16)
        return other, (ix, other // 4, lax.rem(other, 4))

    def x_peer(r):
        other = lax.rem(ix + r, 8)
        return other, (other, iy, iz)

    def greet_yz(r, c):
        pl.semaphore_signal(barrier, inc=1, device_id=yz_peer(r)[1], device_id_type=MESH)
        return c

    def greet_x(r, c):
        pl.semaphore_signal(barrier, inc=1, device_id=x_peer(r)[1], device_id_type=MESH)
        return c

    lax.fori_loop(1, 16, greet_yz, 0)
    lax.fori_loop(1, 8, greet_x, 0)

    def halo_peer(index):
        ox, oy, oz = index // 9 - 1, index // 3 % 3 - 1, index % 3 - 1
        return (lax.rem(ix + ox + 8, 8), lax.rem(iy + oy + 4, 4), lax.rem(iz + oz + 4, 4))

    def halo_span(step, cells):
        if step == 0:
            return pl.ds(0, cells), pl.ds(1, cells)
        return (pl.ds(cells - 1, 1), pl.ds(0, 1)) if step > 0 else (pl.ds(0, 1), pl.ds(cells + 1, 1))

    halo_ids = [n for n in range(27) if n != 13]
    near_ids = [n for n in halo_ids if n // 9 == 1]
    far_ids = [n for n in halo_ids if n // 9 != 1]

    def halo_copies(index):
        steps = (index // 9 - 1, index // 3 % 3 - 1, index % 3 - 1)
        spans = [halo_span(step, cells) for step, cells in zip(steps, (3, 2, 8))]
        group = 0 if steps[0] == 0 else 1
        source = tuple(span[0] for span in spans)
        target = tuple(span[1] for span in spans)
        row = {0: pl.ds(1, 2), 1: pl.ds(0, 1), -1: pl.ds(3, 1)}[steps[2]]
        return [
            pltpu.make_async_remote_copy(
                src_ref=src.at[source[:2] + (from_z,)],
                dst_ref=dst.at[target[:2] + (to_z,)],
                send_sem=send.at[group],
                recv_sem=recv.at[group],
                device_id=halo_peer(index),
                device_id_type=MESH,
            )
            for src, dst, send, recv, from_z, to_z in (
                (feat_ref, feat_ext, sf, rf, source[2], target[2]),
                (pos_ref, pos_ext, sq, rq, row, row),
            )
        ]

    def halo_group(group):
        cells = (pl.ds(0, 2 if group else 3), pl.ds(0, 4), pl.ds(0, 10 if group else 6))
        rows = (pl.ds(0, 2 if group else 3), pl.ds(0, 4), pl.ds(0, 4 if group else 3))
        return [
            pltpu.make_async_remote_copy(
                src_ref=ext.at[part],
                dst_ref=ext.at[part],
                send_sem=send.at[group],
                recv_sem=recv.at[group],
                device_id=halo_peer(0),
                device_id_type=MESH,
            )
            for ext, part, send, recv in ((feat_ext, cells, sf, rf), (pos_ext, rows, sq, rq))
        ]

    for index in far_ids:
        if index % 9 != 4:
            pl.semaphore_signal(
                barrier, inc=1, device_id=halo_peer(index), device_id_type=MESH
            )

    for load in loads[:5] + small[:1]:
        load.wait()

    sub_l = lax.broadcasted_iota(jnp.int32, (8, 128), 0)
    lane_l = lax.broadcasted_iota(jnp.int32, (8, 128), 1)
    for half in range(2):
        own_rows = feat_ref[:, half].astype(f32).reshape(192, 128).astype(bf16)
        weights = jnp.broadcast_to(wc_ref[...].astype(f32), (16, 128)).astype(bf16)
        readout = lax.dot_general(weights, own_rows, NT, preferred_element_type=f32)[0:8]
        laid = []
        for cx in range(3):
            place = place_ref[cx, half]
            for row, cells in ((0, (7,)), (1, (0, 1, 2, 3)), (2, (4, 5, 6, 7)), (3, (0,))):
                pieces = [place[cz : cz + 1] for cz in cells]
                pieces.append(jnp.zeros((1, 128 - 24 * len(cells)), f32))
                pos_ref[cx, half, row] = jnp.concatenate(pieces, axis=1)
            source = jnp.concatenate(
                [
                    place,
                    anchor_ref[cx, half].astype(f32),
                    species_ref[cx, half].astype(f32),
                    jnp.zeros((8, 72), f32),
                ],
                axis=1,
            )
            rows = jnp.zeros((8, 128), f32)
            for cz in range(8):
                row = jnp.broadcast_to(source[cz : cz + 1], (8, 128))
                moved = jnp.take_along_axis(row, sub_l * 8 + lane_l % 8, axis=1)
                rows = jnp.where(lane_l // 8 == cz, moved, rows)
            laid.append(rows)
        rows = jnp.concatenate(
            [jnp.where(lane_l < 64, laid[0], pltpu.roll(laid[1], 64, 1)), laid[2]], axis=1
        )
        kinds = rows[6:7]
        base = jnp.where(kinds == 0.0, kind_ref[0], jnp.where(kinds == 1.0, kind_ref[1], 0.0))
        total = jnp.concatenate(
            [base[:, 0:192] + readout[0:1, :], jnp.zeros((1, 64), f32)], axis=1
        )
        tx_atoms[half, 0:3, :] = rows[0:3] - (rows[3:6] + 1.0)
        tx_atoms[half, 3:6, :] = rows[3:6]
        tx_atoms[half, 6:7, :] = total
        tx_atoms[half, 7:8, :] = jnp.zeros((1, 256), f32)

    pl.semaphore_wait(barrier, 38)

    routes = [(0, 3, 3, 1), (0, 0, 0, 1), (0, 1, 0, 0), (0, 2, 0, 0)]
    routes += [(1, 1, 0, 1), (1, 2, 0, 1), (1, 3, 0, 0), (1, 0, 1, 0)]

    def atom_copy(half, to_z, step_y, place):
        return pltpu.make_async_remote_copy(
            src_ref=tx_atoms.at[half],
            dst_ref=rx_atoms.at[iz * 2 + place],
            send_sem=sa,
            recv_sem=ra.at[iz, place],
            device_id=(ix, lax.rem(iy + step_y, 4), to_z),
            device_id_type=MESH,
        )

    for half, to_z, step_y, place in routes:
        if step_y:
            atom_copy(half, to_z, step_y, place).start()
        else:

            @pl.when(iz != to_z)
            def _():
                atom_copy(half, to_z, step_y, place).start()

            @pl.when(iz == to_z)
            def _():
                rx_atoms[iz * 2 + place] = tx_atoms[half]

    for index in near_ids:
        for copy in halo_copies(index):
            copy.start()
    for load in loads[5:] + small[1:]:
        load.start()
    feat_ext[1:4, 1:3, 1:9] = feat_ref[...]
    pos_ext[1:4, 1:3, 1:3] = pos_ref[:, :, 1:3]
    for load in loads[5:] + small[1:]:
        load.wait()
    first_w[:, 0:128] = (wn_ref[...].astype(f32) * 0.5).T.astype(bf16)
    first_w[:, 128:256] = (ws_ref[...].astype(f32) * 0.5).T.astype(bf16)
    pair1_w[...] = (w1_ref[...].astype(f32) * 0.5).T.astype(bf16)
    pair2_w[...] = (w2_ref[...].astype(f32) * 0.5).T.astype(bf16)
    radial_pad = jnp.concatenate(
        [jnp.zeros((88, 128), f32), wr_ref[...].astype(f32) * 0.5, jnp.zeros((32, 128), f32)], axis=0
    ).T
    cell_x0, cell_y0, cell_z0 = ix * 3, iy * 2, iz * 8

    sub8 = lax.broadcasted_iota(jnp.int32, (8, 512), 0)
    lane8 = lax.broadcasted_iota(jnp.int32, (8, 512), 1)
    rates = jnp.zeros((8, 512), f32)
    for k in range(8):
        rates = jnp.where(sub8 == k, rate_ref[k], rates)
    own_mask = (lane8 // 64) == sub8
    own_hot = jnp.where(own_mask, 1.0, 0.0).astype(f32)
    own_hot32 = jnp.concatenate([own_hot, own_hot, jnp.zeros((16, 512), f32)], axis=0).astype(bf16)
    lane_t = lax.broadcasted_iota(jnp.int32, (128, 128), 1)
    low_part = (lane_t >= 104) & (lane_t < 112)
    half_sub = sub_l // 4
    axis_sub = sub_l % 4
    box = jnp.where(axis_sub == 0, 192.0, jnp.where(axis_sub == 1, 64.0, 256.0)).astype(f32)
    box_inv = 1.0 / box
    atom_lane = lax.broadcasted_iota(jnp.int32, (8, 128), 1) // 64
    def half_column(index, carry):
        later = (index - 4) // 2
        col = jnp.where(index < 4, 2 + index // 2, jnp.where(later < 2, later, later + 2))
        cx = col // 2
        cy = lax.rem(col, 2)
        ids = nbr_ref[cx, cy]
        slot = ids & 7
        z = (ids >> 3) & 31
        y = (ids >> 8) & 7
        x = ids >> 11
        dz = (z - (cell_z0 + sub8) + 1) & 31
        dy = (y - (cell_y0 + cy) + 1) & 7
        dx = x - (cell_x0 + cx) + 1
        dx = jnp.where(dx < 0, dx + 24, dx)
        dx = jnp.where(dx >= 24, dx - 24, dx)
        strip = dx * 3 + dy
        hot_row[...] = strip * 24 + dz * 8 + slot
        lane_row[...] = ((dz + sub8) * 8 + slot) * 16 + strip
        counts = jnp.concatenate([count_ref[cx, cy], jnp.zeros((8, 120), jnp.int32)], axis=1)
        pieces = []
        for g in range(4):
            owner = atom_lane + 2 * g
            count_g = jnp.take_along_axis(counts, owner, axis=1)
            slot_g = lax.broadcasted_iota(jnp.int32, (8, 128), 1) % 64
            pieces.append(jnp.where(slot_g < count_g, 1.0, 0.0).astype(f32))
        live_row[...] = jnp.concatenate(pieces, axis=1)

        def cell(cz):
            rows = []
            for dx_ in range(3):
                for dy_ in range(3):
                    base = ((cx + dx_) * 4 + cy + dy_) * 80 + cz * 8
                    rows.append(feat32[pl.ds(pl.multiple_of(base, 8), 24), :])
            own_base = ((cx + 1) * 4 + cy + 1) * 80 + cz * 8 + 8
            own = feat32[pl.ds(pl.multiple_of(own_base, 8), 8), :]
            left = jnp.concatenate(rows + [jnp.zeros((40, 128), f32)], axis=0)
            right = jnp.concatenate(
                [jnp.zeros((224, 128), f32), own, own, jnp.zeros((16, 128), f32)], axis=0
            )
            table = jnp.concatenate([left, right], axis=1).astype(bf16)
            proj = lax.dot_general(first_w[...], table, NT, preferred_element_type=f32)
            tail = proj[:, 128:256]
            tail_hi = tail.astype(bf16).astype(f32)
            tail = jnp.where(low_part, tail - tail_hi, tail_hi) + radial_pad
            lhs = jnp.concatenate([proj[:, 0:128].astype(bf16), tail.astype(bf16)], axis=1)

            place = []
            hot = hot_row[pl.ds(cz, 1), :]
            packed = lane_row[pl.ds(cz, 1), :]
            live = live_row[pl.ds(cz, 1), :]
            for g in range(4):
                packed_g = jnp.broadcast_to(packed[:, g * 128 : g * 128 + 128], (8, 128))
                where_g = packed_g >> 4
                strip_g = packed_g & 15
                got = jnp.zeros((8, 128), f32)
                for t in range(5):
                    hit = strip_g == (2 * t + half_sub)
                    got = jnp.where(
                        hit,
                        jnp.take_along_axis(pos_tab[col, t * 8 : t * 8 + 8, :], where_g, axis=1),
                        got,
                    )
                got = got + pltpu.roll(got, 4, 0)
                mine = jnp.take_along_axis(
                    pos_tab[col, 40:48, :], atom_lane + 2 * g + (cz + 1) * 8, axis=1
                )
                gap = got - mine
                gap = gap - box * jnp.floor(gap * box_inv + 0.5)
                place.append(gap * 0.125)
            scaled = jnp.concatenate(place, axis=1)
            square = scaled * scaled
            square = square[0:1] + square[1:2] + square[2:3]
            basis = jnp.exp(-jnp.broadcast_to(square, (8, 512)) * rates)
            cell_iota = lax.broadcasted_iota(jnp.int32, (216, 512), 0)
            hots = jnp.where(cell_iota == hot, 1.0, 0.0).astype(f32)
            rhs = jnp.concatenate(
                [jnp.concatenate([hots, basis], axis=0).astype(bf16), own_hot32], axis=0
            )
            half = jnp.dot(lhs, rhs, preferred_element_type=f32)
            yield
            latent = (half + half * jnp.tanh(half)).astype(bf16)
            half = jnp.dot(pair1_w[...], latent, preferred_element_type=f32)
            yield
            second = (half + half * jnp.tanh(half)).astype(bf16)
            half = jnp.dot(pair2_w[...], second, preferred_element_type=f32)
            yield
            third = (half + half * jnp.tanh(half)).astype(bf16)

            weighted = scaled * live
            w_hi = weighted.astype(bf16).astype(f32)
            w_lo = weighted - w_hi
            parts = [live]
            for d in range(3):
                parts += [w_hi[d : d + 1], w_lo[d : d + 1]]
            spread = jnp.concatenate(
                [jnp.where(own_mask, jnp.broadcast_to(p, (8, 512)), 0.0) for p in parts]
                + [jnp.zeros((8, 512), f32)],
                axis=0,
            ).astype(bf16)
            total = lax.dot_general(spread, third, NT, preferred_element_type=f32)
            yield
            at = pl.multiple_of((col * 8 + cz) * 8, 8)
            sums[0, pl.ds(at, 8), :] = total[0:8]
            for d in range(3):
                sums[1 + d, pl.ds(at, 8), :] = (
                    total[8 + 16 * d : 16 + 16 * d] + total[16 + 16 * d : 24 + 16 * d]
                )

        running = [cell(lax.rem(index, 2) * 4 + u) for u in range(4)]
        while running:
            running = [one for one in running if next(one, 1) is None]
        return carry

    def half_columns(first, last):
        lax.fori_loop(first, last, half_column, 0)

    from_y = [
        lax.rem(iy + jnp.where(iz == 0, 3, 0), 4),
        lax.rem(iy + jnp.where(iz == 3, 1, 0), 4),
    ]
    edge = jnp.where((iz == 0) | (iz == 3), 1, 0)
    from_half = [edge, 1 - edge]

    def atom_wait(s, u):
        @pl.when((s != iz) | (from_y[u] != iy))
        def _():
            pltpu.make_async_remote_copy(
                src_ref=tx_atoms.at[0],
                dst_ref=rx_atoms.at[s * 2 + u],
                send_sem=sa,
                recv_sem=ra.at[s, u],
                device_id=(ix, from_y[u], s),
                device_id_type=MESH,
            ).wait_recv()

    y_first = iy * 16 + iz * 4

    z_ids = lax.broadcasted_iota(jnp.int32, (256, 384), 0)
    x_ids = lax.broadcasted_iota(jnp.int32, (32, 384), 0) + (ix * 24 - 1)
    lane_384 = lax.broadcasted_iota(jnp.int32, (8, 128), 1)

    def spread(source):
        low_part_, high_part_ = rx_atoms[source * 2], rx_atoms[source * 2 + 1]
        moved = pltpu.roll(high_part_, 64, 1)
        rows = jnp.concatenate(
            [
                low_part_[:, 0:128],
                jnp.where(lane_384 < 64, low_part_[:, 128:256], moved[:, 0:128]),
                moved[:, 128:256],
            ],
            axis=1,
        )
        anchor = rows[3:6].astype(jnp.int32)
        weights_z = pick_taps((z_ids - anchor[2:3]) & 255, tap_rows(rows[2:3]))
        high, low = split(weights_z)
        z_high[source] = high
        z_low[source] = low
        weights_x = pick_taps(x_ids - anchor[0:1], tap_rows(rows[0:1]))
        taps_y = tap_rows(rows[1:2])
        blocks = [
            weights_x * pick_taps((y_first + i - anchor[1:2]) & 63, taps_y) for i in range(4)
        ]
        both = jnp.concatenate(blocks, axis=0)
        stencil[source] = both
        return dot3(split(both * rows[6:7]), (high, low), NT)

    lines = None
    for steps in ((1, 3), (0, 2)):
        sources = [lax.rem(iz + step, 4) for step in steps]
        for source in sources:
            for u in range(2):
                atom_wait(source, u)
        for source in sources:
            part = spread(source)
            lines = part if lines is None else lines + part
    spectrum = dot3((bz_ref[0], bz_ref[1]), split(lines), NT)
    tx_b[...] = spectrum.reshape(16, 16, 128)
    rx_b[me] = tx_b[me]

    def exchange(tx, rx, send, recv, peer, count, mine):
        for r in range(1, count):
            other, where = peer(r)
            pltpu.make_async_remote_copy(
                src_ref=tx.at[other],
                dst_ref=rx.at[mine],
                send_sem=send,
                recv_sem=recv,
                device_id=where,
                device_id_type=MESH,
            ).start()
        whole = pltpu.make_async_remote_copy(
            src_ref=tx.at[pl.ds(0, count - 1)],
            dst_ref=rx.at[pl.ds(0, count - 1)],
            send_sem=send,
            recv_sem=recv,
            device_id=peer(1)[1],
            device_id_type=MESH,
        )
        return whole.wait_recv, whole.wait_send

    arrive_b, drain_b = exchange(tx_b, rx_b, sb, rb, yz_peer, 16, me)

    for index in far_ids:
        for copy in halo_copies(index):
            copy.start()
    strip_lane = lax.broadcasted_iota(jnp.int32, (8, 128), 1)
    strip_cell = strip_lane // 8
    within = axis_sub * 8 + strip_lane % 8
    starts = jnp.where(strip_cell == 0, 0, jnp.where(strip_cell == 9, 0, lax.rem(strip_cell + 3, 4)))
    strip_at = jnp.where(axis_sub == 3, 127, jnp.minimum(starts * 24 + within, 127))
    strips = {}

    def lay_strips(sx):
        feat32[320 * sx : 320 * sx + 320, :] = feat_ext[sx].astype(f32).reshape(320, 128)
        for sy in range(4):
            table = jnp.zeros((8, 128), f32)
            for row, first, last in ((0, 0, 1), (1, 1, 5), (2, 5, 9), (3, 9, 10)):
                source = jnp.broadcast_to(pos_ext[sx, sy, row], (8, 128))
                moved = jnp.take_along_axis(source, strip_at, axis=1)
                table = jnp.where((strip_cell >= first) & (strip_cell < last), moved, table)
            strips[sx, sy] = table

    def lay_column(n):
        near = [strips[n // 2 + d // 3, n % 2 + d % 3] for d in range(9)]
        near += [near[4]] * 3
        for t in range(6):
            pos_tab[n, 8 * t : 8 * t + 8, :] = jnp.where(half_sub == 0, near[2 * t], near[2 * t + 1])

    for copy in halo_group(0):
        copy.wait_recv()
    for sx in (1, 2, 3):
        lay_strips(sx)
    for n in (2, 3):
        lay_column(n)
    half_columns(CUTS[0], CUTS[1])
    arrive_b()
    rows_b = rx_b.reshape(256, 128)
    columns = []
    for group in range(4):
        pieces = [rows_b[pl.ds(group * 4 + k, 16, 16), :] for k in range(4)]
        columns.append(jnp.concatenate([swap_groups(pieces, i) for i in range(4)], axis=0))
    lines_y = jnp.concatenate(columns, axis=1)
    modes_y = dot3((by_ref[0, 0], by_ref[0, 1]), split(lines_y))
    tx_c[...] = modes_y.reshape(8, 8, 512)
    rx_c[ix] = tx_c[ix]
    arrive_c, drain_c = exchange(tx_c, rx_c, sc, rc, x_peer, 8, ix)

    gain_z = gz_ref[0, pl.ds(pl.multiple_of(me * 16, 16), 16), :]
    square_z = gz_ref[1, pl.ds(pl.multiple_of(me * 16, 16), 16), :]
    gain_y = gy_ref[0, pl.ds(pl.multiple_of(ix * 8, 8), 8), :]
    square_y = gy_ref[1, pl.ds(pl.multiple_of(ix * 8, 8), 8), :]
    gain_yz = (gain_z[:, None, :] * gain_y[None, :, :]).reshape(128, 128)
    square_yz = (square_z[:, None, :] + square_y[None, :, :]).reshape(128, 128)
    greens = []
    for h in range(2):
        lanes = slice(128 * h, 128 * h + 128)
        total = square_yz + gx_ref[1, 0:1, lanes]
        value = gain_yz * gx_ref[0, 0:1, lanes] / (total + 1.0 / 1024.0)
        greens.append(jnp.where(total == 0.0, 0.0, value))
    green = jnp.concatenate(greens, axis=1)
    for copy in halo_group(1):
        copy.wait_recv()
    for sx in (0, 4):
        lay_strips(sx)
    for n in (0, 1, 4, 5):
        lay_column(n)
    half_columns(CUTS[1], CUTS[2])

    arrive_c()
    rows_x = []
    for group in range(4):
        for k in range(4):
            halves = [
                swap_groups(
                    [rx_c[4 * h + g, :, group * 128 : group * 128 + 128] for g in range(4)], k
                )
                for h in range(2)
            ]
            rows_x.append(jnp.concatenate(halves, axis=1))
    lines_x = jnp.concatenate(rows_x, axis=0)
    basis_x = (bx_ref[0], bx_ref[1])
    filtered = dot3(split(lines_x), basis_x, NT) * green
    back_x = dot3(split(filtered), basis_x)
    for g in range(8):
        half = g // 4
        for group in range(4):
            pieces = [
                back_x[(group * 4 + k) * 8 : (group * 4 + k) * 8 + 8, half * 128 : half * 128 + 128]
                for k in range(4)
            ]
            flat_c[g, :, group * 128 : group * 128 + 128] = swap_groups(pieces, g % 4)
    tx_c2[...] = flat_c[...].astype(bf16)
    rx_c2[ix] = tx_c2[ix]
    arrive_c2, drain_c2 = exchange(tx_c2, rx_c2, sc2, rc2, x_peer, 8, ix)
    half_columns(CUTS[2], CUTS[3])
    arrive_c2()
    lines_y2 = rx_c2[...].astype(f32).reshape(64, 512).astype(bf16)
    back_y = jnp.dot(by_ref[1, 0], lines_y2, preferred_element_type=f32)
    back_y = back_y + jnp.dot(by_ref[1, 1], lines_y2, preferred_element_type=f32)
    for group in range(4):
        pieces = [back_y[16 * i : 16 * i + 16, group * 128 : group * 128 + 128] for i in range(4)]
        for k in range(4):
            flat_b[pl.ds(group * 4 + k, 16, 16), :] = swap_groups(pieces, k)
    tx_b2[...] = flat_b[...].astype(bf16).reshape(16, 16, 128)
    rx_b2[me] = tx_b2[me]
    arrive_b2, drain_b2 = exchange(tx_b2, rx_b2, sb2, rb2, yz_peer, 16, me)
    half_columns(CUTS[3], CUTS[4])
    arrive_b2()
    back_z = rx_b2[...].astype(f32).reshape(256, 128).T.astype(bf16)
    lines_z = jnp.dot(back_z, bz_ref[0], preferred_element_type=f32)
    potential = split(lines_z + jnp.dot(back_z, bz_ref[1], preferred_element_type=f32))

    sampled = [dot3(potential, (z_high[n], z_low[n])) for n in range(4)]
    for n in range(4):
        total = jnp.sum(sampled[n] * stencil[n], axis=0, keepdims=True)
        parts[2 * n] = total[:, 0:256]
        tail = jnp.broadcast_to(total[:, 128:384], (8, 256))
        parts[2 * n + 1] = pltpu.roll(tail, 192, 1)[0:1]

    def part_copy(s, u):
        return pltpu.make_async_remote_copy(
            src_ref=parts.at[2 * s + u],
            dst_ref=rx_parts.at[from_half[u] * 4 + iz],
            send_sem=sp,
            recv_sem=rp,
            device_id=(ix, from_y[u], s),
            device_id_type=MESH,
        )

    for s in range(4):
        for u in range(2):

            @pl.when((s != iz) | (from_y[u] != iy))
            def _():
                part_copy(s, u).start()

            @pl.when((s == iz) & (from_y[u] == iy))
            def _():
                rx_parts[from_half[u] * 4 + iz] = parts[2 * s + u]

    half_columns(CUTS[4], 12)
    wv = wv_ref[...]
    invariant = jnp.zeros((384, 128), f32)
    for d in range(3):
        t = sums[1 + d]
        hi = t.astype(bf16)
        lo = (t - hi.astype(f32)).astype(bf16)
        vec = jnp.dot(hi, wv, preferred_element_type=f32) + jnp.dot(
            lo, wv, preferred_element_type=f32
        )
        invariant = invariant + vec * vec
    update = (sums[0] * (1.0 / 64.0) + invariant * (1.0 / 64.0)).astype(bf16)
    out_ref[...] = (
        feat_ref[...].astype(f32).reshape(384, 128) + jnp.dot(update, wo_ref[...], preferred_element_type=f32)
    ).astype(bf16)

    def bulk(ref, send, recv, arriving):
        for blocks, ends in ((7, 1), (6, 0)):

            @pl.when(edge == ends)
            def _():
                whole = pltpu.make_async_remote_copy(
                    src_ref=ref.at[pl.ds(0, blocks)],
                    dst_ref=ref.at[pl.ds(0, blocks)],
                    send_sem=send,
                    recv_sem=recv,
                    device_id=yz_peer(1)[1],
                    device_id_type=MESH,
                )
                if arriving:
                    whole.wait_recv()
                else:
                    whole.wait_send()

    bulk(rx_atoms, sa, ra.at[0, 0], False)
    drain_b()
    drain_c()
    drain_c2()
    drain_b2()
    for group in range(2):
        for copy in halo_group(group):
            copy.wait_send()

    bulk(rx_parts, sp, rp, True)

    for half in range(2):
        site = (rx_parts[half * 4] + rx_parts[half * 4 + 1]) + (
            rx_parts[half * 4 + 2] + rx_parts[half * 4 + 3]
        )
        for cx in range(3):
            block = site[:, 0:128] if cx < 2 else site[:, 128:256]
            block = jnp.broadcast_to(block, (8, 128))
            at = sub_l * 8 + lane_l % 8 + 64 * (cx % 2)
            site_ref[cx, half] = jnp.take_along_axis(block, at, axis=1)[:, 0:8]

    bulk(rx_parts, sp, rp, False)


def layer(operands):
    f32, bf16 = jnp.float32, jnp.bfloat16
    vm = pl.BlockSpec(memory_space=pltpu.VMEM)
    dma = pltpu.SemaphoreType.DMA
    tables = [jnp.asarray(t) for t in ewald_tables()]
    hbm = pl.BlockSpec(memory_space=pltpu.HBM)
    specs = [hbm] * 22
    shapes = [operands[n] for n in (0, 1, 2, 3, 14, 6, 7, 8, 10, 11, 4, 5)] + tables
    shapes += [operands[n] for n in (12, 13)]
    staged = [pltpu.VMEM(x.shape, x.dtype) for x in shapes]
    return pl.pallas_call(
        layer_kernel,
        out_shape=(
            jax.ShapeDtypeStruct((384, 128), bf16),
            jax.ShapeDtypeStruct((3, 2, 8, 8), f32),
        ),
        in_specs=specs,
        out_specs=(vm, vm),
        scratch_shapes=staged
        + [
            pltpu.SMEM((2,), f32),
            pltpu.SMEM((8,), f32),
            dma((20,)),
            dma((2,)),
            pltpu.VMEM((3, 2, 4, 1, 128), f32),
            pltpu.VMEM((5, 4, 10, 8, 128), bf16),
            pltpu.VMEM((5, 4, 4, 1, 128), f32),
            pltpu.VMEM((6, 48, 128), f32),
            pltpu.VMEM((1600, 128), f32),
            pltpu.VMEM((128, 256), bf16),
            pltpu.VMEM((128, 128), bf16),
            pltpu.VMEM((128, 128), bf16),
            pltpu.VMEM((8, 512), jnp.int32),
            pltpu.VMEM((8, 512), jnp.int32),
            pltpu.VMEM((8, 512), f32),
            pltpu.VMEM((4, 384, 128), f32),
            pltpu.VMEM((2, 8, 256), f32),
            pltpu.VMEM((8, 8, 256), f32),
            pltpu.VMEM((4, 256, 384), bf16),
            pltpu.VMEM((4, 256, 384), bf16),
            pltpu.VMEM((4, 128, 384), f32),
            pltpu.VMEM((16, 16, 128), f32),
            pltpu.VMEM((16, 16, 128), f32),
            pltpu.VMEM((8, 8, 512), f32),
            pltpu.VMEM((8, 8, 512), f32),
            pltpu.VMEM((8, 8, 512), bf16),
            pltpu.VMEM((8, 8, 512), bf16),
            pltpu.VMEM((16, 16, 128), bf16),
            pltpu.VMEM((16, 16, 128), bf16),
            pltpu.VMEM((256, 128), f32),
            pltpu.VMEM((8, 8, 512), f32),
            pltpu.VMEM((8, 1, 256), f32),
            pltpu.VMEM((8, 1, 256), f32),
            pltpu.SemaphoreType.DMA,
            dma((4, 2)),
            *[pltpu.SemaphoreType.DMA] * 10,
            dma((2,)),
            dma((2,)),
            dma((2,)),
            dma((2,)),
        ],
        compiler_params=pltpu.CompilerParams(
            collective_id=0, has_side_effects=True, vmem_limit_bytes=48 * 1024 * 1024
        ),
        cost_estimate=pl.CostEstimate(flops=4 * 10**9, bytes_accessed=4 * 10**6, transcendentals=10**7),
        name="layer",
    )(*[pltpu.with_memory_space_constraint(x, pltpu.HBM) for x in (*operands, *tables)])


def shards(
    features,
    positions,
    grid_anchor,
    species,
    neighbours,
    neighbour_count,
    w_self,
    w_neighbour,
    w_radial,
    radial_rates,
    w_pair1,
    w_pair2,
    w_vector,
    w_out,
    w_charge,
    species_charge,
):
    updated, site_potential = layer(
        (
            features,
            positions,
            grid_anchor,
            species,
            neighbours,
            neighbour_count,
            w_neighbour,
            w_self,
            w_radial,
            radial_rates,
            w_pair1,
            w_pair2,
            w_vector,
            w_out,
            w_charge.reshape(1, 128),
            species_charge,
        )
    )
    return (updated.reshape(features.shape), site_potential)


def solution(mesh):
    return jax.shard_map(
        shards,
        mesh=mesh,
        in_specs=(
            P("gx", "gy", "gz", None, None),
            P("gx", "gy", "gz", None),
            P("gx", "gy", "gz", None),
            P("gx", "gy", "gz", None),
            P("gx", "gy", "gz", None),
            P("gx", "gy", "gz", None),
            P(),
            P(),
            P(),
            P(),
            P(),
            P(),
            P(),
            P(),
            P(),
            P(),
        ),
        out_specs=(P("gx", "gy", "gz", None, None), P("gx", "gy", "gz", None)),
        check_vma=False,
    )
```

```python
import jax
import jax.numpy as jnp
import numpy as np
from jax import lax
from jax.experimental import pallas as pl
from jax.experimental.pallas import tpu as pltpu
from jax.sharding import PartitionSpec as P


coulomb_scale = 0.25
smearing = 1.0


NT = (((1,), (1,)), ((), ()))
CUTS = (0, 4, 7, 9, 11)


def real_basis(length):
    modes = np.arange(length)[:, None]
    cells = np.arange(length)[None, :]
    turns = 2.0 * np.pi * ((modes * cells) % length) / length
    flipped = 2.0 * np.pi * (((length - modes) * cells) % length) / length
    return np.where(modes <= length // 2, np.cos(turns), np.sin(flipped))


def two_parts(table):
    table = np.asarray(table, np.float32)
    high = table.astype(jnp.bfloat16)
    low = (table - high.astype(np.float32)).astype(jnp.bfloat16)
    return np.stack([high, low])


def mode_tables(length):
    modes = np.arange(length)
    signed = np.where(modes > length // 2, modes - length, modes)
    wave = signed * (2.0 * np.pi / length)
    modulus = ((4.0 + 2.0 * np.cos(2.0 * np.pi * modes / length)) / 6.0) ** 2
    weight = np.where((modes == 0) | (modes == length // 2), 1.0, 2.0) / length
    return np.exp(-0.5 * smearing * smearing * wave * wave) / modulus * weight, wave * wave


def ewald_tables():
    basis_z = two_parts(real_basis(256))
    order_y = np.array([4 * p + i for i in range(4) for p in range(16)])
    forward_y = real_basis(64)[:, order_y]
    basis_y = np.stack([two_parts(forward_y), two_parts(forward_y.T)])
    wide = np.zeros((256, 256))
    full_x = real_basis(192)
    for g in range(8):
        wide[:192, 32 * g : 32 * g + 27] = full_x[:, (24 * g - 1 + np.arange(27)) % 192]
    basis_x = two_parts(wide)
    green_x = np.zeros((2, 8, 256))
    gain, square = mode_tables(192)
    green_x[0, :, :192] = gain * (coulomb_scale * 4.0 * np.pi)
    green_x[1, :, :192] = square
    green_x[1, :, 192:] = 1.0
    green_y = np.repeat(np.stack(mode_tables(64))[:, :, None], 128, 2)
    green_z = np.repeat(np.stack(mode_tables(256))[:, :, None], 128, 2)
    return (
        basis_z,
        basis_y,
        basis_x,
        green_x.astype(np.float32),
        green_y.astype(np.float32),
        green_z.astype(np.float32),
    )


def split(value):
    high = value.astype(jnp.bfloat16)
    return high, (value - high.astype(jnp.float32)).astype(jnp.bfloat16)


def dot3(a, b, dims=(((1,), (0,)), ((), ()))):
    def one(u, v):
        return lax.dot_general(u, v, dims, preferred_element_type=jnp.float32)

    rows = a[0].shape[0]
    both = one(jnp.concatenate([a[0], a[1]], axis=0), b[0])
    return both[0:rows] + (one(a[0], b[1]) + both[rows : 2 * rows])


def swap_groups(pieces, shift):
    lane = lax.broadcasted_iota(jnp.int32, pieces[0].shape, 1) // 32
    out = None
    for k, piece in enumerate(pieces):
        moved = pltpu.roll(piece, (32 * (k - shift)) % 128, 1) if k != shift else piece
        out = moved if out is None else jnp.where(lane == k, moved, out)
    return out


def tap_rows(fraction):
    square = fraction * fraction
    cube = square * fraction
    remain = 1.0 - fraction
    return (
        remain * remain * remain / 6.0,
        (3.0 * cube - 6.0 * square + 4.0) / 6.0,
        (-3.0 * cube + 3.0 * square + 3.0 * fraction + 1.0) / 6.0,
        cube / 6.0,
    )


def pick_taps(offset, taps):
    out = jnp.zeros(offset.shape, jnp.float32)
    for t in range(4):
        out = jnp.where(offset == t, taps[t], out)
    return out


def layer_kernel(
    feat_hbm,
    place_hbm,
    anchor_hbm,
    species_hbm,
    nbr_hbm,
    count_hbm,
    wn_hbm,
    ws_hbm,
    wr_hbm,
    rate_hbm,
    w1_hbm,
    w2_hbm,
    wv_hbm,
    wo_hbm,
    wc_hbm,
    kind_hbm,
    bz_hbm,
    by_hbm,
    bx_hbm,
    gx_hbm,
    gy_hbm,
    gz_hbm,
    out_ref,
    site_ref,
    feat_ref,
    place_ref,
    anchor_ref,
    species_ref,
    wc_ref,
    wn_ref,
    ws_ref,
    wr_ref,
    w1_ref,
    w2_ref,
    nbr_ref,
    count_ref,
    bz_ref,
    by_ref,
    bx_ref,
    gx_ref,
    gy_ref,
    gz_ref,
    wv_ref,
    wo_ref,
    kind_ref,
    rate_ref,
    load_sem,
    small_sem,
    pos_ref,
    feat_ext,
    pos_ext,
    pos_tab,
    feat32,
    first_w,
    pair1_w,
    pair2_w,
    hot_row,
    lane_row,
    live_row,
    sums,
    tx_atoms,
    rx_atoms,
    z_high,
    z_low,
    stencil,
    tx_b,
    rx_b,
    tx_c,
    rx_c,
    tx_c2,
    rx_c2,
    tx_b2,
    rx_b2,
    flat_b,
    flat_c,
    parts,
    rx_parts,
    sa,
    ra,
    sb,
    rb,
    sc,
    rc,
    sc2,
    rc2,
    sb2,
    rb2,
    sp,
    rp,
    sf,
    rf,
    sq,
    rq,
):
    bf16 = jnp.bfloat16
    f32 = jnp.float32
    MESH = pl.DeviceIdType.MESH
    ix, iy, iz = lax.axis_index("gx"), lax.axis_index("gy"), lax.axis_index("gz")
    me = iy * 4 + iz
    barrier = pltpu.get_barrier_semaphore()
    pairs = (
        (feat_hbm, feat_ref),
        (place_hbm, place_ref),
        (anchor_hbm, anchor_ref),
        (species_hbm, species_ref),
        (wc_hbm, wc_ref),
        (wn_hbm, wn_ref),
        (ws_hbm, ws_ref),
        (wr_hbm, wr_ref),
        (w1_hbm, w1_ref),
        (w2_hbm, w2_ref),
        (nbr_hbm, nbr_ref),
        (count_hbm, count_ref),
        (bz_hbm, bz_ref),
        (by_hbm, by_ref),
        (bx_hbm, bx_ref),
        (gx_hbm, gx_ref),
        (gy_hbm, gy_ref),
        (gz_hbm, gz_ref),
        (wv_hbm, wv_ref),
        (wo_hbm, wo_ref),
    )
    loads = [
        pltpu.make_async_copy(src, dst, load_sem.at[n]) for n, (src, dst) in enumerate(pairs)
    ]
    small = [
        pltpu.make_async_copy(kind_hbm, kind_ref, small_sem.at[0]),
        pltpu.make_async_copy(rate_hbm, rate_ref, small_sem.at[1]),
    ]
    for load in loads[:5] + small[:1]:
        load.start()

    yz_steps = [(x, c, z) for x in (1, 0) for z in (2, 1, 3, 0) for c in (1, 0)]
    x_steps = [(2, 1), (2, 0), (1, 1), (3, 1), (1, 0), (3, 0), (0, 1)]

    def yz_peer(r):
        x, c, z = yz_steps[r - 1]
        other_y = lax.rem(iy // 2 + x, 2) * 2 + lax.rem(lax.rem(iy, 2) + c, 2)
        other_z = lax.rem(iz + z, 4)
        return other_y * 4 + other_z, (ix, other_y, other_z)

    def x_peer(r):
        y, x = x_steps[r - 1]
        other = lax.rem(ix // 2 + y, 4) * 2 + lax.rem(lax.rem(ix, 2) + x, 2)
        return other, (other, iy, iz)

    for r in range(1, 16):
        pl.semaphore_signal(barrier, inc=1, device_id=yz_peer(r)[1], device_id_type=MESH)
    for r in range(1, 8):
        pl.semaphore_signal(barrier, inc=1, device_id=x_peer(r)[1], device_id_type=MESH)

    def halo_peer(index):
        ox, oy, oz = index // 9 - 1, index // 3 % 3 - 1, index % 3 - 1
        return (lax.rem(ix + ox + 8, 8), lax.rem(iy + oy + 4, 4), lax.rem(iz + oz + 4, 4))

    def halo_span(step, cells):
        if step == 0:
            return pl.ds(0, cells), pl.ds(1, cells)
        return (pl.ds(cells - 1, 1), pl.ds(0, 1)) if step > 0 else (pl.ds(0, 1), pl.ds(cells + 1, 1))

    halo_ids = [n for n in range(27) if n != 13]
    near_ids = [n for n in halo_ids if n // 9 == 1]
    far_ids = [n for n in halo_ids if n // 9 != 1]

    def halo_copies(index):
        steps = (index // 9 - 1, index // 3 % 3 - 1, index % 3 - 1)
        spans = [halo_span(step, cells) for step, cells in zip(steps, (3, 2, 8))]
        group = 0 if steps[0] == 0 else 1
        source = tuple(span[0] for span in spans)
        target = tuple(span[1] for span in spans)
        row = {0: pl.ds(1, 2), 1: pl.ds(0, 1), -1: pl.ds(3, 1)}[steps[2]]
        return [
            pltpu.make_async_remote_copy(
                src_ref=src.at[source[:2] + (from_z,)],
                dst_ref=dst.at[target[:2] + (to_z,)],
                send_sem=send.at[group],
                recv_sem=recv.at[group],
                device_id=halo_peer(index),
                device_id_type=MESH,
            )
            for src, dst, send, recv, from_z, to_z in (
                (feat_ref, feat_ext, sf, rf, source[2], target[2]),
                (pos_ref, pos_ext, sq, rq, row, row),
            )
        ]

    def halo_group(group):
        cells = (pl.ds(0, 2 if group else 3), pl.ds(0, 4), pl.ds(0, 10 if group else 6))
        rows = (pl.ds(0, 2 if group else 3), pl.ds(0, 4), pl.ds(0, 4 if group else 3))
        return [
            pltpu.make_async_remote_copy(
                src_ref=ext.at[part],
                dst_ref=ext.at[part],
                send_sem=send.at[group],
                recv_sem=recv.at[group],
                device_id=halo_peer(0),
                device_id_type=MESH,
            )
            for ext, part, send, recv in ((feat_ext, cells, sf, rf), (pos_ext, rows, sq, rq))
        ]

    for index in far_ids:
        if index % 9 != 4:
            pl.semaphore_signal(
                barrier, inc=1, device_id=halo_peer(index), device_id_type=MESH
            )

    for load in loads[:5] + small[:1]:
        load.wait()

    sub_l = lax.broadcasted_iota(jnp.int32, (8, 128), 0)
    lane_l = lax.broadcasted_iota(jnp.int32, (8, 128), 1)
    for half in range(2):
        own_rows = feat_ref[:, half].astype(f32).reshape(192, 128).astype(bf16)
        weights = jnp.broadcast_to(wc_ref[...].astype(f32), (16, 128)).astype(bf16)
        readout = lax.dot_general(weights, own_rows, NT, preferred_element_type=f32)[0:8]
        laid = []
        for cx in range(3):
            place = place_ref[cx, half]
            for row, cells in ((0, (7,)), (1, (0, 1, 2, 3)), (2, (4, 5, 6, 7)), (3, (0,))):
                pieces = [place[cz : cz + 1] for cz in cells]
                pieces.append(jnp.zeros((1, 128 - 24 * len(cells)), f32))
                pos_ref[cx, half, row] = jnp.concatenate(pieces, axis=1)
            source = jnp.concatenate(
                [
                    place,
                    anchor_ref[cx, half].astype(f32),
                    species_ref[cx, half].astype(f32),
                    jnp.zeros((8, 72), f32),
                ],
                axis=1,
            )
            rows = jnp.zeros((8, 128), f32)
            for cz in range(8):
                row = jnp.broadcast_to(source[cz : cz + 1], (8, 128))
                moved = jnp.take_along_axis(row, sub_l * 8 + lane_l % 8, axis=1)
                rows = jnp.where(lane_l // 8 == cz, moved, rows)
            laid.append(rows)
        rows = jnp.concatenate(
            [jnp.where(lane_l < 64, laid[0], pltpu.roll(laid[1], 64, 1)), laid[2]], axis=1
        )
        kinds = rows[6:7]
        base = jnp.where(kinds == 0.0, kind_ref[0], jnp.where(kinds == 1.0, kind_ref[1], 0.0))
        total = jnp.concatenate(
            [base[:, 0:192] + readout[0:1, :], jnp.zeros((1, 64), f32)], axis=1
        )
        tx_atoms[half, 0:3, :] = rows[0:3] - (rows[3:6] + 1.0)
        tx_atoms[half, 3:6, :] = rows[3:6]
        tx_atoms[half, 6:7, :] = total
        tx_atoms[half, 7:8, :] = jnp.zeros((1, 256), f32)

    pl.semaphore_wait(barrier, 38)

    routes = [(0, 3, 3, 1), (0, 0, 0, 1), (0, 1, 0, 0), (0, 2, 0, 0)]
    routes += [(1, 1, 0, 1), (1, 2, 0, 1), (1, 3, 0, 0), (1, 0, 1, 0)]

    def atom_copy(half, to_z, step_y, place):
        return pltpu.make_async_remote_copy(
            src_ref=tx_atoms.at[half],
            dst_ref=rx_atoms.at[iz * 2 + place],
            send_sem=sa,
            recv_sem=ra.at[iz, place],
            device_id=(ix, lax.rem(iy + step_y, 4), to_z),
            device_id_type=MESH,
        )

    for half, to_z, step_y, place in routes:
        if step_y:
            atom_copy(half, to_z, step_y, place).start()
        else:

            @pl.when(iz != to_z)
            def _():
                atom_copy(half, to_z, step_y, place).start()

            @pl.when(iz == to_z)
            def _():
                rx_atoms[iz * 2 + place] = tx_atoms[half]

    for index in near_ids:
        for copy in halo_copies(index):
            copy.start()
    for index in far_ids:
        for copy in halo_copies(index):
            copy.start()
    for load in loads[5:] + small[1:]:
        load.start()
    feat_ext[1:4, 1:3, 1:9] = feat_ref[...]
    pos_ext[1:4, 1:3, 1:3] = pos_ref[:, :, 1:3]
    for load in loads[5:] + small[1:]:
        load.wait()
    first_w[:, 0:128] = (wn_ref[...].astype(f32) * 0.5).T.astype(bf16)
    first_w[:, 128:256] = (ws_ref[...].astype(f32) * 0.5).T.astype(bf16)
    pair1_w[...] = (w1_ref[...].astype(f32) * 0.5).T.astype(bf16)
    pair2_w[...] = (w2_ref[...].astype(f32) * 0.5).T.astype(bf16)
    radial_pad = jnp.concatenate(
        [jnp.zeros((88, 128), f32), wr_ref[...].astype(f32) * 0.5, jnp.zeros((32, 128), f32)], axis=0
    ).T
    cell_x0, cell_y0, cell_z0 = ix * 3, iy * 2, iz * 8

    sub8 = lax.broadcasted_iota(jnp.int32, (8, 512), 0)
    lane8 = lax.broadcasted_iota(jnp.int32, (8, 512), 1)
    rates = jnp.zeros((8, 512), f32)
    for k in range(8):
        rates = jnp.where(sub8 == k, rate_ref[k], rates)
    own_mask = (lane8 // 64) == sub8
    own_hot = jnp.where(own_mask, 1.0, 0.0).astype(f32)
    own_hot32 = jnp.concatenate([own_hot, own_hot, jnp.zeros((16, 512), f32)], axis=0).astype(bf16)
    lane_t = lax.broadcasted_iota(jnp.int32, (128, 128), 1)
    low_part = (lane_t >= 104) & (lane_t < 112)
    half_sub = sub_l // 4
    axis_sub = sub_l % 4
    box = jnp.where(axis_sub == 0, 192.0, jnp.where(axis_sub == 1, 64.0, 256.0)).astype(f32)
    box_inv = 1.0 / box
    atom_lane = lax.broadcasted_iota(jnp.int32, (8, 128), 1) // 64
    def half_column(index, carry):
        later = (index - 4) // 2
        col = jnp.where(index < 4, 2 + index // 2, jnp.where(later < 2, later, later + 2))
        cx = col // 2
        cy = lax.rem(col, 2)
        ids = nbr_ref[cx, cy]
        slot = ids & 7
        z = (ids >> 3) & 31
        y = (ids >> 8) & 7
        x = ids >> 11
        dz = (z - (cell_z0 + sub8) + 1) & 31
        dy = (y - (cell_y0 + cy) + 1) & 7
        dx = x - (cell_x0 + cx) + 1
        dx = jnp.where(dx < 0, dx + 24, dx)
        dx = jnp.where(dx >= 24, dx - 24, dx)
        strip = dx * 3 + dy
        hot_row[...] = strip * 24 + dz * 8 + slot
        lane_row[...] = ((dz + sub8) * 8 + slot) * 16 + strip
        counts = jnp.concatenate([count_ref[cx, cy], jnp.zeros((8, 120), jnp.int32)], axis=1)
        pieces = []
        for g in range(4):
            owner = atom_lane + 2 * g
            count_g = jnp.take_along_axis(counts, owner, axis=1)
            slot_g = lax.broadcasted_iota(jnp.int32, (8, 128), 1) % 64
            pieces.append(jnp.where(slot_g < count_g, 1.0, 0.0).astype(f32))
        live_row[...] = jnp.concatenate(pieces, axis=1)

        def cell(cz):
            rows = []
            for dx_ in range(3):
                for dy_ in range(3):
                    base = ((cx + dx_) * 4 + cy + dy_) * 80 + cz * 8
                    rows.append(feat32[pl.ds(pl.multiple_of(base, 8), 24), :])
            own_base = ((cx + 1) * 4 + cy + 1) * 80 + cz * 8 + 8
            own = feat32[pl.ds(pl.multiple_of(own_base, 8), 8), :]
            left = jnp.concatenate(rows + [jnp.zeros((40, 128), f32)], axis=0)
            right = jnp.concatenate(
                [jnp.zeros((224, 128), f32), own, own, jnp.zeros((16, 128), f32)], axis=0
            )
            table = jnp.concatenate([left, right], axis=1).astype(bf16)
            proj = lax.dot_general(first_w[...], table, NT, preferred_element_type=f32)
            tail = proj[:, 128:256]
            tail_hi = tail.astype(bf16).astype(f32)
            tail = jnp.where(low_part, tail - tail_hi, tail_hi) + radial_pad
            lhs = jnp.concatenate([proj[:, 0:128].astype(bf16), tail.astype(bf16)], axis=1)

            place = []
            hot = hot_row[pl.ds(cz, 1), :]
            packed = lane_row[pl.ds(cz, 1), :]
            live = live_row[pl.ds(cz, 1), :]
            for g in range(4):
                packed_g = jnp.broadcast_to(packed[:, g * 128 : g * 128 + 128], (8, 128))
                where_g = packed_g >> 4
                strip_g = packed_g & 15
                got = jnp.zeros((8, 128), f32)
                for t in range(5):
                    hit = strip_g == (2 * t + half_sub)
                    got = jnp.where(
                        hit,
                        jnp.take_along_axis(pos_tab[col, t * 8 : t * 8 + 8, :], where_g, axis=1),
                        got,
                    )
                got = got + pltpu.roll(got, 4, 0)
                mine = jnp.take_along_axis(
                    pos_tab[col, 40:48, :], atom_lane + 2 * g + (cz + 1) * 8, axis=1
                )
                gap = got - mine
                gap = gap - box * jnp.floor(gap * box_inv + 0.5)
                place.append(gap * 0.125)
            scaled = jnp.concatenate(place, axis=1)
            square = scaled * scaled
            square = square[0:1] + square[1:2] + square[2:3]
            basis = jnp.exp(-jnp.broadcast_to(square, (8, 512)) * rates)
            cell_iota = lax.broadcasted_iota(jnp.int32, (216, 512), 0)
            hots = jnp.where(cell_iota == hot, 1.0, 0.0).astype(f32)
            rhs = jnp.concatenate(
                [jnp.concatenate([hots, basis], axis=0).astype(bf16), own_hot32], axis=0
            )
            half = jnp.dot(lhs, rhs, preferred_element_type=f32)
            yield
            latent = (half + half * jnp.tanh(half)).astype(bf16)
            half = jnp.dot(pair1_w[...], latent, preferred_element_type=f32)
            yield
            second = (half + half * jnp.tanh(half)).astype(bf16)
            half = jnp.dot(pair2_w[...], second, preferred_element_type=f32)
            yield
            third = (half + half * jnp.tanh(half)).astype(bf16)

            weighted = scaled * live
            w_hi = weighted.astype(bf16).astype(f32)
            w_lo = weighted - w_hi
            parts = [live]
            for d in range(3):
                parts += [w_hi[d : d + 1], w_lo[d : d + 1]]
            spread = jnp.concatenate(
                [jnp.where(own_mask, jnp.broadcast_to(p, (8, 512)), 0.0) for p in parts]
                + [jnp.zeros((8, 512), f32)],
                axis=0,
            ).astype(bf16)
            total = lax.dot_general(spread, third, NT, preferred_element_type=f32)
            yield
            at = pl.multiple_of((col * 8 + cz) * 8, 8)
            sums[0, pl.ds(at, 8), :] = total[0:8]
            for d in range(3):
                sums[1 + d, pl.ds(at, 8), :] = (
                    total[8 + 16 * d : 16 + 16 * d] + total[16 + 16 * d : 24 + 16 * d]
                )

        running = [cell(lax.rem(index, 2) * 4 + u) for u in range(4)]
        while running:
            running = [one for one in running if next(one, 1) is None]
        return carry

    def half_columns(first, last):
        lax.fori_loop(first, last, half_column, 0)

    from_y = [
        lax.rem(iy + jnp.where(iz == 0, 3, 0), 4),
        lax.rem(iy + jnp.where(iz == 3, 1, 0), 4),
    ]
    edge = jnp.where((iz == 0) | (iz == 3), 1, 0)
    from_half = [edge, 1 - edge]

    def atom_wait(s, u):
        @pl.when((s != iz) | (from_y[u] != iy))
        def _():
            pltpu.make_async_remote_copy(
                src_ref=tx_atoms.at[0],
                dst_ref=rx_atoms.at[s * 2 + u],
                send_sem=sa,
                recv_sem=ra.at[s, u],
                device_id=(ix, from_y[u], s),
                device_id_type=MESH,
            ).wait_recv()

    y_first = iy * 16 + iz * 4

    z_ids = lax.broadcasted_iota(jnp.int32, (256, 384), 0)
    x_ids = lax.broadcasted_iota(jnp.int32, (32, 384), 0) + (ix * 24 - 1)
    lane_384 = lax.broadcasted_iota(jnp.int32, (8, 128), 1)

    def spread(source):
        low_part_, high_part_ = rx_atoms[source * 2], rx_atoms[source * 2 + 1]
        moved = pltpu.roll(high_part_, 64, 1)
        rows = jnp.concatenate(
            [
                low_part_[:, 0:128],
                jnp.where(lane_384 < 64, low_part_[:, 128:256], moved[:, 0:128]),
                moved[:, 128:256],
            ],
            axis=1,
        )
        anchor = rows[3:6].astype(jnp.int32)
        weights_z = pick_taps((z_ids - anchor[2:3]) & 255, tap_rows(rows[2:3]))
        high, low = split(weights_z)
        z_high[source] = high
        z_low[source] = low
        weights_x = pick_taps(x_ids - anchor[0:1], tap_rows(rows[0:1]))
        taps_y = tap_rows(rows[1:2])
        blocks = [
            weights_x * pick_taps((y_first + i - anchor[1:2]) & 63, taps_y) for i in range(4)
        ]
        both = jnp.concatenate(blocks, axis=0)
        stencil[source] = both
        return dot3(split(both * rows[6:7]), (high, low), NT)

    lines = None
    for steps in ((1, 3), (0, 2)):
        sources = [lax.rem(iz + step, 4) for step in steps]
        for source in sources:
            for u in range(2):
                atom_wait(source, u)
        for source in sources:
            part = spread(source)
            lines = part if lines is None else lines + part
    spectrum = dot3((bz_ref[0], bz_ref[1]), split(lines), NT)
    tx_b[...] = spectrum.reshape(16, 16, 128)
    rx_b[me] = tx_b[me]

    def exchange(tx, rx, send, recv, peer, count, mine):
        for r in range(1, count):
            other, where = peer(r)
            pltpu.make_async_remote_copy(
                src_ref=tx.at[other],
                dst_ref=rx.at[mine],
                send_sem=send,
                recv_sem=recv,
                device_id=where,
                device_id_type=MESH,
            ).start()
        whole = pltpu.make_async_remote_copy(
            src_ref=tx.at[pl.ds(0, count - 1)],
            dst_ref=rx.at[pl.ds(0, count - 1)],
            send_sem=send,
            recv_sem=recv,
            device_id=peer(1)[1],
            device_id_type=MESH,
        )
        return whole.wait_recv, whole.wait_send

    arrive_b, drain_b = exchange(tx_b, rx_b, sb, rb, yz_peer, 16, me)

    strip_lane = lax.broadcasted_iota(jnp.int32, (8, 128), 1)
    strip_cell = strip_lane // 8
    within = axis_sub * 8 + strip_lane % 8
    starts = jnp.where(strip_cell == 0, 0, jnp.where(strip_cell == 9, 0, lax.rem(strip_cell + 3, 4)))
    strip_at = jnp.where(axis_sub == 3, 127, jnp.minimum(starts * 24 + within, 127))
    strips = {}

    def lay_strips(sx):
        feat32[320 * sx : 320 * sx + 320, :] = feat_ext[sx].astype(f32).reshape(320, 128)
        for sy in range(4):
            table = jnp.zeros((8, 128), f32)
            for row, first, last in ((0, 0, 1), (1, 1, 5), (2, 5, 9), (3, 9, 10)):
                source = jnp.broadcast_to(pos_ext[sx, sy, row], (8, 128))
                moved = jnp.take_along_axis(source, strip_at, axis=1)
                table = jnp.where((strip_cell >= first) & (strip_cell < last), moved, table)
            strips[sx, sy] = table

    def lay_column(n):
        near = [strips[n // 2 + d // 3, n % 2 + d % 3] for d in range(9)]
        near += [near[4]] * 3
        for t in range(6):
            pos_tab[n, 8 * t : 8 * t + 8, :] = jnp.where(half_sub == 0, near[2 * t], near[2 * t + 1])

    for copy in halo_group(0):
        copy.wait_recv()
    for sx in (1, 2, 3):
        lay_strips(sx)
    for n in (2, 3):
        lay_column(n)
    half_columns(CUTS[0], CUTS[1])
    arrive_b()
    rows_b = rx_b.reshape(256, 128)
    columns = []
    for group in range(4):
        pieces = [rows_b[pl.ds(group * 4 + k, 16, 16), :] for k in range(4)]
        columns.append(jnp.concatenate([swap_groups(pieces, i) for i in range(4)], axis=0))
    lines_y = jnp.concatenate(columns, axis=1)
    modes_y = dot3((by_ref[0, 0], by_ref[0, 1]), split(lines_y))
    tx_c[...] = modes_y.reshape(8, 8, 512)
    rx_c[ix] = tx_c[ix]
    arrive_c, drain_c = exchange(tx_c, rx_c, sc, rc, x_peer, 8, ix)

    gain_z = gz_ref[0, pl.ds(pl.multiple_of(me * 16, 16), 16), :]
    square_z = gz_ref[1, pl.ds(pl.multiple_of(me * 16, 16), 16), :]
    gain_y = gy_ref[0, pl.ds(pl.multiple_of(ix * 8, 8), 8), :]
    square_y = gy_ref[1, pl.ds(pl.multiple_of(ix * 8, 8), 8), :]
    gain_yz = (gain_z[:, None, :] * gain_y[None, :, :]).reshape(128, 128)
    square_yz = (square_z[:, None, :] + square_y[None, :, :]).reshape(128, 128)
    greens = []
    for h in range(2):
        lanes = slice(128 * h, 128 * h + 128)
        total = square_yz + gx_ref[1, 0:1, lanes]
        value = gain_yz * gx_ref[0, 0:1, lanes] / (total + 1.0 / 1024.0)
        greens.append(jnp.where(total == 0.0, 0.0, value))
    green = jnp.concatenate(greens, axis=1)
    for copy in halo_group(1):
        copy.wait_recv()
    for sx in (0, 4):
        lay_strips(sx)
    for n in (0, 1, 4, 5):
        lay_column(n)
    half_columns(CUTS[1], CUTS[2])

    arrive_c()
    rows_x = []
    for group in range(4):
        for k in range(4):
            halves = [
                swap_groups(
                    [rx_c[4 * h + g, :, group * 128 : group * 128 + 128] for g in range(4)], k
                )
                for h in range(2)
            ]
            rows_x.append(jnp.concatenate(halves, axis=1))
    lines_x = jnp.concatenate(rows_x, axis=0)
    basis_x = (bx_ref[0], bx_ref[1])
    filtered = dot3(split(lines_x), basis_x, NT) * green
    back_x = dot3(split(filtered), basis_x)
    for g in range(8):
        half = g // 4
        for group in range(4):
            pieces = [
                back_x[(group * 4 + k) * 8 : (group * 4 + k) * 8 + 8, half * 128 : half * 128 + 128]
                for k in range(4)
            ]
            flat_c[g, :, group * 128 : group * 128 + 128] = swap_groups(pieces, g % 4)
    tx_c2[...] = flat_c[...].astype(bf16)
    rx_c2[ix] = tx_c2[ix]
    arrive_c2, drain_c2 = exchange(tx_c2, rx_c2, sc2, rc2, x_peer, 8, ix)
    half_columns(CUTS[2], CUTS[3])
    arrive_c2()
    lines_y2 = rx_c2[...].astype(f32).reshape(64, 512).astype(bf16)
    back_y = jnp.dot(by_ref[1, 0], lines_y2, preferred_element_type=f32)
    back_y = back_y + jnp.dot(by_ref[1, 1], lines_y2, preferred_element_type=f32)
    for group in range(4):
        pieces = [back_y[16 * i : 16 * i + 16, group * 128 : group * 128 + 128] for i in range(4)]
        for k in range(4):
            flat_b[pl.ds(group * 4 + k, 16, 16), :] = swap_groups(pieces, k)
    tx_b2[...] = flat_b[...].astype(bf16).reshape(16, 16, 128)
    rx_b2[me] = tx_b2[me]
    arrive_b2, drain_b2 = exchange(tx_b2, rx_b2, sb2, rb2, yz_peer, 16, me)
    half_columns(CUTS[3], CUTS[4])
    arrive_b2()
    back_z = rx_b2[...].astype(f32).reshape(256, 128).T.astype(bf16)
    lines_z = jnp.dot(back_z, bz_ref[0], preferred_element_type=f32)
    potential = split(lines_z + jnp.dot(back_z, bz_ref[1], preferred_element_type=f32))

    sampled = [dot3(potential, (z_high[n], z_low[n])) for n in range(4)]
    for n in range(4):
        total = jnp.sum(sampled[n] * stencil[n], axis=0, keepdims=True)
        parts[2 * n] = total[:, 0:256]
        tail = jnp.broadcast_to(total[:, 128:384], (8, 256))
        parts[2 * n + 1] = pltpu.roll(tail, 192, 1)[0:1]

    def part_copy(s, u):
        return pltpu.make_async_remote_copy(
            src_ref=parts.at[2 * s + u],
            dst_ref=rx_parts.at[from_half[u] * 4 + iz],
            send_sem=sp,
            recv_sem=rp,
            device_id=(ix, from_y[u], s),
            device_id_type=MESH,
        )

    for s in range(4):
        for u in range(2):

            @pl.when((s != iz) | (from_y[u] != iy))
            def _():
                part_copy(s, u).start()

            @pl.when((s == iz) & (from_y[u] == iy))
            def _():
                rx_parts[from_half[u] * 4 + iz] = parts[2 * s + u]

    half_columns(CUTS[4], 12)
    wv = wv_ref[...]
    invariant = jnp.zeros((384, 128), f32)
    for d in range(3):
        t = sums[1 + d]
        hi = t.astype(bf16)
        lo = (t - hi.astype(f32)).astype(bf16)
        vec = jnp.dot(hi, wv, preferred_element_type=f32) + jnp.dot(
            lo, wv, preferred_element_type=f32
        )
        invariant = invariant + vec * vec
    update = (sums[0] * (1.0 / 64.0) + invariant * (1.0 / 64.0)).astype(bf16)
    out_ref[...] = (
        feat_ref[...].astype(f32).reshape(384, 128) + jnp.dot(update, wo_ref[...], preferred_element_type=f32)
    ).astype(bf16)

    def bulk(ref, send, recv, arriving):
        for blocks, ends in ((7, 1), (6, 0)):

            @pl.when(edge == ends)
            def _():
                whole = pltpu.make_async_remote_copy(
                    src_ref=ref.at[pl.ds(0, blocks)],
                    dst_ref=ref.at[pl.ds(0, blocks)],
                    send_sem=send,
                    recv_sem=recv,
                    device_id=yz_peer(1)[1],
                    device_id_type=MESH,
                )
                if arriving:
                    whole.wait_recv()
                else:
                    whole.wait_send()

    bulk(rx_atoms, sa, ra.at[0, 0], False)
    drain_b()
    drain_c()
    drain_c2()
    drain_b2()
    for group in range(2):
        for copy in halo_group(group):
            copy.wait_send()

    bulk(rx_parts, sp, rp, True)

    for half in range(2):
        site = (rx_parts[half * 4] + rx_parts[half * 4 + 1]) + (
            rx_parts[half * 4 + 2] + rx_parts[half * 4 + 3]
        )
        for cx in range(3):
            block = site[:, 0:128] if cx < 2 else site[:, 128:256]
            block = jnp.broadcast_to(block, (8, 128))
            at = sub_l * 8 + lane_l % 8 + 64 * (cx % 2)
            site_ref[cx, half] = jnp.take_along_axis(block, at, axis=1)[:, 0:8]

    bulk(rx_parts, sp, rp, False)


def layer(operands):
    f32, bf16 = jnp.float32, jnp.bfloat16
    vm = pl.BlockSpec(memory_space=pltpu.VMEM)
    dma = pltpu.SemaphoreType.DMA
    tables = [jnp.asarray(t) for t in ewald_tables()]
    hbm = pl.BlockSpec(memory_space=pltpu.HBM)
    specs = [hbm] * 22
    shapes = [operands[n] for n in (0, 1, 2, 3, 14, 6, 7, 8, 10, 11, 4, 5)] + tables
    shapes += [operands[n] for n in (12, 13)]
    staged = [pltpu.VMEM(x.shape, x.dtype) for x in shapes]
    return pl.pallas_call(
        layer_kernel,
        out_shape=(
            jax.ShapeDtypeStruct((384, 128), bf16),
            jax.ShapeDtypeStruct((3, 2, 8, 8), f32),
        ),
        in_specs=specs,
        out_specs=(vm, vm),
        scratch_shapes=staged
        + [
            pltpu.SMEM((2,), f32),
            pltpu.SMEM((8,), f32),
            dma((20,)),
            dma((2,)),
            pltpu.VMEM((3, 2, 4, 1, 128), f32),
            pltpu.VMEM((5, 4, 10, 8, 128), bf16),
            pltpu.VMEM((5, 4, 4, 1, 128), f32),
            pltpu.VMEM((6, 48, 128), f32),
            pltpu.VMEM((1600, 128), f32),
            pltpu.VMEM((128, 256), bf16),
            pltpu.VMEM((128, 128), bf16),
            pltpu.VMEM((128, 128), bf16),
            pltpu.VMEM((8, 512), jnp.int32),
            pltpu.VMEM((8, 512), jnp.int32),
            pltpu.VMEM((8, 512), f32),
            pltpu.VMEM((4, 384, 128), f32),
            pltpu.VMEM((2, 8, 256), f32),
            pltpu.VMEM((8, 8, 256), f32),
            pltpu.VMEM((4, 256, 384), bf16),
            pltpu.VMEM((4, 256, 384), bf16),
            pltpu.VMEM((4, 128, 384), f32),
            pltpu.VMEM((16, 16, 128), f32),
            pltpu.VMEM((16, 16, 128), f32),
            pltpu.VMEM((8, 8, 512), f32),
            pltpu.VMEM((8, 8, 512), f32),
            pltpu.VMEM((8, 8, 512), bf16),
            pltpu.VMEM((8, 8, 512), bf16),
            pltpu.VMEM((16, 16, 128), bf16),
            pltpu.VMEM((16, 16, 128), bf16),
            pltpu.VMEM((256, 128), f32),
            pltpu.VMEM((8, 8, 512), f32),
            pltpu.VMEM((8, 1, 256), f32),
            pltpu.VMEM((8, 1, 256), f32),
            pltpu.SemaphoreType.DMA,
            dma((4, 2)),
            *[pltpu.SemaphoreType.DMA] * 10,
            dma((2,)),
            dma((2,)),
            dma((2,)),
            dma((2,)),
        ],
        compiler_params=pltpu.CompilerParams(
            collective_id=0, has_side_effects=True, vmem_limit_bytes=48 * 1024 * 1024
        ),
        cost_estimate=pl.CostEstimate(flops=4 * 10**9, bytes_accessed=4 * 10**6, transcendentals=10**7),
        name="layer",
    )(*[pltpu.with_memory_space_constraint(x, pltpu.HBM) for x in (*operands, *tables)])


def shards(
    features,
    positions,
    grid_anchor,
    species,
    neighbours,
    neighbour_count,
    w_self,
    w_neighbour,
    w_radial,
    radial_rates,
    w_pair1,
    w_pair2,
    w_vector,
    w_out,
    w_charge,
    species_charge,
):
    updated, site_potential = layer(
        (
            features,
            positions,
            grid_anchor,
            species,
            neighbours,
            neighbour_count,
            w_neighbour,
            w_self,
            w_radial,
            radial_rates,
            w_pair1,
            w_pair2,
            w_vector,
            w_out,
            w_charge.reshape(1, 128),
            species_charge,
        )
    )
    return (updated.reshape(features.shape), site_potential)


def solution(mesh):
    return jax.shard_map(
        shards,
        mesh=mesh,
        in_specs=(
            P("gx", "gy", "gz", None, None),
            P("gx", "gy", "gz", None),
            P("gx", "gy", "gz", None),
            P("gx", "gy", "gz", None),
            P("gx", "gy", "gz", None),
            P("gx", "gy", "gz", None),
            P(),
            P(),
            P(),
            P(),
            P(),
            P(),
            P(),
            P(),
            P(),
            P(),
        ),
        out_specs=(P("gx", "gy", "gz", None, None), P("gx", "gy", "gz", None)),
        check_vma=False,
    )
```

```python
import jax
import jax.numpy as jnp
import numpy as np
from jax import lax
from jax.experimental import pallas as pl
from jax.experimental.pallas import tpu as pltpu
from jax.sharding import PartitionSpec as P


coulomb_scale = 0.25
smearing = 1.0


NT = (((1,), (1,)), ((), ()))
CUTS = (0, 4, 6, 8, 11)


def real_basis(length):
    modes = np.arange(length)[:, None]
    cells = np.arange(length)[None, :]
    turns = 2.0 * np.pi * ((modes * cells) % length) / length
    flipped = 2.0 * np.pi * (((length - modes) * cells) % length) / length
    return np.where(modes <= length // 2, np.cos(turns), np.sin(flipped))


def two_parts(table):
    table = np.asarray(table, np.float32)
    high = table.astype(jnp.bfloat16)
    low = (table - high.astype(np.float32)).astype(jnp.bfloat16)
    return np.stack([high, low])


def mode_tables(length):
    modes = np.arange(length)
    signed = np.where(modes > length // 2, modes - length, modes)
    wave = signed * (2.0 * np.pi / length)
    modulus = ((4.0 + 2.0 * np.cos(2.0 * np.pi * modes / length)) / 6.0) ** 2
    weight = np.where((modes == 0) | (modes == length // 2), 1.0, 2.0) / length
    return np.exp(-0.5 * smearing * smearing * wave * wave) / modulus * weight, wave * wave


def ewald_tables():
    basis_z = two_parts(real_basis(256))
    order_y = np.array([4 * p + i for i in range(4) for p in range(16)])
    forward_y = real_basis(64)[:, order_y]
    basis_y = np.stack([two_parts(forward_y), two_parts(forward_y.T)])
    wide = np.zeros((256, 256))
    full_x = real_basis(192)
    for g in range(8):
        wide[:192, 32 * g : 32 * g + 27] = full_x[:, (24 * g - 1 + np.arange(27)) % 192]
    basis_x = two_parts(wide)
    green_x = np.zeros((2, 8, 256))
    gain, square = mode_tables(192)
    green_x[0, :, :192] = gain * (coulomb_scale * 4.0 * np.pi)
    green_x[1, :, :192] = square
    green_x[1, :, 192:] = 1.0
    green_y = np.repeat(np.stack(mode_tables(64))[:, :, None], 128, 2)
    green_z = np.repeat(np.stack(mode_tables(256))[:, :, None], 128, 2)
    return (
        basis_z,
        basis_y,
        basis_x,
        green_x.astype(np.float32),
        green_y.astype(np.float32),
        green_z.astype(np.float32),
    )


def split(value):
    high = value.astype(jnp.bfloat16)
    return high, (value - high.astype(jnp.float32)).astype(jnp.bfloat16)


def dot3(a, b, dims=(((1,), (0,)), ((), ()))):
    def one(u, v):
        return lax.dot_general(u, v, dims, preferred_element_type=jnp.float32)

    rows = a[0].shape[0]
    both = one(jnp.concatenate([a[0], a[1]], axis=0), b[0])
    return both[0:rows] + (one(a[0], b[1]) + both[rows : 2 * rows])


def swap_groups(pieces, shift):
    lane = lax.broadcasted_iota(jnp.int32, pieces[0].shape, 1) // 32
    out = None
    for k, piece in enumerate(pieces):
        moved = pltpu.roll(piece, (32 * (k - shift)) % 128, 1) if k != shift else piece
        out = moved if out is None else jnp.where(lane == k, moved, out)
    return out


def tap_rows(fraction):
    square = fraction * fraction
    cube = square * fraction
    remain = 1.0 - fraction
    return (
        remain * remain * remain / 6.0,
        (3.0 * cube - 6.0 * square + 4.0) / 6.0,
        (-3.0 * cube + 3.0 * square + 3.0 * fraction + 1.0) / 6.0,
        cube / 6.0,
    )


def pick_taps(offset, taps):
    out = jnp.zeros(offset.shape, jnp.float32)
    for t in range(4):
        out = jnp.where(offset == t, taps[t], out)
    return out


def layer_kernel(
    feat_hbm,
    place_hbm,
    anchor_hbm,
    species_hbm,
    nbr_hbm,
    count_hbm,
    wn_hbm,
    ws_hbm,
    wr_hbm,
    rate_hbm,
    w1_hbm,
    w2_hbm,
    wv_hbm,
    wo_hbm,
    wc_hbm,
    kind_hbm,
    bz_hbm,
    by_hbm,
    bx_hbm,
    gx_hbm,
    gy_hbm,
    gz_hbm,
    out_ref,
    site_ref,
    feat_ref,
    place_ref,
    anchor_ref,
    species_ref,
    wc_ref,
    wn_ref,
    ws_ref,
    wr_ref,
    w1_ref,
    w2_ref,
    nbr_ref,
    count_ref,
    bz_ref,
    by_ref,
    bx_ref,
    gx_ref,
    gy_ref,
    gz_ref,
    wv_ref,
    wo_ref,
    kind_ref,
    rate_ref,
    load_sem,
    small_sem,
    pos_ref,
    feat_ext,
    pos_ext,
    pos_tab,
    feat32,
    first_w,
    pair1_w,
    pair2_w,
    hot_row,
    lane_row,
    live_row,
    sums,
    tx_atoms,
    rx_atoms,
    z_high,
    z_low,
    stencil,
    tx_b,
    rx_b,
    tx_c,
    rx_c,
    tx_c2,
    rx_c2,
    tx_b2,
    rx_b2,
    flat_b,
    flat_c,
    parts,
    rx_parts,
    sa,
    ra,
    sb,
    rb,
    sc,
    rc,
    sc2,
    rc2,
    sb2,
    rb2,
    sp,
    rp,
    sf,
    rf,
    sq,
    rq,
):
    bf16 = jnp.bfloat16
    f32 = jnp.float32
    MESH = pl.DeviceIdType.MESH
    ix, iy, iz = lax.axis_index("gx"), lax.axis_index("gy"), lax.axis_index("gz")
    me = iy * 4 + iz
    barrier = pltpu.get_barrier_semaphore()
    pairs = (
        (feat_hbm, feat_ref),
        (place_hbm, place_ref),
        (anchor_hbm, anchor_ref),
        (species_hbm, species_ref),
        (wc_hbm, wc_ref),
        (wn_hbm, wn_ref),
        (ws_hbm, ws_ref),
        (wr_hbm, wr_ref),
        (w1_hbm, w1_ref),
        (w2_hbm, w2_ref),
        (nbr_hbm, nbr_ref),
        (count_hbm, count_ref),
        (bz_hbm, bz_ref),
        (by_hbm, by_ref),
        (bx_hbm, bx_ref),
        (gx_hbm, gx_ref),
        (gy_hbm, gy_ref),
        (gz_hbm, gz_ref),
        (wv_hbm, wv_ref),
        (wo_hbm, wo_ref),
    )
    loads = [
        pltpu.make_async_copy(src, dst, load_sem.at[n]) for n, (src, dst) in enumerate(pairs)
    ]
    small = [
        pltpu.make_async_copy(kind_hbm, kind_ref, small_sem.at[0]),
        pltpu.make_async_copy(rate_hbm, rate_ref, small_sem.at[1]),
    ]

    yz_steps = [(x, c, z) for x in (1, 0) for z in (2, 1, 3, 0) for c in (1, 0)]
    x_steps = [(2, 1), (2, 0), (1, 1), (3, 1), (1, 0), (3, 0), (0, 1)]

    def yz_peer(r):
        x, c, z = yz_steps[r - 1]
        other_y = lax.rem(iy // 2 + x, 2) * 2 + lax.rem(lax.rem(iy, 2) + c, 2)
        other_z = lax.rem(iz + z, 4)
        return other_y * 4 + other_z, (ix, other_y, other_z)

    def x_peer(r):
        y, x = x_steps[r - 1]
        other = lax.rem(ix // 2 + y, 4) * 2 + lax.rem(lax.rem(ix, 2) + x, 2)
        return other, (other, iy, iz)

    for r in range(1, 16):
        pl.semaphore_signal(barrier, inc=1, device_id=yz_peer(r)[1], device_id_type=MESH)
    for r in range(1, 8):
        pl.semaphore_signal(barrier, inc=1, device_id=x_peer(r)[1], device_id_type=MESH)

    def halo_peer(index):
        ox, oy, oz = index // 9 - 1, index // 3 % 3 - 1, index % 3 - 1
        return (lax.rem(ix + ox + 8, 8), lax.rem(iy + oy + 4, 4), lax.rem(iz + oz + 4, 4))

    def halo_span(step, cells):
        if step == 0:
            return pl.ds(0, cells), pl.ds(1, cells)
        return (pl.ds(cells - 1, 1), pl.ds(0, 1)) if step > 0 else (pl.ds(0, 1), pl.ds(cells + 1, 1))

    halo_ids = [n for n in range(27) if n != 13]
    near_ids = [n for n in halo_ids if n // 9 == 1]
    far_ids = [n for n in halo_ids if n // 9 != 1]

    def halo_copies(index):
        steps = (index // 9 - 1, index // 3 % 3 - 1, index % 3 - 1)
        spans = [halo_span(step, cells) for step, cells in zip(steps, (3, 2, 8))]
        group = 0 if steps[0] == 0 else 1
        source = tuple(span[0] for span in spans)
        target = tuple(span[1] for span in spans)
        row = {0: pl.ds(1, 2), 1: pl.ds(0, 1), -1: pl.ds(3, 1)}[steps[2]]
        return [
            pltpu.make_async_remote_copy(
                src_ref=src.at[source[:2] + (from_z,)],
                dst_ref=dst.at[target[:2] + (to_z,)],
                send_sem=send.at[group],
                recv_sem=recv.at[group],
                device_id=halo_peer(index),
                device_id_type=MESH,
            )
            for src, dst, send, recv, from_z, to_z in (
                (feat_ref, feat_ext, sf, rf, source[2], target[2]),
                (pos_ref, pos_ext, sq, rq, row, row),
            )
        ]

    def halo_group(group):
        cells = (pl.ds(0, 2 if group else 3), pl.ds(0, 4), pl.ds(0, 10 if group else 6))
        rows = (pl.ds(0, 2 if group else 3), pl.ds(0, 4), pl.ds(0, 4 if group else 3))
        return [
            pltpu.make_async_remote_copy(
                src_ref=ext.at[part],
                dst_ref=ext.at[part],
                send_sem=send.at[group],
                recv_sem=recv.at[group],
                device_id=halo_peer(0),
                device_id_type=MESH,
            )
            for ext, part, send, recv in ((feat_ext, cells, sf, rf), (pos_ext, rows, sq, rq))
        ]

    for load in loads[:5] + small[:1]:
        load.start()
    for index in far_ids:
        if index % 9 != 4:
            pl.semaphore_signal(
                barrier, inc=1, device_id=halo_peer(index), device_id_type=MESH
            )

    for load in loads[:5] + small[:1]:
        load.wait()

    sub_l = lax.broadcasted_iota(jnp.int32, (8, 128), 0)
    lane_l = lax.broadcasted_iota(jnp.int32, (8, 128), 1)
    for half in range(2):
        own_rows = feat_ref[:, half].astype(f32).reshape(192, 128).astype(bf16)
        weights = jnp.broadcast_to(wc_ref[...].astype(f32), (16, 128)).astype(bf16)
        readout = lax.dot_general(weights, own_rows, NT, preferred_element_type=f32)[0:8]
        laid = []
        for cx in range(3):
            place = place_ref[cx, half]
            for row, cells in ((0, (7,)), (1, (0, 1, 2, 3)), (2, (4, 5, 6, 7)), (3, (0,))):
                pieces = [place[cz : cz + 1] for cz in cells]
                pieces.append(jnp.zeros((1, 128 - 24 * len(cells)), f32))
                pos_ref[cx, half, row] = jnp.concatenate(pieces, axis=1)
            source = jnp.concatenate(
                [
                    place,
                    anchor_ref[cx, half].astype(f32),
                    species_ref[cx, half].astype(f32),
                    jnp.zeros((8, 72), f32),
                ],
                axis=1,
            )
            rows = jnp.zeros((8, 128), f32)
            for cz in range(8):
                row = jnp.broadcast_to(source[cz : cz + 1], (8, 128))
                moved = jnp.take_along_axis(row, sub_l * 8 + lane_l % 8, axis=1)
                rows = jnp.where(lane_l // 8 == cz, moved, rows)
            laid.append(rows)
        rows = jnp.concatenate(
            [jnp.where(lane_l < 64, laid[0], pltpu.roll(laid[1], 64, 1)), laid[2]], axis=1
        )
        kinds = rows[6:7]
        base = jnp.where(kinds == 0.0, kind_ref[0], jnp.where(kinds == 1.0, kind_ref[1], 0.0))
        total = jnp.concatenate(
            [base[:, 0:192] + readout[0:1, :], jnp.zeros((1, 64), f32)], axis=1
        )
        tx_atoms[half, 0:3, :] = rows[0:3] - (rows[3:6] + 1.0)
        tx_atoms[half, 3:6, :] = rows[3:6]
        tx_atoms[half, 6:7, :] = total
        tx_atoms[half, 7:8, :] = jnp.zeros((1, 256), f32)

    pl.semaphore_wait(barrier, 38)

    routes = [(0, 3, 3, 1), (0, 0, 0, 1), (0, 1, 0, 0), (0, 2, 0, 0)]
    routes += [(1, 1, 0, 1), (1, 2, 0, 1), (1, 3, 0, 0), (1, 0, 1, 0)]

    def atom_copy(half, to_z, step_y, place):
        return pltpu.make_async_remote_copy(
            src_ref=tx_atoms.at[half],
            dst_ref=rx_atoms.at[iz * 2 + place],
            send_sem=sa,
            recv_sem=ra.at[iz, place],
            device_id=(ix, lax.rem(iy + step_y, 4), to_z),
            device_id_type=MESH,
        )

    for half, to_z, step_y, place in routes:
        if step_y:
            atom_copy(half, to_z, step_y, place).start()
        else:

            @pl.when(iz != to_z)
            def _():
                atom_copy(half, to_z, step_y, place).start()

            @pl.when(iz == to_z)
            def _():
                rx_atoms[iz * 2 + place] = tx_atoms[half]

    for index in near_ids:
        for copy in halo_copies(index):
            copy.start()
    for index in far_ids:
        for copy in halo_copies(index):
            copy.start()
    for load in loads[5:] + small[1:]:
        load.start()
    feat_ext[1:4, 1:3, 1:9] = feat_ref[...]
    pos_ext[1:4, 1:3, 1:3] = pos_ref[:, :, 1:3]
    for load in loads[5:] + small[1:]:
        load.wait()
    first_w[:, 0:128] = (wn_ref[...].astype(f32) * 0.5).T.astype(bf16)
    first_w[:, 128:256] = (ws_ref[...].astype(f32) * 0.5).T.astype(bf16)
    pair1_w[...] = (w1_ref[...].astype(f32) * 0.5).T.astype(bf16)
    pair2_w[...] = (w2_ref[...].astype(f32) * 0.5).T.astype(bf16)
    radial_pad = jnp.concatenate(
        [jnp.zeros((88, 128), f32), wr_ref[...].astype(f32) * 0.5, jnp.zeros((32, 128), f32)], axis=0
    ).T
    cell_x0, cell_y0, cell_z0 = ix * 3, iy * 2, iz * 8

    sub8 = lax.broadcasted_iota(jnp.int32, (8, 512), 0)
    lane8 = lax.broadcasted_iota(jnp.int32, (8, 512), 1)
    rates = jnp.zeros((8, 512), f32)
    for k in range(8):
        rates = jnp.where(sub8 == k, rate_ref[k], rates)
    own_mask = (lane8 // 64) == sub8
    own_hot = jnp.where(own_mask, 1.0, 0.0).astype(f32)
    own_hot32 = jnp.concatenate([own_hot, own_hot, jnp.zeros((16, 512), f32)], axis=0).astype(bf16)
    lane_t = lax.broadcasted_iota(jnp.int32, (128, 128), 1)
    low_part = (lane_t >= 104) & (lane_t < 112)
    half_sub = sub_l // 4
    axis_sub = sub_l % 4
    box = jnp.where(axis_sub == 0, 192.0, jnp.where(axis_sub == 1, 64.0, 256.0)).astype(f32)
    box_inv = 1.0 / box
    atom_lane = lax.broadcasted_iota(jnp.int32, (8, 128), 1) // 64
    def half_column(index, carry):
        later = (index - 4) // 2
        col = jnp.where(index < 4, 2 + index // 2, jnp.where(later < 2, later, later + 2))
        cx = col // 2
        cy = lax.rem(col, 2)
        ids = nbr_ref[cx, cy]
        slot = ids & 7
        z = (ids >> 3) & 31
        y = (ids >> 8) & 7
        x = ids >> 11
        dz = (z - (cell_z0 + sub8) + 1) & 31
        dy = (y - (cell_y0 + cy) + 1) & 7
        dx = x - (cell_x0 + cx) + 1
        dx = jnp.where(dx < 0, dx + 24, dx)
        dx = jnp.where(dx >= 24, dx - 24, dx)
        strip = dx * 3 + dy
        hot_row[...] = strip * 24 + dz * 8 + slot
        lane_row[...] = ((dz + sub8) * 8 + slot) * 16 + strip
        counts = jnp.concatenate([count_ref[cx, cy], jnp.zeros((8, 120), jnp.int32)], axis=1)
        pieces = []
        for g in range(4):
            owner = atom_lane + 2 * g
            count_g = jnp.take_along_axis(counts, owner, axis=1)
            slot_g = lax.broadcasted_iota(jnp.int32, (8, 128), 1) % 64
            pieces.append(jnp.where(slot_g < count_g, 1.0, 0.0).astype(f32))
        live_row[...] = jnp.concatenate(pieces, axis=1)

        def cell(cz):
            rows = []
            for dx_ in range(3):
                for dy_ in range(3):
                    base = ((cx + dx_) * 4 + cy + dy_) * 80 + cz * 8
                    rows.append(feat32[pl.ds(pl.multiple_of(base, 8), 24), :])
            own_base = ((cx + 1) * 4 + cy + 1) * 80 + cz * 8 + 8
            own = feat32[pl.ds(pl.multiple_of(own_base, 8), 8), :]
            left = jnp.concatenate(rows + [jnp.zeros((40, 128), f32)], axis=0)
            right = jnp.concatenate(
                [jnp.zeros((224, 128), f32), own, own, jnp.zeros((16, 128), f32)], axis=0
            )
            table = jnp.concatenate([left, right], axis=1).astype(bf16)
            proj = lax.dot_general(first_w[...], table, NT, preferred_element_type=f32)
            tail = proj[:, 128:256]
            tail_hi = tail.astype(bf16).astype(f32)
            tail = jnp.where(low_part, tail - tail_hi, tail_hi) + radial_pad
            lhs = jnp.concatenate([proj[:, 0:128].astype(bf16), tail.astype(bf16)], axis=1)

            place = []
            hot = hot_row[pl.ds(cz, 1), :]
            packed = lane_row[pl.ds(cz, 1), :]
            live = live_row[pl.ds(cz, 1), :]
            for g in range(4):
                packed_g = jnp.broadcast_to(packed[:, g * 128 : g * 128 + 128], (8, 128))
                where_g = packed_g >> 4
                strip_g = packed_g & 15
                got = jnp.zeros((8, 128), f32)
                for t in range(5):
                    hit = strip_g == (2 * t + half_sub)
                    got = jnp.where(
                        hit,
                        jnp.take_along_axis(pos_tab[col, t * 8 : t * 8 + 8, :], where_g, axis=1),
                        got,
                    )
                got = got + pltpu.roll(got, 4, 0)
                mine = jnp.take_along_axis(
                    pos_tab[col, 40:48, :], atom_lane + 2 * g + (cz + 1) * 8, axis=1
                )
                gap = got - mine
                gap = gap - box * jnp.floor(gap * box_inv + 0.5)
                place.append(gap * 0.125)
            scaled = jnp.concatenate(place, axis=1)
            square = scaled * scaled
            square = square[0:1] + square[1:2] + square[2:3]
            basis = jnp.exp(-jnp.broadcast_to(square, (8, 512)) * rates)
            cell_iota = lax.broadcasted_iota(jnp.int32, (216, 512), 0)
            hots = jnp.where(cell_iota == hot, 1.0, 0.0).astype(f32)
            rhs = jnp.concatenate(
                [jnp.concatenate([hots, basis], axis=0).astype(bf16), own_hot32], axis=0
            )
            half = jnp.dot(lhs, rhs, preferred_element_type=f32)
            yield
            latent = (half + half * jnp.tanh(half)).astype(bf16)
            half = jnp.dot(pair1_w[...], latent, preferred_element_type=f32)
            yield
            second = (half + half * jnp.tanh(half)).astype(bf16)
            half = jnp.dot(pair2_w[...], second, preferred_element_type=f32)
            yield
            third = (half + half * jnp.tanh(half)).astype(bf16)

            weighted = scaled * live
            w_hi = weighted.astype(bf16).astype(f32)
            w_lo = weighted - w_hi
            parts = [live]
            for d in range(3):
                parts += [w_hi[d : d + 1], w_lo[d : d + 1]]
            spread = jnp.concatenate(
                [jnp.where(own_mask, jnp.broadcast_to(p, (8, 512)), 0.0) for p in parts]
                + [jnp.zeros((8, 512), f32)],
                axis=0,
            ).astype(bf16)
            total = lax.dot_general(spread, third, NT, preferred_element_type=f32)
            yield
            at = pl.multiple_of((col * 8 + cz) * 8, 8)
            sums[0, pl.ds(at, 8), :] = total[0:8]
            for d in range(3):
                sums[1 + d, pl.ds(at, 8), :] = (
                    total[8 + 16 * d : 16 + 16 * d] + total[16 + 16 * d : 24 + 16 * d]
                )

        running = [cell(lax.rem(index, 2) * 4 + u) for u in range(4)]
        while running:
            running = [one for one in running if next(one, 1) is None]
        return carry

    def half_columns(first, last):
        lax.fori_loop(first, last, half_column, 0)

    from_y = [
        lax.rem(iy + jnp.where(iz == 0, 3, 0), 4),
        lax.rem(iy + jnp.where(iz == 3, 1, 0), 4),
    ]
    edge = jnp.where((iz == 0) | (iz == 3), 1, 0)
    from_half = [edge, 1 - edge]

    def atom_wait(s, u):
        @pl.when((s != iz) | (from_y[u] != iy))
        def _():
            pltpu.make_async_remote_copy(
                src_ref=tx_atoms.at[0],
                dst_ref=rx_atoms.at[s * 2 + u],
                send_sem=sa,
                recv_sem=ra.at[s, u],
                device_id=(ix, from_y[u], s),
                device_id_type=MESH,
            ).wait_recv()

    y_first = iy * 16 + iz * 4

    z_ids = lax.broadcasted_iota(jnp.int32, (256, 384), 0)
    x_ids = lax.broadcasted_iota(jnp.int32, (32, 384), 0) + (ix * 24 - 1)
    lane_384 = lax.broadcasted_iota(jnp.int32, (8, 128), 1)

    def spread(source):
        low_part_, high_part_ = rx_atoms[source * 2], rx_atoms[source * 2 + 1]
        moved = pltpu.roll(high_part_, 64, 1)
        rows = jnp.concatenate(
            [
                low_part_[:, 0:128],
                jnp.where(lane_384 < 64, low_part_[:, 128:256], moved[:, 0:128]),
                moved[:, 128:256],
            ],
            axis=1,
        )
        anchor = rows[3:6].astype(jnp.int32)
        weights_z = pick_taps((z_ids - anchor[2:3]) & 255, tap_rows(rows[2:3]))
        high, low = split(weights_z)
        z_high[source] = high
        z_low[source] = low
        weights_x = pick_taps(x_ids - anchor[0:1], tap_rows(rows[0:1]))
        taps_y = tap_rows(rows[1:2])
        blocks = [
            weights_x * pick_taps((y_first + i - anchor[1:2]) & 63, taps_y) for i in range(4)
        ]
        both = jnp.concatenate(blocks, axis=0)
        stencil[source] = both
        return dot3(split(both * rows[6:7]), (high, low), NT)

    lines = None
    for steps in ((1, 3), (0, 2)):
        sources = [lax.rem(iz + step, 4) for step in steps]
        for source in sources:
            for u in range(2):
                atom_wait(source, u)
        for source in sources:
            part = spread(source)
            lines = part if lines is None else lines + part
    spectrum = dot3((bz_ref[0], bz_ref[1]), split(lines), NT)
    tx_b[...] = spectrum.reshape(16, 16, 128)
    rx_b[me] = tx_b[me]

    def exchange(tx, rx, send, recv, peer, count, mine):
        for r in range(1, count):
            other, where = peer(r)
            pltpu.make_async_remote_copy(
                src_ref=tx.at[other],
                dst_ref=rx.at[mine],
                send_sem=send,
                recv_sem=recv,
                device_id=where,
                device_id_type=MESH,
            ).start()
        whole = pltpu.make_async_remote_copy(
            src_ref=tx.at[pl.ds(0, count - 1)],
            dst_ref=rx.at[pl.ds(0, count - 1)],
            send_sem=send,
            recv_sem=recv,
            device_id=peer(1)[1],
            device_id_type=MESH,
        )
        return whole.wait_recv, whole.wait_send

    arrive_b, drain_b = exchange(tx_b, rx_b, sb, rb, yz_peer, 16, me)

    strip_lane = lax.broadcasted_iota(jnp.int32, (8, 128), 1)
    strip_cell = strip_lane // 8
    within = axis_sub * 8 + strip_lane % 8
    starts = jnp.where(strip_cell == 0, 0, jnp.where(strip_cell == 9, 0, lax.rem(strip_cell + 3, 4)))
    strip_at = jnp.where(axis_sub == 3, 127, jnp.minimum(starts * 24 + within, 127))
    strips = {}

    def lay_strips(sx):
        feat32[320 * sx : 320 * sx + 320, :] = feat_ext[sx].astype(f32).reshape(320, 128)
        for sy in range(4):
            table = jnp.zeros((8, 128), f32)
            for row, first, last in ((0, 0, 1), (1, 1, 5), (2, 5, 9), (3, 9, 10)):
                source = jnp.broadcast_to(pos_ext[sx, sy, row], (8, 128))
                moved = jnp.take_along_axis(source, strip_at, axis=1)
                table = jnp.where((strip_cell >= first) & (strip_cell < last), moved, table)
            strips[sx, sy] = table

    def lay_column(n):
        near = [strips[n // 2 + d // 3, n % 2 + d % 3] for d in range(9)]
        near += [near[4]] * 3
        for t in range(6):
            pos_tab[n, 8 * t : 8 * t + 8, :] = jnp.where(half_sub == 0, near[2 * t], near[2 * t + 1])

    for copy in halo_group(0):
        copy.wait_recv()
    for sx in (1, 2, 3):
        lay_strips(sx)
    for n in (2, 3):
        lay_column(n)
    half_columns(CUTS[0], CUTS[1])
    arrive_b()
    rows_b = rx_b.reshape(256, 128)
    columns = []
    for group in range(4):
        pieces = [rows_b[pl.ds(group * 4 + k, 16, 16), :] for k in range(4)]
        columns.append(jnp.concatenate([swap_groups(pieces, i) for i in range(4)], axis=0))
    lines_y = jnp.concatenate(columns, axis=1)
    modes_y = dot3((by_ref[0, 0], by_ref[0, 1]), split(lines_y))
    tx_c[...] = modes_y.reshape(8, 8, 512)
    rx_c[ix] = tx_c[ix]
    arrive_c, drain_c = exchange(tx_c, rx_c, sc, rc, x_peer, 8, ix)

    gain_z = gz_ref[0, pl.ds(pl.multiple_of(me * 16, 16), 16), :]
    square_z = gz_ref[1, pl.ds(pl.multiple_of(me * 16, 16), 16), :]
    gain_y = gy_ref[0, pl.ds(pl.multiple_of(ix * 8, 8), 8), :]
    square_y = gy_ref[1, pl.ds(pl.multiple_of(ix * 8, 8), 8), :]
    gain_yz = (gain_z[:, None, :] * gain_y[None, :, :]).reshape(128, 128)
    square_yz = (square_z[:, None, :] + square_y[None, :, :]).reshape(128, 128)
    greens = []
    for h in range(2):
        lanes = slice(128 * h, 128 * h + 128)
        total = square_yz + gx_ref[1, 0:1, lanes]
        value = gain_yz * gx_ref[0, 0:1, lanes] / (total + 1.0 / 1024.0)
        greens.append(jnp.where(total == 0.0, 0.0, value))
    green = jnp.concatenate(greens, axis=1)
    for copy in halo_group(1):
        copy.wait_recv()
    for sx in (0, 4):
        lay_strips(sx)
    for n in (0, 1, 4, 5):
        lay_column(n)
    half_columns(CUTS[1], CUTS[2])

    arrive_c()
    rows_x = []
    for group in range(4):
        for k in range(4):
            halves = [
                swap_groups(
                    [rx_c[4 * h + g, :, group * 128 : group * 128 + 128] for g in range(4)], k
                )
                for h in range(2)
            ]
            rows_x.append(jnp.concatenate(halves, axis=1))
    lines_x = jnp.concatenate(rows_x, axis=0)
    basis_x = (bx_ref[0], bx_ref[1])
    filtered = dot3(split(lines_x), basis_x, NT) * green
    back_x = dot3(split(filtered), basis_x)
    for g in range(8):
        half = g // 4
        for group in range(4):
            pieces = [
                back_x[(group * 4 + k) * 8 : (group * 4 + k) * 8 + 8, half * 128 : half * 128 + 128]
                for k in range(4)
            ]
            flat_c[g, :, group * 128 : group * 128 + 128] = swap_groups(pieces, g % 4)
    tx_c2[...] = flat_c[...].astype(bf16)
    rx_c2[ix] = tx_c2[ix]
    arrive_c2, drain_c2 = exchange(tx_c2, rx_c2, sc2, rc2, x_peer, 8, ix)
    half_columns(CUTS[2], CUTS[3])
    arrive_c2()
    lines_y2 = rx_c2[...].astype(f32).reshape(64, 512).astype(bf16)
    back_y = jnp.dot(by_ref[1, 0], lines_y2, preferred_element_type=f32)
    back_y = back_y + jnp.dot(by_ref[1, 1], lines_y2, preferred_element_type=f32)
    for group in range(4):
        pieces = [back_y[16 * i : 16 * i + 16, group * 128 : group * 128 + 128] for i in range(4)]
        for k in range(4):
            flat_b[pl.ds(group * 4 + k, 16, 16), :] = swap_groups(pieces, k)
    tx_b2[...] = flat_b[...].astype(bf16).reshape(16, 16, 128)
    rx_b2[me] = tx_b2[me]
    arrive_b2, drain_b2 = exchange(tx_b2, rx_b2, sb2, rb2, yz_peer, 16, me)
    half_columns(CUTS[3], CUTS[4])
    arrive_b2()
    back_z = rx_b2[...].astype(f32).reshape(256, 128).T.astype(bf16)
    lines_z = jnp.dot(back_z, bz_ref[0], preferred_element_type=f32)
    potential = split(lines_z + jnp.dot(back_z, bz_ref[1], preferred_element_type=f32))

    sampled = [dot3(potential, (z_high[n], z_low[n])) for n in range(4)]
    for n in range(4):
        total = jnp.sum(sampled[n] * stencil[n], axis=0, keepdims=True)
        parts[2 * n] = total[:, 0:256]
        tail = jnp.broadcast_to(total[:, 128:384], (8, 256))
        parts[2 * n + 1] = pltpu.roll(tail, 192, 1)[0:1]

    def part_copy(s, u):
        return pltpu.make_async_remote_copy(
            src_ref=parts.at[2 * s + u],
            dst_ref=rx_parts.at[from_half[u] * 4 + iz],
            send_sem=sp,
            recv_sem=rp,
            device_id=(ix, from_y[u], s),
            device_id_type=MESH,
        )

    for step in (2, 1, 3):
        for u in range(2):
            part_copy(lax.rem(iz + step, 4), u).start()
    for u in range(2):

        @pl.when(from_y[u] != iy)
        def _():
            part_copy(iz, u).start()

        @pl.when(from_y[u] == iy)
        def _():
            rx_parts[from_half[u] * 4 + iz] = parts[2 * iz + u]

    half_columns(CUTS[4], 12)
    wv = wv_ref[...]
    invariant = jnp.zeros((384, 128), f32)
    for d in range(3):
        t = sums[1 + d]
        hi = t.astype(bf16)
        lo = (t - hi.astype(f32)).astype(bf16)
        vec = jnp.dot(hi, wv, preferred_element_type=f32) + jnp.dot(
            lo, wv, preferred_element_type=f32
        )
        invariant = invariant + vec * vec
    update = (sums[0] * (1.0 / 64.0) + invariant * (1.0 / 64.0)).astype(bf16)
    out_ref[...] = (
        feat_ref[...].astype(f32).reshape(384, 128) + jnp.dot(update, wo_ref[...], preferred_element_type=f32)
    ).astype(bf16)

    def bulk(ref, send, recv, arriving):
        for blocks, ends in ((7, 1), (6, 0)):

            @pl.when(edge == ends)
            def _():
                whole = pltpu.make_async_remote_copy(
                    src_ref=ref.at[pl.ds(0, blocks)],
                    dst_ref=ref.at[pl.ds(0, blocks)],
                    send_sem=send,
                    recv_sem=recv,
                    device_id=yz_peer(1)[1],
                    device_id_type=MESH,
                )
                if arriving:
                    whole.wait_recv()
                else:
                    whole.wait_send()

    bulk(rx_atoms, sa, ra.at[0, 0], False)
    drain_b()
    drain_c()
    drain_c2()
    drain_b2()
    for group in range(2):
        for copy in halo_group(group):
            copy.wait_send()

    bulk(rx_parts, sp, rp, True)

    for half in range(2):
        site = (rx_parts[half * 4] + rx_parts[half * 4 + 1]) + (
            rx_parts[half * 4 + 2] + rx_parts[half * 4 + 3]
        )
        for cx in range(3):
            block = site[:, 0:128] if cx < 2 else site[:, 128:256]
            block = jnp.broadcast_to(block, (8, 128))
            at = sub_l * 8 + lane_l % 8 + 64 * (cx % 2)
            site_ref[cx, half] = jnp.take_along_axis(block, at, axis=1)[:, 0:8]

    bulk(rx_parts, sp, rp, False)


def layer(operands):
    f32, bf16 = jnp.float32, jnp.bfloat16
    vm = pl.BlockSpec(memory_space=pltpu.VMEM)
    dma = pltpu.SemaphoreType.DMA
    tables = [jnp.asarray(t) for t in ewald_tables()]
    hbm = pl.BlockSpec(memory_space=pltpu.HBM)
    specs = [hbm] * 22
    shapes = [operands[n] for n in (0, 1, 2, 3, 14, 6, 7, 8, 10, 11, 4, 5)] + tables
    shapes += [operands[n] for n in (12, 13)]
    staged = [pltpu.VMEM(x.shape, x.dtype) for x in shapes]
    return pl.pallas_call(
        layer_kernel,
        out_shape=(
            jax.ShapeDtypeStruct((384, 128), bf16),
            jax.ShapeDtypeStruct((3, 2, 8, 8), f32),
        ),
        in_specs=specs,
        out_specs=(vm, vm),
        scratch_shapes=staged
        + [
            pltpu.SMEM((2,), f32),
            pltpu.SMEM((8,), f32),
            dma((20,)),
            dma((2,)),
            pltpu.VMEM((3, 2, 4, 1, 128), f32),
            pltpu.VMEM((5, 4, 10, 8, 128), bf16),
            pltpu.VMEM((5, 4, 4, 1, 128), f32),
            pltpu.VMEM((6, 48, 128), f32),
            pltpu.VMEM((1600, 128), f32),
            pltpu.VMEM((128, 256), bf16),
            pltpu.VMEM((128, 128), bf16),
            pltpu.VMEM((128, 128), bf16),
            pltpu.VMEM((8, 512), jnp.int32),
            pltpu.VMEM((8, 512), jnp.int32),
            pltpu.VMEM((8, 512), f32),
            pltpu.VMEM((4, 384, 128), f32),
            pltpu.VMEM((2, 8, 256), f32),
            pltpu.VMEM((8, 8, 256), f32),
            pltpu.VMEM((4, 256, 384), bf16),
            pltpu.VMEM((4, 256, 384), bf16),
            pltpu.VMEM((4, 128, 384), f32),
            pltpu.VMEM((16, 16, 128), f32),
            pltpu.VMEM((16, 16, 128), f32),
            pltpu.VMEM((8, 8, 512), f32),
            pltpu.VMEM((8, 8, 512), f32),
            pltpu.VMEM((8, 8, 512), bf16),
            pltpu.VMEM((8, 8, 512), bf16),
            pltpu.VMEM((16, 16, 128), bf16),
            pltpu.VMEM((16, 16, 128), bf16),
            pltpu.VMEM((256, 128), f32),
            pltpu.VMEM((8, 8, 512), f32),
            pltpu.VMEM((8, 1, 256), f32),
            pltpu.VMEM((8, 1, 256), f32),
            pltpu.SemaphoreType.DMA,
            dma((4, 2)),
            *[pltpu.SemaphoreType.DMA] * 10,
            dma((2,)),
            dma((2,)),
            dma((2,)),
            dma((2,)),
        ],
        compiler_params=pltpu.CompilerParams(
            collective_id=0, has_side_effects=True, vmem_limit_bytes=48 * 1024 * 1024
        ),
        cost_estimate=pl.CostEstimate(flops=4 * 10**9, bytes_accessed=4 * 10**6, transcendentals=10**7),
        name="layer",
    )(*[pltpu.with_memory_space_constraint(x, pltpu.HBM) for x in (*operands, *tables)])


def shards(
    features,
    positions,
    grid_anchor,
    species,
    neighbours,
    neighbour_count,
    w_self,
    w_neighbour,
    w_radial,
    radial_rates,
    w_pair1,
    w_pair2,
    w_vector,
    w_out,
    w_charge,
    species_charge,
):
    updated, site_potential = layer(
        (
            features,
            positions,
            grid_anchor,
            species,
            neighbours,
            neighbour_count,
            w_neighbour,
            w_self,
            w_radial,
            radial_rates,
            w_pair1,
            w_pair2,
            w_vector,
            w_out,
            w_charge.reshape(1, 128),
            species_charge,
        )
    )
    return (updated.reshape(features.shape), site_potential)


def solution(mesh):
    return jax.shard_map(
        shards,
        mesh=mesh,
        in_specs=(
            P("gx", "gy", "gz", None, None),
            P("gx", "gy", "gz", None),
            P("gx", "gy", "gz", None),
            P("gx", "gy", "gz", None),
            P("gx", "gy", "gz", None),
            P("gx", "gy", "gz", None),
            P(),
            P(),
            P(),
            P(),
            P(),
            P(),
            P(),
            P(),
            P(),
            P(),
        ),
        out_specs=(P("gx", "gy", "gz", None, None), P("gx", "gy", "gz", None)),
        check_vma=False,
    )
```

```python
import jax
import jax.numpy as jnp
import numpy as np
from jax import lax
from jax.experimental import pallas as pl
from jax.experimental.pallas import tpu as pltpu
from jax.sharding import PartitionSpec as P


coulomb_scale = 0.25
smearing = 1.0


NT = (((1,), (1,)), ((), ()))
CUTS = (0, 4, 7, 9, 11)


def real_basis(length):
    modes = np.arange(length)[:, None]
    cells = np.arange(length)[None, :]
    turns = 2.0 * np.pi * ((modes * cells) % length) / length
    flipped = 2.0 * np.pi * (((length - modes) * cells) % length) / length
    return np.where(modes <= length // 2, np.cos(turns), np.sin(flipped))


def two_parts(table):
    table = np.asarray(table, np.float32)
    high = table.astype(jnp.bfloat16)
    low = (table - high.astype(np.float32)).astype(jnp.bfloat16)
    return np.stack([high, low])


def mode_tables(length):
    modes = np.arange(length)
    signed = np.where(modes > length // 2, modes - length, modes)
    wave = signed * (2.0 * np.pi / length)
    modulus = ((4.0 + 2.0 * np.cos(2.0 * np.pi * modes / length)) / 6.0) ** 2
    weight = np.where((modes == 0) | (modes == length // 2), 1.0, 2.0) / length
    return np.exp(-0.5 * smearing * smearing * wave * wave) / modulus * weight, wave * wave


def ewald_tables():
    basis_z = two_parts(real_basis(256))
    order_y = np.array([4 * p + i for i in range(4) for p in range(16)])
    forward_y = real_basis(64)[:, order_y]
    basis_y = np.stack([two_parts(forward_y), two_parts(forward_y.T)])
    wide = np.zeros((256, 256))
    full_x = real_basis(192)
    for g in range(8):
        wide[:192, 32 * g : 32 * g + 27] = full_x[:, (24 * g - 1 + np.arange(27)) % 192]
    basis_x = two_parts(wide)
    green_x = np.zeros((2, 8, 256))
    gain, square = mode_tables(192)
    green_x[0, :, :192] = gain * (coulomb_scale * 4.0 * np.pi)
    green_x[1, :, :192] = square
    green_x[1, :, 192:] = 1.0
    green_y = np.repeat(np.stack(mode_tables(64))[:, :, None], 128, 2)
    green_z = np.repeat(np.stack(mode_tables(256))[:, :, None], 128, 2)
    return (
        basis_z,
        basis_y,
        basis_x,
        green_x.astype(np.float32),
        green_y.astype(np.float32),
        green_z.astype(np.float32),
    )


def split(value):
    high = value.astype(jnp.bfloat16)
    return high, (value - high.astype(jnp.float32)).astype(jnp.bfloat16)


def dot3(a, b, dims=(((1,), (0,)), ((), ()))):
    def one(u, v):
        return lax.dot_general(u, v, dims, preferred_element_type=jnp.float32)

    rows = a[0].shape[0]
    both = one(jnp.concatenate([a[0], a[1]], axis=0), b[0])
    return both[0:rows] + (one(a[0], b[1]) + both[rows : 2 * rows])


def swap_groups(pieces, shift):
    lane = lax.broadcasted_iota(jnp.int32, pieces[0].shape, 1) // 32
    out = None
    for k, piece in enumerate(pieces):
        moved = pltpu.roll(piece, (32 * (k - shift)) % 128, 1) if k != shift else piece
        out = moved if out is None else jnp.where(lane == k, moved, out)
    return out


def tap_rows(fraction):
    square = fraction * fraction
    cube = square * fraction
    remain = 1.0 - fraction
    return (
        remain * remain * remain / 6.0,
        (3.0 * cube - 6.0 * square + 4.0) / 6.0,
        (-3.0 * cube + 3.0 * square + 3.0 * fraction + 1.0) / 6.0,
        cube / 6.0,
    )


def pick_taps(offset, taps):
    out = jnp.zeros(offset.shape, jnp.float32)
    for t in range(4):
        out = jnp.where(offset == t, taps[t], out)
    return out


def layer_kernel(
    feat_hbm,
    place_hbm,
    anchor_hbm,
    species_hbm,
    nbr_hbm,
    count_hbm,
    wn_hbm,
    ws_hbm,
    wr_hbm,
    rate_hbm,
    w1_hbm,
    w2_hbm,
    wv_hbm,
    wo_hbm,
    wc_hbm,
    kind_hbm,
    bz_hbm,
    by_hbm,
    bx_hbm,
    gx_hbm,
    gy_hbm,
    gz_hbm,
    out_ref,
    site_ref,
    feat_ref,
    place_ref,
    anchor_ref,
    species_ref,
    wc_ref,
    wn_ref,
    ws_ref,
    wr_ref,
    w1_ref,
    w2_ref,
    nbr_ref,
    count_ref,
    bz_ref,
    by_ref,
    bx_ref,
    gx_ref,
    gy_ref,
    gz_ref,
    wv_ref,
    wo_ref,
    kind_ref,
    rate_ref,
    load_sem,
    small_sem,
    pos_ref,
    feat_ext,
    pos_ext,
    pos_tab,
    feat32,
    first_w,
    pair1_w,
    pair2_w,
    hot_row,
    lane_row,
    live_row,
    sums,
    tx_atoms,
    rx_atoms,
    z_high,
    z_low,
    stencil,
    tx_b,
    rx_b,
    tx_c,
    rx_c,
    tx_c2,
    rx_c2,
    tx_b2,
    rx_b2,
    flat_b,
    flat_c,
    parts,
    rx_parts,
    sa,
    ra,
    sb,
    rb,
    sc,
    rc,
    sc2,
    rc2,
    sb2,
    rb2,
    sp,
    rp,
    sf,
    rf,
    sq,
    rq,
):
    bf16 = jnp.bfloat16
    f32 = jnp.float32
    MESH = pl.DeviceIdType.MESH
    ix, iy, iz = lax.axis_index("gx"), lax.axis_index("gy"), lax.axis_index("gz")
    me = iy * 4 + iz
    barrier = pltpu.get_barrier_semaphore()
    pairs = (
        (feat_hbm, feat_ref),
        (place_hbm, place_ref),
        (anchor_hbm, anchor_ref),
        (species_hbm, species_ref),
        (wc_hbm, wc_ref),
        (wn_hbm, wn_ref),
        (ws_hbm, ws_ref),
        (wr_hbm, wr_ref),
        (w1_hbm, w1_ref),
        (w2_hbm, w2_ref),
        (nbr_hbm, nbr_ref),
        (count_hbm, count_ref),
        (bz_hbm, bz_ref),
        (by_hbm, by_ref),
        (bx_hbm, bx_ref),
        (gx_hbm, gx_ref),
        (gy_hbm, gy_ref),
        (gz_hbm, gz_ref),
        (wv_hbm, wv_ref),
        (wo_hbm, wo_ref),
    )
    loads = [
        pltpu.make_async_copy(src, dst, load_sem.at[n]) for n, (src, dst) in enumerate(pairs)
    ]
    small = [
        pltpu.make_async_copy(kind_hbm, kind_ref, small_sem.at[0]),
        pltpu.make_async_copy(rate_hbm, rate_ref, small_sem.at[1]),
    ]
    for load in loads[:5] + small[:1]:
        load.start()

    yz_steps = [(x, c, z) for x in (1, 0) for z in (2, 1, 3, 0) for c in (1, 0)]
    x_steps = [(2, 1), (2, 0), (1, 1), (3, 1), (1, 0), (3, 0), (0, 1)]

    def yz_peer(r):
        x, c, z = yz_steps[r - 1]
        other_y = lax.rem(iy // 2 + x, 2) * 2 + lax.rem(lax.rem(iy, 2) + c, 2)
        other_z = lax.rem(iz + z, 4)
        return other_y * 4 + other_z, (ix, other_y, other_z)

    def x_peer(r):
        y, x = x_steps[r - 1]
        other = lax.rem(ix // 2 + y, 4) * 2 + lax.rem(lax.rem(ix, 2) + x, 2)
        return other, (other, iy, iz)

    for r in range(1, 16):
        pl.semaphore_signal(barrier, inc=1, device_id=yz_peer(r)[1], device_id_type=MESH)
    for r in range(1, 8):
        pl.semaphore_signal(barrier, inc=1, device_id=x_peer(r)[1], device_id_type=MESH)

    def halo_peer(index):
        ox, oy, oz = index // 9 - 1, index // 3 % 3 - 1, index % 3 - 1
        return (lax.rem(ix + ox + 8, 8), lax.rem(iy + oy + 4, 4), lax.rem(iz + oz + 4, 4))

    def halo_span(step, cells):
        if step == 0:
            return pl.ds(0, cells), pl.ds(1, cells)
        return (pl.ds(cells - 1, 1), pl.ds(0, 1)) if step > 0 else (pl.ds(0, 1), pl.ds(cells + 1, 1))

    halo_ids = [n for n in range(27) if n != 13]
    near_ids = [n for n in halo_ids if n // 9 == 1]
    far_ids = [n for n in halo_ids if n // 9 != 1]

    def halo_copies(index):
        steps = (index // 9 - 1, index // 3 % 3 - 1, index % 3 - 1)
        spans = [halo_span(step, cells) for step, cells in zip(steps, (3, 2, 8))]
        group = 0 if steps[0] == 0 else 1
        source = tuple(span[0] for span in spans)
        target = tuple(span[1] for span in spans)
        row = {0: pl.ds(1, 2), 1: pl.ds(0, 1), -1: pl.ds(3, 1)}[steps[2]]
        return [
            pltpu.make_async_remote_copy(
                src_ref=src.at[source[:2] + (from_z,)],
                dst_ref=dst.at[target[:2] + (to_z,)],
                send_sem=send.at[group],
                recv_sem=recv.at[group],
                device_id=halo_peer(index),
                device_id_type=MESH,
            )
            for src, dst, send, recv, from_z, to_z in (
                (feat_ref, feat_ext, sf, rf, source[2], target[2]),
                (pos_ref, pos_ext, sq, rq, row, row),
            )
        ]

    def halo_group(group):
        cells = (pl.ds(0, 2 if group else 3), pl.ds(0, 4), pl.ds(0, 10 if group else 6))
        rows = (pl.ds(0, 2 if group else 3), pl.ds(0, 4), pl.ds(0, 4 if group else 3))
        return [
            pltpu.make_async_remote_copy(
                src_ref=ext.at[part],
                dst_ref=ext.at[part],
                send_sem=send.at[group],
                recv_sem=recv.at[group],
                device_id=halo_peer(0),
                device_id_type=MESH,
            )
            for ext, part, send, recv in ((feat_ext, cells, sf, rf), (pos_ext, rows, sq, rq))
        ]

    for index in far_ids:
        if index % 9 != 4:
            pl.semaphore_signal(
                barrier, inc=1, device_id=halo_peer(index), device_id_type=MESH
            )

    for load in loads[:5] + small[:1]:
        load.wait()

    sub_l = lax.broadcasted_iota(jnp.int32, (8, 128), 0)
    lane_l = lax.broadcasted_iota(jnp.int32, (8, 128), 1)
    for half in range(2):
        own_rows = feat_ref[:, half].astype(f32).reshape(192, 128).astype(bf16)
        weights = jnp.broadcast_to(wc_ref[...].astype(f32), (16, 128)).astype(bf16)
        readout = lax.dot_general(weights, own_rows, NT, preferred_element_type=f32)[0:8]
        laid = []
        for cx in range(3):
            place = place_ref[cx, half]
            for row, cells in ((0, (7,)), (1, (0, 1, 2, 3)), (2, (4, 5, 6, 7)), (3, (0,))):
                pieces = [place[cz : cz + 1] for cz in cells]
                pieces.append(jnp.zeros((1, 128 - 24 * len(cells)), f32))
                pos_ref[cx, half, row] = jnp.concatenate(pieces, axis=1)
            source = jnp.concatenate(
                [
                    place,
                    anchor_ref[cx, half].astype(f32),
                    species_ref[cx, half].astype(f32),
                    jnp.zeros((8, 72), f32),
                ],
                axis=1,
            )
            rows = jnp.zeros((8, 128), f32)
            for cz in range(8):
                row = jnp.broadcast_to(source[cz : cz + 1], (8, 128))
                moved = jnp.take_along_axis(row, sub_l * 8 + lane_l % 8, axis=1)
                rows = jnp.where(lane_l // 8 == cz, moved, rows)
            laid.append(rows)
        rows = jnp.concatenate(
            [jnp.where(lane_l < 64, laid[0], pltpu.roll(laid[1], 64, 1)), laid[2]], axis=1
        )
        kinds = rows[6:7]
        base = jnp.where(kinds == 0.0, kind_ref[0], jnp.where(kinds == 1.0, kind_ref[1], 0.0))
        total = jnp.concatenate(
            [base[:, 0:192] + readout[0:1, :], jnp.zeros((1, 64), f32)], axis=1
        )
        tx_atoms[half, 0:3, :] = rows[0:3] - (rows[3:6] + 1.0)
        tx_atoms[half, 3:6, :] = rows[3:6]
        tx_atoms[half, 6:7, :] = total
        tx_atoms[half, 7:8, :] = jnp.zeros((1, 256), f32)

    pl.semaphore_wait(barrier, 38)

    routes = [(0, 3, 3, 1), (0, 0, 0, 1), (0, 1, 0, 0), (0, 2, 0, 0)]
    routes += [(1, 1, 0, 1), (1, 2, 0, 1), (1, 3, 0, 0), (1, 0, 1, 0)]

    def atom_copy(half, to_z, step_y, place):
        return pltpu.make_async_remote_copy(
            src_ref=tx_atoms.at[half],
            dst_ref=rx_atoms.at[iz * 2 + place],
            send_sem=sa,
            recv_sem=ra,
            device_id=(ix, lax.rem(iy + step_y, 4), to_z),
            device_id_type=MESH,
        )

    for half, to_z, step_y, place in routes:
        if step_y:
            atom_copy(half, to_z, step_y, place).start()
        else:

            @pl.when(iz != to_z)
            def _():
                atom_copy(half, to_z, step_y, place).start()

            @pl.when(iz == to_z)
            def _():
                rx_atoms[iz * 2 + place] = tx_atoms[half]

    for index in near_ids:
        for copy in halo_copies(index):
            copy.start()
    for index in far_ids:
        for copy in halo_copies(index):
            copy.start()
    for load in loads[5:] + small[1:]:
        load.start()
    feat_ext[1:4, 1:3, 1:9] = feat_ref[...]
    pos_ext[1:4, 1:3, 1:3] = pos_ref[:, :, 1:3]
    for load in loads[5:] + small[1:]:
        load.wait()
    first_w[:, 0:128] = (wn_ref[...].astype(f32) * 0.5).T.astype(bf16)
    first_w[:, 128:256] = (ws_ref[...].astype(f32) * 0.5).T.astype(bf16)
    pair1_w[...] = (w1_ref[...].astype(f32) * 0.5).T.astype(bf16)
    pair2_w[...] = (w2_ref[...].astype(f32) * 0.5).T.astype(bf16)
    radial_pad = jnp.concatenate(
        [jnp.zeros((88, 128), f32), wr_ref[...].astype(f32) * 0.5, jnp.zeros((32, 128), f32)], axis=0
    ).T
    cell_x0, cell_y0, cell_z0 = ix * 3, iy * 2, iz * 8

    sub8 = lax.broadcasted_iota(jnp.int32, (8, 512), 0)
    lane8 = lax.broadcasted_iota(jnp.int32, (8, 512), 1)
    rates = jnp.zeros((8, 512), f32)
    for k in range(8):
        rates = jnp.where(sub8 == k, rate_ref[k], rates)
    own_mask = (lane8 // 64) == sub8
    own_hot = jnp.where(own_mask, 1.0, 0.0).astype(f32)
    own_hot32 = jnp.concatenate([own_hot, own_hot, jnp.zeros((16, 512), f32)], axis=0).astype(bf16)
    lane_t = lax.broadcasted_iota(jnp.int32, (128, 128), 1)
    low_part = (lane_t >= 104) & (lane_t < 112)
    half_sub = sub_l // 4
    axis_sub = sub_l % 4
    box = jnp.where(axis_sub == 0, 192.0, jnp.where(axis_sub == 1, 64.0, 256.0)).astype(f32)
    box_inv = 1.0 / box
    atom_lane = lax.broadcasted_iota(jnp.int32, (8, 128), 1) // 64
    def half_column(index, carry):
        later = (index - 4) // 2
        col = jnp.where(index < 4, 2 + index // 2, jnp.where(later < 2, later, later + 2))
        cx = col // 2
        cy = lax.rem(col, 2)
        ids = nbr_ref[cx, cy]
        slot = ids & 7
        z = (ids >> 3) & 31
        y = (ids >> 8) & 7
        x = ids >> 11
        dz = (z - (cell_z0 + sub8) + 1) & 31
        dy = (y - (cell_y0 + cy) + 1) & 7
        dx = x - (cell_x0 + cx) + 1
        dx = jnp.where(dx < 0, dx + 24, dx)
        dx = jnp.where(dx >= 24, dx - 24, dx)
        strip = dx * 3 + dy
        hot_row[...] = strip * 24 + dz * 8 + slot
        lane_row[...] = ((dz + sub8) * 8 + slot) * 16 + strip
        counts = jnp.concatenate([count_ref[cx, cy], jnp.zeros((8, 120), jnp.int32)], axis=1)
        pieces = []
        for g in range(4):
            owner = atom_lane + 2 * g
            count_g = jnp.take_along_axis(counts, owner, axis=1)
            slot_g = lax.broadcasted_iota(jnp.int32, (8, 128), 1) % 64
            pieces.append(jnp.where(slot_g < count_g, 1.0, 0.0).astype(f32))
        live_row[...] = jnp.concatenate(pieces, axis=1)

        def cell(cz):
            rows = []
            for dx_ in range(3):
                for dy_ in range(3):
                    base = ((cx + dx_) * 4 + cy + dy_) * 80 + cz * 8
                    rows.append(feat32[pl.ds(pl.multiple_of(base, 8), 24), :])
            own_base = ((cx + 1) * 4 + cy + 1) * 80 + cz * 8 + 8
            own = feat32[pl.ds(pl.multiple_of(own_base, 8), 8), :]
            left = jnp.concatenate(rows + [jnp.zeros((40, 128), f32)], axis=0)
            right = jnp.concatenate(
                [jnp.zeros((224, 128), f32), own, own, jnp.zeros((16, 128), f32)], axis=0
            )
            table = jnp.concatenate([left, right], axis=1).astype(bf16)
            proj = lax.dot_general(first_w[...], table, NT, preferred_element_type=f32)
            tail = proj[:, 128:256]
            tail_hi = tail.astype(bf16).astype(f32)
            tail = jnp.where(low_part, tail - tail_hi, tail_hi) + radial_pad
            lhs = jnp.concatenate([proj[:, 0:128].astype(bf16), tail.astype(bf16)], axis=1)

            place = []
            hot = hot_row[pl.ds(cz, 1), :]
            packed = lane_row[pl.ds(cz, 1), :]
            live = live_row[pl.ds(cz, 1), :]
            for g in range(4):
                packed_g = jnp.broadcast_to(packed[:, g * 128 : g * 128 + 128], (8, 128))
                where_g = packed_g >> 4
                strip_g = packed_g & 15
                got = jnp.zeros((8, 128), f32)
                for t in range(5):
                    hit = strip_g == (2 * t + half_sub)
                    got = jnp.where(
                        hit,
                        jnp.take_along_axis(pos_tab[col, t * 8 : t * 8 + 8, :], where_g, axis=1),
                        got,
                    )
                got = got + pltpu.roll(got, 4, 0)
                mine = jnp.take_along_axis(
                    pos_tab[col, 40:48, :], atom_lane + 2 * g + (cz + 1) * 8, axis=1
                )
                gap = got - mine
                gap = gap - box * jnp.floor(gap * box_inv + 0.5)
                place.append(gap * 0.125)
            scaled = jnp.concatenate(place, axis=1)
            square = scaled * scaled
            square = square[0:1] + square[1:2] + square[2:3]
            basis = jnp.exp(-jnp.broadcast_to(square, (8, 512)) * rates)
            cell_iota = lax.broadcasted_iota(jnp.int32, (216, 512), 0)
            hots = jnp.where(cell_iota == hot, 1.0, 0.0).astype(f32)
            rhs = jnp.concatenate(
                [jnp.concatenate([hots, basis], axis=0).astype(bf16), own_hot32], axis=0
            )
            half = jnp.dot(lhs, rhs, preferred_element_type=f32)
            yield
            latent = (half + half * jnp.tanh(half)).astype(bf16)
            half = jnp.dot(pair1_w[...], latent, preferred_element_type=f32)
            yield
            second = (half + half * jnp.tanh(half)).astype(bf16)
            half = jnp.dot(pair2_w[...], second, preferred_element_type=f32)
            yield
            third = (half + half * jnp.tanh(half)).astype(bf16)

            weighted = scaled * live
            w_hi = weighted.astype(bf16).astype(f32)
            w_lo = weighted - w_hi
            parts = [live]
            for d in range(3):
                parts += [w_hi[d : d + 1], w_lo[d : d + 1]]
            spread = jnp.concatenate(
                [jnp.where(own_mask, jnp.broadcast_to(p, (8, 512)), 0.0) for p in parts]
                + [jnp.zeros((8, 512), f32)],
                axis=0,
            ).astype(bf16)
            total = lax.dot_general(spread, third, NT, preferred_element_type=f32)
            yield
            at = pl.multiple_of((col * 8 + cz) * 8, 8)
            sums[0, pl.ds(at, 8), :] = total[0:8]
            for d in range(3):
                sums[1 + d, pl.ds(at, 8), :] = (
                    total[8 + 16 * d : 16 + 16 * d] + total[16 + 16 * d : 24 + 16 * d]
                )

        running = [cell(lax.rem(index, 2) * 4 + u) for u in range(4)]
        while running:
            running = [one for one in running if next(one, 1) is None]
        return carry

    def half_columns(first, last):
        lax.fori_loop(first, last, half_column, 0)

    from_y = [
        lax.rem(iy + jnp.where(iz == 0, 3, 0), 4),
        lax.rem(iy + jnp.where(iz == 3, 1, 0), 4),
    ]
    edge = jnp.where((iz == 0) | (iz == 3), 1, 0)
    from_half = [edge, 1 - edge]

    def bulk(ref, send, recv, arriving):
        for blocks, ends in ((7, 1), (6, 0)):

            @pl.when(edge == ends)
            def _():
                whole = pltpu.make_async_remote_copy(
                    src_ref=ref.at[pl.ds(0, blocks)],
                    dst_ref=ref.at[pl.ds(0, blocks)],
                    send_sem=send,
                    recv_sem=recv,
                    device_id=yz_peer(1)[1],
                    device_id_type=MESH,
                )
                if arriving:
                    whole.wait_recv()
                else:
                    whole.wait_send()

    y_first = iy * 16 + iz * 4

    z_ids = lax.broadcasted_iota(jnp.int32, (256, 384), 0)
    x_ids = lax.broadcasted_iota(jnp.int32, (32, 384), 0) + (ix * 24 - 1)
    lane_384 = lax.broadcasted_iota(jnp.int32, (8, 128), 1)

    def spread(source):
        low_part_, high_part_ = rx_atoms[source * 2], rx_atoms[source * 2 + 1]
        moved = pltpu.roll(high_part_, 64, 1)
        rows = jnp.concatenate(
            [
                low_part_[:, 0:128],
                jnp.where(lane_384 < 64, low_part_[:, 128:256], moved[:, 0:128]),
                moved[:, 128:256],
            ],
            axis=1,
        )
        anchor = rows[3:6].astype(jnp.int32)
        weights_z = pick_taps((z_ids - anchor[2:3]) & 255, tap_rows(rows[2:3]))
        high, low = split(weights_z)
        z_high[source] = high
        z_low[source] = low
        weights_x = pick_taps(x_ids - anchor[0:1], tap_rows(rows[0:1]))
        taps_y = tap_rows(rows[1:2])
        blocks = [
            weights_x * pick_taps((y_first + i - anchor[1:2]) & 63, taps_y) for i in range(4)
        ]
        both = jnp.concatenate(blocks, axis=0)
        stencil[source] = both
        return dot3(split(both * rows[6:7]), (high, low), NT)

    bulk(rx_atoms, sa, ra, True)
    lines = None
    for steps in ((1, 3), (0, 2)):
        sources = [lax.rem(iz + step, 4) for step in steps]
        for source in sources:
            part = spread(source)
            lines = part if lines is None else lines + part
    spectrum = dot3((bz_ref[0], bz_ref[1]), split(lines), NT)
    tx_b[...] = spectrum.reshape(16, 16, 128)
    rx_b[me] = tx_b[me]

    def exchange(tx, rx, send, recv, peer, count, mine):
        for r in range(1, count):
            other, where = peer(r)
            pltpu.make_async_remote_copy(
                src_ref=tx.at[other],
                dst_ref=rx.at[mine],
                send_sem=send,
                recv_sem=recv,
                device_id=where,
                device_id_type=MESH,
            ).start()
        whole = pltpu.make_async_remote_copy(
            src_ref=tx.at[pl.ds(0, count - 1)],
            dst_ref=rx.at[pl.ds(0, count - 1)],
            send_sem=send,
            recv_sem=recv,
            device_id=peer(1)[1],
            device_id_type=MESH,
        )
        return whole.wait_recv, whole.wait_send

    arrive_b, drain_b = exchange(tx_b, rx_b, sb, rb, yz_peer, 16, me)

    strip_lane = lax.broadcasted_iota(jnp.int32, (8, 128), 1)
    strip_cell = strip_lane // 8
    within = axis_sub * 8 + strip_lane % 8
    starts = jnp.where(strip_cell == 0, 0, jnp.where(strip_cell == 9, 0, lax.rem(strip_cell + 3, 4)))
    strip_at = jnp.where(axis_sub == 3, 127, jnp.minimum(starts * 24 + within, 127))
    strips = {}

    def lay_strips(sx):
        feat32[320 * sx : 320 * sx + 320, :] = feat_ext[sx].astype(f32).reshape(320, 128)
        for sy in range(4):
            table = jnp.zeros((8, 128), f32)
            for row, first, last in ((0, 0, 1), (1, 1, 5), (2, 5, 9), (3, 9, 10)):
                source = jnp.broadcast_to(pos_ext[sx, sy, row], (8, 128))
                moved = jnp.take_along_axis(source, strip_at, axis=1)
                table = jnp.where((strip_cell >= first) & (strip_cell < last), moved, table)
            strips[sx, sy] = table

    def lay_column(n):
        near = [strips[n // 2 + d // 3, n % 2 + d % 3] for d in range(9)]
        near += [near[4]] * 3
        for t in range(6):
            pos_tab[n, 8 * t : 8 * t + 8, :] = jnp.where(half_sub == 0, near[2 * t], near[2 * t + 1])

    for copy in halo_group(0):
        copy.wait_recv()
    for sx in (1, 2, 3):
        lay_strips(sx)
    for n in (2, 3):
        lay_column(n)
    half_columns(CUTS[0], CUTS[1])
    arrive_b()
    rows_b = rx_b.reshape(256, 128)
    columns = []
    for group in range(4):
        pieces = [rows_b[pl.ds(group * 4 + k, 16, 16), :] for k in range(4)]
        columns.append(jnp.concatenate([swap_groups(pieces, i) for i in range(4)], axis=0))
    lines_y = jnp.concatenate(columns, axis=1)
    modes_y = dot3((by_ref[0, 0], by_ref[0, 1]), split(lines_y))
    tx_c[...] = modes_y.reshape(8, 8, 512)
    rx_c[ix] = tx_c[ix]
    arrive_c, drain_c = exchange(tx_c, rx_c, sc, rc, x_peer, 8, ix)

    gain_z = gz_ref[0, pl.ds(pl.multiple_of(me * 16, 16), 16), :]
    square_z = gz_ref[1, pl.ds(pl.multiple_of(me * 16, 16), 16), :]
    gain_y = gy_ref[0, pl.ds(pl.multiple_of(ix * 8, 8), 8), :]
    square_y = gy_ref[1, pl.ds(pl.multiple_of(ix * 8, 8), 8), :]
    gain_yz = (gain_z[:, None, :] * gain_y[None, :, :]).reshape(128, 128)
    square_yz = (square_z[:, None, :] + square_y[None, :, :]).reshape(128, 128)
    greens = []
    for h in range(2):
        lanes = slice(128 * h, 128 * h + 128)
        total = square_yz + gx_ref[1, 0:1, lanes]
        value = gain_yz * gx_ref[0, 0:1, lanes] / (total + 1.0 / 1024.0)
        greens.append(jnp.where(total == 0.0, 0.0, value))
    green = jnp.concatenate(greens, axis=1)
    for copy in halo_group(1):
        copy.wait_recv()
    for sx in (0, 4):
        lay_strips(sx)
    for n in (0, 1, 4, 5):
        lay_column(n)
    half_columns(CUTS[1], CUTS[2])

    arrive_c()
    rows_x = []
    for group in range(4):
        for k in range(4):
            halves = [
                swap_groups(
                    [rx_c[4 * h + g, :, group * 128 : group * 128 + 128] for g in range(4)], k
                )
                for h in range(2)
            ]
            rows_x.append(jnp.concatenate(halves, axis=1))
    lines_x = jnp.concatenate(rows_x, axis=0)
    basis_x = (bx_ref[0], bx_ref[1])
    filtered = dot3(split(lines_x), basis_x, NT) * green
    back_x = dot3(split(filtered), basis_x)
    for g in range(8):
        half = g // 4
        for group in range(4):
            pieces = [
                back_x[(group * 4 + k) * 8 : (group * 4 + k) * 8 + 8, half * 128 : half * 128 + 128]
                for k in range(4)
            ]
            flat_c[g, :, group * 128 : group * 128 + 128] = swap_groups(pieces, g % 4)
    tx_c2[...] = flat_c[...].astype(bf16)
    rx_c2[ix] = tx_c2[ix]
    arrive_c2, drain_c2 = exchange(tx_c2, rx_c2, sc2, rc2, x_peer, 8, ix)
    half_columns(CUTS[2], CUTS[3])
    arrive_c2()
    lines_y2 = rx_c2[...].astype(f32).reshape(64, 512).astype(bf16)
    back_y = jnp.dot(by_ref[1, 0], lines_y2, preferred_element_type=f32)
    back_y = back_y + jnp.dot(by_ref[1, 1], lines_y2, preferred_element_type=f32)
    for group in range(4):
        pieces = [back_y[16 * i : 16 * i + 16, group * 128 : group * 128 + 128] for i in range(4)]
        for k in range(4):
            flat_b[pl.ds(group * 4 + k, 16, 16), :] = swap_groups(pieces, k)
    tx_b2[...] = flat_b[...].astype(bf16).reshape(16, 16, 128)
    rx_b2[me] = tx_b2[me]
    arrive_b2, drain_b2 = exchange(tx_b2, rx_b2, sb2, rb2, yz_peer, 16, me)
    half_columns(CUTS[3], CUTS[4])
    arrive_b2()
    back_z = rx_b2[...].astype(f32).reshape(256, 128).T.astype(bf16)
    lines_z = jnp.dot(back_z, bz_ref[0], preferred_element_type=f32)
    potential = split(lines_z + jnp.dot(back_z, bz_ref[1], preferred_element_type=f32))

    sampled = [dot3(potential, (z_high[n], z_low[n])) for n in range(4)]
    for n in range(4):
        total = jnp.sum(sampled[n] * stencil[n], axis=0, keepdims=True)
        parts[2 * n] = total[:, 0:256]
        tail = jnp.broadcast_to(total[:, 128:384], (8, 256))
        parts[2 * n + 1] = pltpu.roll(tail, 192, 1)[0:1]

    def part_copy(s, u):
        return pltpu.make_async_remote_copy(
            src_ref=parts.at[2 * s + u],
            dst_ref=rx_parts.at[from_half[u] * 4 + iz],
            send_sem=sp,
            recv_sem=rp,
            device_id=(ix, from_y[u], s),
            device_id_type=MESH,
        )

    for s in range(4):
        for u in range(2):

            @pl.when((s != iz) | (from_y[u] != iy))
            def _():
                part_copy(s, u).start()

            @pl.when((s == iz) & (from_y[u] == iy))
            def _():
                rx_parts[from_half[u] * 4 + iz] = parts[2 * s + u]

    half_columns(CUTS[4], 12)
    wv = wv_ref[...]
    invariant = jnp.zeros((384, 128), f32)
    for d in range(3):
        t = sums[1 + d]
        hi = t.astype(bf16)
        lo = (t - hi.astype(f32)).astype(bf16)
        vec = jnp.dot(hi, wv, preferred_element_type=f32) + jnp.dot(
            lo, wv, preferred_element_type=f32
        )
        invariant = invariant + vec * vec
    update = (sums[0] * (1.0 / 64.0) + invariant * (1.0 / 64.0)).astype(bf16)
    out_ref[...] = (
        feat_ref[...].astype(f32).reshape(384, 128) + jnp.dot(update, wo_ref[...], preferred_element_type=f32)
    ).astype(bf16)

    bulk(rx_atoms, sa, ra, False)
    drain_b()
    drain_c()
    drain_c2()
    drain_b2()
    for group in range(2):
        for copy in halo_group(group):
            copy.wait_send()

    bulk(rx_parts, sp, rp, True)

    for half in range(2):
        site = (rx_parts[half * 4] + rx_parts[half * 4 + 1]) + (
            rx_parts[half * 4 + 2] + rx_parts[half * 4 + 3]
        )
        for cx in range(3):
            block = site[:, 0:128] if cx < 2 else site[:, 128:256]
            block = jnp.broadcast_to(block, (8, 128))
            at = sub_l * 8 + lane_l % 8 + 64 * (cx % 2)
            site_ref[cx, half] = jnp.take_along_axis(block, at, axis=1)[:, 0:8]

    bulk(rx_parts, sp, rp, False)


def layer(operands):
    f32, bf16 = jnp.float32, jnp.bfloat16
    vm = pl.BlockSpec(memory_space=pltpu.VMEM)
    dma = pltpu.SemaphoreType.DMA
    tables = [jnp.asarray(t) for t in ewald_tables()]
    hbm = pl.BlockSpec(memory_space=pltpu.HBM)
    specs = [hbm] * 22
    shapes = [operands[n] for n in (0, 1, 2, 3, 14, 6, 7, 8, 10, 11, 4, 5)] + tables
    shapes += [operands[n] for n in (12, 13)]
    staged = [pltpu.VMEM(x.shape, x.dtype) for x in shapes]
    return pl.pallas_call(
        layer_kernel,
        out_shape=(
            jax.ShapeDtypeStruct((384, 128), bf16),
            jax.ShapeDtypeStruct((3, 2, 8, 8), f32),
        ),
        in_specs=specs,
        out_specs=(vm, vm),
        scratch_shapes=staged
        + [
            pltpu.SMEM((2,), f32),
            pltpu.SMEM((8,), f32),
            dma((20,)),
            dma((2,)),
            pltpu.VMEM((3, 2, 4, 1, 128), f32),
            pltpu.VMEM((5, 4, 10, 8, 128), bf16),
            pltpu.VMEM((5, 4, 4, 1, 128), f32),
            pltpu.VMEM((6, 48, 128), f32),
            pltpu.VMEM((1600, 128), f32),
            pltpu.VMEM((128, 256), bf16),
            pltpu.VMEM((128, 128), bf16),
            pltpu.VMEM((128, 128), bf16),
            pltpu.VMEM((8, 512), jnp.int32),
            pltpu.VMEM((8, 512), jnp.int32),
            pltpu.VMEM((8, 512), f32),
            pltpu.VMEM((4, 384, 128), f32),
            pltpu.VMEM((2, 8, 256), f32),
            pltpu.VMEM((8, 8, 256), f32),
            pltpu.VMEM((4, 256, 384), bf16),
            pltpu.VMEM((4, 256, 384), bf16),
            pltpu.VMEM((4, 128, 384), f32),
            pltpu.VMEM((16, 16, 128), f32),
            pltpu.VMEM((16, 16, 128), f32),
            pltpu.VMEM((8, 8, 512), f32),
            pltpu.VMEM((8, 8, 512), f32),
            pltpu.VMEM((8, 8, 512), bf16),
            pltpu.VMEM((8, 8, 512), bf16),
            pltpu.VMEM((16, 16, 128), bf16),
            pltpu.VMEM((16, 16, 128), bf16),
            pltpu.VMEM((256, 128), f32),
            pltpu.VMEM((8, 8, 512), f32),
            pltpu.VMEM((8, 1, 256), f32),
            pltpu.VMEM((8, 1, 256), f32),
            pltpu.SemaphoreType.DMA,
            pltpu.SemaphoreType.DMA,
            *[pltpu.SemaphoreType.DMA] * 10,
            dma((2,)),
            dma((2,)),
            dma((2,)),
            dma((2,)),
        ],
        compiler_params=pltpu.CompilerParams(
            collective_id=0, has_side_effects=True, vmem_limit_bytes=48 * 1024 * 1024
        ),
        cost_estimate=pl.CostEstimate(flops=4 * 10**9, bytes_accessed=4 * 10**6, transcendentals=10**7),
        name="layer",
    )(*[pltpu.with_memory_space_constraint(x, pltpu.HBM) for x in (*operands, *tables)])


def shards(
    features,
    positions,
    grid_anchor,
    species,
    neighbours,
    neighbour_count,
    w_self,
    w_neighbour,
    w_radial,
    radial_rates,
    w_pair1,
    w_pair2,
    w_vector,
    w_out,
    w_charge,
    species_charge,
):
    updated, site_potential = layer(
        (
            features,
            positions,
            grid_anchor,
            species,
            neighbours,
            neighbour_count,
            w_neighbour,
            w_self,
            w_radial,
            radial_rates,
            w_pair1,
            w_pair2,
            w_vector,
            w_out,
            w_charge.reshape(1, 128),
            species_charge,
        )
    )
    return (updated.reshape(features.shape), site_potential)


def solution(mesh):
    return jax.shard_map(
        shards,
        mesh=mesh,
        in_specs=(
            P("gx", "gy", "gz", None, None),
            P("gx", "gy", "gz", None),
            P("gx", "gy", "gz", None),
            P("gx", "gy", "gz", None),
            P("gx", "gy", "gz", None),
            P("gx", "gy", "gz", None),
            P(),
            P(),
            P(),
            P(),
            P(),
            P(),
            P(),
            P(),
            P(),
            P(),
        ),
        out_specs=(P("gx", "gy", "gz", None, None), P("gx", "gy", "gz", None)),
        check_vma=False,
    )
```

```python
import jax
import jax.numpy as jnp
import numpy as np
from jax import lax
from jax.experimental import pallas as pl
from jax.experimental.pallas import tpu as pltpu
from jax.sharding import PartitionSpec as P


coulomb_scale = 0.25
smearing = 1.0


NT = (((1,), (1,)), ((), ()))
CUTS = (0, 4, 6, 8, 11)


def real_basis(length):
    modes = np.arange(length)[:, None]
    cells = np.arange(length)[None, :]
    turns = 2.0 * np.pi * ((modes * cells) % length) / length
    flipped = 2.0 * np.pi * (((length - modes) * cells) % length) / length
    return np.where(modes <= length // 2, np.cos(turns), np.sin(flipped))


def two_parts(table):
    table = np.asarray(table, np.float32)
    high = table.astype(jnp.bfloat16)
    low = (table - high.astype(np.float32)).astype(jnp.bfloat16)
    return np.stack([high, low])


def mode_tables(length):
    modes = np.arange(length)
    signed = np.where(modes > length // 2, modes - length, modes)
    wave = signed * (2.0 * np.pi / length)
    modulus = ((4.0 + 2.0 * np.cos(2.0 * np.pi * modes / length)) / 6.0) ** 2
    weight = np.where((modes == 0) | (modes == length // 2), 1.0, 2.0) / length
    return np.exp(-0.5 * smearing * smearing * wave * wave) / modulus * weight, wave * wave


def ewald_tables():
    basis_z = two_parts(real_basis(256))
    order_y = np.array([4 * p + i for i in range(4) for p in range(16)])
    forward_y = real_basis(64)[:, order_y]
    basis_y = np.stack([two_parts(forward_y), two_parts(forward_y.T)])
    wide = np.zeros((256, 256))
    full_x = real_basis(192)
    for g in range(8):
        wide[:192, 32 * g : 32 * g + 27] = full_x[:, (24 * g - 1 + np.arange(27)) % 192]
    basis_x = two_parts(wide)
    green_x = np.zeros((2, 8, 256))
    gain, square = mode_tables(192)
    green_x[0, :, :192] = gain * (coulomb_scale * 4.0 * np.pi)
    green_x[1, :, :192] = square
    green_x[1, :, 192:] = 1.0
    green_y = np.repeat(np.stack(mode_tables(64))[:, :, None], 128, 2)
    green_z = np.repeat(np.stack(mode_tables(256))[:, :, None], 128, 2)
    return (
        basis_z,
        basis_y,
        basis_x,
        green_x.astype(np.float32),
        green_y.astype(np.float32),
        green_z.astype(np.float32),
    )


def split(value):
    high = value.astype(jnp.bfloat16)
    return high, (value - high.astype(jnp.float32)).astype(jnp.bfloat16)


def dot3(a, b, dims=(((1,), (0,)), ((), ()))):
    def one(u, v):
        return lax.dot_general(u, v, dims, preferred_element_type=jnp.float32)

    rows = a[0].shape[0]
    both = one(jnp.concatenate([a[0], a[1]], axis=0), b[0])
    return both[0:rows] + (one(a[0], b[1]) + both[rows : 2 * rows])


def swap_groups(pieces, shift):
    lane = lax.broadcasted_iota(jnp.int32, pieces[0].shape, 1) // 32
    out = None
    for k, piece in enumerate(pieces):
        moved = pltpu.roll(piece, (32 * (k - shift)) % 128, 1) if k != shift else piece
        out = moved if out is None else jnp.where(lane == k, moved, out)
    return out


def tap_rows(fraction):
    square = fraction * fraction
    cube = square * fraction
    remain = 1.0 - fraction
    return (
        remain * remain * remain / 6.0,
        (3.0 * cube - 6.0 * square + 4.0) / 6.0,
        (-3.0 * cube + 3.0 * square + 3.0 * fraction + 1.0) / 6.0,
        cube / 6.0,
    )


def pick_taps(offset, taps):
    out = jnp.zeros(offset.shape, jnp.float32)
    for t in range(4):
        out = jnp.where(offset == t, taps[t], out)
    return out


def layer_kernel(
    feat_hbm,
    place_hbm,
    anchor_hbm,
    species_hbm,
    nbr_hbm,
    count_hbm,
    wn_hbm,
    ws_hbm,
    wr_hbm,
    rate_hbm,
    w1_hbm,
    w2_hbm,
    wv_hbm,
    wo_hbm,
    wc_hbm,
    kind_hbm,
    bz_hbm,
    by_hbm,
    bx_hbm,
    gx_hbm,
    gy_hbm,
    gz_hbm,
    out_ref,
    site_ref,
    feat_ref,
    place_ref,
    anchor_ref,
    species_ref,
    wc_ref,
    wn_ref,
    ws_ref,
    wr_ref,
    w1_ref,
    w2_ref,
    nbr_ref,
    count_ref,
    bz_ref,
    by_ref,
    bx_ref,
    gx_ref,
    gy_ref,
    gz_ref,
    wv_ref,
    wo_ref,
    kind_ref,
    rate_ref,
    load_sem,
    small_sem,
    pos_ref,
    feat_ext,
    pos_ext,
    pos_tab,
    feat32,
    first_w,
    pair1_w,
    pair2_w,
    hot_row,
    lane_row,
    live_row,
    sums,
    tx_atoms,
    rx_atoms,
    z_high,
    z_low,
    stencil,
    tx_b,
    rx_b,
    tx_c,
    rx_c,
    tx_c2,
    rx_c2,
    tx_b2,
    rx_b2,
    flat_b,
    flat_c,
    parts,
    rx_parts,
    sa,
    ra,
    sb,
    rb,
    sc,
    rc,
    sc2,
    rc2,
    sb2,
    rb2,
    sp,
    rp,
    sf,
    rf,
    sq,
    rq,
):
    bf16 = jnp.bfloat16
    f32 = jnp.float32
    MESH = pl.DeviceIdType.MESH
    ix, iy, iz = lax.axis_index("gx"), lax.axis_index("gy"), lax.axis_index("gz")
    me = iy * 4 + iz
    barrier = pltpu.get_barrier_semaphore()
    pairs = (
        (feat_hbm, feat_ref),
        (place_hbm, place_ref),
        (anchor_hbm, anchor_ref),
        (species_hbm, species_ref),
        (wc_hbm, wc_ref),
        (wn_hbm, wn_ref),
        (ws_hbm, ws_ref),
        (wr_hbm, wr_ref),
        (w1_hbm, w1_ref),
        (w2_hbm, w2_ref),
        (nbr_hbm, nbr_ref),
        (count_hbm, count_ref),
        (bz_hbm, bz_ref),
        (by_hbm, by_ref),
        (bx_hbm, bx_ref),
        (gx_hbm, gx_ref),
        (gy_hbm, gy_ref),
        (gz_hbm, gz_ref),
        (wv_hbm, wv_ref),
        (wo_hbm, wo_ref),
    )
    loads = [
        pltpu.make_async_copy(src, dst, load_sem.at[n]) for n, (src, dst) in enumerate(pairs)
    ]
    small = [
        pltpu.make_async_copy(kind_hbm, kind_ref, small_sem.at[0]),
        pltpu.make_async_copy(rate_hbm, rate_ref, small_sem.at[1]),
    ]

    yz_steps = [(x, c, z) for x in (1, 0) for z in (2, 1, 3, 0) for c in (1, 0)]
    x_steps = [(2, 1), (2, 0), (1, 1), (3, 1), (1, 0), (3, 0), (0, 1)]

    def yz_peer(r):
        x, c, z = yz_steps[r - 1]
        other_y = lax.rem(iy // 2 + x, 2) * 2 + lax.rem(lax.rem(iy, 2) + c, 2)
        other_z = lax.rem(iz + z, 4)
        return other_y * 4 + other_z, (ix, other_y, other_z)

    def x_peer(r):
        y, x = x_steps[r - 1]
        other = lax.rem(ix // 2 + y, 4) * 2 + lax.rem(lax.rem(ix, 2) + x, 2)
        return other, (other, iy, iz)

    for r in range(1, 16):
        pl.semaphore_signal(barrier, inc=1, device_id=yz_peer(r)[1], device_id_type=MESH)
    for r in range(1, 8):
        pl.semaphore_signal(barrier, inc=1, device_id=x_peer(r)[1], device_id_type=MESH)

    def halo_peer(index):
        ox, oy, oz = index // 9 - 1, index // 3 % 3 - 1, index % 3 - 1
        return (lax.rem(ix + ox + 8, 8), lax.rem(iy + oy + 4, 4), lax.rem(iz + oz + 4, 4))

    def halo_span(step, cells):
        if step == 0:
            return pl.ds(0, cells), pl.ds(1, cells)
        return (pl.ds(cells - 1, 1), pl.ds(0, 1)) if step > 0 else (pl.ds(0, 1), pl.ds(cells + 1, 1))

    halo_ids = [n for n in range(27) if n != 13]
    near_ids = [n for n in halo_ids if n // 9 == 1]
    far_ids = [n for n in halo_ids if n // 9 != 1]

    def halo_copies(index):
        steps = (index // 9 - 1, index // 3 % 3 - 1, index % 3 - 1)
        spans = [halo_span(step, cells) for step, cells in zip(steps, (3, 2, 8))]
        group = 0 if steps[0] == 0 else 1
        source = tuple(span[0] for span in spans)
        target = tuple(span[1] for span in spans)
        row = {0: pl.ds(1, 2), 1: pl.ds(0, 1), -1: pl.ds(3, 1)}[steps[2]]
        return [
            pltpu.make_async_remote_copy(
                src_ref=src.at[source[:2] + (from_z,)],
                dst_ref=dst.at[target[:2] + (to_z,)],
                send_sem=send.at[group],
                recv_sem=recv.at[group],
                device_id=halo_peer(index),
                device_id_type=MESH,
            )
            for src, dst, send, recv, from_z, to_z in (
                (feat_ref, feat_ext, sf, rf, source[2], target[2]),
                (pos_ref, pos_ext, sq, rq, row, row),
            )
        ]

    def halo_group(group):
        cells = (pl.ds(0, 2 if group else 3), pl.ds(0, 4), pl.ds(0, 10 if group else 6))
        rows = (pl.ds(0, 2 if group else 3), pl.ds(0, 4), pl.ds(0, 4 if group else 3))
        return [
            pltpu.make_async_remote_copy(
                src_ref=ext.at[part],
                dst_ref=ext.at[part],
                send_sem=send.at[group],
                recv_sem=recv.at[group],
                device_id=halo_peer(0),
                device_id_type=MESH,
            )
            for ext, part, send, recv in ((feat_ext, cells, sf, rf), (pos_ext, rows, sq, rq))
        ]

    for load in loads[:5] + small[:1]:
        load.start()
    for index in far_ids:
        if index % 9 != 4:
            pl.semaphore_signal(
                barrier, inc=1, device_id=halo_peer(index), device_id_type=MESH
            )

    for load in loads[:5] + small[:1]:
        load.wait()

    sub_l = lax.broadcasted_iota(jnp.int32, (8, 128), 0)
    lane_l = lax.broadcasted_iota(jnp.int32, (8, 128), 1)
    for half in range(2):
        own_rows = feat_ref[:, half].astype(f32).reshape(192, 128).astype(bf16)
        weights = jnp.broadcast_to(wc_ref[...].astype(f32), (16, 128)).astype(bf16)
        readout = lax.dot_general(weights, own_rows, NT, preferred_element_type=f32)[0:8]
        laid = []
        for cx in range(3):
            place = place_ref[cx, half]
            for row, cells in ((0, (7,)), (1, (0, 1, 2, 3)), (2, (4, 5, 6, 7)), (3, (0,))):
                pieces = [place[cz : cz + 1] for cz in cells]
                pieces.append(jnp.zeros((1, 128 - 24 * len(cells)), f32))
                pos_ref[cx, half, row] = jnp.concatenate(pieces, axis=1)
            source = jnp.concatenate(
                [
                    place,
                    anchor_ref[cx, half].astype(f32),
                    species_ref[cx, half].astype(f32),
                    jnp.zeros((8, 72), f32),
                ],
                axis=1,
            )
            rows = jnp.zeros((8, 128), f32)
            for cz in range(8):
                row = jnp.broadcast_to(source[cz : cz + 1], (8, 128))
                moved = jnp.take_along_axis(row, sub_l * 8 + lane_l % 8, axis=1)
                rows = jnp.where(lane_l // 8 == cz, moved, rows)
            laid.append(rows)
        rows = jnp.concatenate(
            [jnp.where(lane_l < 64, laid[0], pltpu.roll(laid[1], 64, 1)), laid[2]], axis=1
        )
        kinds = rows[6:7]
        base = jnp.where(kinds == 0.0, kind_ref[0], jnp.where(kinds == 1.0, kind_ref[1], 0.0))
        total = jnp.concatenate(
            [base[:, 0:192] + readout[0:1, :], jnp.zeros((1, 64), f32)], axis=1
        )
        tx_atoms[half, 0:3, :] = rows[0:3] - (rows[3:6] + 1.0)
        tx_atoms[half, 3:6, :] = rows[3:6]
        tx_atoms[half, 6:7, :] = total
        tx_atoms[half, 7:8, :] = jnp.zeros((1, 256), f32)

    pl.semaphore_wait(barrier, 38)

    routes = [(0, 3, 3, 1), (0, 0, 0, 1), (0, 1, 0, 0), (0, 2, 0, 0)]
    routes += [(1, 1, 0, 1), (1, 2, 0, 1), (1, 3, 0, 0), (1, 0, 1, 0)]

    def atom_copy(half, to_z, step_y, place):
        return pltpu.make_async_remote_copy(
            src_ref=tx_atoms.at[half],
            dst_ref=rx_atoms.at[iz * 2 + place],
            send_sem=sa,
            recv_sem=ra,
            device_id=(ix, lax.rem(iy + step_y, 4), to_z),
            device_id_type=MESH,
        )

    for half, to_z, step_y, place in routes:
        if step_y:
            atom_copy(half, to_z, step_y, place).start()
        else:

            @pl.when(iz != to_z)
            def _():
                atom_copy(half, to_z, step_y, place).start()

            @pl.when(iz == to_z)
            def _():
                rx_atoms[iz * 2 + place] = tx_atoms[half]

    for index in near_ids:
        for copy in halo_copies(index):
            copy.start()
    for index in far_ids:
        for copy in halo_copies(index):
            copy.start()
    for load in loads[5:] + small[1:]:
        load.start()
    feat_ext[1:4, 1:3, 1:9] = feat_ref[...]
    pos_ext[1:4, 1:3, 1:3] = pos_ref[:, :, 1:3]
    for load in loads[5:] + small[1:]:
        load.wait()
    first_w[:, 0:128] = (wn_ref[...].astype(f32) * 0.5).T.astype(bf16)
    first_w[:, 128:256] = (ws_ref[...].astype(f32) * 0.5).T.astype(bf16)
    pair1_w[...] = (w1_ref[...].astype(f32) * 0.5).T.astype(bf16)
    pair2_w[...] = (w2_ref[...].astype(f32) * 0.5).T.astype(bf16)
    radial_pad = jnp.concatenate(
        [jnp.zeros((88, 128), f32), wr_ref[...].astype(f32) * 0.5, jnp.zeros((32, 128), f32)], axis=0
    ).T
    cell_x0, cell_y0, cell_z0 = ix * 3, iy * 2, iz * 8

    sub8 = lax.broadcasted_iota(jnp.int32, (8, 512), 0)
    lane8 = lax.broadcasted_iota(jnp.int32, (8, 512), 1)
    rates = jnp.zeros((8, 512), f32)
    for k in range(8):
        rates = jnp.where(sub8 == k, rate_ref[k], rates)
    own_mask = (lane8 // 64) == sub8
    own_hot = jnp.where(own_mask, 1.0, 0.0).astype(f32)
    own_hot32 = jnp.concatenate([own_hot, own_hot, jnp.zeros((16, 512), f32)], axis=0).astype(bf16)
    lane_t = lax.broadcasted_iota(jnp.int32, (128, 128), 1)
    low_part = (lane_t >= 104) & (lane_t < 112)
    half_sub = sub_l // 4
    axis_sub = sub_l % 4
    box = jnp.where(axis_sub == 0, 192.0, jnp.where(axis_sub == 1, 64.0, 256.0)).astype(f32)
    box_inv = 1.0 / box
    atom_lane = lax.broadcasted_iota(jnp.int32, (8, 128), 1) // 64
    def half_column(index, carry):
        later = (index - 4) // 2
        col = jnp.where(index < 4, 2 + index // 2, jnp.where(later < 2, later, later + 2))
        cx = col // 2
        cy = lax.rem(col, 2)
        ids = nbr_ref[cx, cy]
        slot = ids & 7
        z = (ids >> 3) & 31
        y = (ids >> 8) & 7
        x = ids >> 11
        dz = (z - (cell_z0 + sub8) + 1) & 31
        dy = (y - (cell_y0 + cy) + 1) & 7
        dx = x - (cell_x0 + cx) + 1
        dx = jnp.where(dx < 0, dx + 24, dx)
        dx = jnp.where(dx >= 24, dx - 24, dx)
        strip = dx * 3 + dy
        hot_row[...] = strip * 24 + dz * 8 + slot
        lane_row[...] = ((dz + sub8) * 8 + slot) * 16 + strip
        counts = jnp.concatenate([count_ref[cx, cy], jnp.zeros((8, 120), jnp.int32)], axis=1)
        pieces = []
        for g in range(4):
            owner = atom_lane + 2 * g
            count_g = jnp.take_along_axis(counts, owner, axis=1)
            slot_g = lax.broadcasted_iota(jnp.int32, (8, 128), 1) % 64
            pieces.append(jnp.where(slot_g < count_g, 1.0, 0.0).astype(f32))
        live_row[...] = jnp.concatenate(pieces, axis=1)

        def cell(cz):
            rows = []
            for dx_ in range(3):
                for dy_ in range(3):
                    base = ((cx + dx_) * 4 + cy + dy_) * 80 + cz * 8
                    rows.append(feat32[pl.ds(pl.multiple_of(base, 8), 24), :])
            own_base = ((cx + 1) * 4 + cy + 1) * 80 + cz * 8 + 8
            own = feat32[pl.ds(pl.multiple_of(own_base, 8), 8), :]
            left = jnp.concatenate(rows + [jnp.zeros((40, 128), f32)], axis=0)
            right = jnp.concatenate(
                [jnp.zeros((224, 128), f32), own, own, jnp.zeros((16, 128), f32)], axis=0
            )
            table = jnp.concatenate([left, right], axis=1).astype(bf16)
            proj = lax.dot_general(first_w[...], table, NT, preferred_element_type=f32)
            tail = proj[:, 128:256]
            tail_hi = tail.astype(bf16).astype(f32)
            tail = jnp.where(low_part, tail - tail_hi, tail_hi) + radial_pad
            lhs = jnp.concatenate([proj[:, 0:128].astype(bf16), tail.astype(bf16)], axis=1)

            place = []
            hot = hot_row[pl.ds(cz, 1), :]
            packed = lane_row[pl.ds(cz, 1), :]
            live = live_row[pl.ds(cz, 1), :]
            for g in range(4):
                packed_g = jnp.broadcast_to(packed[:, g * 128 : g * 128 + 128], (8, 128))
                where_g = packed_g >> 4
                strip_g = packed_g & 15
                got = jnp.zeros((8, 128), f32)
                for t in range(5):
                    hit = strip_g == (2 * t + half_sub)
                    got = jnp.where(
                        hit,
                        jnp.take_along_axis(pos_tab[col, t * 8 : t * 8 + 8, :], where_g, axis=1),
                        got,
                    )
                got = got + pltpu.roll(got, 4, 0)
                mine = jnp.take_along_axis(
                    pos_tab[col, 40:48, :], atom_lane + 2 * g + (cz + 1) * 8, axis=1
                )
                gap = got - mine
                gap = gap - box * jnp.floor(gap * box_inv + 0.5)
                place.append(gap * 0.125)
            scaled = jnp.concatenate(place, axis=1)
            square = scaled * scaled
            square = square[0:1] + square[1:2] + square[2:3]
            basis = jnp.exp(-jnp.broadcast_to(square, (8, 512)) * rates)
            cell_iota = lax.broadcasted_iota(jnp.int32, (216, 512), 0)
            hots = jnp.where(cell_iota == hot, 1.0, 0.0).astype(f32)
            rhs = jnp.concatenate(
                [jnp.concatenate([hots, basis], axis=0).astype(bf16), own_hot32], axis=0
            )
            half = jnp.dot(lhs, rhs, preferred_element_type=f32)
            yield
            latent = (half + half * jnp.tanh(half)).astype(bf16)
            half = jnp.dot(pair1_w[...], latent, preferred_element_type=f32)
            yield
            second = (half + half * jnp.tanh(half)).astype(bf16)
            half = jnp.dot(pair2_w[...], second, preferred_element_type=f32)
            yield
            third = (half + half * jnp.tanh(half)).astype(bf16)

            weighted = scaled * live
            w_hi = weighted.astype(bf16).astype(f32)
            w_lo = weighted - w_hi
            parts = [live]
            for d in range(3):
                parts += [w_hi[d : d + 1], w_lo[d : d + 1]]
            spread = jnp.concatenate(
                [jnp.where(own_mask, jnp.broadcast_to(p, (8, 512)), 0.0) for p in parts]
                + [jnp.zeros((8, 512), f32)],
                axis=0,
            ).astype(bf16)
            total = lax.dot_general(spread, third, NT, preferred_element_type=f32)
            yield
            at = pl.multiple_of((col * 8 + cz) * 8, 8)
            sums[0, pl.ds(at, 8), :] = total[0:8]
            for d in range(3):
                sums[1 + d, pl.ds(at, 8), :] = (
                    total[8 + 16 * d : 16 + 16 * d] + total[16 + 16 * d : 24 + 16 * d]
                )

        running = [cell(lax.rem(index, 2) * 4 + u) for u in range(4)]
        while running:
            running = [one for one in running if next(one, 1) is None]
        return carry

    def half_columns(first, last):
        lax.fori_loop(first, last, half_column, 0)

    from_y = [
        lax.rem(iy + jnp.where(iz == 0, 3, 0), 4),
        lax.rem(iy + jnp.where(iz == 3, 1, 0), 4),
    ]
    edge = jnp.where((iz == 0) | (iz == 3), 1, 0)
    from_half = [edge, 1 - edge]

    def bulk(ref, send, recv, arriving):
        for blocks, ends in ((7, 1), (6, 0)):

            @pl.when(edge == ends)
            def _():
                whole = pltpu.make_async_remote_copy(
                    src_ref=ref.at[pl.ds(0, blocks)],
                    dst_ref=ref.at[pl.ds(0, blocks)],
                    send_sem=send,
                    recv_sem=recv,
                    device_id=yz_peer(1)[1],
                    device_id_type=MESH,
                )
                if arriving:
                    whole.wait_recv()
                else:
                    whole.wait_send()

    y_first = iy * 16 + iz * 4

    z_ids = lax.broadcasted_iota(jnp.int32, (256, 384), 0)
    x_ids = lax.broadcasted_iota(jnp.int32, (32, 384), 0) + (ix * 24 - 1)
    lane_384 = lax.broadcasted_iota(jnp.int32, (8, 128), 1)

    def spread(source):
        low_part_, high_part_ = rx_atoms[source * 2], rx_atoms[source * 2 + 1]
        moved = pltpu.roll(high_part_, 64, 1)
        rows = jnp.concatenate(
            [
                low_part_[:, 0:128],
                jnp.where(lane_384 < 64, low_part_[:, 128:256], moved[:, 0:128]),
                moved[:, 128:256],
            ],
            axis=1,
        )
        anchor = rows[3:6].astype(jnp.int32)
        weights_z = pick_taps((z_ids - anchor[2:3]) & 255, tap_rows(rows[2:3]))
        high, low = split(weights_z)
        z_high[source] = high
        z_low[source] = low
        weights_x = pick_taps(x_ids - anchor[0:1], tap_rows(rows[0:1]))
        taps_y = tap_rows(rows[1:2])
        blocks = [
            weights_x * pick_taps((y_first + i - anchor[1:2]) & 63, taps_y) for i in range(4)
        ]
        both = jnp.concatenate(blocks, axis=0)
        stencil[source] = both
        return dot3(split(both * rows[6:7]), (high, low), NT)

    bulk(rx_atoms, sa, ra, True)
    lines = None
    for steps in ((1, 3), (0, 2)):
        sources = [lax.rem(iz + step, 4) for step in steps]
        for source in sources:
            part = spread(source)
            lines = part if lines is None else lines + part
    spectrum = dot3((bz_ref[0], bz_ref[1]), split(lines), NT)
    tx_b[...] = spectrum.reshape(16, 16, 128)
    rx_b[me] = tx_b[me]

    def exchange(tx, rx, send, recv, peer, count, mine):
        for r in range(1, count):
            other, where = peer(r)
            pltpu.make_async_remote_copy(
                src_ref=tx.at[other],
                dst_ref=rx.at[mine],
                send_sem=send,
                recv_sem=recv,
                device_id=where,
                device_id_type=MESH,
            ).start()
        whole = pltpu.make_async_remote_copy(
            src_ref=tx.at[pl.ds(0, count - 1)],
            dst_ref=rx.at[pl.ds(0, count - 1)],
            send_sem=send,
            recv_sem=recv,
            device_id=peer(1)[1],
            device_id_type=MESH,
        )
        return whole.wait_recv, whole.wait_send

    arrive_b, drain_b = exchange(tx_b, rx_b, sb, rb, yz_peer, 16, me)

    strip_lane = lax.broadcasted_iota(jnp.int32, (8, 128), 1)
    strip_cell = strip_lane // 8
    within = axis_sub * 8 + strip_lane % 8
    starts = jnp.where(strip_cell == 0, 0, jnp.where(strip_cell == 9, 0, lax.rem(strip_cell + 3, 4)))
    strip_at = jnp.where(axis_sub == 3, 127, jnp.minimum(starts * 24 + within, 127))
    strips = {}

    def lay_strips(sx):
        feat32[320 * sx : 320 * sx + 320, :] = feat_ext[sx].astype(f32).reshape(320, 128)
        for sy in range(4):
            table = jnp.zeros((8, 128), f32)
            for row, first, last in ((0, 0, 1), (1, 1, 5), (2, 5, 9), (3, 9, 10)):
                source = jnp.broadcast_to(pos_ext[sx, sy, row], (8, 128))
                moved = jnp.take_along_axis(source, strip_at, axis=1)
                table = jnp.where((strip_cell >= first) & (strip_cell < last), moved, table)
            strips[sx, sy] = table

    def lay_column(n):
        near = [strips[n // 2 + d // 3, n % 2 + d % 3] for d in range(9)]
        near += [near[4]] * 3
        for t in range(6):
            pos_tab[n, 8 * t : 8 * t + 8, :] = jnp.where(half_sub == 0, near[2 * t], near[2 * t + 1])

    for copy in halo_group(0):
        copy.wait_recv()
    for sx in (1, 2, 3):
        lay_strips(sx)
    for n in (2, 3):
        lay_column(n)
    half_columns(CUTS[0], CUTS[1])
    arrive_b()
    rows_b = rx_b.reshape(256, 128)
    columns = []
    for group in range(4):
        pieces = [rows_b[pl.ds(group * 4 + k, 16, 16), :] for k in range(4)]
        columns.append(jnp.concatenate([swap_groups(pieces, i) for i in range(4)], axis=0))
    lines_y = jnp.concatenate(columns, axis=1)
    modes_y = dot3((by_ref[0, 0], by_ref[0, 1]), split(lines_y))
    tx_c[...] = modes_y.reshape(8, 8, 512)
    rx_c[ix] = tx_c[ix]
    arrive_c, drain_c = exchange(tx_c, rx_c, sc, rc, x_peer, 8, ix)

    gain_z = gz_ref[0, pl.ds(pl.multiple_of(me * 16, 16), 16), :]
    square_z = gz_ref[1, pl.ds(pl.multiple_of(me * 16, 16), 16), :]
    gain_y = gy_ref[0, pl.ds(pl.multiple_of(ix * 8, 8), 8), :]
    square_y = gy_ref[1, pl.ds(pl.multiple_of(ix * 8, 8), 8), :]
    gain_yz = (gain_z[:, None, :] * gain_y[None, :, :]).reshape(128, 128)
    square_yz = (square_z[:, None, :] + square_y[None, :, :]).reshape(128, 128)
    greens = []
    for h in range(2):
        lanes = slice(128 * h, 128 * h + 128)
        total = square_yz + gx_ref[1, 0:1, lanes]
        value = gain_yz * gx_ref[0, 0:1, lanes] / (total + 1.0 / 1024.0)
        greens.append(jnp.where(total == 0.0, 0.0, value))
    green = jnp.concatenate(greens, axis=1)
    for copy in halo_group(1):
        copy.wait_recv()
    for sx in (0, 4):
        lay_strips(sx)
    for n in (0, 1, 4, 5):
        lay_column(n)
    half_columns(CUTS[1], CUTS[2])

    arrive_c()
    rows_x = []
    for group in range(4):
        for k in range(4):
            halves = [
                swap_groups(
                    [rx_c[4 * h + g, :, group * 128 : group * 128 + 128] for g in range(4)], k
                )
                for h in range(2)
            ]
            rows_x.append(jnp.concatenate(halves, axis=1))
    lines_x = jnp.concatenate(rows_x, axis=0)
    basis_x = (bx_ref[0], bx_ref[1])
    filtered = dot3(split(lines_x), basis_x, NT) * green
    back_x = dot3(split(filtered), basis_x)
    for g in range(8):
        half = g // 4
        for group in range(4):
            pieces = [
                back_x[(group * 4 + k) * 8 : (group * 4 + k) * 8 + 8, half * 128 : half * 128 + 128]
                for k in range(4)
            ]
            flat_c[g, :, group * 128 : group * 128 + 128] = swap_groups(pieces, g % 4)
    tx_c2[...] = flat_c[...].astype(bf16)
    rx_c2[ix] = tx_c2[ix]
    arrive_c2, drain_c2 = exchange(tx_c2, rx_c2, sc2, rc2, x_peer, 8, ix)
    half_columns(CUTS[2], CUTS[3])
    arrive_c2()
    lines_y2 = rx_c2[...].astype(f32).reshape(64, 512).astype(bf16)
    back_y = jnp.dot(by_ref[1, 0], lines_y2, preferred_element_type=f32)
    back_y = back_y + jnp.dot(by_ref[1, 1], lines_y2, preferred_element_type=f32)
    for group in range(4):
        pieces = [back_y[16 * i : 16 * i + 16, group * 128 : group * 128 + 128] for i in range(4)]
        for k in range(4):
            flat_b[pl.ds(group * 4 + k, 16, 16), :] = swap_groups(pieces, k)
    tx_b2[...] = flat_b[...].astype(bf16).reshape(16, 16, 128)
    rx_b2[me] = tx_b2[me]
    arrive_b2, drain_b2 = exchange(tx_b2, rx_b2, sb2, rb2, yz_peer, 16, me)
    half_columns(CUTS[3], CUTS[4])
    arrive_b2()
    back_z = rx_b2[...].astype(f32).reshape(256, 128).T.astype(bf16)
    lines_z = jnp.dot(back_z, bz_ref[0], preferred_element_type=f32)
    potential = split(lines_z + jnp.dot(back_z, bz_ref[1], preferred_element_type=f32))

    sampled = [dot3(potential, (z_high[n], z_low[n])) for n in range(4)]
    for n in range(4):
        total = jnp.sum(sampled[n] * stencil[n], axis=0, keepdims=True)
        parts[2 * n] = total[:, 0:256]
        tail = jnp.broadcast_to(total[:, 128:384], (8, 256))
        parts[2 * n + 1] = pltpu.roll(tail, 192, 1)[0:1]

    def part_copy(s, u):
        return pltpu.make_async_remote_copy(
            src_ref=parts.at[2 * s + u],
            dst_ref=rx_parts.at[from_half[u] * 4 + iz],
            send_sem=sp,
            recv_sem=rp,
            device_id=(ix, from_y[u], s),
            device_id_type=MESH,
        )

    for step in (2, 1, 3):
        for u in range(2):
            part_copy(lax.rem(iz + step, 4), u).start()
    for u in range(2):

        @pl.when(from_y[u] != iy)
        def _():
            part_copy(iz, u).start()

        @pl.when(from_y[u] == iy)
        def _():
            rx_parts[from_half[u] * 4 + iz] = parts[2 * iz + u]

    half_columns(CUTS[4], 12)
    wv = wv_ref[...]
    invariant = jnp.zeros((384, 128), f32)
    for d in range(3):
        t = sums[1 + d]
        hi = t.astype(bf16)
        lo = (t - hi.astype(f32)).astype(bf16)
        vec = jnp.dot(hi, wv, preferred_element_type=f32) + jnp.dot(
            lo, wv, preferred_element_type=f32
        )
        invariant = invariant + vec * vec
    update = (sums[0] * (1.0 / 64.0) + invariant * (1.0 / 64.0)).astype(bf16)
    out_ref[...] = (
        feat_ref[...].astype(f32).reshape(384, 128) + jnp.dot(update, wo_ref[...], preferred_element_type=f32)
    ).astype(bf16)

    bulk(rx_atoms, sa, ra, False)
    drain_b()
    drain_c()
    drain_c2()
    drain_b2()
    for group in range(2):
        for copy in halo_group(group):
            copy.wait_send()

    bulk(rx_parts, sp, rp, True)

    for half in range(2):
        site = (rx_parts[half * 4] + rx_parts[half * 4 + 1]) + (
            rx_parts[half * 4 + 2] + rx_parts[half * 4 + 3]
        )
        for cx in range(3):
            block = site[:, 0:128] if cx < 2 else site[:, 128:256]
            block = jnp.broadcast_to(block, (8, 128))
            at = sub_l * 8 + lane_l % 8 + 64 * (cx % 2)
            site_ref[cx, half] = jnp.take_along_axis(block, at, axis=1)[:, 0:8]

    bulk(rx_parts, sp, rp, False)


def layer(operands):
    f32, bf16 = jnp.float32, jnp.bfloat16
    vm = pl.BlockSpec(memory_space=pltpu.VMEM)
    dma = pltpu.SemaphoreType.DMA
    tables = [jnp.asarray(t) for t in ewald_tables()]
    hbm = pl.BlockSpec(memory_space=pltpu.HBM)
    specs = [hbm] * 22
    shapes = [operands[n] for n in (0, 1, 2, 3, 14, 6, 7, 8, 10, 11, 4, 5)] + tables
    shapes += [operands[n] for n in (12, 13)]
    staged = [pltpu.VMEM(x.shape, x.dtype) for x in shapes]
    return pl.pallas_call(
        layer_kernel,
        out_shape=(
            jax.ShapeDtypeStruct((384, 128), bf16),
            jax.ShapeDtypeStruct((3, 2, 8, 8), f32),
        ),
        in_specs=specs,
        out_specs=(vm, vm),
        scratch_shapes=staged
        + [
            pltpu.SMEM((2,), f32),
            pltpu.SMEM((8,), f32),
            dma((20,)),
            dma((2,)),
            pltpu.VMEM((3, 2, 4, 1, 128), f32),
            pltpu.VMEM((5, 4, 10, 8, 128), bf16),
            pltpu.VMEM((5, 4, 4, 1, 128), f32),
            pltpu.VMEM((6, 48, 128), f32),
            pltpu.VMEM((1600, 128), f32),
            pltpu.VMEM((128, 256), bf16),
            pltpu.VMEM((128, 128), bf16),
            pltpu.VMEM((128, 128), bf16),
            pltpu.VMEM((8, 512), jnp.int32),
            pltpu.VMEM((8, 512), jnp.int32),
            pltpu.VMEM((8, 512), f32),
            pltpu.VMEM((4, 384, 128), f32),
            pltpu.VMEM((2, 8, 256), f32),
            pltpu.VMEM((8, 8, 256), f32),
            pltpu.VMEM((4, 256, 384), bf16),
            pltpu.VMEM((4, 256, 384), bf16),
            pltpu.VMEM((4, 128, 384), f32),
            pltpu.VMEM((16, 16, 128), f32),
            pltpu.VMEM((16, 16, 128), f32),
            pltpu.VMEM((8, 8, 512), f32),
            pltpu.VMEM((8, 8, 512), f32),
            pltpu.VMEM((8, 8, 512), bf16),
            pltpu.VMEM((8, 8, 512), bf16),
            pltpu.VMEM((16, 16, 128), bf16),
            pltpu.VMEM((16, 16, 128), bf16),
            pltpu.VMEM((256, 128), f32),
            pltpu.VMEM((8, 8, 512), f32),
            pltpu.VMEM((8, 1, 256), f32),
            pltpu.VMEM((8, 1, 256), f32),
            pltpu.SemaphoreType.DMA,
            pltpu.SemaphoreType.DMA,
            *[pltpu.SemaphoreType.DMA] * 10,
            dma((2,)),
            dma((2,)),
            dma((2,)),
            dma((2,)),
        ],
        compiler_params=pltpu.CompilerParams(
            collective_id=0, has_side_effects=True, vmem_limit_bytes=48 * 1024 * 1024
        ),
        cost_estimate=pl.CostEstimate(flops=4 * 10**9, bytes_accessed=4 * 10**6, transcendentals=10**7),
        name="layer",
    )(*[pltpu.with_memory_space_constraint(x, pltpu.HBM) for x in (*operands, *tables)])


def shards(
    features,
    positions,
    grid_anchor,
    species,
    neighbours,
    neighbour_count,
    w_self,
    w_neighbour,
    w_radial,
    radial_rates,
    w_pair1,
    w_pair2,
    w_vector,
    w_out,
    w_charge,
    species_charge,
):
    updated, site_potential = layer(
        (
            features,
            positions,
            grid_anchor,
            species,
            neighbours,
            neighbour_count,
            w_neighbour,
            w_self,
            w_radial,
            radial_rates,
            w_pair1,
            w_pair2,
            w_vector,
            w_out,
            w_charge.reshape(1, 128),
            species_charge,
        )
    )
    return (updated.reshape(features.shape), site_potential)


def solution(mesh):
    return jax.shard_map(
        shards,
        mesh=mesh,
        in_specs=(
            P("gx", "gy", "gz", None, None),
            P("gx", "gy", "gz", None),
            P("gx", "gy", "gz", None),
            P("gx", "gy", "gz", None),
            P("gx", "gy", "gz", None),
            P("gx", "gy", "gz", None),
            P(),
            P(),
            P(),
            P(),
            P(),
            P(),
            P(),
            P(),
            P(),
            P(),
        ),
        out_specs=(P("gx", "gy", "gz", None, None), P("gx", "gy", "gz", None)),
        check_vma=False,
    )
```
